768 devices in a mesh: slab: 768 (over y, z, x, core).
Axes of the slice: x: 4, y: 8, z: 12, core: 2. Of those that a mesh axis runs over, the one named last changes fastest.
Arguments:
- load_terms: float32 [8, 8, 8, 98304], P(None, None, None, 'slab'), may hold values from -12 to 12
- geometry: float32 [3, 8, 8, 8, 98304], P(None, None, None, None, 'slab'), may hold values from 0.02 to 0.2
- mass_terms: float32 [8, 8, 8, 98304], P(None, None, None, 'slab'), may hold values from 1 to 4
- element_order: int32 [768, 128], P('slab'), may hold values from 0 to 127, each once within a row
Outputs:
- solution: float32 [8, 8, 8, 98304], P(None, None, None, 'slab')
- residual: float32 [8, 8, 8, 98304], P(None, None, None, 'slab')
The draws below stay inside these ranges and needn't reach their ends.
Inputs may be any that keep to these rules, and one draw needn't show every extreme that they name: `element_order`: each device's row lists each of its 128 cells once.
All inputs are finite; a program needn't handle non-finite values.
Results may differ from the reference program's by a relative error of at most 0.0001.
Values sent between devices are 32-bit elements; how exact they have to be, the bound alone decides.
A program may use at most 32 MiB of HBM per device.

```python
import math
import jax
import jax.numpy as jnp
import numpy as np
from jax import lax

POINTS = 8
EL_X = 1
EL_Y = 8
EL_Z = 16
SECTIONS = 2
ELEM_DEV = 128
NELEM = 98304
N_SLAB = 768


def draw_load_terms(key, part):
    noise = jax.random.normal(key, (POINTS, POINTS, POINTS, NELEM), jnp.float32)
    device_pos = (jnp.arange(NELEM) // ELEM_DEV).astype(jnp.float32)
    ramp = 1.0 + 0.8 * device_pos / max(NELEM // ELEM_DEV - 1, 1)
    return jnp.clip(noise * ramp, -12.0, 12.0)


def level_of(own_key, dims, split, smallest, high):
    level = 1.0
    for position, shards_of in split:
        steps = jax.random.uniform(jax.random.fold_in(jax.random.fold_in(own_key, 6), position), (shards_of,), jnp.float32, smallest / len(split), high / len(split))
        level = level * jnp.repeat(jnp.exp(steps), dims[position] // shards_of).reshape((-1,) + (1,) * (len(dims) - 1 - position))
    return level


def setup_inputs(seed: int = 0) -> dict:
    key_of = jax.random.split(jax.random.key(seed), 5)
    load_terms = draw_load_terms(jax.random.fold_in(key_of[4], 71), 0)
    geometry = jnp.clip(jnp.exp(math.log(0.2) - 2.3025851 * jax.random.uniform(key_of[1], (3, POINTS, POINTS, POINTS, NELEM), jnp.float32) ** level_of(key_of[1], (3, POINTS, POINTS, POINTS, NELEM), ((4, 768),), -0.2, 0.2)), 0.02, 0.2)
    mass_terms = jnp.clip(jnp.exp(math.log(4.0) - 1.3862944 * jax.random.uniform(key_of[2], (POINTS, POINTS, POINTS, NELEM), jnp.float32) ** level_of(key_of[2], (POINTS, POINTS, POINTS, NELEM), ((3, 768),), -0.2, 0.2)), 1.0, 4.0)
    element_order = jax.vmap(lambda own: jax.random.permutation(own, ELEM_DEV))(jax.random.split(key_of[3], N_SLAB)).reshape((N_SLAB, ELEM_DEV)).astype(jnp.int32)
    return dict(load_terms=load_terms, geometry=geometry, mass_terms=mass_terms, element_order=element_order)


spectrum_centre = 1.65
spectrum_half = 1.35


def legendre_table(positions, points):
    columns = [positions * 0.0 + 1.0, positions]
    for degree_now in range(2, points):
        columns.append(((2 * degree_now - 1) * positions * columns[-1] - (degree_now - 1) * columns[-2]) / degree_now)
    return np.stack(columns, axis=1)


def gll_derivative(points):
    degree = points - 1
    grid_nodes = -np.cos(np.pi * np.arange(points) / degree)
    for repeat in range(100):
        legendre = legendre_table(grid_nodes, points)
        grid_nodes = grid_nodes - (grid_nodes * legendre[:, degree] - legendre[:, degree - 1]) / (points * legendre[:, degree])
    legendre = legendre_table(grid_nodes, points)
    top_values = legendre[:, degree]
    index_list = np.arange(points)
    same_index = index_list[:, None] == index_list[None, :]
    spacing = grid_nodes[:, None] - grid_nodes[None, :]
    spacing = np.where(same_index, 1.0, spacing)
    deriv_table = top_values[:, None] / (top_values[None, :] * spacing)
    deriv_table = np.where(same_index, 0.0, deriv_table)
    deriv_table[0, 0] = -degree * points / 4.0
    deriv_table[degree, degree] = degree * points / 4.0
    return deriv_table


def local_apply(values, geometry, mass_terms, deriv_table):
    highest = lax.Precision.HIGHEST
    grad_one = jnp.einsum("ma,abce->mbce", deriv_table, values, precision=highest)
    result = jnp.einsum("ma,mbce->abce", deriv_table, geometry[0] * grad_one, precision=highest)
    grad_two = jnp.einsum("mb,abce->amce", deriv_table, values, precision=highest)
    result = result + jnp.einsum("mb,amce->abce", deriv_table, geometry[1] * grad_two, precision=highest)
    grad_three = jnp.einsum("mc,abce->abme", deriv_table, values, precision=highest)
    result = result + jnp.einsum("mc,abme->abce", deriv_table, geometry[2] * grad_three, precision=highest)
    return result + mass_terms * values


def local_diagonal(geometry, mass_terms, deriv_table):
    highest = lax.Precision.HIGHEST
    squared = deriv_table * deriv_table
    result = jnp.einsum("ma,mbce->abce", squared, geometry[0], precision=highest)
    result = result + jnp.einsum("mb,amce->abce", squared, geometry[1], precision=highest)
    result = result + jnp.einsum("mc,abme->abce", squared, geometry[2], precision=highest)
    return result + mass_terms


def to_grid(values, element_order):
    points = values.shape[0]
    inverse = jnp.argsort(element_order, axis=1).astype(jnp.int32)
    row_base = jnp.arange(N_SLAB, dtype=jnp.int32)[:, None] * ELEM_DEV
    picks = (row_base + inverse).reshape(-1).astype(jnp.int32)
    grid = jnp.take(values, picks, axis=3)
    return grid.reshape(points, points, points, N_SLAB * EL_X, EL_Y, EL_Z)


def to_store(grid, element_order):
    points = grid.shape[0]
    row_base = jnp.arange(N_SLAB, dtype=jnp.int32)[:, None] * ELEM_DEV
    picks = (row_base + element_order.astype(jnp.int32)).reshape(-1).astype(jnp.int32)
    return jnp.take(grid.reshape(points, points, points, NELEM), picks, axis=3)


def assemble_grid(grid):
    low_face = grid[0]
    high_face = grid[-1]
    shared = high_face + jnp.roll(low_face, -1, axis=2)
    grid = jnp.concatenate([jnp.roll(shared, 1, axis=2)[None], grid[1:-1], shared[None]], axis=0)
    low_face = grid[:, 0]
    high_face = grid[:, -1]
    zero_column = jnp.zeros_like(low_face[:, :, :, :1])
    new_high = high_face + jnp.concatenate([low_face[:, :, :, 1:], zero_column], axis=3)
    new_low = low_face + jnp.concatenate([zero_column, high_face[:, :, :, :-1]], axis=3)
    grid = jnp.concatenate([new_low[:, None], grid[:, 1:-1], new_high[:, None]], axis=1)
    low_face = grid[:, :, 0]
    high_face = grid[:, :, -1]
    shared = high_face + jnp.roll(low_face, -1, axis=4)
    grid = jnp.concatenate([jnp.roll(shared, 1, axis=4)[:, :, None], grid[:, :, 1:-1], shared[:, :, None]], axis=2)
    return grid


def grid_weights(points):
    node_ids = jnp.arange(points)
    end_node = (node_ids == 0) | (node_ids == points - 1)
    edge_mult = jnp.where(end_node, 2.0, 1.0).astype(jnp.float32)
    cross_ids = jnp.arange(EL_Y)
    low_shared = (node_ids == 0)[:, None] & (cross_ids > 0)[None, :]
    high_shared = (node_ids == points - 1)[:, None] & (cross_ids < EL_Y - 1)[None, :]
    mid_mult = jnp.where(low_shared | high_shared, 2.0, 1.0).astype(jnp.float32)
    total = edge_mult[:, None, None, None, None, None] * mid_mult[None, :, None, None, :, None] * edge_mult[None, None, :, None, None, None]
    full = jnp.broadcast_to(total, (points, points, points, N_SLAB * EL_X, EL_Y, EL_Z))
    return 1.0 / full


def reference(load_terms, geometry, mass_terms, element_order):
    points = load_terms.shape[0]
    deriv_table = jnp.asarray(gll_derivative(points), jnp.float32)

    def stiffness_sum(values):
        return to_store(assemble_grid(to_grid(values, element_order)), element_order)

    def operate(values):
        return stiffness_sum(local_apply(values, geometry, mass_terms, deriv_table))

    weight = to_store(grid_weights(points), element_order)
    start = stiffness_sum(load_terms)
    inv_diag = 1.0 / stiffness_sum(local_diagonal(geometry, mass_terms, deriv_table))
    ratio_sigma = spectrum_centre / spectrum_half
    step_vec = inv_diag * start / spectrum_centre
    precond = step_vec
    rho_prev = 1.0 / ratio_sigma
    for section in range(SECTIONS - 1):
        rho_next = 1.0 / (2.0 * ratio_sigma - rho_prev)
        misfit = start - operate(precond)
        step_vec = rho_next * rho_prev * step_vec + (2.0 * rho_next / spectrum_half) * inv_diag * misfit
        precond = precond + step_vec
        rho_prev = rho_next
    numerator = jnp.sum(weight * start * precond)
    image_vec = operate(precond)
    denominator = jnp.sum(weight * precond * image_vec)
    step_size = numerator / denominator
    return step_size * precond, start - step_size * image_vec
```

```python
import functools

import jax
import jax.numpy as jnp
import numpy as np
from jax import lax
from jax.experimental import pallas as pl
from jax.experimental.pallas import tpu as pltpu
from jax.sharding import PartitionSpec as P

N = 8
EL_Y = 8
EL_Z = 16
LANES = 128
ROWS = N * N * N
FACE = N * N
CENTRE = 1.65
HALF = 1.35
MESH = pl.DeviceIdType.MESH
PHASES = ((8, 1), (8, 96), (12, 8))


def legendre_table(positions, points):
    columns = [positions * 0.0 + 1.0, positions]
    for degree in range(2, points):
        columns.append(
            ((2 * degree - 1) * positions * columns[-1] - (degree - 1) * columns[-2]) / degree
        )
    return np.stack(columns, axis=1)


def gll_derivative(points):
    degree = points - 1
    nodes = -np.cos(np.pi * np.arange(points) / degree)
    for _ in range(100):
        legendre = legendre_table(nodes, points)
        nodes = nodes - (nodes * legendre[:, degree] - legendre[:, degree - 1]) / (
            points * legendre[:, degree]
        )
    legendre = legendre_table(nodes, points)
    top = legendre[:, degree]
    same = np.eye(points, dtype=bool)
    spacing = np.where(same, 1.0, nodes[:, None] - nodes[None, :])
    table = np.where(same, 0.0, top[:, None] / (top[None, :] * spacing))
    table[0, 0] = -degree * points / 4.0
    table[degree, degree] = degree * points / 4.0
    return table


DERIV = gll_derivative(N).astype(np.float32).astype(np.float64)
SQUARED = DERIV * DERIV
SIGMA = CENTRE / HALF
RHO0 = 1.0 / SIGMA
RHO1 = 1.0 / (2.0 * SIGMA - RHO0)
COEF_Z = (1.0 + RHO1 * RHO0) / CENTRE + 2.0 * RHO1 / HALF
COEF_Q = 2.0 * RHO1 / HALF / CENTRE


def contract(table, terms, sign):
    half = N // 2
    even = [terms[j] + terms[N - 1 - j] for j in range(half)]
    odd = [terms[j] - terms[N - 1 - j] for j in range(half)]
    out = [None] * N
    for i in range(half):
        e = o = None
        for j in range(half):
            ce = float(table[i, j] + table[i, N - 1 - j]) / 2
            co = float(table[i, j] - table[i, N - 1 - j]) / 2
            e = ce * even[j] if e is None else e + ce * even[j]
            o = co * odd[j] if o is None else o + co * odd[j]
        out[i] = e + o
        out[N - 1 - i] = (o - e) if sign < 0 else (e - o)
    return out


def tile(row):
    return pl.ds(pl.multiple_of(row, 8), 8)


def normal(ref, a, b):
    return ref[tile((a * N + b) * N), :]


def across(a, c):
    return pl.ds(a * FACE + c, N, stride=N)


def stiffness(v, g0, g1, g2t, ms, out, tmp):
    def along_c(a, _):
        vt = [v[across(a, c), :] for c in range(N)]
        s = contract(DERIV, vt, -1)
        s = [s[c] * normal(g2t, a, c) for c in range(N)]
        s = contract(DERIV.T, s, -1)
        for c in range(N):
            tmp[across(a, c), :] = s[c]
        return 0

    lax.fori_loop(0, N, along_c, 0)

    def along_b(a, _):
        vb = [normal(v, a, b) for b in range(N)]
        s = contract(DERIV, vb, -1)
        s = [s[b] * normal(g1, a, b) for b in range(N)]
        s = contract(DERIV.T, s, -1)
        for b in range(N):
            out[tile((a * N + b) * N), :] = (
                s[b] + normal(ms, a, b) * vb[b] + normal(tmp, a, b)
            )
        return 0

    lax.fori_loop(0, N, along_b, 0)

    def along_a(b, _):
        va = [normal(v, a, b) for a in range(N)]
        s = contract(DERIV, va, -1)
        s = [s[a] * normal(g0, a, b) for a in range(N)]
        s = contract(DERIV.T, s, -1)
        for a in range(N):
            out[tile((a * N + b) * N), :] = normal(out, a, b) + s[a]
        return 0

    lax.fori_loop(0, N, along_a, 0)


def local_diagonal(g0, g1, g2t, ms, out, tmp):
    def along_c(a, _):
        s = contract(SQUARED.T, [normal(g2t, a, c) for c in range(N)], 1)
        for c in range(N):
            tmp[across(a, c), :] = s[c]
        return 0

    lax.fori_loop(0, N, along_c, 0)

    def along_b(a, _):
        s = contract(SQUARED.T, [normal(g1, a, b) for b in range(N)], 1)
        for b in range(N):
            out[tile((a * N + b) * N), :] = s[b] + normal(ms, a, b) + normal(tmp, a, b)
        return 0

    lax.fori_loop(0, N, along_b, 0)

    def along_a(b, _):
        s = contract(SQUARED.T, [normal(g0, a, b) for a in range(N)], 1)
        for a in range(N):
            out[tile((a * N + b) * N), :] = normal(out, a, b) + s[a]
        return 0

    lax.fori_loop(0, N, along_a, 0)


def assemble_yz(v):
    lane = lax.broadcasted_iota(jnp.int32, (8, LANES), 1)
    up = lane < LANES - EL_Z
    down = lane >= EL_Z
    wrap_up = (lane & (EL_Z - 1)) == EL_Z - 1
    wrap_down = (lane & (EL_Z - 1)) == 0

    def one(a, _):
        low = normal(v, a, 0)
        high = normal(v, a, N - 1)
        v[tile((a * N + N - 1) * N), :] = high + jnp.where(
            up, pltpu.roll(low, LANES - EL_Z, 1), 0.0
        )
        v[tile(a * FACE), :] = low + jnp.where(down, pltpu.roll(high, EL_Z, 1), 0.0)
        low = v[across(a, 0), :]
        high = v[across(a, N - 1), :]
        nxt = jnp.where(wrap_up, pltpu.roll(low, EL_Z - 1, 1), pltpu.roll(low, LANES - 1, 1))
        prv = jnp.where(wrap_down, pltpu.roll(high, LANES - EL_Z + 1, 1), pltpu.roll(high, 1, 1))
        v[across(a, N - 1), :] = high + nxt
        v[across(a, 0), :] = low + prv
        return 0

    lax.fori_loop(0, N, one, 0)


def lane_pick(x, idx):
    return jnp.take_along_axis(x, idx, axis=1, mode="promise_in_bounds")


def step_kernel(
    load_h, geom_h, mass_h, order_h, p_h, r_h, im_h, al_o,
    ld, g0, g1, g2, g2t, ms, r, dg, z, y, u, tmp,
    face_r, face_d, face_y, face_u, dots, got0, got1, got2,
    order_v, in_sems, out_sems, x_send, x_recv, s_send, s_recv,
):
    count = lax.axis_size("slab")
    me = lax.axis_index("slab")
    right = lax.rem(me + 1, count)
    left = lax.rem(me + count - 1, count)
    loads = [
        pltpu.make_async_copy(src, dst, in_sems.at[k])
        for k, (src, dst) in enumerate(
            (
                (order_h, order_v),
                (load_h, ld),
                (geom_h.at[0], g0),
                (geom_h.at[1], g1),
                (geom_h.at[2], g2),
                (mass_h, ms),
            )
        )
    ]
    for copy in loads:
        copy.start()

    peers = []
    for members, stride in PHASES:
        pos = lax.rem(me // stride, members)
        peers.append(
            [me + (lax.rem(pos + j, members) - pos) * stride for j in range(1, members)]
        )
    barrier = pltpu.get_barrier_semaphore()
    everyone = [left, right] + [q for ring in peers for q in ring]
    for q in everyone:
        pl.semaphore_signal(barrier, inc=1, device_id=(q,), device_id_type=MESH)

    loads[0].wait()
    order = jnp.broadcast_to(order_v[...], (8, LANES))
    hit = (
        jnp.broadcast_to(order_v[...], (LANES, LANES))
        == lax.broadcasted_iota(jnp.int32, (LANES, LANES), 0)
    ).astype(jnp.float32)
    columns = lax.broadcasted_iota(jnp.int32, (8, LANES), 1).astype(jnp.float32)
    inverse = lax.dot_general(
        columns, hit, (((1,), (1,)), ((), ())), preferred_element_type=jnp.float32
    )
    inverse = (inverse + 0.5).astype(jnp.int32)

    def reorder(src, dst, idx):
        def one(k, _):
            for i in range(4):
                rows = tile((k * 4 + i) * 8)
                dst[rows, :] = lane_pick(src[rows, :], idx)
            return 0

        lax.fori_loop(0, ROWS // 32, one, 0)

    loads[1].wait()
    reorder(ld, ld, inverse)

    def copy_rows(src, dst):
        def one(k, _):
            for i in range(8):
                rows = tile((k * 8 + i) * 8)
                dst[rows, :] = src[rows, :]
            return 0

        lax.fori_loop(0, ROWS // 64, one, 0)

    copy_rows(ld, r)
    assemble_yz(r)
    loads[2].wait()
    reorder(g0, g0, inverse)
    loads[3].wait()
    reorder(g1, g1, inverse)
    loads[4].wait()

    def turn(a, _):
        for c in range(N):
            g2t[tile((a * N + c) * N), :] = lane_pick(g2[across(a, c), :], inverse)
        return 0

    lax.fori_loop(0, N, turn, 0)
    loads[5].wait()
    reorder(ms, ms, inverse)
    local_diagonal(g0, g1, g2t, ms, dg, tmp)
    assemble_yz(dg)

    pl.semaphore_wait(barrier, len(everyone))

    low, high = pl.ds(0, FACE), pl.ds(ROWS - FACE, FACE)

    def exchange(v, faces, k):
        copies = [
            pltpu.make_async_remote_copy(
                src_ref=v.at[high if i == 0 else low],
                dst_ref=faces.at[i],
                send_sem=x_send.at[2 * k + i],
                recv_sem=x_recv.at[2 * k + i],
                device_id=(right if i == 0 else left,),
                device_id_type=MESH,
            )
            for i in range(2)
        ]
        for copy in copies:
            copy.start()
        return copies

    def merge(v, faces, copies):
        for copy in copies:
            copy.wait()
        v[low, :] = v[low, :] + faces[0]
        v[high, :] = v[high, :] + faces[1]

    first = exchange(r, face_r, 0)
    second = exchange(dg, face_d, 1)
    merge(r, face_r, first)
    merge(dg, face_d, second)

    def each(body, init=0, per=4):
        def one(k, carry):
            for i in range(per):
                carry = body(tile((k * per + i) * 8), carry)
            return carry

        return lax.fori_loop(0, ROWS // 8 // per, one, init)

    def to_z(rows, carry):
        inv = 1.0 / dg[rows, :]
        dg[rows, :] = inv
        z[rows, :] = inv * r[rows, :]
        return carry

    each(to_z)
    stiffness(z, g0, g1, g2t, ms, y, tmp)
    assemble_yz(y)
    third = exchange(y, face_y, 2)
    merge(y, face_y, third)

    def to_p(rows, carry):
        p = COEF_Z * z[rows, :] - COEF_Q * (dg[rows, :] * y[rows, :])
        z[rows, :] = p
        return carry + ld[rows, :] * p

    zero = jnp.zeros((8, LANES), jnp.float32)
    num = each(to_p, zero)
    stiffness(z, g0, g1, g2t, ms, u, tmp)
    den = each(lambda rows, carry: carry + z[rows, :] * u[rows, :], zero)
    dots[0, 0:1, :] = jnp.sum(num, axis=0, keepdims=True)
    dots[0, 1:2, :] = jnp.sum(den, axis=0, keepdims=True)

    gots = (got0, got1, got2)

    def spread(k):
        base = sum(m - 1 for m, _ in PHASES[:k])
        copies = [
            pltpu.make_async_remote_copy(
                src_ref=dots.at[k],
                dst_ref=gots[k].at[j],
                send_sem=s_send.at[base + j],
                recv_sem=s_recv.at[base + j],
                device_id=(q,),
                device_id_type=MESH,
            )
            for j, q in enumerate(peers[k])
        ]
        for copy in copies:
            copy.start()
        return copies

    def gather(k, copies):
        total = dots[k]
        for j, copy in enumerate(copies):
            copy.wait_recv()
        for j in range(len(copies)):
            total = total + gots[k][j]
        return total

    ring0 = spread(0)
    assemble_yz(u)
    fourth = exchange(u, face_u, 3)

    dots[1] = gather(0, ring0)
    ring1 = spread(1)
    reorder(z, y, order)
    reorder(r, tmp, order)
    puts = [
        pltpu.make_async_copy(y, p_h, out_sems.at[0]),
        pltpu.make_async_copy(tmp, r_h, out_sems.at[1]),
        pltpu.make_async_copy(u, im_h, out_sems.at[2]),
    ]
    puts[0].start()
    puts[1].start()
    dots[2] = gather(1, ring1)
    ring2 = spread(2)
    merge(u, face_u, fourth)
    reorder(u, u, order)
    puts[2].start()
    total = gather(2, ring2)
    sums = jnp.sum(total, axis=1, keepdims=True)
    al_o[...] = jnp.broadcast_to(sums[0:1, :] / sums[1:2, :], (8, LANES))
    for copy in ring0 + ring1 + ring2:
        copy.wait_send()
    for copy in puts:
        copy.wait()


def on_device(load_terms, geometry, mass_terms, element_order):
    flat = jax.ShapeDtypeStruct((ROWS, LANES), jnp.float32)
    vm = lambda *shape: pltpu.VMEM(shape, jnp.float32)
    field = vm(ROWS, LANES)
    face = vm(2, FACE, LANES)
    links = sum(m - 1 for m, _ in PHASES)
    p, r, im, alpha = pl.pallas_call(
        step_kernel,
        out_shape=(flat, flat, flat, jax.ShapeDtypeStruct((8, LANES), jnp.float32)),
        in_specs=[pl.BlockSpec(memory_space=pl.ANY)] * 4,
        out_specs=(
            *[pl.BlockSpec(memory_space=pl.ANY)] * 3,
            pl.BlockSpec(memory_space=pltpu.VMEM),
        ),
        scratch_shapes=[
            *[field] * 12,
            face, face, face, face,
            vm(3, 2, LANES), *[vm(m - 1, 2, LANES) for m, _ in PHASES],
            pltpu.VMEM((1, LANES), jnp.int32),
            pltpu.SemaphoreType.DMA((6,)),
            pltpu.SemaphoreType.DMA((3,)),
            pltpu.SemaphoreType.DMA((8,)),
            pltpu.SemaphoreType.DMA((8,)),
            pltpu.SemaphoreType.DMA((links,)),
            pltpu.SemaphoreType.DMA((links,)),
        ],
        compiler_params=pltpu.CompilerParams(collective_id=0, has_side_effects=True),
        name="cg_step",
    )(
        load_terms.reshape(ROWS, LANES),
        geometry.reshape(3, ROWS, LANES),
        mass_terms.reshape(ROWS, LANES),
        element_order,
    )
    alpha = alpha[0:1, :]
    shape = load_terms.shape
    return (alpha * p).reshape(shape), (r - alpha * im).reshape(shape)


def solution(mesh):
    last = P(None, None, None, "slab")
    return jax.shard_map(
        on_device,
        mesh=mesh,
        in_specs=(last, P(None, None, None, None, "slab"), last, P("slab", None)),
        out_specs=(last, last),
        check_vma=False,
    )
```

```python
import functools

import jax
import jax.numpy as jnp
import numpy as np
from jax import lax
from jax.experimental import pallas as pl
from jax.experimental.pallas import tpu as pltpu
from jax.sharding import PartitionSpec as P

N = 8
LAST = N - 1
EL_Y = 8
EL_Z = 16
LANES = 128
ROWS = N * N * N
FACE = N * N
CENTRE = 1.65
HALF = 1.35
MESH = pl.DeviceIdType.MESH
PHASES = ((8, 1), (8, 96), (12, 8))
INSIDE = range(1, LAST)


def legendre_table(positions, points):
    columns = [positions * 0.0 + 1.0, positions]
    for degree in range(2, points):
        columns.append(
            ((2 * degree - 1) * positions * columns[-1] - (degree - 1) * columns[-2]) / degree
        )
    return np.stack(columns, axis=1)


def gll_derivative(points):
    degree = points - 1
    nodes = -np.cos(np.pi * np.arange(points) / degree)
    for _ in range(100):
        legendre = legendre_table(nodes, points)
        nodes = nodes - (nodes * legendre[:, degree] - legendre[:, degree - 1]) / (
            points * legendre[:, degree]
        )
    legendre = legendre_table(nodes, points)
    top = legendre[:, degree]
    same = np.eye(points, dtype=bool)
    spacing = np.where(same, 1.0, nodes[:, None] - nodes[None, :])
    table = np.where(same, 0.0, top[:, None] / (top[None, :] * spacing))
    table[0, 0] = -degree * points / 4.0
    table[degree, degree] = degree * points / 4.0
    return table


DERIV = gll_derivative(N).astype(np.float32).astype(np.float64)
SQUARED = DERIV * DERIV
SIGMA = CENTRE / HALF
RHO0 = 1.0 / SIGMA
RHO1 = 1.0 / (2.0 * SIGMA - RHO0)
COEF_Z = (1.0 + RHO1 * RHO0) / CENTRE + 2.0 * RHO1 / HALF
COEF_Q = 2.0 * RHO1 / HALF / CENTRE


def plus(x, y):
    return y if x is None else x + y


def contract(table, terms, sign, rows=range(N)):
    used = [j for j in range(N // 2) if terms[j] is not None]
    even = {j: terms[j] + terms[LAST - j] for j in used}
    odd = {j: terms[j] - terms[LAST - j] for j in used}
    out = [None] * N
    for i in range(N // 2):
        if i not in rows and LAST - i not in rows:
            continue
        e = o = None
        for j in used:
            e = plus(e, float(table[i, j] + table[i, LAST - j]) / 2 * even[j])
            o = plus(o, float(table[i, j] - table[i, LAST - j]) / 2 * odd[j])
        if i in rows:
            out[i] = e + o
        if LAST - i in rows:
            out[LAST - i] = (o - e) if sign < 0 else (e - o)
    return out


def tile(row):
    return pl.ds(row if isinstance(row, int) else pl.multiple_of(row, 8), 8)


def at(a, b):
    return tile((a * N + b) * N)


def across(a, c):
    return pl.ds(a * FACE + c, N, stride=N)


def loop(start, stop, body):
    lax.fori_loop(start, stop, lambda i, _: (body(i), 0)[1], 0)


def inner_stiffness(v, g0, g1, g2t, ms, out, tmp):
    def along_c(a):
        s = contract(DERIV, [v[across(a, c), :] for c in range(N)], -1)
        s = contract(DERIV.T, [s[c] * g2t[at(a, c), :] for c in range(N)], -1)
        for c in range(N):
            tmp[across(a, c), :] = s[c]

    loop(1, LAST, along_c)

    def along_b(a):
        vb = [v[at(a, b), :] for b in range(N)]
        s = contract(DERIV, vb, -1)
        s = contract(DERIV.T, [s[b] * g1[at(a, b), :] for b in range(N)], -1)
        for b in range(N):
            out[at(a, b), :] = s[b] + ms[at(a, b), :] * vb[b] + tmp[at(a, b), :]

    loop(1, LAST, along_b)

    def along_a(b):
        va = [v[at(a, b), :] if a in INSIDE else None for a in range(N)]
        s = contract(DERIV, va, -1)
        s = contract(DERIV.T, [s[a] * g0[at(a, b), :] for a in range(N)], -1)
        for a in range(N):
            out[at(a, b), :] = out[at(a, b), :] + s[a] if a in INSIDE else s[a]

    loop(0, N, along_a)


def inner_diagonal(g0, g1, g2t, ms, out, tmp, ends, cross):
    def along_c(a):
        s = contract(SQUARED.T, [g2t[at(a, c), :] for c in range(N)], 1)
        for c in range(N):
            tmp[across(a, c), :] = s[c]

    loop(1, LAST, along_c)

    def along_b(a):
        s = contract(SQUARED.T, [g1[at(a, b), :] for b in range(N)], 1)
        for b in range(N):
            out[at(a, b), :] = s[b] + ms[at(a, b), :] + tmp[at(a, b), :]

    loop(1, LAST, along_b)

    def along_a(b):
        g = [g0[at(a, b), :] for a in range(N)]
        s = contract(SQUARED.T, g, 1)
        for a in INSIDE:
            out[at(a, b), :] = out[at(a, b), :] + s[a]
        ends[at(0, b), :] = s[0] + ms[at(0, b), :]
        ends[at(1, b), :] = s[LAST] + ms[at(LAST, b), :]
        both = None
        for m in range(N):
            both = plus(both, float(DERIV[m, 0] * DERIV[m, LAST]) * g[m])
        cross[at(0, b), :] = both

    loop(0, N, along_a)


def end_stiffness(v, g1, g2t, ends, cross, tmp):
    for f, a in ((0, 0), (1, LAST)):
        s = contract(DERIV, [v[across(f, c), :] for c in range(N)], -1)
        s = contract(DERIV.T, [s[c] * g2t[at(a, c), :] for c in range(N)], -1)
        for c in range(N):
            tmp[across(f, c), :] = s[c]
    out = []
    for f, a in ((0, 0), (1, LAST)):
        vb = [v[at(f, b), :] for b in range(N)]
        s = contract(DERIV, vb, -1)
        s = contract(DERIV.T, [s[b] * g1[at(a, b), :] for b in range(N)], -1)
        out.append(
            [
                s[b]
                + ends[at(f, b), :] * vb[b]
                + cross[at(0, b), :] * v[at(1 - f, b), :]
                + tmp[at(f, b), :]
                for b in range(N)
            ]
        )
    return out


def add_ends_inside(v, g0, out):
    def one(b):
        ends = [None] * N
        ends[0], ends[LAST] = v[at(0, b), :], v[at(1, b), :]
        s = contract(DERIV, ends, -1)
        s = contract(DERIV.T, [s[a] * g0[at(a, b), :] for a in range(N)], -1, INSIDE)
        for a in INSIDE:
            out[at(a, b), :] = out[at(a, b), :] + s[a]

    loop(0, N, one)


def lane_pick(x, idx):
    return jnp.take_along_axis(x, idx, axis=1, mode="promise_in_bounds")


def sum_yz(v, planes, lanes):
    for a in planes:
        low, high = v[at(a, 0), :], v[at(a, LAST), :]
        v[at(a, LAST), :] = high + jnp.where(lanes["up"], pltpu.roll(low, LANES - EL_Z, 1), 0.0)
        v[at(a, 0), :] = low + jnp.where(lanes["down"], pltpu.roll(high, EL_Z, 1), 0.0)
    lows = [v[across(a, 0), :] for a in planes]
    highs = [v[across(a, LAST), :] for a in planes]
    nexts = [lane_pick(low, lanes["next"]) for low in lows]
    prevs = [lane_pick(high, lanes["prev"]) for high in highs]
    for k, a in enumerate(planes):
        v[across(a, LAST), :] = highs[k] + nexts[k]
        v[across(a, 0), :] = lows[k] + prevs[k]


def step_kernel(
    load_h, geom_h, mass_h, order_h, p_o, r_o, im_o, al_o,
    ld, g0, g1, g2, g2t, ms, r, dg, z, y, u, tmp,
    r_got, d_got, y_got, u_got, zf, pf, tmpf, ends, cross, dots, got0, got1, got2,
    order_v, in_sems, x_send, x_recv, s_send, s_recv,
):
    stack = []

    def scope(name):
        if stack:
            stack.pop().__exit__(None, None, None)
        if name:
            stack.append(jax.named_scope(name))
            stack[-1].__enter__()

    scope("enter")
    count = lax.axis_size("slab")
    me = lax.axis_index("slab")
    right = lax.rem(me + 1, count)
    left = lax.rem(me + count - 1, count)
    loads = [
        pltpu.make_async_copy(src, dst, in_sems.at[k])
        for k, (src, dst) in enumerate(
            (
                (order_h, order_v),
                (load_h, ld),
                (geom_h.at[0], g0),
                (geom_h.at[1], g1),
                (geom_h.at[2], g2),
                (mass_h, ms),
            )
        )
    ]
    for copy in loads:
        copy.start()

    peers = []
    for members, stride in PHASES:
        pos = lax.rem(me // stride, members)
        peers.append(
            [me + (lax.rem(pos + j, members) - pos) * stride for j in range(1, members)]
        )
    barrier = pltpu.get_barrier_semaphore()
    everyone = [left, right] + [q for ring in peers for q in ring]
    for q in everyone:
        pl.semaphore_signal(barrier, inc=1, device_id=(q,), device_id_type=MESH)

    scope("idx")
    loads[0].wait()
    order = jnp.broadcast_to(order_v[...], (8, LANES))
    hit = (
        jnp.broadcast_to(order_v[...], (LANES, LANES))
        == lax.broadcasted_iota(jnp.int32, (LANES, LANES), 0)
    ).astype(jnp.float32)
    lane = lax.broadcasted_iota(jnp.int32, (8, LANES), 1)
    inverse = lax.dot_general(
        lane.astype(jnp.float32), hit, (((1,), (1,)), ((), ())), preferred_element_type=jnp.float32
    )
    inverse = (inverse + 0.5).astype(jnp.int32)
    in_row = lane & (EL_Z - 1)
    lanes = {
        "up": lane < LANES - EL_Z,
        "down": lane >= EL_Z,
        "next": lane - in_row + ((in_row + 1) & (EL_Z - 1)),
        "prev": lane - in_row + ((in_row + EL_Z - 1) & (EL_Z - 1)),
    }

    def reorder(src, dst, idx, planes=range(N)):
        for a in planes:
            for b in range(N):
                dst[at(a, b), :] = lane_pick(src[at(a, b), :], idx)

    def exchange(v, got, k):
        copies = [
            pltpu.make_async_remote_copy(
                src_ref=v.at[pl.ds(ROWS - FACE if i == 0 else 0, FACE)],
                dst_ref=got.at[pl.ds(i * FACE, FACE)],
                send_sem=x_send.at[2 * k + i],
                recv_sem=x_recv.at[2 * k + i],
                device_id=(right if i == 0 else left,),
                device_id_type=MESH,
            )
            for i in range(2)
        ]
        for copy in copies:
            copy.start()
        return copies

    planes = ((0, 0), (1, LAST))
    both = (0, LAST)
    scope("load_ends")
    loads[1].wait()
    reorder(ld, r, inverse, both)
    sum_yz(r, both, lanes)
    scope("barrier")
    pl.semaphore_wait(barrier, len(everyone))
    scope("diag_ends")
    first = exchange(r, r_got, 0)
    for copy in loads[2:]:
        copy.wait()
    for f, a in planes:
        s = contract(SQUARED.T, [g2[across(a, c), :] for c in range(N)], 1)
        for c in range(N):
            tmpf[across(f, c), :] = s[c]
    for b in range(N):
        s = contract(SQUARED.T, [g0[at(a, b), :] for a in range(N)], 1, both)
        for a in both:
            dg[at(a, b), :] = s[a]
    for f, a in planes:
        s = contract(SQUARED.T, [g1[at(a, b), :] for b in range(N)], 1)
        for b in range(N):
            rows = at(a, b)
            dg[rows, :] = lane_pick(
                s[b] + dg[rows, :] + ms[rows, :] + tmpf[at(f, b), :], inverse
            )
    sum_yz(dg, both, lanes)
    second = exchange(dg, d_got, 1)

    scope("reorder")
    reorder(ld, ld, inverse)
    reorder(g0, g0, inverse)
    reorder(g1, g1, inverse)
    for a in range(N):
        for c in range(N):
            g2t[at(a, c), :] = lane_pick(g2[across(a, c), :], inverse)
    reorder(ms, ms, inverse)
    scope("diag")
    inner_diagonal(g0, g1, g2t, ms, dg, tmp, ends, cross)
    scope("sums")
    sum_yz(dg, INSIDE, lanes)
    for a in INSIDE:
        for b in (0, LAST):
            r[at(a, b), :] = ld[at(a, b), :]
    loop(1, LAST, lambda a: [r.__setitem__((at(a, b), slice(None)), ld[at(a, b), :]) for b in range(1, LAST)])
    sum_yz(r, INSIDE, lanes)

    def inner_z(a):
        for b in range(N):
            inv = 1.0 / dg[at(a, b), :]
            dg[at(a, b), :] = inv
            z[at(a, b), :] = inv * r[at(a, b), :]

    loop(1, LAST, inner_z)
    scope("L1")
    inner_stiffness(z, g0, g1, g2t, ms, y, tmp)

    scope("x1r")
    for copy in first:
        copy.wait()
    scope("x1d")
    for copy in second:
        copy.wait()
    scope("ends1")
    for f, a in planes:
        for b in range(N):
            total = r[at(a, b), :] + r_got[at(f, b), :]
            inv = 1.0 / (dg[at(a, b), :] + d_got[at(f, b), :])
            r[at(a, b), :] = total
            dg[at(a, b), :] = inv
            zf[at(f, b), :] = inv * total
    s = end_stiffness(zf, g1, g2t, ends, cross, tmpf)
    for f, a in planes:
        for b in range(N):
            y[at(a, b), :] = y[at(a, b), :] + s[f][b]
    sum_yz(y, both, lanes)
    third = exchange(y, y_got, 2)

    scope("inner2")
    add_ends_inside(zf, g0, y)
    sum_yz(y, INSIDE, lanes)

    def inner_p(a, num):
        for b in range(N):
            rows = at(a, b)
            p = COEF_Z * z[rows, :] - COEF_Q * (dg[rows, :] * y[rows, :])
            z[rows, :] = p
            num = num + ld[rows, :] * p
        return num

    zero = jnp.zeros((8, LANES), jnp.float32)
    num = lax.fori_loop(1, LAST, inner_p, zero)
    scope("L2")
    inner_stiffness(z, g0, g1, g2t, ms, u, tmp)

    def inner_den(a, den):
        for b in range(N):
            den = den + z[at(a, b), :] * u[at(a, b), :]
        return den

    den = lax.fori_loop(1, LAST, inner_den, zero)

    scope("x2")
    for copy in third:
        copy.wait()
    scope("ends2")
    for f, a in planes:
        for b in range(N):
            rows = at(f, b)
            p = COEF_Z * zf[rows, :] - COEF_Q * (
                dg[at(a, b), :] * (y[at(a, b), :] + y_got[rows, :])
            )
            pf[rows, :] = p
            num = num + ld[at(a, b), :] * p
    s = end_stiffness(pf, g1, g2t, ends, cross, tmpf)
    for f, a in planes:
        for b in range(N):
            old = u[at(a, b), :]
            new = old + s[f][b]
            den = den + pf[at(f, b), :] * (old + new)
            u[at(a, b), :] = new
    dots[0, 0:1, :] = jnp.sum(num, axis=0, keepdims=True)
    dots[0, 1:2, :] = jnp.sum(den, axis=0, keepdims=True)

    gots = (got0, got1, got2)

    def spread(k):
        base = sum(m - 1 for m, _ in PHASES[:k])
        copies = [
            pltpu.make_async_remote_copy(
                src_ref=dots.at[k],
                dst_ref=gots[k].at[j],
                send_sem=s_send.at[base + j],
                recv_sem=s_recv.at[base + j],
                device_id=(q,),
                device_id_type=MESH,
            )
            for j, q in enumerate(peers[k])
        ]
        for copy in copies:
            copy.start()
        return copies

    def gather(k, copies):
        total = dots[k]
        for copy in copies:
            copy.wait_recv()
        for j in range(len(copies)):
            total = total + gots[k][j]
        return total

    ring0 = spread(0)
    scope("u_ends")
    sum_yz(u, both, lanes)
    fourth = exchange(u, u_got, 3)
    add_ends_inside(pf, g0, u)
    scope("ar0")
    dots[1] = gather(0, ring0)
    ring1 = spread(1)
    scope("out_p_r")
    for f, a in planes:
        for b in range(N):
            z[at(a, b), :] = pf[at(f, b), :]
    reorder(z, p_o, order)
    reorder(r, r_o, order)
    sum_yz(u, INSIDE, lanes)
    reorder(u, im_o, order, INSIDE)
    scope("ar1")
    dots[2] = gather(1, ring1)
    ring2 = spread(2)
    scope("x3")
    for copy in fourth:
        copy.wait()
    for f, a in planes:
        for b in range(N):
            im_o[at(a, b), :] = lane_pick(u[at(a, b), :] + u_got[at(f, b), :], order)
    scope("ar2")
    total = gather(2, ring2)
    scope("alpha")
    sums = jnp.sum(total, axis=1, keepdims=True)
    al_o[...] = jnp.broadcast_to(sums[0:1, :] / sums[1:2, :], (8, LANES))
    for copy in ring0 + ring1 + ring2:
        copy.wait_send()
    scope(None)


def finish_kernel(p, r, im, al, x_o, r_o):
    alpha = al[...]

    def one(k):
        for i in range(N):
            rows = tile((k * N + i) * N)
            x_o[rows, :] = alpha * p[rows, :]
            r_o[rows, :] = r[rows, :] - alpha * im[rows, :]

    loop(0, N, one)


def on_device(load_terms, geometry, mass_terms, element_order):
    flat = jax.ShapeDtypeStruct((ROWS, LANES), jnp.float32)
    vm = lambda *shape: pltpu.VMEM(shape, jnp.float32)
    field = vm(ROWS, LANES)
    pair = vm(2 * FACE, LANES)
    links = sum(m - 1 for m, _ in PHASES)
    in_vmem = pl.BlockSpec(memory_space=pltpu.VMEM)
    parts = pl.pallas_call(
        step_kernel,
        out_shape=(flat, flat, flat, jax.ShapeDtypeStruct((8, LANES), jnp.float32)),
        in_specs=[pl.BlockSpec(memory_space=pl.ANY)] * 4,
        out_specs=[in_vmem] * 4,
        scratch_shapes=[
            *[field] * 12,
            *[pair] * 8, vm(FACE, LANES),
            vm(3, 2, LANES), *[vm(m - 1, 2, LANES) for m, _ in PHASES],
            pltpu.VMEM((1, LANES), jnp.int32),
            pltpu.SemaphoreType.DMA((6,)),
            pltpu.SemaphoreType.DMA((8,)),
            pltpu.SemaphoreType.DMA((8,)),
            pltpu.SemaphoreType.DMA((links,)),
            pltpu.SemaphoreType.DMA((links,)),
        ],
        compiler_params=pltpu.CompilerParams(collective_id=0, has_side_effects=True),
        name="cg_step",
    )(
        load_terms.reshape(ROWS, LANES),
        geometry.reshape(3, ROWS, LANES),
        mass_terms.reshape(ROWS, LANES),
        element_order,
    )
    x, res = pl.pallas_call(
        finish_kernel,
        out_shape=(flat, flat),
        in_specs=[in_vmem] * 4,
        out_specs=[in_vmem] * 2,
        name="cg_finish",
    )(*parts)
    shape = load_terms.shape
    return x.reshape(shape), res.reshape(shape)


def solution(mesh):
    last = P(None, None, None, "slab")
    return jax.shard_map(
        on_device,
        mesh=mesh,
        in_specs=(last, P(None, None, None, None, "slab"), last, P("slab", None)),
        out_specs=(last, last),
        check_vma=False,
    )
```

```python
import functools

import jax
import jax.numpy as jnp
import numpy as np
from jax import lax
from jax.experimental import pallas as pl
from jax.experimental.pallas import tpu as pltpu
from jax.sharding import PartitionSpec as P

N = 8
LAST = N - 1
EL_Y = 8
EL_Z = 16
LANES = 128
ROWS = N * N * N
FACE = N * N
CENTRE = 1.65
HALF = 1.35
MESH = pl.DeviceIdType.MESH
TORUS = (8, 12, 4, 2)
INSIDE = range(1, LAST)


def legendre_table(positions, points):
    columns = [positions * 0.0 + 1.0, positions]
    for degree in range(2, points):
        columns.append(
            ((2 * degree - 1) * positions * columns[-1] - (degree - 1) * columns[-2]) / degree
        )
    return np.stack(columns, axis=1)


def gll_derivative(points):
    degree = points - 1
    nodes = -np.cos(np.pi * np.arange(points) / degree)
    for _ in range(100):
        legendre = legendre_table(nodes, points)
        nodes = nodes - (nodes * legendre[:, degree] - legendre[:, degree - 1]) / (
            points * legendre[:, degree]
        )
    legendre = legendre_table(nodes, points)
    top = legendre[:, degree]
    same = np.eye(points, dtype=bool)
    spacing = np.where(same, 1.0, nodes[:, None] - nodes[None, :])
    table = np.where(same, 0.0, top[:, None] / (top[None, :] * spacing))
    table[0, 0] = -degree * points / 4.0
    table[degree, degree] = degree * points / 4.0
    return table


DERIV = gll_derivative(N).astype(np.float32).astype(np.float64)
SQUARED = DERIV * DERIV
SIGMA = CENTRE / HALF
RHO0 = 1.0 / SIGMA
RHO1 = 1.0 / (2.0 * SIGMA - RHO0)
COEF_Z = (1.0 + RHO1 * RHO0) / CENTRE + 2.0 * RHO1 / HALF
COEF_Q = 2.0 * RHO1 / HALF / CENTRE


def plus(x, y):
    return y if x is None else x + y


def contract(table, terms, sign, rows=range(N)):
    used = [j for j in range(N // 2) if terms[j] is not None]
    even = {j: terms[j] + terms[LAST - j] for j in used}
    odd = {j: terms[j] - terms[LAST - j] for j in used}
    out = [None] * N
    for i in range(N // 2):
        if i not in rows and LAST - i not in rows:
            continue
        e = o = None
        for j in used:
            e = plus(e, float(table[i, j] + table[i, LAST - j]) / 2 * even[j])
            o = plus(o, float(table[i, j] - table[i, LAST - j]) / 2 * odd[j])
        if i in rows:
            out[i] = e + o
        if LAST - i in rows:
            out[LAST - i] = (o - e) if sign < 0 else (e - o)
    return out


def tile(row):
    return pl.ds(row if isinstance(row, int) else pl.multiple_of(row, 8), 8)


def at(a, b):
    return tile((a * N + b) * N)


def across(a, c):
    return pl.ds(a * FACE + c, N, stride=N)


LOAD, DIAG, G1, G2 = range(4)


def part(f, kind, i):
    return tile(((f * 4 + kind) * N + i) * N)


def loop(start, stop, body):
    lax.fori_loop(start, stop, lambda i, _: (body(i), 0)[1], 0)


def inner_stiffness(v, g0, g1, g2t, ms, out, tmp):
    def along_c(a):
        s = contract(DERIV, [v[across(a, c), :] for c in range(N)], -1)
        s = contract(DERIV.T, [s[c] * g2t[at(a, c), :] for c in range(N)], -1)
        for c in range(N):
            tmp[across(a, c), :] = s[c]

    loop(1, LAST, along_c)

    def along_b(a):
        vb = [v[at(a, b), :] for b in range(N)]
        s = contract(DERIV, vb, -1)
        s = contract(DERIV.T, [s[b] * g1[at(a, b), :] for b in range(N)], -1)
        for b in range(N):
            out[at(a, b), :] = s[b] + ms[at(a, b), :] * vb[b] + tmp[at(a, b), :]

    loop(1, LAST, along_b)

    def along_a(b):
        va = [v[at(a, b), :] if a in INSIDE else None for a in range(N)]
        s = contract(DERIV, va, -1)
        s = contract(DERIV.T, [s[a] * g0[at(a, b), :] for a in range(N)], -1)
        for a in range(N):
            out[at(a, b), :] = out[at(a, b), :] + s[a] if a in INSIDE else s[a]

    loop(0, N, along_a)


def inner_diagonal(g0, g1, g2t, ms, out, tmp, cross):
    def along_c(a):
        s = contract(SQUARED.T, [g2t[at(a, c), :] for c in range(N)], 1)
        for c in range(N):
            tmp[across(a, c), :] = s[c]

    loop(1, LAST, along_c)

    def along_b(a):
        s = contract(SQUARED.T, [g1[at(a, b), :] for b in range(N)], 1)
        for b in range(N):
            out[at(a, b), :] = s[b] + ms[at(a, b), :] + tmp[at(a, b), :]

    loop(1, LAST, along_b)

    def along_a(b):
        g = [g0[at(a, b), :] for a in range(N)]
        s = contract(SQUARED.T, g, 1, INSIDE)
        for a in INSIDE:
            out[at(a, b), :] = out[at(a, b), :] + s[a]
        both = None
        for m in range(N):
            both = plus(both, float(DERIV[m, 0] * DERIV[m, LAST]) * g[m])
        cross[at(0, b), :] = both

    loop(0, N, along_a)


def face_terms(v, f, mine, theirs, a_sum, tmp):
    s = contract(DERIV, [v[across(f, c), :] for c in range(N)], -1)
    s = contract(DERIV.T, [s[c] * theirs[part(f, G2, c), :] for c in range(N)], -1)
    for c in range(N):
        tmp[across(f, c), :] = s[c]
    vb = [v[at(f, b), :] for b in range(N)]
    s = contract(DERIV, vb, -1)
    s = contract(DERIV.T, [s[b] * theirs[part(f, G1, b), :] for b in range(N)], -1)
    return [s[b] + a_sum[at(f, b), :] * vb[b] + tmp[at(f, b), :] for b in range(N)]


def face_sums(f, mine, theirs, diag, a_sum, tmp):
    g = [[mine[part(f, k, i), :] + theirs[part(f, k, i), :] for i in range(N)] for k in (G1, G2)]
    for k in (G1, G2):
        for i in range(N):
            theirs[part(f, k, i), :] = g[k - G1][i]
    s = contract(SQUARED.T, g[1], 1)
    for c in range(N):
        tmp[across(f, c), :] = s[c]
    s = contract(SQUARED.T, g[0], 1)
    for b in range(N):
        a_sum[at(f, b), :] = diag[at(f, b), :] - s[b] - tmp[at(f, b), :]


def add_ends_inside(v, first, g0, out):
    def one(b):
        ends = [None] * N
        ends[0] = v[tile(first + b * N), :]
        ends[LAST] = v[tile(FACE - first + b * N), :]
        s = contract(DERIV, ends, -1)
        s = contract(DERIV.T, [s[a] * g0[at(a, b), :] for a in range(N)], -1, INSIDE)
        for a in INSIDE:
            out[at(a, b), :] = out[at(a, b), :] + s[a]

    loop(0, N, one)


def lane_pick(x, idx):
    return jnp.take_along_axis(x, idx, axis=1, mode="promise_in_bounds")


def sum_yz(planes, lanes):
    for v, a in planes:
        low, high = v[at(a, 0), :], v[at(a, LAST), :]
        v[at(a, LAST), :] = high + jnp.where(lanes["up"], pltpu.roll(low, LANES - EL_Z, 1), 0.0)
        v[at(a, 0), :] = low + jnp.where(lanes["down"], pltpu.roll(high, EL_Z, 1), 0.0)
    lows = [v[across(a, 0), :] for v, a in planes]
    highs = [v[across(a, LAST), :] for v, a in planes]
    nexts = [lane_pick(low, lanes["next"]) for low in lows]
    prevs = [lane_pick(high, lanes["prev"]) for high in highs]
    for k, (v, a) in enumerate(planes):
        v[across(a, LAST), :] = highs[k] + nexts[k]
        v[across(a, 0), :] = lows[k] + prevs[k]


def step_kernel(
    load_h, geom_h, mass_h, order_h, p_o, r_o, im_o, al_o,
    ld, g0, g1, g2, g2t, ms, r, dg, z, y, u, tmp,
    mine, theirs, w_mine, w_theirs, i_mine, i_theirs, rf, df, zf, pf, yf, a_sum, tmpf, cross,
    dots, got_a, got_b, order_v, in_sems, x_send, x_recv, s_send, s_recv, hello,
):
    stack = []

    def scope(name):
        if stack:
            stack.pop().__exit__(None, None, None)
        if name:
            stack.append(jax.named_scope(name))
            stack[-1].__enter__()

    scope("enter")
    ys, zs, xs, cores = TORUS
    count = lax.axis_size("slab")
    me = lax.axis_index("slab")
    core = lax.rem(me, cores)
    x = lax.rem(me // cores, xs)
    z_at = lax.rem(me // (cores * xs), zs)
    y_at = me // (cores * xs * zs)
    near_to = me + 1 - 2 * core
    far_to = lax.rem(me + count + 2 * core - 1, count)
    sides = (near_to, far_to)
    row_of = (pl.multiple_of((1 - core) * (ROWS - FACE), FACE), pl.multiple_of(core * (ROWS - FACE), FACE))
    face_of = {0: 1 - core, LAST: core}

    def moved(dy=0, dz=0, dx=0):
        to = me
        if dy:
            to = to + (lax.rem(y_at + dy, ys) - y_at) * (cores * xs * zs)
        if dz:
            to = to + (lax.rem(z_at + dz, zs) - z_at) * (cores * xs)
        if dx:
            to = to + (lax.rem(x + dx, xs) - x) * cores
        return to

    def ring(size, stop, start=1):
        return sorted({j % size for k in range(start, stop) for j in (k, -k)} - {0})

    def greet(sem, who):
        for q in who:
            pl.semaphore_signal(sem, inc=1, device_id=(q,), device_id_type=MESH)

    def heard(sem, who):
        if who:
            pl.semaphore_wait(sem, len(who))

    row = [moved(dx=k) + c for k in range(xs) for c in (0, 1 - 2 * core) if k or not isinstance(c, int)]
    y_near = [moved(dy=k) for k in ring(ys, 3)]
    z_near = [moved(dz=k) for k in ring(zs, 3)]
    barrier = pltpu.get_barrier_semaphore()
    near = [near_to, far_to] + row + y_near + z_near
    greet(barrier, near)
    loads = [
        pltpu.make_async_copy(src, dst, in_sems.at[k])
        for k, (src, dst) in enumerate(
            (
                (order_h, order_v),
                (load_h, ld),
                (geom_h.at[0], g0),
                (geom_h.at[1], g1),
                (geom_h.at[2], g2),
                (mass_h, ms),
            )
        )
    ]
    for copy in loads:
        copy.start()

    scope("idx")
    loads[0].wait()
    order = jnp.broadcast_to(order_v[...], (8, LANES))
    hit = (
        jnp.broadcast_to(order_v[...], (LANES, LANES))
        == lax.broadcasted_iota(jnp.int32, (LANES, LANES), 0)
    ).astype(jnp.float32)
    lane = lax.broadcasted_iota(jnp.int32, (8, LANES), 1)
    inverse = lax.dot_general(
        lane.astype(jnp.float32), hit, (((1,), (1,)), ((), ())), preferred_element_type=jnp.float32
    )
    inverse = (inverse + 0.5).astype(jnp.int32)
    in_row = lane & (EL_Z - 1)
    lanes = {
        "up": lane < LANES - EL_Z,
        "down": lane >= EL_Z,
        "next": lane - in_row + ((in_row + 1) & (EL_Z - 1)),
        "prev": lane - in_row + ((in_row + EL_Z - 1) & (EL_Z - 1)),
    }

    def reorder(src, dst, idx, planes=range(N)):
        for a in planes:
            for b in range(N):
                dst[at(a, b), :] = lane_pick(src[at(a, b), :], idx)

    def swap(src, dst, f, first, rows, k):
        copy = pltpu.make_async_remote_copy(
            src_ref=src.at[pl.ds(first, rows)],
            dst_ref=dst.at[pl.ds(first, rows)],
            send_sem=x_send.at[k, f],
            recv_sem=x_recv.at[k, f],
            device_id=(sides[f],),
            device_id_type=MESH,
        )
        copy.start()
        return copy

    both = (0, LAST)
    faces = (0, 1)
    started = []
    scope("load_ends")
    loads[1].wait()
    for a in both:
        for b in range(N):
            mine[part(face_of[a], LOAD, b), :] = lane_pick(ld[at(a, b), :], inverse)
    scope("barrier")
    pl.semaphore_wait(barrier, len(near))
    scope("diag_ends")
    sent_l = [swap(mine, theirs, f, f * 4 * FACE, FACE, 0) for f in faces]
    greet(hello.at[0], y_near)
    greet(hello.at[1], z_near)
    for copy in loads[2:]:
        copy.wait()
    for k, a in enumerate(both):
        s = contract(SQUARED.T, [g2[across(a, c), :] for c in range(N)], 1)
        for c in range(N):
            tmpf[across(k, c), :] = s[c]
    for b in range(N):
        s = contract(SQUARED.T, [g0[at(a, b), :] for a in range(N)], 1, both)
        for k, a in enumerate(both):
            yf[at(k, b), :] = s[a]
    for k, a in enumerate(both):
        s = contract(SQUARED.T, [g1[at(a, b), :] for b in range(N)], 1)
        for b in range(N):
            mine[part(face_of[a], DIAG, b), :] = lane_pick(
                s[b] + yf[at(k, b), :] + ms[at(a, b), :] + tmpf[at(k, b), :], inverse
            )
    sent_d = [swap(mine, theirs, f, (f * 4 + DIAG) * FACE, FACE, 1) for f in faces]
    for a in both:
        for i in range(N):
            mine[part(face_of[a], G1, i), :] = lane_pick(g1[at(a, i), :], inverse)
            mine[part(face_of[a], G2, i), :] = lane_pick(g2[across(a, i), :], inverse)
    sent_g = [swap(mine, theirs, f, (f * 4 + G1) * FACE, 2 * FACE, 2) for f in faces]

    scope("reorder")
    reorder(ld, ld, inverse, INSIDE)
    reorder(g0, g0, inverse)
    reorder(g1, g1, inverse, INSIDE)
    for a in INSIDE:
        for c in range(N):
            g2t[at(a, c), :] = lane_pick(g2[across(a, c), :], inverse)
    reorder(ms, ms, inverse, INSIDE)
    scope("diag")
    inner_diagonal(g0, g1, g2t, ms, dg, tmp, cross)
    scope("sums")
    sum_yz([(dg, a) for a in INSIDE], lanes)

    def copy_plane(a):
        for b in range(N):
            r[at(a, b), :] = ld[at(a, b), :]

    loop(1, LAST, copy_plane)
    sum_yz([(r, a) for a in INSIDE], lanes)

    def inner_z(a):
        for b in range(N):
            inv = 1.0 / dg[at(a, b), :]
            dg[at(a, b), :] = inv
            z[at(a, b), :] = inv * r[at(a, b), :]

    loop(1, LAST, inner_z)
    scope("L1")
    inner_stiffness(z, g0, g1, g2t, ms, y, tmp)

    def full(f, b):
        return tile(row_of[f] + b * N)

    def face_z(f):
        for b in range(N):
            rf[at(f, b), :] = mine[part(f, LOAD, b), :] + theirs[part(f, LOAD, b), :]
            total = mine[part(f, DIAG, b), :] + theirs[part(f, DIAG, b), :]
            a_sum[at(f, b), :] = total
            df[at(f, b), :] = total
        sum_yz([(rf, f), (df, f)], lanes)
        for b in range(N):
            inv = 1.0 / df[at(f, b), :]
            df[at(f, b), :] = inv
            zf[at(f, b), :] = inv * rf[at(f, b), :]

    def tell(f, v, ends, src, dst, k):
        for b in range(N):
            src[at(f, b), :] = v[full(f, b), :] + cross[at(0, b), :] * ends[at(1 - f, b), :]
        return swap(src, dst, f, f * FACE, FACE, k)

    scope("hello2")
    heard(hello.at[0], y_near)
    y_far = [moved(dy=k) for k in ring(ys, ys // 2 + 1, 3)]
    greet(hello.at[2], y_far)
    heard(hello.at[1], z_near)
    z_mid = [moved(dz=k) for k in ring(zs, 5, 3)]
    greet(hello.at[3], z_mid)
    scope("x_near")
    sent_l[0].wait()
    sent_d[0].wait()
    scope("z_near")
    face_z(0)
    sent_w = [None, tell(1, y, zf, w_mine, w_theirs, 3)]
    sent_g[0].wait()
    face_sums(0, mine, theirs, a_sum, a_sum, tmpf)
    s = face_terms(zf, 0, mine, theirs, a_sum, tmpf)
    for b in range(N):
        yf[at(0, b), :] = s[b]
    scope("x_far")
    sent_l[1].wait()
    sent_d[1].wait()
    scope("z_far")
    face_z(1)
    sent_w[0] = tell(0, y, zf, w_mine, w_theirs, 3)

    scope("inner2")
    first = pl.multiple_of((1 - core) * FACE, FACE)
    add_ends_inside(zf, first, g0, y)
    sum_yz([(y, a) for a in INSIDE], lanes)

    def inner_p(a, num):
        for b in range(N):
            rows = at(a, b)
            p = COEF_Z * z[rows, :] - COEF_Q * (dg[rows, :] * y[rows, :])
            z[rows, :] = p
            num = num + ld[rows, :] * p
        return num

    zero = jnp.zeros((8, LANES), jnp.float32)
    num = lax.fori_loop(1, LAST, inner_p, zero)
    scope("L2")
    inner_stiffness(z, g0, g1, g2t, ms, u, tmp)

    def inner_den(a, den):
        for b in range(N):
            den = den + z[at(a, b), :] * u[at(a, b), :]
        return den

    den = lax.fori_loop(1, LAST, inner_den, zero)
    scope("g_far")
    sent_g[1].wait()
    face_sums(1, mine, theirs, a_sum, a_sum, tmpf)
    s = face_terms(zf, 1, mine, theirs, a_sum, tmpf)
    for b in range(N):
        yf[at(1, b), :] = s[b]
    scope("hello3")
    heard(hello.at[3], z_mid)
    z_far = [moved(dz=k) for k in ring(zs, zs // 2 + 1, 5)]
    greet(hello.at[4], z_far)
    scope("w_far")
    sent_w[1].wait()
    scope("w_near")
    sent_w[0].wait()
    scope("ends2")
    for f in faces:
        for b in range(N):
            rows = at(f, b)
            yf[rows, :] = yf[rows, :] + (w_mine[rows, :] + w_theirs[rows, :])
    sum_yz([(yf, f) for f in faces], lanes)
    for f in faces:
        for b in range(N):
            rows = at(f, b)
            p = COEF_Z * zf[rows, :] - COEF_Q * (df[rows, :] * yf[rows, :])
            pf[rows, :] = p
            num = num + mine[part(f, LOAD, b), :] * p
    for f in faces:
        s = face_terms(pf, f, mine, theirs, a_sum, tmpf)
        for b in range(N):
            yf[at(f, b), :] = s[b]
            part_sum = u[full(f, b), :] + 0.5 * s[b]
            if f == 0:
                part_sum = part_sum + cross[at(0, b), :] * pf[at(1, b), :]
            else:
                part_sum = part_sum + cross[at(0, b), :] * pf[at(0, b), :]
            den = den + pf[at(f, b), :] * (part_sum + u[full(f, b), :])
    dots[0, 0:1, :] = jnp.sum(num, axis=0, keepdims=True)
    dots[0, 1:2, :] = jnp.sum(den, axis=0, keepdims=True)

    hops = sorted(
        ((dy, dx) for dy in range(ys) for dx in range(xs) if dy or dx),
        key=lambda d: -min(d[0], ys - d[0]) - min(d[1], xs - d[1]),
    )
    others = 2 * len(hops) + 1

    def send(src, dst, k, to):
        copy = pltpu.make_async_remote_copy(
            src_ref=src,
            dst_ref=dst,
            send_sem=s_send.at[k],
            recv_sem=s_recv.at[k],
            device_id=(to,),
            device_id_type=MESH,
        )
        copy.start()

    def arrived(ref, sem):
        pltpu.make_async_copy(ref, ref, sem).wait()

    def added(ref, first, total):
        part = [first, None, None, None]
        for j in range(total):
            part[j % 4] = plus(part[j % 4], ref[j])
        return functools.reduce(plus, [t for t in part if t is not None])

    heard(hello.at[2], y_far)
    for j, (dy, dx) in enumerate(hops):
        send(dots.at[0], got_a.at[2 * j + core], 0, moved(dy=dy, dx=dx) + 1 - core)

    @pl.when(core == 0)
    def _():
        send(dots.at[0], got_a.at[others - 1], 0, me + 1)

    scope("u_ends")
    sent_i = [tell(f, u, pf, i_mine, i_theirs, 4) for f in faces]
    add_ends_inside(pf, first, g0, u)
    scope("plane")

    @pl.when(core == 1)
    def _():
        arrived(got_a.at[pl.ds(0, others)], s_recv.at[0])
        dots[1] = added(got_a, dots[0], others)
        heard(hello.at[4], z_far)
        for k in sorted(range(1, zs), key=lambda k: -min(k, zs - k)):
            for c in (0, 1):
                send(dots.at[1], got_b.at[k - 1], 1, moved(dz=k) - c)
        send(dots.at[1], got_b.at[zs - 1], 1, me - 1)
        got_b[zs - 1] = dots[1]

    scope("out_p_r")
    for src, ends, dst in ((z, pf, p_o), (r, rf, r_o)):
        reorder(src, dst, order, INSIDE)
        for f in faces:
            for b in range(N):
                dst[full(f, b), :] = lane_pick(ends[at(f, b), :], order)
    sum_yz([(u, a) for a in INSIDE], lanes)
    reorder(u, im_o, order, INSIDE)
    scope("x3")
    for copy in sent_i:
        copy.wait()
    for f in faces:
        for b in range(N):
            rows = at(f, b)
            yf[rows, :] = yf[rows, :] + (i_mine[rows, :] + i_theirs[rows, :])
    sum_yz([(yf, f) for f in faces], lanes)
    for f in faces:
        for b in range(N):
            im_o[full(f, b), :] = lane_pick(yf[at(f, b), :], order)
    scope("lines")

    @pl.when(core == 0)
    def _():
        heard(hello.at[4], z_far)
        arrived(got_b, s_recv.at[1])

    @pl.when(core == 1)
    def _():
        arrived(got_b.at[pl.ds(0, zs - 1)], s_recv.at[1])

    total = added(got_b, None, zs)
    scope("alpha")
    sums = jnp.sum(total, axis=1, keepdims=True)
    al_o[...] = jnp.broadcast_to(sums[0:1, :] / sums[1:2, :], (8, LANES))
    @pl.when(core == 0)
    def _():
        arrived(got_a.at[pl.ds(0, len(hops) + 1)], s_send.at[0])

    @pl.when(core == 1)
    def _():
        arrived(got_a.at[pl.ds(0, len(hops))], s_send.at[0])
        arrived(got_a.at[pl.ds(0, 2 * zs - 1)], s_send.at[1])

    scope(None)


CHUNKS = 4


def finish_kernel(p, r, im, al, x_h, r_h, x_v, r_v, sems):
    alpha = al[...]
    size = ROWS // CHUNKS
    copies = []
    for k in range(CHUNKS):
        for i in range(k * size, (k + 1) * size, N):
            x_v[tile(i), :] = alpha * p[tile(i), :]
        rows = pl.ds(k * size, size)
        copies.append(pltpu.make_async_copy(x_v.at[rows], x_h.at[rows], sems.at[0, k]))
        copies[-1].start()
        for i in range(k * size, (k + 1) * size, N):
            r_v[tile(i), :] = r[tile(i), :] - alpha * im[tile(i), :]
        copies.append(pltpu.make_async_copy(r_v.at[rows], r_h.at[rows], sems.at[1, k]))
        copies[-1].start()
    for copy in copies:
        copy.wait()


def on_device(load_terms, geometry, mass_terms, element_order):
    flat = jax.ShapeDtypeStruct((ROWS, LANES), jnp.float32)
    vm = lambda *shape: pltpu.VMEM(shape, jnp.float32)
    field = vm(ROWS, LANES)
    pair = vm(2 * FACE, LANES)
    ys, zs, xs, cores = TORUS
    in_vmem = pl.BlockSpec(memory_space=pltpu.VMEM)
    in_hbm = pl.BlockSpec(memory_space=pltpu.HBM)
    parts = pl.pallas_call(
        step_kernel,
        out_shape=(field, field, field, vm(8, LANES)),
        in_specs=[in_hbm] * 4,
        out_specs=[in_vmem] * 4,
        scratch_shapes=[
            *[field] * 12,
            *[vm(8 * FACE, LANES)] * 2,
            *[pair] * 11, vm(FACE, LANES),
            vm(2, 2, LANES), vm(2 * ys * xs - 1, 2, LANES), vm(zs, 2, LANES),
            pltpu.VMEM((1, LANES), jnp.int32),
            pltpu.SemaphoreType.DMA((6,)),
            pltpu.SemaphoreType.DMA((5, 2)),
            pltpu.SemaphoreType.DMA((5, 2)),
            pltpu.SemaphoreType.DMA((2,)),
            pltpu.SemaphoreType.DMA((2,)),
            pltpu.SemaphoreType.REGULAR((5,)),
        ],
        compiler_params=pltpu.CompilerParams(
            collective_id=0, has_side_effects=True, vmem_limit_bytes=24 << 20
        ),
        name="cg_step",
    )(
        *[
            pltpu.with_memory_space_constraint(t, pltpu.HBM)
            for t in (
                load_terms.reshape(ROWS, LANES),
                geometry.reshape(3, ROWS, LANES),
                mass_terms.reshape(ROWS, LANES),
                element_order,
            )
        ]
    )
    x, res = pl.pallas_call(
        finish_kernel,
        out_shape=(flat, flat),
        in_specs=[in_vmem] * 4,
        out_specs=[in_hbm] * 2,
        scratch_shapes=[field, field, pltpu.SemaphoreType.DMA((2, CHUNKS))],
        compiler_params=pltpu.CompilerParams(vmem_limit_bytes=8 << 20),
        name="cg_finish",
    )(*[pltpu.with_memory_space_constraint(t, pltpu.VMEM) for t in parts])
    shape = load_terms.shape
    return x.reshape(shape), res.reshape(shape)


def solution(mesh):
    last = P(None, None, None, "slab")
    return jax.shard_map(
        on_device,
        mesh=mesh,
        in_specs=(last, P(None, None, None, None, "slab"), last, P("slab", None)),
        out_specs=(last, last),
        check_vma=False,
    )
```

```python
import functools

import jax
import jax.numpy as jnp
import numpy as np
from jax import lax
from jax.experimental import pallas as pl
from jax.experimental.pallas import tpu as pltpu
from jax.sharding import PartitionSpec as P

N = 8
LAST = N - 1
EL_Y = 8
EL_Z = 16
LANES = 128
ROWS = N * N * N
FACE = N * N
CENTRE = 1.65
HALF = 1.35
MESH = pl.DeviceIdType.MESH
TORUS = (8, 12, 4, 2)
INSIDE = range(1, LAST)


def legendre_table(positions, points):
    columns = [positions * 0.0 + 1.0, positions]
    for degree in range(2, points):
        columns.append(
            ((2 * degree - 1) * positions * columns[-1] - (degree - 1) * columns[-2]) / degree
        )
    return np.stack(columns, axis=1)


def gll_derivative(points):
    degree = points - 1
    nodes = -np.cos(np.pi * np.arange(points) / degree)
    for _ in range(100):
        legendre = legendre_table(nodes, points)
        nodes = nodes - (nodes * legendre[:, degree] - legendre[:, degree - 1]) / (
            points * legendre[:, degree]
        )
    legendre = legendre_table(nodes, points)
    top = legendre[:, degree]
    same = np.eye(points, dtype=bool)
    spacing = np.where(same, 1.0, nodes[:, None] - nodes[None, :])
    table = np.where(same, 0.0, top[:, None] / (top[None, :] * spacing))
    table[0, 0] = -degree * points / 4.0
    table[degree, degree] = degree * points / 4.0
    return table


DERIV = gll_derivative(N).astype(np.float32).astype(np.float64)
SQUARED = DERIV * DERIV
SIGMA = CENTRE / HALF
RHO0 = 1.0 / SIGMA
RHO1 = 1.0 / (2.0 * SIGMA - RHO0)
COEF_Z = (1.0 + RHO1 * RHO0) / CENTRE + 2.0 * RHO1 / HALF
COEF_Q = 2.0 * RHO1 / HALF / CENTRE


def plus(x, y):
    return y if x is None else x + y


def contract(table, terms, sign, rows=range(N)):
    used = [j for j in range(N // 2) if terms[j] is not None]
    even = {j: terms[j] + terms[LAST - j] for j in used}
    odd = {j: terms[j] - terms[LAST - j] for j in used}
    out = [None] * N
    for i in range(N // 2):
        if i not in rows and LAST - i not in rows:
            continue
        e = o = None
        for j in used:
            e = plus(e, float(table[i, j] + table[i, LAST - j]) / 2 * even[j])
            o = plus(o, float(table[i, j] - table[i, LAST - j]) / 2 * odd[j])
        if i in rows:
            out[i] = e + o
        if LAST - i in rows:
            out[LAST - i] = (o - e) if sign < 0 else (e - o)
    return out


def tile(row):
    return pl.ds(row if isinstance(row, int) else pl.multiple_of(row, 8), 8)


def at(a, b):
    return tile((a * N + b) * N)


def across(a, c):
    return pl.ds(a * FACE + c, N, stride=N)


LOAD, DIAG, G1, G2 = range(4)


def part(f, kind, i):
    return tile(((f * 4 + kind) * N + i) * N)


def loop(start, stop, body):
    lax.fori_loop(start, stop, lambda i, _: (body(i), 0)[1], 0)


def inner_stiffness(v, g0, g1, g2t, ms, out, tmp):
    def along_c(a):
        s = contract(DERIV, [v[across(a, c), :] for c in range(N)], -1)
        s = contract(DERIV.T, [s[c] * g2t[at(a, c), :] for c in range(N)], -1)
        for c in range(N):
            tmp[across(a, c), :] = s[c]

    loop(1, LAST, along_c)

    def along_b(a):
        vb = [v[at(a, b), :] for b in range(N)]
        s = contract(DERIV, vb, -1)
        s = contract(DERIV.T, [s[b] * g1[at(a, b), :] for b in range(N)], -1)
        for b in range(N):
            out[at(a, b), :] = s[b] + ms[at(a, b), :] * vb[b] + tmp[at(a, b), :]

    loop(1, LAST, along_b)

    def along_a(b):
        va = [v[at(a, b), :] if a in INSIDE else None for a in range(N)]
        s = contract(DERIV, va, -1)
        s = contract(DERIV.T, [s[a] * g0[at(a, b), :] for a in range(N)], -1)
        for a in range(N):
            out[at(a, b), :] = out[at(a, b), :] + s[a] if a in INSIDE else s[a]

    loop(0, N, along_a)


def inner_diagonal(g0, g1, g2t, ms, out, tmp, cross):
    def along_c(a):
        s = contract(SQUARED.T, [g2t[at(a, c), :] for c in range(N)], 1)
        for c in range(N):
            tmp[across(a, c), :] = s[c]

    loop(1, LAST, along_c)

    def along_b(a):
        s = contract(SQUARED.T, [g1[at(a, b), :] for b in range(N)], 1)
        for b in range(N):
            out[at(a, b), :] = s[b] + ms[at(a, b), :] + tmp[at(a, b), :]

    loop(1, LAST, along_b)

    def along_a(b):
        g = [g0[at(a, b), :] for a in range(N)]
        s = contract(SQUARED.T, g, 1, INSIDE)
        for a in INSIDE:
            out[at(a, b), :] = out[at(a, b), :] + s[a]
        both = None
        for m in range(N):
            both = plus(both, float(DERIV[m, 0] * DERIV[m, LAST]) * g[m])
        cross[at(0, b), :] = both

    loop(0, N, along_a)


def face_terms(v, f, mine, theirs, a_sum, tmp):
    s = contract(DERIV, [v[across(f, c), :] for c in range(N)], -1)
    s = contract(DERIV.T, [s[c] * theirs[part(f, G2, c), :] for c in range(N)], -1)
    for c in range(N):
        tmp[across(f, c), :] = s[c]
    vb = [v[at(f, b), :] for b in range(N)]
    s = contract(DERIV, vb, -1)
    s = contract(DERIV.T, [s[b] * theirs[part(f, G1, b), :] for b in range(N)], -1)
    return [s[b] + a_sum[at(f, b), :] * vb[b] + tmp[at(f, b), :] for b in range(N)]


def face_sums(f, mine, theirs, diag, a_sum, tmp):
    g = [[mine[part(f, k, i), :] + theirs[part(f, k, i), :] for i in range(N)] for k in (G1, G2)]
    for k in (G1, G2):
        for i in range(N):
            theirs[part(f, k, i), :] = g[k - G1][i]
    s = contract(SQUARED.T, g[1], 1)
    for c in range(N):
        tmp[across(f, c), :] = s[c]
    s = contract(SQUARED.T, g[0], 1)
    for b in range(N):
        a_sum[at(f, b), :] = diag[at(f, b), :] - s[b] - tmp[at(f, b), :]


def add_ends_inside(v, first, g0, out):
    def one(b):
        ends = [None] * N
        ends[0] = v[tile(first + b * N), :]
        ends[LAST] = v[tile(FACE - first + b * N), :]
        s = contract(DERIV, ends, -1)
        s = contract(DERIV.T, [s[a] * g0[at(a, b), :] for a in range(N)], -1, INSIDE)
        for a in INSIDE:
            out[at(a, b), :] = out[at(a, b), :] + s[a]

    loop(0, N, one)


def lane_pick(x, idx):
    return jnp.take_along_axis(x, idx, axis=1, mode="promise_in_bounds")


def sum_yz(planes, lanes):
    for v, a in planes:
        low, high = v[at(a, 0), :], v[at(a, LAST), :]
        v[at(a, LAST), :] = high + jnp.where(lanes["up"], pltpu.roll(low, LANES - EL_Z, 1), 0.0)
        v[at(a, 0), :] = low + jnp.where(lanes["down"], pltpu.roll(high, EL_Z, 1), 0.0)
    lows = [v[across(a, 0), :] for v, a in planes]
    highs = [v[across(a, LAST), :] for v, a in planes]
    nexts = [lane_pick(low, lanes["next"]) for low in lows]
    prevs = [lane_pick(high, lanes["prev"]) for high in highs]
    for k, (v, a) in enumerate(planes):
        v[across(a, LAST), :] = highs[k] + nexts[k]
        v[across(a, 0), :] = lows[k] + prevs[k]


def step_kernel(
    load_h, geom_h, mass_h, order_h, p_o, r_o, im_o, al_o,
    ld, g0, g1, g2, g2t, ms, r, dg, z, y, u, tmp,
    mine, theirs, w_mine, w_theirs, i_mine, i_theirs, bag, rf, df, zf, pf, yf, a_sum, tmpf, cross,
    dots, got_a, got_b, order_v, in_sems, x_send, x_recv, bag_send, bag_recv, s_send, s_recv, hello,
):
    stack = []

    def scope(name):
        if stack:
            stack.pop().__exit__(None, None, None)
        if name:
            stack.append(jax.named_scope(name))
            stack[-1].__enter__()

    scope("enter")
    ys, zs, xs, cores = TORUS
    count = lax.axis_size("slab")
    me = lax.axis_index("slab")
    core = lax.rem(me, cores)
    x = lax.rem(me // cores, xs)
    z_at = lax.rem(me // (cores * xs), zs)
    y_at = me // (cores * xs * zs)
    near_to = me + 1 - 2 * core
    far_to = lax.rem(me + count + 2 * core - 1, count)
    sides = (near_to, far_to)
    row_of = (pl.multiple_of((1 - core) * (ROWS - FACE), FACE), pl.multiple_of(core * (ROWS - FACE), FACE))
    face_of = {0: 1 - core, LAST: core}

    def moved(dy=0, dz=0, dx=0):
        to = me
        if dy:
            to = to + (lax.rem(y_at + dy, ys) - y_at) * (cores * xs * zs)
        if dz:
            to = to + (lax.rem(z_at + dz, zs) - z_at) * (cores * xs)
        if dx:
            to = to + (lax.rem(x + dx, xs) - x) * cores
        return to

    def ring(size, stop, start=1):
        return sorted({j % size for k in range(start, stop) for j in (k, -k)} - {0})

    def greet(sem, who):
        for q in who:
            pl.semaphore_signal(sem, inc=1, device_id=(q,), device_id_type=MESH)

    def heard(sem, who):
        if who:
            pl.semaphore_wait(sem, len(who))

    early = (z_at == 0) & (x == 0) & (core == 0)
    carrier = (z_at == 0) & (x == xs - 1) & (core == 1)
    late = (z_at == zs - 1) & (x == xs - 1) & (core == 1)
    plane_size = zs * xs * cores
    carrier_of_early = lax.rem(y_at + ys - 1, ys) * plane_size + xs * cores - 1
    carrier_of_late = y_at * plane_size + xs * cores - 1
    early_of_carrier = lax.rem(y_at + 1, ys) * plane_size
    late_of_carrier = y_at * plane_size + plane_size - 1

    row = [moved(dx=k) + c for k in range(xs) for c in (0, 1 - 2 * core) if k or not isinstance(c, int)]
    y_near = [moved(dy=k) for k in ring(ys, 3)]
    y_far = [moved(dy=k) for k in ring(ys, ys // 2 + 1, 3)]
    barrier = pltpu.get_barrier_semaphore()
    greet(barrier, [jnp.where(late, carrier_of_late, far_to), near_to])
    greet(barrier, row + y_near)

    @pl.when(early | carrier)
    def _():
        greet(barrier, [jnp.where(early, carrier_of_early, early_of_carrier)])

    for k in range(1, zs):

        @pl.when(z_at + k < zs)
        def _(k=k):
            greet(barrier, [me + k * xs * cores + 1 - core])

    expected = len(row) + len(y_near) + 2 + 2 * carrier.astype(jnp.int32) + cores * core * z_at

    loads = [
        pltpu.make_async_copy(src, dst, in_sems.at[k])
        for k, (src, dst) in enumerate(
            (
                (order_h, order_v),
                (load_h, ld),
                (geom_h.at[0], g0),
                (geom_h.at[1], g1),
                (geom_h.at[2], g2),
                (mass_h, ms),
            )
        )
    ]
    for copy in loads:
        copy.start()

    scope("idx")
    loads[0].wait()
    order = jnp.broadcast_to(order_v[...], (8, LANES))
    hit = (
        jnp.broadcast_to(order_v[...], (LANES, LANES))
        == lax.broadcasted_iota(jnp.int32, (LANES, LANES), 0)
    ).astype(jnp.float32)
    lane = lax.broadcasted_iota(jnp.int32, (8, LANES), 1)
    inverse = lax.dot_general(
        lane.astype(jnp.float32), hit, (((1,), (1,)), ((), ())), preferred_element_type=jnp.float32
    )
    inverse = (inverse + 0.5).astype(jnp.int32)
    in_row = lane & (EL_Z - 1)
    lanes = {
        "up": lane < LANES - EL_Z,
        "down": lane >= EL_Z,
        "next": lane - in_row + ((in_row + 1) & (EL_Z - 1)),
        "prev": lane - in_row + ((in_row + EL_Z - 1) & (EL_Z - 1)),
    }

    def reorder(src, dst, idx, planes=range(N)):
        for a in planes:
            for b in range(N):
                dst[at(a, b), :] = lane_pick(src[at(a, b), :], idx)

    def swap(src, dst, f, first, rows, k, carried=None):
        copy = pltpu.make_async_remote_copy(
            src_ref=src.at[pl.ds(first, rows)],
            dst_ref=dst.at[pl.ds(first, rows)],
            send_sem=x_send.at[k, f],
            recv_sem=x_recv.at[k, f],
            device_id=(sides[f],),
            device_id_type=MESH,
        )
        if f == 0 or carried is None:
            copy.start()
            return copy

        @pl.when(early)
        def _():
            pltpu.make_async_remote_copy(
                src_ref=src.at[pl.ds(first, rows)],
                dst_ref=bag.at[pl.ds(carried, rows)],
                send_sem=x_send.at[k, f],
                recv_sem=bag_recv.at[k],
                device_id=(carrier_of_early,),
                device_id_type=MESH,
            ).start()

        pl.when(jnp.logical_not(early))(copy.start)
        return copy

    def carry(dst, carried, first, rows, k):
        return pltpu.make_async_remote_copy(
            src_ref=bag.at[pl.ds(carried, rows)],
            dst_ref=dst.at[pl.ds(first, rows)],
            send_sem=bag_send.at[k],
            recv_sem=x_recv.at[k, 1],
            device_id=(late_of_carrier,),
            device_id_type=MESH,
        )

    both = (0, LAST)
    faces = (0, 1)
    scope("load_ends")
    loads[1].wait()
    for a in both:
        for b in range(N):
            mine[part(face_of[a], LOAD, b), :] = lane_pick(ld[at(a, b), :], inverse)
    for copy in loads[2:]:
        copy.wait()
    for k, a in enumerate(both):
        s = contract(SQUARED.T, [g2[across(a, c), :] for c in range(N)], 1)
        for c in range(N):
            tmpf[across(k, c), :] = s[c]
    for b in range(N):
        s = contract(SQUARED.T, [g0[at(a, b), :] for a in range(N)], 1, both)
        for k, a in enumerate(both):
            yf[at(k, b), :] = s[a]
    for k, a in enumerate(both):
        s = contract(SQUARED.T, [g1[at(a, b), :] for b in range(N)], 1)
        for b in range(N):
            mine[part(face_of[a], DIAG, b), :] = lane_pick(
                s[b] + yf[at(k, b), :] + ms[at(a, b), :] + tmpf[at(k, b), :], inverse
            )
    for a in both:
        for i in range(N):
            mine[part(face_of[a], G1, i), :] = lane_pick(g1[at(a, i), :], inverse)
            mine[part(face_of[a], G2, i), :] = lane_pick(g2[across(a, i), :], inverse)
    scope("barrier")
    pl.semaphore_wait(barrier, expected)
    scope("send1")
    carried1 = ((0, 4 * FACE, 2 * FACE), (1, 4 * FACE + 2 * FACE, 2 * FACE))

    @pl.when(carrier)
    def _():
        for k, first, rows in carried1:
            got = bag.at[pl.ds(first - 4 * FACE, rows)]
            pltpu.make_async_copy(got, got, bag_recv.at[k]).wait()
            carry(theirs, first - 4 * FACE, first, rows, k).start()

    sent_ld = [swap(mine, theirs, f, f * 4 * FACE, 2 * FACE, 0, 0) for f in (1, 0)][::-1]
    sent_g = [swap(mine, theirs, f, (f * 4 + 2) * FACE, 2 * FACE, 1, 2 * FACE) for f in (1, 0)][::-1]
    greet(hello.at[0], y_near)

    @pl.when(core == 1)
    def _():
        for k in range(1, zs):

            @pl.when(z_at >= k)
            def _(k=k):
                greet(hello.at[2], [me - k * xs * cores])

    scope("reorder")
    reorder(ld, ld, inverse, INSIDE)
    reorder(g0, g0, inverse)
    reorder(g1, g1, inverse, INSIDE)
    for a in INSIDE:
        for c in range(N):
            g2t[at(a, c), :] = lane_pick(g2[across(a, c), :], inverse)
    reorder(ms, ms, inverse, INSIDE)
    scope("diag")
    inner_diagonal(g0, g1, g2t, ms, dg, tmp, cross)
    scope("sums")
    sum_yz([(dg, a) for a in INSIDE], lanes)

    def copy_plane(a):
        for b in range(N):
            r[at(a, b), :] = ld[at(a, b), :]

    loop(1, LAST, copy_plane)
    sum_yz([(r, a) for a in INSIDE], lanes)

    def inner_z(a):
        for b in range(N):
            inv = 1.0 / dg[at(a, b), :]
            dg[at(a, b), :] = inv
            z[at(a, b), :] = inv * r[at(a, b), :]

    loop(1, LAST, inner_z)
    scope("L1")
    inner_stiffness(z, g0, g1, g2t, ms, y, tmp)

    def full(f, b):
        return tile(row_of[f] + b * N)

    def face_z(f):
        for b in range(N):
            rf[at(f, b), :] = mine[part(f, LOAD, b), :] + theirs[part(f, LOAD, b), :]
            total = mine[part(f, DIAG, b), :] + theirs[part(f, DIAG, b), :]
            a_sum[at(f, b), :] = total
            df[at(f, b), :] = total
        sum_yz([(rf, f), (df, f)], lanes)
        for b in range(N):
            inv = 1.0 / df[at(f, b), :]
            df[at(f, b), :] = inv
            zf[at(f, b), :] = inv * rf[at(f, b), :]

    def tell(f, v, ends, src, dst, k, carried=None):
        for b in range(N):
            src[at(f, b), :] = v[full(f, b), :] + cross[at(0, b), :] * ends[at(1 - f, b), :]
        return swap(src, dst, f, f * FACE, FACE, k, carried)

    scope("hello")

    @pl.when(carrier)
    def _():
        got = bag.at[pl.ds(4 * FACE, FACE)]
        pltpu.make_async_copy(got, got, bag_recv.at[2]).wait()
        carry(w_theirs, 4 * FACE, FACE, FACE, 2).start()

    heard(hello.at[0], y_near)
    greet(hello.at[1], y_far)
    scope("x_near")
    sent_ld[0].wait()
    scope("z_near")
    face_z(0)
    sent_w = [None, tell(1, y, zf, w_mine, w_theirs, 2, 4 * FACE)]
    sent_g[0].wait()
    face_sums(0, mine, theirs, a_sum, a_sum, tmpf)
    s = face_terms(zf, 0, mine, theirs, a_sum, tmpf)
    for b in range(N):
        yf[at(0, b), :] = s[b]
    scope("x_far")
    sent_ld[1].wait()
    scope("z_far")
    face_z(1)
    sent_w[0] = tell(0, y, zf, w_mine, w_theirs, 2)

    scope("inner2")
    first = pl.multiple_of((1 - core) * FACE, FACE)
    add_ends_inside(zf, first, g0, y)
    sum_yz([(y, a) for a in INSIDE], lanes)

    def inner_p(a, num):
        for b in range(N):
            rows = at(a, b)
            p = COEF_Z * z[rows, :] - COEF_Q * (dg[rows, :] * y[rows, :])
            z[rows, :] = p
            num = num + ld[rows, :] * p
        return num

    zero = jnp.zeros((8, LANES), jnp.float32)
    num = lax.fori_loop(1, LAST, inner_p, zero)
    scope("L2")
    inner_stiffness(z, g0, g1, g2t, ms, u, tmp)

    def inner_den(a, den):
        for b in range(N):
            den = den + z[at(a, b), :] * u[at(a, b), :]
        return den

    den = lax.fori_loop(1, LAST, inner_den, zero)
    scope("g_far")
    sent_g[1].wait()
    face_sums(1, mine, theirs, a_sum, a_sum, tmpf)
    s = face_terms(zf, 1, mine, theirs, a_sum, tmpf)
    for b in range(N):
        yf[at(1, b), :] = s[b]
    scope("w_far")
    sent_w[1].wait()
    scope("w_near")
    sent_w[0].wait()
    scope("ends2")
    for f in faces:
        for b in range(N):
            rows = at(f, b)
            yf[rows, :] = yf[rows, :] + (w_mine[rows, :] + w_theirs[rows, :])
    sum_yz([(yf, f) for f in faces], lanes)
    for f in faces:
        for b in range(N):
            rows = at(f, b)
            p = COEF_Z * zf[rows, :] - COEF_Q * (df[rows, :] * yf[rows, :])
            pf[rows, :] = p
            num = num + mine[part(f, LOAD, b), :] * p
    for f in faces:
        s = face_terms(pf, f, mine, theirs, a_sum, tmpf)
        for b in range(N):
            yf[at(f, b), :] = s[b]
            part_sum = u[full(f, b), :] + 0.5 * s[b]
            if f == 0:
                part_sum = part_sum + cross[at(0, b), :] * pf[at(1, b), :]
            else:
                part_sum = part_sum + cross[at(0, b), :] * pf[at(0, b), :]
            den = den + pf[at(f, b), :] * (part_sum + u[full(f, b), :])
    dots[0, 0:1, :] = jnp.sum(num, axis=0, keepdims=True)
    dots[0, 1:2, :] = jnp.sum(den, axis=0, keepdims=True)

    hops = sorted(
        ((dy, dx) for dy in range(ys) for dx in range(xs) if dy or dx),
        key=lambda d: -min(d[0], ys - d[0]) - min(d[1], xs - d[1]),
    )
    others = 2 * len(hops) + 1

    def send(src, dst, k, to):
        copy = pltpu.make_async_remote_copy(
            src_ref=src,
            dst_ref=dst,
            send_sem=s_send.at[k],
            recv_sem=s_recv.at[k],
            device_id=(to,),
            device_id_type=MESH,
        )
        copy.start()

    def arrived(ref, sem):
        pltpu.make_async_copy(ref, ref, sem).wait()

    def added(ref, first, total):
        part = [first, None, None, None]
        for j in range(total):
            part[j % 4] = plus(part[j % 4], ref[j])
        return functools.reduce(plus, [t for t in part if t is not None])

    heard(hello.at[1], y_far)
    for j, (dy, dx) in enumerate(hops):
        send(dots.at[0], got_a.at[2 * j + core], 0, moved(dy=dy, dx=dx) + 1 - core)

    @pl.when(core == 0)
    def _():
        send(dots.at[0], got_a.at[others - 1], 0, me + 1)

    scope("u_ends")
    sent_i = [tell(f, u, pf, i_mine, i_theirs, 3) for f in faces]
    add_ends_inside(pf, first, g0, u)
    scope("plane")

    @pl.when(core == 1)
    def _():
        arrived(got_a.at[pl.ds(0, others)], s_recv.at[0])
        dots[1] = added(got_a, dots[0], others)

        @pl.when(z_at < zs - 1)
        def _():
            pl.semaphore_wait(hello.at[2], zs - 1 - z_at)

        for k in sorted(range(1, zs), key=lambda k: -min(k, zs - k)):
            for c in (0, 1):
                send(dots.at[1], got_b.at[k - 1], 1, moved(dz=k) - c)
        send(dots.at[1], got_b.at[zs - 1], 1, me - 1)
        got_b[zs - 1] = dots[1]

    scope("out_p_r")
    for src, ends, dst in ((z, pf, p_o), (r, rf, r_o)):
        reorder(src, dst, order, INSIDE)
        for f in faces:
            for b in range(N):
                dst[full(f, b), :] = lane_pick(ends[at(f, b), :], order)
    sum_yz([(u, a) for a in INSIDE], lanes)
    reorder(u, im_o, order, INSIDE)
    scope("x3")
    for copy in sent_i:
        copy.wait()
    for f in faces:
        for b in range(N):
            rows = at(f, b)
            yf[rows, :] = yf[rows, :] + (i_mine[rows, :] + i_theirs[rows, :])
    sum_yz([(yf, f) for f in faces], lanes)
    for f in faces:
        for b in range(N):
            im_o[full(f, b), :] = lane_pick(yf[at(f, b), :], order)
    scope("lines")

    @pl.when(core == 0)
    def _():
        arrived(got_b, s_recv.at[1])

    @pl.when(core == 1)
    def _():
        arrived(got_b.at[pl.ds(0, zs - 1)], s_recv.at[1])

    total = added(got_b, None, zs)
    scope("alpha")
    sums = jnp.sum(total, axis=1, keepdims=True)
    al_o[...] = jnp.broadcast_to(sums[0:1, :] / sums[1:2, :], (8, LANES))
    @pl.when(carrier)
    def _():
        for k, first, rows in carried1:
            carry(theirs, first - 4 * FACE, first, rows, k).wait_send()
        carry(w_theirs, 4 * FACE, FACE, FACE, 2).wait_send()

    @pl.when(core == 0)
    def _():
        arrived(got_a.at[pl.ds(0, len(hops) + 1)], s_send.at[0])

    @pl.when(core == 1)
    def _():
        arrived(got_a.at[pl.ds(0, len(hops))], s_send.at[0])
        arrived(got_a.at[pl.ds(0, 2 * zs - 1)], s_send.at[1])

    scope(None)


CHUNKS = 4


def finish_kernel(p, r, im, al, x_h, r_h, x_v, r_v, sems):
    alpha = al[...]
    size = ROWS // CHUNKS
    copies = []
    for k in range(CHUNKS):
        for i in range(k * size, (k + 1) * size, N):
            x_v[tile(i), :] = alpha * p[tile(i), :]
        rows = pl.ds(k * size, size)
        copies.append(pltpu.make_async_copy(x_v.at[rows], x_h.at[rows], sems.at[0, k]))
        copies[-1].start()
        for i in range(k * size, (k + 1) * size, N):
            r_v[tile(i), :] = r[tile(i), :] - alpha * im[tile(i), :]
        copies.append(pltpu.make_async_copy(r_v.at[rows], r_h.at[rows], sems.at[1, k]))
        copies[-1].start()
    for copy in copies:
        copy.wait()


def on_device(load_terms, geometry, mass_terms, element_order):
    flat = jax.ShapeDtypeStruct((ROWS, LANES), jnp.float32)
    vm = lambda *shape: pltpu.VMEM(shape, jnp.float32)
    field = vm(ROWS, LANES)
    pair = vm(2 * FACE, LANES)
    ys, zs, xs, cores = TORUS
    in_vmem = pl.BlockSpec(memory_space=pltpu.VMEM)
    in_hbm = pl.BlockSpec(memory_space=pltpu.HBM)
    parts = pl.pallas_call(
        step_kernel,
        out_shape=(field, field, field, vm(8, LANES)),
        in_specs=[in_hbm] * 4,
        out_specs=[in_vmem] * 4,
        scratch_shapes=[
            *[field] * 12,
            *[vm(8 * FACE, LANES)] * 2,
            *[pair] * 4, vm(5 * FACE, LANES), *[pair] * 7, vm(FACE, LANES),
            vm(2, 2, LANES), vm(2 * ys * xs - 1, 2, LANES), vm(zs, 2, LANES),
            pltpu.VMEM((1, LANES), jnp.int32),
            pltpu.SemaphoreType.DMA((6,)),
            pltpu.SemaphoreType.DMA((4, 2)),
            pltpu.SemaphoreType.DMA((4, 2)),
            pltpu.SemaphoreType.DMA((3,)),
            pltpu.SemaphoreType.DMA((3,)),
            pltpu.SemaphoreType.DMA((2,)),
            pltpu.SemaphoreType.DMA((2,)),
            pltpu.SemaphoreType.REGULAR((3,)),
        ],
        compiler_params=pltpu.CompilerParams(
            collective_id=0, has_side_effects=True, vmem_limit_bytes=24 << 20
        ),
        name="cg_step",
    )(
        *[
            pltpu.with_memory_space_constraint(t, pltpu.HBM)
            for t in (
                load_terms.reshape(ROWS, LANES),
                geometry.reshape(3, ROWS, LANES),
                mass_terms.reshape(ROWS, LANES),
                element_order,
            )
        ]
    )
    x, res = pl.pallas_call(
        finish_kernel,
        out_shape=(flat, flat),
        in_specs=[in_vmem] * 4,
        out_specs=[in_hbm] * 2,
        scratch_shapes=[field, field, pltpu.SemaphoreType.DMA((2, CHUNKS))],
        compiler_params=pltpu.CompilerParams(vmem_limit_bytes=8 << 20),
        name="cg_finish",
    )(*[pltpu.with_memory_space_constraint(t, pltpu.VMEM) for t in parts])
    shape = load_terms.shape
    return x.reshape(shape), res.reshape(shape)


def solution(mesh):
    last = P(None, None, None, "slab")
    return jax.shard_map(
        on_device,
        mesh=mesh,
        in_specs=(last, P(None, None, None, None, "slab"), last, P("slab", None)),
        out_specs=(last, last),
        check_vma=False,
    )
```

```python
import functools

import jax
import jax.numpy as jnp
import numpy as np
from jax import lax
from jax.experimental import pallas as pl
from jax.experimental.pallas import tpu as pltpu
from jax.sharding import PartitionSpec as P

N = 8
LAST = N - 1
EL_Y = 8
EL_Z = 16
LANES = 128
ROWS = N * N * N
FACE = N * N
CENTRE = 1.65
HALF = 1.35
MESH = pl.DeviceIdType.MESH
TORUS = (8, 12, 4, 2)
INSIDE = range(1, LAST)
UNROLL_A = 4
UNROLL_BC = 3


def legendre_table(positions, points):
    columns = [positions * 0.0 + 1.0, positions]
    for degree in range(2, points):
        columns.append(
            ((2 * degree - 1) * positions * columns[-1] - (degree - 1) * columns[-2]) / degree
        )
    return np.stack(columns, axis=1)


def gll_derivative(points):
    degree = points - 1
    nodes = -np.cos(np.pi * np.arange(points) / degree)
    for _ in range(100):
        legendre = legendre_table(nodes, points)
        nodes = nodes - (nodes * legendre[:, degree] - legendre[:, degree - 1]) / (
            points * legendre[:, degree]
        )
    legendre = legendre_table(nodes, points)
    top = legendre[:, degree]
    same = np.eye(points, dtype=bool)
    spacing = np.where(same, 1.0, nodes[:, None] - nodes[None, :])
    table = np.where(same, 0.0, top[:, None] / (top[None, :] * spacing))
    table[0, 0] = -degree * points / 4.0
    table[degree, degree] = degree * points / 4.0
    return table


DERIV = gll_derivative(N).astype(np.float32).astype(np.float64)
SQUARED = DERIV * DERIV
SIGMA = CENTRE / HALF
RHO0 = 1.0 / SIGMA
RHO1 = 1.0 / (2.0 * SIGMA - RHO0)
COEF_Z = (1.0 + RHO1 * RHO0) / CENTRE + 2.0 * RHO1 / HALF
COEF_Q = 2.0 * RHO1 / HALF / CENTRE


def plus(x, y):
    return y if x is None else x + y


def contract(table, terms, sign, rows=range(N)):
    used = [j for j in range(N // 2) if terms[j] is not None]
    even = {j: terms[j] + terms[LAST - j] for j in used}
    odd = {j: terms[j] - terms[LAST - j] for j in used}
    out = [None] * N
    for i in range(N // 2):
        if i not in rows and LAST - i not in rows:
            continue
        e = o = None
        for j in used:
            e = plus(e, float(table[i, j] + table[i, LAST - j]) / 2 * even[j])
            o = plus(o, float(table[i, j] - table[i, LAST - j]) / 2 * odd[j])
        if i in rows:
            out[i] = e + o
        if LAST - i in rows:
            out[LAST - i] = (o - e) if sign < 0 else (e - o)
    return out


def tile(row):
    return pl.ds(row if isinstance(row, int) else pl.multiple_of(row, 8), 8)


def at(a, b):
    return tile((a * N + b) * N)


def across(a, c):
    return pl.ds(a * FACE + c, N, stride=N)


LOAD, DIAG, G1, G2 = range(4)


def part(f, kind, i):
    return tile(((f * 4 + kind) * N + i) * N)


def loop(start, stop, body):
    lax.fori_loop(start, stop, lambda i, _: (body(i), 0)[1], 0)


def stiffness_a(v, g0, out, rows=range(N), more=None):
    def along_a(b, _):
        va = [v[at(a, b), :] if a in INSIDE else None for a in range(N)]
        s = contract(DERIV, va, -1)
        s = contract(DERIV.T, [s[a] * g0[at(a, b), :] for a in range(N)], -1, rows)
        for a in rows:
            out[at(a, b), :] = s[a] if more is None else s[a] + more[at(a, b), :]
        return 0

    lax.fori_loop(0, N, along_a, 0, unroll=UNROLL_A)


def energy_a(v, g0, ends, first, total):
    def along_a(b, total):
        t = contract(DERIV, [v[at(a, b), :] if a in INSIDE else None for a in range(N)], -1)
        s = [t[a] * g0[at(a, b), :] for a in range(N)]
        total = [total[k] + s[k] * t[k] + s[k + 4] * t[k + 4] for k in range(4)]
        s = contract(DERIV.T, s, -1, (0, LAST))
        ends[tile(first + b * N), :] = s[0]
        ends[tile(FACE - first + b * N), :] = s[LAST]
        return total

    return lax.fori_loop(0, N, along_a, total, unroll=UNROLL_A)


def energy_bc(v, g1, g2t, ms, total):
    def along_bc(a, total):
        vb = [v[at(a, b), :] for b in range(N)]
        for own, g in (([v[across(a, c), :] for c in range(N)], g2t), (vb, g1)):
            t = contract(DERIV, own, -1)
            e = [t[i] * g[at(a, i), :] * t[i] for i in range(N)]
            total = [total[k] + (e[k] + e[k + 4]) for k in range(4)]
        e = [vb[b] * ms[at(a, b), :] * vb[b] for b in range(N)]
        return [total[k] + (e[k] + e[k + 4]) for k in range(4)]

    return lax.fori_loop(1, LAST, along_bc, total, unroll=UNROLL_BC)


def stiffness_bc(v, g1, g2t, ms, out, tmp, more=None):
    def along_bc(a, _):
        vt = [v[across(a, c), :] for c in range(N)]
        vb = [v[at(a, b), :] for b in range(N)]
        t = contract(DERIV, vt, -1)
        t = contract(DERIV.T, [t[c] * g2t[at(a, c), :] for c in range(N)], -1)
        for c in range(N):
            tmp[across(a, c), :] = t[c]
        s = contract(DERIV, vb, -1)
        s = contract(DERIV.T, [s[b] * g1[at(a, b), :] for b in range(N)], -1)
        for b in range(N):
            s[b] = s[b] + ms[at(a, b), :] * vb[b]
            if more is not None:
                s[b] = s[b] + more[at(a, b), :]
        for b in range(N):
            out[at(a, b), :] = s[b] + tmp[at(a, b), :]
        return 0

    lax.fori_loop(1, LAST, along_bc, 0, unroll=UNROLL_BC)


def inner_diagonal(g0, g1, g2t, ms, out, tmp, cross):
    def along_c(a):
        s = contract(SQUARED.T, [g2t[at(a, c), :] for c in range(N)], 1)
        for c in range(N):
            tmp[across(a, c), :] = s[c]

    loop(1, LAST, along_c)

    def along_b(a):
        s = contract(SQUARED.T, [g1[at(a, b), :] for b in range(N)], 1)
        for b in range(N):
            out[at(a, b), :] = s[b] + ms[at(a, b), :] + tmp[at(a, b), :]

    loop(1, LAST, along_b)

    def along_a(b):
        g = [g0[at(a, b), :] for a in range(N)]
        s = contract(SQUARED.T, g, 1, INSIDE)
        for a in INSIDE:
            out[at(a, b), :] = out[at(a, b), :] + s[a]
        both = None
        for m in range(N):
            both = plus(both, float(DERIV[m, 0] * DERIV[m, LAST]) * g[m])
        cross[at(0, b), :] = both

    loop(0, N, along_a)


def face_terms(v, f, mine, theirs, a_sum, tmp):
    s = contract(DERIV, [v[across(f, c), :] for c in range(N)], -1)
    s = contract(DERIV.T, [s[c] * theirs[part(f, G2, c), :] for c in range(N)], -1)
    for c in range(N):
        tmp[across(f, c), :] = s[c]
    vb = [v[at(f, b), :] for b in range(N)]
    s = contract(DERIV, vb, -1)
    s = contract(DERIV.T, [s[b] * theirs[part(f, G1, b), :] for b in range(N)], -1)
    return [s[b] + a_sum[at(f, b), :] * vb[b] + tmp[at(f, b), :] for b in range(N)]


def face_energy(v, f, theirs, a_sum):
    vb = [v[at(f, b), :] for b in range(N)]
    e = [a_sum[at(f, b), :] * vb[b] * vb[b] for b in range(N)]
    for own, kind in (([v[across(f, c), :] for c in range(N)], G2), (vb, G1)):
        t = contract(DERIV, own, -1)
        e = [e[i] + t[i] * theirs[part(f, kind, i), :] * t[i] for i in range(N)]
    return added_up(e)


def added_up(terms):
    while len(terms) > 1:
        terms = [functools.reduce(plus, terms[i : i + 2]) for i in range(0, len(terms), 2)]
    return terms[0]


def face_sums(f, mine, theirs, diag, a_sum, tmp):
    g = [[mine[part(f, k, i), :] + theirs[part(f, k, i), :] for i in range(N)] for k in (G1, G2)]
    for k in (G1, G2):
        for i in range(N):
            theirs[part(f, k, i), :] = g[k - G1][i]
    s = contract(SQUARED.T, g[1], 1)
    for c in range(N):
        tmp[across(f, c), :] = s[c]
    s = contract(SQUARED.T, g[0], 1)
    for b in range(N):
        a_sum[at(f, b), :] = diag[at(f, b), :] - s[b] - tmp[at(f, b), :]


def couplings(g0, first, out):
    def one(b, _):
        g = [g0[at(a, b), :] for a in range(N)]
        for a_end, row in ((0, first), (LAST, FACE - first)):
            s = contract(DERIV.T, [float(DERIV[m, a_end]) * g[m] for m in range(N)], -1, INSIDE)
            for a in INSIDE:
                out[tile(row * 6 + ((a - 1) * N + b) * N), :] = s[a]
        return 0

    lax.fori_loop(0, N, one, 0, unroll=2)


def couple(v, f, coupling, out, a):
    for b in range(N):
        out[at(a, b), :] = (
            out[at(a, b), :] + coupling[tile(((f * 6 + a - 1) * N + b) * N), :] * v[at(f, b), :]
        )


def lane_pick(x, idx):
    return jnp.take_along_axis(x, idx, axis=1, mode="promise_in_bounds")


def sum_yz(planes, lanes):
    ends = [(v[at(a, 0), :], v[at(a, LAST), :]) for v, a in planes]
    rims = [(v[across(a, 0), :], v[across(a, LAST), :]) for v, a in planes]
    ups = [jnp.where(lanes["up"], pltpu.roll(low, LANES - EL_Z, 1), 0.0) for low, _ in ends]
    downs = [jnp.where(lanes["down"], pltpu.roll(high, EL_Z, 1), 0.0) for _, high in ends]
    nexts = [lane_pick(low, lanes["next"]) for low, _ in rims]
    prevs = [lane_pick(high, lanes["prev"]) for _, high in rims]

    def corners(rim, idx):
        turned = jnp.where(lanes["first"], pltpu.roll(rim, 1, 0), pltpu.roll(rim, LAST, 0))
        return jnp.where(lanes["corner"], lane_pick(turned, idx), 0.0)

    far_nexts = [corners(low, lanes["corner_next"]) for low, _ in rims]
    far_prevs = [corners(high, lanes["corner_prev"]) for _, high in rims]
    for k, (v, a) in enumerate(planes):
        v[across(a, LAST), :] = rims[k][1] + (nexts[k] + far_nexts[k])
        v[across(a, 0), :] = rims[k][0] + (prevs[k] + far_prevs[k])
        v[at(a, LAST), :] = v[at(a, LAST), :] + ups[k]
        v[at(a, 0), :] = v[at(a, 0), :] + downs[k]


def step_kernel(
    load_h, geom_h, mass_h, order_h, p_o, r_o, im_o, al_o,
    ld, g0, g1, g2, g2t, ms, r, dg, z, y, u, tmp,
    mine, theirs, w_mine, w_theirs, i_mine, i_theirs, bag, rf, df, zf, pf, yf, a_sum, tmpf,
    u_ends, cross, q_mine, q_theirs, coupling, acc,
    dots, got_a, got_b, order_v, in_sems, x_send, x_recv, bag_send, bag_recv, s_send, s_recv, hello,
):
    stack = []

    def scope(name):
        if stack:
            stack.pop().__exit__(None, None, None)
        if name:
            stack.append(jax.named_scope(name))
            stack[-1].__enter__()

    scope("enter")
    ys, zs, xs, cores = TORUS
    count = lax.axis_size("slab")
    me = lax.axis_index("slab")
    core = lax.rem(me, cores)
    x = lax.rem(me // cores, xs)
    z_at = lax.rem(me // (cores * xs), zs)
    y_at = me // (cores * xs * zs)
    near_to = me + 1 - 2 * core
    far_to = lax.rem(me + count + 2 * core - 1, count)
    sides = (near_to, far_to)
    row_of = (pl.multiple_of((1 - core) * (ROWS - FACE), FACE), pl.multiple_of(core * (ROWS - FACE), FACE))
    face_of = {0: 1 - core, LAST: core}

    def moved(dy=0, dz=0, dx=0):
        to = me
        if dy:
            to = to + (lax.rem(y_at + dy, ys) - y_at) * (cores * xs * zs)
        if dz:
            to = to + (lax.rem(z_at + dz, zs) - z_at) * (cores * xs)
        if dx:
            to = to + (lax.rem(x + dx, xs) - x) * cores
        return to

    def ring(size, stop, start=1):
        return sorted({j % size for k in range(start, stop) for j in (k, -k)} - {0})

    def greet(sem, who):
        for q in who:
            pl.semaphore_signal(sem, inc=1, device_id=(q,), device_id_type=MESH)

    def heard(sem, who):
        if who:
            pl.semaphore_wait(sem, len(who))

    early = (z_at == 0) & (x == 0) & (core == 0)
    carrier = (z_at == 0) & (x == xs - 1) & (core == 1)
    late = (z_at == zs - 1) & (x == xs - 1) & (core == 1)
    plane_size = zs * xs * cores
    carrier_of_early = lax.rem(y_at + ys - 1, ys) * plane_size + xs * cores - 1
    carrier_of_late = y_at * plane_size + xs * cores - 1
    early_of_carrier = lax.rem(y_at + 1, ys) * plane_size
    late_of_carrier = y_at * plane_size + plane_size - 1

    row = [moved(dx=k) + c for k in range(xs) for c in (0, 1 - 2 * core) if k or not isinstance(c, int)]
    y_near = [moved(dy=k) for k in ring(ys, 3)]
    y_far = [moved(dy=k) for k in ring(ys, ys // 2 + 1, 3)]
    barrier = pltpu.get_barrier_semaphore()
    greet(barrier, [jnp.where(late, carrier_of_late, far_to), near_to])
    greet(barrier, row + y_near)

    @pl.when(early | carrier)
    def _():
        greet(barrier, [jnp.where(early, carrier_of_early, early_of_carrier)])

    expected = len(row) + len(y_near) + 2 + 2 * carrier.astype(jnp.int32) + cores * core * z_at

    loads = [
        pltpu.make_async_copy(src, dst, in_sems.at[k])
        for k, (src, dst) in enumerate(
            (
                (order_h, order_v),
                (load_h, ld),
                (geom_h.at[0], g0),
                (geom_h.at[1], g1),
                (geom_h.at[2], g2),
                (mass_h, ms),
            )
        )
    ]
    for copy in loads:
        copy.start()

    for k in range(1, zs):

        @pl.when(z_at + k < zs)
        def _(k=k):
            greet(barrier, [me + k * xs * cores + 1 - core])

    scope("idx")
    loads[0].wait()
    order = jnp.broadcast_to(order_v[...], (8, LANES))
    hit = (
        jnp.broadcast_to(order_v[...], (LANES, LANES))
        == lax.broadcasted_iota(jnp.int32, (LANES, LANES), 0)
    ).astype(jnp.float32)
    lane = lax.broadcasted_iota(jnp.int32, (8, LANES), 1)
    inverse = lax.dot_general(
        lane.astype(jnp.float32), hit, (((1,), (1,)), ((), ())), preferred_element_type=jnp.float32
    )
    inverse = (inverse + 0.5).astype(jnp.int32)
    in_row = lane & (EL_Z - 1)
    lanes = {
        "up": lane < LANES - EL_Z,
        "down": lane >= EL_Z,
        "next": lane - in_row + ((in_row + 1) & (EL_Z - 1)),
        "prev": lane - in_row + ((in_row + EL_Z - 1) & (EL_Z - 1)),
    }
    b_at = lax.broadcasted_iota(jnp.int32, (8, LANES), 0)
    lanes["first"] = b_at == 0
    lanes["corner"] = (lanes["first"] & lanes["down"]) | ((b_at == LAST) & lanes["up"])
    by_y = jnp.where(lanes["first"], LANES - EL_Z, EL_Z)
    lanes["corner_next"] = (lanes["next"] + by_y) & (LANES - 1)
    lanes["corner_prev"] = (lanes["prev"] + by_y) & (LANES - 1)

    def reorder(src, dst, idx, planes=range(N)):
        for a in planes:
            for b in range(N):
                dst[at(a, b), :] = lane_pick(src[at(a, b), :], idx)

    def swap(src, dst, f, first, rows, k, carried=None):
        copy = pltpu.make_async_remote_copy(
            src_ref=src.at[pl.ds(first, rows)],
            dst_ref=dst.at[pl.ds(first, rows)],
            send_sem=x_send.at[k, f],
            recv_sem=x_recv.at[k, f],
            device_id=(sides[f],),
            device_id_type=MESH,
        )
        if f == 0 or carried is None:
            copy.start()
            return copy

        @pl.when(early)
        def _():
            pltpu.make_async_remote_copy(
                src_ref=src.at[pl.ds(first, rows)],
                dst_ref=bag.at[pl.ds(carried, rows)],
                send_sem=x_send.at[k, f],
                recv_sem=bag_recv.at[k],
                device_id=(carrier_of_early,),
                device_id_type=MESH,
            ).start()

        pl.when(jnp.logical_not(early))(copy.start)
        return copy

    def carry(dst, carried, first, rows, k):
        return pltpu.make_async_remote_copy(
            src_ref=bag.at[pl.ds(carried, rows)],
            dst_ref=dst.at[pl.ds(first, rows)],
            send_sem=bag_send.at[k],
            recv_sem=x_recv.at[k, 1],
            device_id=(late_of_carrier,),
            device_id_type=MESH,
        )

    both = (0, LAST)
    faces = (0, 1)
    scope("load_ends")
    loads[1].wait()
    for a in both:
        for b in range(N):
            mine[part(face_of[a], LOAD, b), :] = lane_pick(ld[at(a, b), :], inverse)
    for copy in loads[2:]:
        copy.wait()
    for k, a in enumerate(both):
        s = contract(SQUARED.T, [g2[across(a, c), :] for c in range(N)], 1)
        for c in range(N):
            tmpf[across(k, c), :] = s[c]
    for b in range(N):
        s = contract(SQUARED.T, [g0[at(a, b), :] for a in range(N)], 1, both)
        for k, a in enumerate(both):
            yf[at(k, b), :] = s[a]
    for k, a in enumerate(both):
        s = contract(SQUARED.T, [g1[at(a, b), :] for b in range(N)], 1)
        for b in range(N):
            mine[part(face_of[a], DIAG, b), :] = lane_pick(
                s[b] + yf[at(k, b), :] + ms[at(a, b), :] + tmpf[at(k, b), :], inverse
            )
    for a in both:
        for i in range(N):
            mine[part(face_of[a], G1, i), :] = lane_pick(g1[at(a, i), :], inverse)
            mine[part(face_of[a], G2, i), :] = lane_pick(g2[across(a, i), :], inverse)
    scope("barrier")
    pl.semaphore_wait(barrier, expected)
    scope("send1")
    carried1 = ((0, 4 * FACE, 2 * FACE), (1, 4 * FACE + 2 * FACE, 2 * FACE))

    @pl.when(carrier)
    def _():
        for k, first, rows in carried1:
            got = bag.at[pl.ds(first - 4 * FACE, rows)]
            pltpu.make_async_copy(got, got, bag_recv.at[k]).wait()
            carry(theirs, first - 4 * FACE, first, rows, k).start()

    sent_ld = [swap(mine, theirs, f, f * 4 * FACE, 2 * FACE, 0, 0) for f in (1, 0)][::-1]
    sent_g = [swap(mine, theirs, f, (f * 4 + 2) * FACE, 2 * FACE, 1, 2 * FACE) for f in (1, 0)][::-1]
    greet(hello.at[0], y_near)

    @pl.when(core == 1)
    def _():
        for k in range(1, zs):

            @pl.when(z_at >= k)
            def _(k=k):
                greet(hello.at[2], [me - k * xs * cores])

    scope("reorder")
    reorder(g0, g0, inverse)
    reorder(g1, g1, inverse, INSIDE)
    for a in INSIDE:
        for c in range(N):
            g2t[at(a, c), :] = lane_pick(g2[across(a, c), :], inverse)
    reorder(ms, ms, inverse, INSIDE)
    for a in INSIDE:
        for b in range(N):
            moved_load = lane_pick(ld[at(a, b), :], inverse)
            ld[at(a, b), :] = moved_load
            r[at(a, b), :] = moved_load
    scope("diag")
    inner_diagonal(g0, g1, g2t, ms, dg, tmp, cross)
    scope("sums")
    sum_yz([(v, a) for a in INSIDE for v in (dg, r)], lanes)

    def inner_z(a):
        for b in range(N):
            inv = 1.0 / dg[at(a, b), :]
            dg[at(a, b), :] = inv
            z[at(a, b), :] = inv * r[at(a, b), :]

    loop(1, LAST, inner_z)
    scope("La1")
    stiffness_a(z, g0, y)

    def full(f, b):
        return tile(row_of[f] + b * N)

    def face_z(f):
        for b in range(N):
            rf[at(f, b), :] = mine[part(f, LOAD, b), :] + theirs[part(f, LOAD, b), :]
            total = mine[part(f, DIAG, b), :] + theirs[part(f, DIAG, b), :]
            a_sum[at(f, b), :] = total
            df[at(f, b), :] = total
        sum_yz([(rf, f), (df, f)], lanes)
        for b in range(N):
            inv = 1.0 / df[at(f, b), :]
            df[at(f, b), :] = inv
            zf[at(f, b), :] = inv * rf[at(f, b), :]

    def tell(f, k, carried=None):
        for b in range(N):
            w_mine[at(f, b), :] = y[full(f, b), :] + cross[at(0, b), :] * zf[at(1 - f, b), :]
        return swap(w_mine, w_theirs, f, f * FACE, FACE, k, carried)

    scope("x_near")
    sent_ld[0].wait()
    scope("z_near")
    face_z(0)
    sent_w = [None, tell(1, 2, 4 * FACE)]
    scope("Lbc1")
    stiffness_bc(z, g1, g2t, ms, y, tmp, y)
    scope("hello")

    @pl.when(carrier)
    def _():
        got = bag.at[pl.ds(4 * FACE, FACE)]
        pltpu.make_async_copy(got, got, bag_recv.at[2]).wait()
        carry(w_theirs, 4 * FACE, FACE, FACE, 2).start()

    heard(hello.at[0], y_near)
    greet(hello.at[1], y_far)
    scope("g_near")
    first = pl.multiple_of((1 - core) * FACE, FACE)
    couplings(g0, first, coupling)
    loop(1, LAST, lambda a: couple(zf, 0, coupling, y, a))
    sent_g[0].wait()
    face_sums(0, mine, theirs, a_sum, a_sum, tmpf)
    s = face_terms(zf, 0, mine, theirs, a_sum, tmpf)
    for b in range(N):
        yf[at(0, b), :] = s[b]
    scope("x_far")
    sent_ld[1].wait()
    scope("z_far")
    face_z(1)
    sent_w[0] = tell(0, 2)

    scope("inner2")
    for a in INSIDE:
        couple(zf, 1, coupling, y, a)
    sum_yz([(y, a) for a in INSIDE], lanes)
    zero = jnp.zeros((8, LANES), jnp.float32)

    def inner_p(a, num):
        for b in range(N):
            rows = at(a, b)
            p = COEF_Z * z[rows, :] - COEF_Q * (dg[rows, :] * y[rows, :])
            z[rows, :] = p
            num[b % 4] = num[b % 4] + ld[rows, :] * p
        return num

    num = lax.fori_loop(1, LAST, inner_p, [zero] * 4, unroll=True)
    scope("L2")
    den = energy_bc(z, g1, g2t, ms, [zero] * 4)
    den = energy_a(z, g0, u_ends, first, den)
    num, den = added_up(num), added_up(den)
    scope("g_far")
    sent_g[1].wait()
    face_sums(1, mine, theirs, a_sum, a_sum, tmpf)
    s = face_terms(zf, 1, mine, theirs, a_sum, tmpf)
    for b in range(N):
        yf[at(1, b), :] = s[b]

    def face_p(f):
        for b in range(N):
            rows = at(f, b)
            yf[rows, :] = yf[rows, :] + (w_mine[rows, :] + w_theirs[rows, :])
        sum_yz([(yf, f)], lanes)
        for b in range(N):
            rows = at(f, b)
            pf[rows, :] = COEF_Z * zf[rows, :] - COEF_Q * (df[rows, :] * yf[rows, :])

    def face_dot(kind, f):
        return added_up([kind[part(f, LOAD, b), :] * pf[at(f, b), :] for b in range(N)])

    scope("w_far")
    sent_w[1].wait()
    scope("ends2")
    face_p(1)
    num = num + face_dot(mine, 1)
    den = (
        den
        + 0.5 * face_energy(pf, 1, theirs, a_sum)
        + added_up([2.0 * u_ends[at(1, b), :] * pf[at(1, b), :] for b in range(N)])
    )
    for b in range(N):
        q_mine[at(0, b), :] = 2.0 * (u_ends[at(0, b), :] + cross[at(0, b), :] * pf[at(1, b), :])
    acc[tile(0), :] = num
    acc[tile(8), :] = den
    takes = jnp.where(2 * x >= xs, core, 1 - core) == 1
    gives = jnp.logical_not(takes)
    sent_q = pltpu.make_async_remote_copy(
        src_ref=q_mine,
        dst_ref=q_theirs,
        send_sem=x_send.at[4, 0],
        recv_sem=x_recv.at[4, 0],
        device_id=(near_to,),
        device_id_type=MESH,
    )
    pl.when(gives)(sent_q.start)

    @pl.when(takes)
    def _():
        sent_w[0].wait()
        face_p(0)
        sent_q.wait_recv()
        acc[tile(0), :] = acc[tile(0), :] + (face_dot(mine, 0) + face_dot(theirs, 0))
        acc[tile(8), :] = (
            acc[tile(8), :]
            + face_energy(pf, 0, theirs, a_sum)
            + added_up(
                [(q_mine[at(0, b), :] + q_theirs[at(0, b), :]) * pf[at(0, b), :] for b in range(N)]
            )
        )

    dots[0, 0:1, :] = jnp.sum(acc[tile(0), :], axis=0, keepdims=True)
    dots[0, 1:2, :] = jnp.sum(acc[tile(8), :], axis=0, keepdims=True)

    hops = sorted(
        ((dy, dx) for dy in range(ys) for dx in range(xs) if dy or dx),
        key=lambda d: -min(d[0], ys - d[0]) - min(d[1], xs - d[1]),
    )
    others = 2 * len(hops) + 1

    def send(src, dst, k, to):
        copy = pltpu.make_async_remote_copy(
            src_ref=src,
            dst_ref=dst,
            send_sem=s_send.at[k],
            recv_sem=s_recv.at[k],
            device_id=(to,),
            device_id_type=MESH,
        )
        copy.start()

    def arrived(ref, sem):
        pltpu.make_async_copy(ref, ref, sem).wait()

    def added(ref, first, total):
        part = [first, None, None, None]
        for j in range(total):
            part[j % 4] = plus(part[j % 4], ref[j])
        return functools.reduce(plus, [t for t in part if t is not None])

    heard(hello.at[1], y_far)
    for j, (dy, dx) in enumerate(hops):
        send(dots.at[0], got_a.at[2 * j + core], 0, moved(dy=dy, dx=dx) + 1 - core)

    @pl.when(core == 0)
    def _():
        send(dots.at[0], got_a.at[others - 1], 0, me + 1)

    scope("u_ends")

    @pl.when(gives)
    def _():
        sent_w[0].wait()
        face_p(0)
        sent_q.wait_send()

    sent_i = []
    for f in faces:
        for b in range(N):
            i_mine[at(f, b), :] = u_ends[at(f, b), :] + cross[at(0, b), :] * pf[at(1 - f, b), :]
        sent_i.append(swap(i_mine, i_theirs, f, f * FACE, FACE, 3))
    for f in faces:
        s = face_terms(pf, f, mine, theirs, a_sum, tmpf)
        for b in range(N):
            yf[at(f, b), :] = s[b]
    stiffness_bc(z, g1, g2t, ms, y, tmp)
    stiffness_a(z, g0, u, INSIDE, y)

    def couple_both(a):
        couple(pf, 0, coupling, u, a)
        couple(pf, 1, coupling, u, a)

    loop(1, LAST, couple_both)
    scope("out_p_r")
    for src, ends, dst in ((z, pf, p_o), (r, rf, r_o)):
        reorder(src, dst, order, INSIDE)
        for f in faces:
            for b in range(N):
                dst[full(f, b), :] = lane_pick(ends[at(f, b), :], order)
    sum_yz([(u, a) for a in INSIDE], lanes)
    reorder(u, im_o, order, INSIDE)
    scope("plane")

    @pl.when(core == 1)
    def _():
        arrived(got_a.at[pl.ds(0, others)], s_recv.at[0])
        dots[1] = added(got_a, dots[0], others)

        @pl.when(z_at < zs - 1)
        def _():
            pl.semaphore_wait(hello.at[2], zs - 1 - z_at)

        for k in sorted(range(1, zs), key=lambda k: -min(k, zs - k)):
            for c in (0, 1):
                send(dots.at[1], got_b.at[k - 1], 1, moved(dz=k) - c)
        send(dots.at[1], got_b.at[zs - 1], 1, me - 1)
        got_b[zs - 1] = dots[1]

    scope("x3")
    for copy in sent_i:
        copy.wait()
    for f in faces:
        for b in range(N):
            rows = at(f, b)
            yf[rows, :] = yf[rows, :] + (i_mine[rows, :] + i_theirs[rows, :])
    sum_yz([(yf, f) for f in faces], lanes)
    for f in faces:
        for b in range(N):
            im_o[full(f, b), :] = lane_pick(yf[at(f, b), :], order)
    scope("lines")

    @pl.when(core == 0)
    def _():
        arrived(got_b, s_recv.at[1])

    @pl.when(core == 1)
    def _():
        arrived(got_b.at[pl.ds(0, zs - 1)], s_recv.at[1])

    total = added(got_b, None, zs)
    scope("alpha")
    sums = jnp.sum(total, axis=1, keepdims=True)
    al_o[...] = jnp.broadcast_to(sums[0:1, :] / sums[1:2, :], (8, LANES))
    @pl.when(carrier)
    def _():
        for k, first, rows in carried1:
            carry(theirs, first - 4 * FACE, first, rows, k).wait_send()
        carry(w_theirs, 4 * FACE, FACE, FACE, 2).wait_send()

    @pl.when(core == 0)
    def _():
        arrived(got_a.at[pl.ds(0, len(hops) + 1)], s_send.at[0])

    @pl.when(core == 1)
    def _():
        arrived(got_a.at[pl.ds(0, len(hops))], s_send.at[0])
        arrived(got_a.at[pl.ds(0, 2 * zs - 1)], s_send.at[1])

    scope(None)


CHUNKS = 4


def finish_kernel(p, r, im, al, x_h, r_h, x_v, r_v, sems):
    alpha = al[...]
    size = ROWS // CHUNKS
    copies = []
    for k in range(CHUNKS):
        for i in range(k * size, (k + 1) * size, N):
            x_v[tile(i), :] = alpha * p[tile(i), :]
        rows = pl.ds(k * size, size)
        copies.append(pltpu.make_async_copy(x_v.at[rows], x_h.at[rows], sems.at[0, k]))
        copies[-1].start()
        for i in range(k * size, (k + 1) * size, N):
            r_v[tile(i), :] = r[tile(i), :] - alpha * im[tile(i), :]
        copies.append(pltpu.make_async_copy(r_v.at[rows], r_h.at[rows], sems.at[1, k]))
        copies[-1].start()
    for copy in copies:
        copy.wait()


def on_device(load_terms, geometry, mass_terms, element_order):
    flat = jax.ShapeDtypeStruct((ROWS, LANES), jnp.float32)
    vm = lambda *shape: pltpu.VMEM(shape, jnp.float32)
    field = vm(ROWS, LANES)
    pair = vm(2 * FACE, LANES)
    ys, zs, xs, cores = TORUS
    in_vmem = pl.BlockSpec(memory_space=pltpu.VMEM)
    in_hbm = pl.BlockSpec(memory_space=pltpu.HBM)
    parts = pl.pallas_call(
        step_kernel,
        out_shape=(field, field, field, vm(8, LANES)),
        in_specs=[in_hbm] * 4,
        out_specs=[in_vmem] * 4,
        scratch_shapes=[
            *[field] * 12,
            *[vm(8 * FACE, LANES)] * 2,
            *[pair] * 4, vm(5 * FACE, LANES), *[pair] * 8, *[vm(FACE, LANES)] * 3,
            vm(12 * FACE, LANES), vm(16, LANES),
            vm(2, 2, LANES), vm(2 * ys * xs - 1, 2, LANES), vm(zs, 2, LANES),
            pltpu.VMEM((1, LANES), jnp.int32),
            pltpu.SemaphoreType.DMA((6,)),
            pltpu.SemaphoreType.DMA((5, 2)),
            pltpu.SemaphoreType.DMA((5, 2)),
            pltpu.SemaphoreType.DMA((3,)),
            pltpu.SemaphoreType.DMA((3,)),
            pltpu.SemaphoreType.DMA((2,)),
            pltpu.SemaphoreType.DMA((2,)),
            pltpu.SemaphoreType.REGULAR((3,)),
        ],
        compiler_params=pltpu.CompilerParams(
            collective_id=0, has_side_effects=True, vmem_limit_bytes=24 << 20
        ),
        name="cg_step",
    )(
        *[
            pltpu.with_memory_space_constraint(t, pltpu.HBM)
            for t in (
                load_terms.reshape(ROWS, LANES),
                geometry.reshape(3, ROWS, LANES),
                mass_terms.reshape(ROWS, LANES),
                element_order,
            )
        ]
    )
    x, res = pl.pallas_call(
        finish_kernel,
        out_shape=(flat, flat),
        in_specs=[in_vmem] * 4,
        out_specs=[in_hbm] * 2,
        scratch_shapes=[field, field, pltpu.SemaphoreType.DMA((2, CHUNKS))],
        compiler_params=pltpu.CompilerParams(vmem_limit_bytes=8 << 20),
        name="cg_finish",
    )(*[pltpu.with_memory_space_constraint(t, pltpu.VMEM) for t in parts])
    shape = load_terms.shape
    return x.reshape(shape), res.reshape(shape)


def solution(mesh):
    last = P(None, None, None, "slab")
    return jax.shard_map(
        on_device,
        mesh=mesh,
        in_specs=(last, P(None, None, None, None, "slab"), last, P("slab", None)),
        out_specs=(last, last),
        check_vma=False,
    )
```

```python
import functools

import jax
import jax.numpy as jnp
import numpy as np
from jax import lax
from jax.experimental import pallas as pl
from jax.experimental.pallas import tpu as pltpu
from jax.sharding import PartitionSpec as P

N = 8
LAST = N - 1
EL_Y = 8
EL_Z = 16
LANES = 128
ROWS = N * N * N
FACE = N * N
CENTRE = 1.65
HALF = 1.35
MESH = pl.DeviceIdType.MESH
TORUS = (8, 12, 4, 2)
INSIDE = range(1, LAST)
UNROLL_A = 4
UNROLL_BC = 3


def legendre_table(positions, points):
    columns = [positions * 0.0 + 1.0, positions]
    for degree in range(2, points):
        columns.append(
            ((2 * degree - 1) * positions * columns[-1] - (degree - 1) * columns[-2]) / degree
        )
    return np.stack(columns, axis=1)


def gll_derivative(points):
    degree = points - 1
    nodes = -np.cos(np.pi * np.arange(points) / degree)
    for _ in range(100):
        legendre = legendre_table(nodes, points)
        nodes = nodes - (nodes * legendre[:, degree] - legendre[:, degree - 1]) / (
            points * legendre[:, degree]
        )
    legendre = legendre_table(nodes, points)
    top = legendre[:, degree]
    same = np.eye(points, dtype=bool)
    spacing = np.where(same, 1.0, nodes[:, None] - nodes[None, :])
    table = np.where(same, 0.0, top[:, None] / (top[None, :] * spacing))
    table[0, 0] = -degree * points / 4.0
    table[degree, degree] = degree * points / 4.0
    return table


DERIV = gll_derivative(N).astype(np.float32).astype(np.float64)
SQUARED = DERIV * DERIV
SIGMA = CENTRE / HALF
RHO0 = 1.0 / SIGMA
RHO1 = 1.0 / (2.0 * SIGMA - RHO0)
COEF_Z = (1.0 + RHO1 * RHO0) / CENTRE + 2.0 * RHO1 / HALF
COEF_Q = 2.0 * RHO1 / HALF / CENTRE


def plus(x, y):
    return y if x is None else x + y


def contract(table, terms, sign, rows=range(N)):
    used = [j for j in range(N // 2) if terms[j] is not None]
    even = {j: terms[j] + terms[LAST - j] for j in used}
    odd = {j: terms[j] - terms[LAST - j] for j in used}
    out = [None] * N
    for i in range(N // 2):
        if i not in rows and LAST - i not in rows:
            continue
        e = o = None
        for j in used:
            e = plus(e, float(table[i, j] + table[i, LAST - j]) / 2 * even[j])
            o = plus(o, float(table[i, j] - table[i, LAST - j]) / 2 * odd[j])
        if i in rows:
            out[i] = e + o
        if LAST - i in rows:
            out[LAST - i] = (o - e) if sign < 0 else (e - o)
    return out


def tile(row):
    return pl.ds(row if isinstance(row, int) else pl.multiple_of(row, 8), 8)


def at(a, b):
    return tile((a * N + b) * N)


def across(a, c):
    return pl.ds(a * FACE + c, N, stride=N)


LOAD, DIAG, G1, G2 = range(4)
NEAR, FAR_LD, FAR_G, NEAR_W, FAR_W, IMAGE, NEAR_Q = range(7)


def part(f, kind, i):
    return tile(((f * 4 + kind) * N + i) * N)


def loop(start, stop, body):
    lax.fori_loop(start, stop, lambda i, _: (body(i), 0)[1], 0)


def stiffness_a(v, g0, out, rows=range(N), more=None):
    def along_a(b, _):
        va = [v[at(a, b), :] if a in INSIDE else None for a in range(N)]
        s = contract(DERIV, va, -1)
        s = contract(DERIV.T, [s[a] * g0[at(a, b), :] for a in range(N)], -1, rows)
        for a in rows:
            out[at(a, b), :] = s[a] if more is None else s[a] + more[at(a, b), :]
        return 0

    lax.fori_loop(0, N, along_a, 0, unroll=UNROLL_A)


def energy_a(v, g0, ends, first, total):
    def along_a(b, total):
        t = contract(DERIV, [v[at(a, b), :] if a in INSIDE else None for a in range(N)], -1)
        s = [t[a] * g0[at(a, b), :] for a in range(N)]
        total = [total[k] + s[k] * t[k] + s[k + 4] * t[k + 4] for k in range(4)]
        s = contract(DERIV.T, s, -1, (0, LAST))
        ends[tile(first + b * N), :] = s[0]
        ends[tile(FACE - first + b * N), :] = s[LAST]
        return total

    return lax.fori_loop(0, N, along_a, total, unroll=UNROLL_A)


def energy_bc(v, g1, g2t, ms, total):
    def along_bc(a, total):
        vb = [v[at(a, b), :] for b in range(N)]
        for own, g in (([v[across(a, c), :] for c in range(N)], g2t), (vb, g1)):
            t = contract(DERIV, own, -1)
            e = [t[i] * g[at(a, i), :] * t[i] for i in range(N)]
            total = [total[k] + (e[k] + e[k + 4]) for k in range(4)]
        e = [vb[b] * ms[at(a, b), :] * vb[b] for b in range(N)]
        return [total[k] + (e[k] + e[k + 4]) for k in range(4)]

    return lax.fori_loop(1, LAST, along_bc, total, unroll=UNROLL_BC)


def stiffness_bc(v, g1, g2t, ms, out, tmp, more=None):
    def along_bc(a, _):
        vt = [v[across(a, c), :] for c in range(N)]
        vb = [v[at(a, b), :] for b in range(N)]
        t = contract(DERIV, vt, -1)
        t = contract(DERIV.T, [t[c] * g2t[at(a, c), :] for c in range(N)], -1)
        for c in range(N):
            tmp[across(a, c), :] = t[c]
        s = contract(DERIV, vb, -1)
        s = contract(DERIV.T, [s[b] * g1[at(a, b), :] for b in range(N)], -1)
        for b in range(N):
            s[b] = s[b] + ms[at(a, b), :] * vb[b]
            if more is not None:
                s[b] = s[b] + more[at(a, b), :]
        for b in range(N):
            out[at(a, b), :] = s[b] + tmp[at(a, b), :]
        return 0

    lax.fori_loop(1, LAST, along_bc, 0, unroll=UNROLL_BC)


def inner_diagonal(g0, g1, g2, ms, out, tmp):
    def along_a(b, _):
        s = contract(SQUARED.T, [g0[at(a, b), :] for a in range(N)], 1, INSIDE)
        for a in INSIDE:
            out[at(a, b), :] = s[a] + ms[at(a, b), :]
        return 0

    lax.fori_loop(0, N, along_a, 0, unroll=UNROLL_A)

    def along_bc(a, _):
        t = contract(SQUARED.T, [g2[across(a, c), :] for c in range(N)], 1)
        for c in range(N):
            tmp[across(a, c), :] = t[c]
        s = contract(SQUARED.T, [g1[at(a, b), :] for b in range(N)], 1)
        for b in range(N):
            s[b] = s[b] + out[at(a, b), :]
        for b in range(N):
            out[at(a, b), :] = s[b] + tmp[at(a, b), :]
        return 0

    lax.fori_loop(1, LAST, along_bc, 0, unroll=UNROLL_BC)


def face_terms(v, f, mine, theirs, a_sum, tmp):
    s = contract(DERIV, [v[across(f, c), :] for c in range(N)], -1)
    s = contract(DERIV.T, [s[c] * theirs[part(f, G2, c), :] for c in range(N)], -1)
    for c in range(N):
        tmp[across(f, c), :] = s[c]
    vb = [v[at(f, b), :] for b in range(N)]
    s = contract(DERIV, vb, -1)
    s = contract(DERIV.T, [s[b] * theirs[part(f, G1, b), :] for b in range(N)], -1)
    return [s[b] + a_sum[at(f, b), :] * vb[b] + tmp[at(f, b), :] for b in range(N)]


def face_energy(v, f, theirs, a_sum):
    vb = [v[at(f, b), :] for b in range(N)]
    e = [a_sum[at(f, b), :] * vb[b] * vb[b] for b in range(N)]
    for own, kind in (([v[across(f, c), :] for c in range(N)], G2), (vb, G1)):
        t = contract(DERIV, own, -1)
        e = [e[i] + t[i] * theirs[part(f, kind, i), :] * t[i] for i in range(N)]
    return added_up(e)


def added_up(terms):
    while len(terms) > 1:
        terms = [functools.reduce(plus, terms[i : i + 2]) for i in range(0, len(terms), 2)]
    return terms[0]


def face_sums(f, mine, theirs, diag, a_sum, tmp):
    g = [[mine[part(f, k, i), :] + theirs[part(f, k, i), :] for i in range(N)] for k in (G1, G2)]
    for k in (G1, G2):
        for i in range(N):
            theirs[part(f, k, i), :] = g[k - G1][i]
    s = contract(SQUARED.T, g[1], 1)
    for c in range(N):
        tmp[across(f, c), :] = s[c]
    s = contract(SQUARED.T, g[0], 1)
    for b in range(N):
        a_sum[at(f, b), :] = diag[at(f, b), :] - s[b] - tmp[at(f, b), :]


def couplings(g0, first, out):
    def one(b, _):
        g = [g0[at(a, b), :] for a in range(N)]
        for a_end, row in ((0, first), (LAST, FACE - first)):
            s = contract(DERIV.T, [float(DERIV[m, a_end]) * g[m] for m in range(N)], -1, INSIDE)
            for a in INSIDE:
                out[tile(row * 6 + ((a - 1) * N + b) * N), :] = s[a]
        return 0

    lax.fori_loop(0, N, one, 0, unroll=2)


def couple(v, f, coupling, out, a):
    for b in range(N):
        out[at(a, b), :] = (
            out[at(a, b), :] + coupling[tile(((f * 6 + a - 1) * N + b) * N), :] * v[at(f, b), :]
        )


def lane_pick(x, idx):
    return jnp.take_along_axis(x, idx, axis=1, mode="promise_in_bounds")


def sum_yz(planes, lanes):
    ends = [(v[at(a, 0), :], v[at(a, LAST), :]) for v, a in planes]
    rims = [(v[across(a, 0), :], v[across(a, LAST), :]) for v, a in planes]
    ups = [jnp.where(lanes["up"], pltpu.roll(low, LANES - EL_Z, 1), 0.0) for low, _ in ends]
    downs = [jnp.where(lanes["down"], pltpu.roll(high, EL_Z, 1), 0.0) for _, high in ends]
    nexts = [lane_pick(low, lanes["next"]) for low, _ in rims]
    prevs = [lane_pick(high, lanes["prev"]) for _, high in rims]

    def corners(rim, idx):
        turned = jnp.where(lanes["first"], pltpu.roll(rim, 1, 0), pltpu.roll(rim, LAST, 0))
        return jnp.where(lanes["corner"], lane_pick(turned, idx), 0.0)

    far_nexts = [corners(low, lanes["corner_next"]) for low, _ in rims]
    far_prevs = [corners(high, lanes["corner_prev"]) for _, high in rims]
    for k, (v, a) in enumerate(planes):
        v[across(a, LAST), :] = rims[k][1] + (nexts[k] + far_nexts[k])
        v[across(a, 0), :] = rims[k][0] + (prevs[k] + far_prevs[k])
        v[at(a, LAST), :] = v[at(a, LAST), :] + ups[k]
        v[at(a, 0), :] = v[at(a, 0), :] + downs[k]


def step_kernel(
    load_h, geom_h, mass_h, order_h, p_o, r_o, im_o, al_o,
    ld, coef, g2t, r, dg, z, y, u, tmp,
    mine, theirs, w_mine, w_theirs, i_mine, i_theirs, bag, rf, df, zf, pf, yf, a_sum, tmpf,
    u_ends, cross, q_mine, q_theirs, coupling, acc,
    dots, got_a, got_b, sent_all, order_v, in_sems, x_send, x_recv, bag_recv, s_send, s_recv, hello,
):
    stack = []

    def scope(name):
        if stack:
            stack.pop().__exit__(None, None, None)
        if name:
            stack.append(jax.named_scope(name))
            stack[-1].__enter__()

    scope("enter")
    ys, zs, xs, cores = TORUS
    line, plane_size, count = xs * cores, zs * xs * cores, ys * zs * xs * cores
    me = lax.axis_index("slab")
    core = lax.rem(me, cores)
    in_plane = lax.rem(me, plane_size)

    def greet(sem, who):
        for q in who:
            pl.semaphore_signal(sem, inc=1, device_id=(q,), device_id_type=MESH)

    def heard(sem, who):
        if who:
            pl.semaphore_wait(sem, len(who))

    near_to = me + 1 - 2 * core
    far_to = me + 2 * core - 1
    far_to = jnp.where(far_to < 0, count - 1, jnp.where(far_to == count, 0, far_to))
    early, carrier, late = in_plane == 0, in_plane == line - 1, in_plane == plane_size - 1
    barrier = pltpu.get_barrier_semaphore()
    greet(barrier, [jnp.where(late, me + line - plane_size, far_to)])
    loads = [
        pltpu.make_async_copy(src, dst, in_sems.at[k])
        for k, src, dst in (
            (0, order_h, order_v),
            (1, load_h, ld),
            (2, geom_h, coef.at[pl.ds(0, 3 * ROWS)]),
            (2, mass_h, coef.at[pl.ds(3 * ROWS, ROWS)]),
        )
    ]
    for copy in loads:
        copy.start()
    g0, g1, g2, ms = (coef.at[pl.ds(k * ROWS, ROWS)] for k in range(4))

    y_at = me // plane_size
    z_at = in_plane // line
    x = lax.rem(me, line) // cores

    def moved(dy=0, dz=0, dx=0):
        to = me
        if dy:
            to = to + (lax.rem(y_at + dy, ys) - y_at) * plane_size
        if dz:
            to = to + (lax.rem(z_at + dz, zs) - z_at) * line
        if dx:
            to = to + (lax.rem(x + dx, xs) - x) * cores
        return to

    def ring(size, stop, start=1):
        return sorted({j % size for k in range(start, stop) for j in (k, -k)} - {0})

    sides = (near_to, far_to)
    row_of = (pl.multiple_of((1 - core) * (ROWS - FACE), FACE), pl.multiple_of(core * (ROWS - FACE), FACE))
    face_of = {0: 1 - core, LAST: core}
    carrier_of_early = lax.rem(y_at + ys - 1, ys) * plane_size + line - 1
    early_of_carrier = lax.rem(y_at + 1, ys) * plane_size
    late_of_carrier = me + plane_size - line

    row = [moved(dx=k) + c for k in range(xs) for c in (0, 1 - 2 * core) if k or not isinstance(c, int)]
    y_near = [moved(dy=k) for k in ring(ys, 3)]
    y_far = [moved(dy=k) for k in ring(ys, ys // 2 + 1, 3)]
    greet(barrier, [near_to] + row + y_near)

    @pl.when(early | carrier)
    def _():
        greet(barrier, [jnp.where(early, carrier_of_early, early_of_carrier)])

    def higher(z_to, _):
        greet(barrier, [me + (z_to - z_at) * line + 1 - core])
        return 0

    lax.fori_loop(z_at + 1, zs, higher, 0)
    expected = len(row) + len(y_near) + 2 + 2 * carrier.astype(jnp.int32) + 2 * core * z_at

    scope("idx")
    loads[0].wait()
    order = jnp.broadcast_to(order_v[...], (8, LANES))
    hit = (
        jnp.broadcast_to(order_v[...], (LANES, LANES))
        == lax.broadcasted_iota(jnp.int32, (LANES, LANES), 0)
    ).astype(jnp.float32)
    lane = lax.broadcasted_iota(jnp.int32, (8, LANES), 1)
    inverse = lax.dot_general(
        lane.astype(jnp.float32), hit, (((1,), (1,)), ((), ())), preferred_element_type=jnp.float32
    )
    inverse = (inverse + 0.5).astype(jnp.int32)
    in_row = lane & (EL_Z - 1)
    lanes = {
        "up": lane < LANES - EL_Z,
        "down": lane >= EL_Z,
        "next": lane - in_row + ((in_row + 1) & (EL_Z - 1)),
        "prev": lane - in_row + ((in_row + EL_Z - 1) & (EL_Z - 1)),
    }
    b_at = lax.broadcasted_iota(jnp.int32, (8, LANES), 0)
    lanes["first"] = b_at == 0
    lanes["corner"] = (lanes["first"] & lanes["down"]) | ((b_at == LAST) & lanes["up"])
    by_y = jnp.where(lanes["first"], LANES - EL_Z, EL_Z)
    lanes["corner_next"] = (lanes["next"] + by_y) & (LANES - 1)
    lanes["corner_prev"] = (lanes["prev"] + by_y) & (LANES - 1)

    def reorder(src, dst, idx, planes=range(N)):
        for a in planes:
            for b in range(N):
                dst[at(a, b), :] = lane_pick(src[at(a, b), :], idx)

    def remote(src, dst, recv, to):
        return pltpu.make_async_remote_copy(
            src_ref=src,
            dst_ref=dst,
            send_sem=x_send,
            recv_sem=recv,
            device_id=(to,),
            device_id_type=MESH,
        )

    def swap(src, dst, f, first, rows, k, carried=None, bag_k=None):
        src, dst = src.at[pl.ds(first, rows)], dst.at[pl.ds(first, rows)]
        copy = remote(src, dst, x_recv.at[k], sides[f])
        if carried is None:
            copy.start()
        else:
            by_bag = remote(src, bag.at[pl.ds(carried, rows)], bag_recv.at[bag_k], carrier_of_early)
            pl.when(early)(by_bag.start)
            pl.when(jnp.logical_not(early))(copy.start)
        return copy

    def carry(dst, carried, first, rows, k):
        src, dst = bag.at[pl.ds(carried, rows)], dst.at[pl.ds(first, rows)]
        remote(src, dst, x_recv.at[k], late_of_carrier).start()

    def landed(ref, sem):
        pltpu.make_async_copy(ref, ref, sem).wait()

    both = (0, LAST)
    faces = (0, 1)
    scope("load_ends")
    loads[1].wait()
    for a in both:
        for b in range(N):
            mine[part(face_of[a], LOAD, b), :] = lane_pick(ld[at(a, b), :], inverse)
    pltpu.make_async_copy(coef, coef, in_sems.at[2]).wait()
    for k, a in enumerate(both):
        s = contract(SQUARED.T, [g2[across(a, c), :] for c in range(N)], 1)
        for c in range(N):
            tmpf[across(k, c), :] = s[c]
    for b in range(N):
        s = contract(SQUARED.T, [g0[at(a, b), :] for a in range(N)], 1, both)
        for k, a in enumerate(both):
            yf[at(k, b), :] = s[a]
    for k, a in enumerate(both):
        s = contract(SQUARED.T, [g1[at(a, b), :] for b in range(N)], 1)
        for b in range(N):
            mine[part(face_of[a], DIAG, b), :] = lane_pick(
                s[b] + yf[at(k, b), :] + ms[at(a, b), :] + tmpf[at(k, b), :], inverse
            )
    for a in both:
        for i in range(N):
            mine[part(face_of[a], G1, i), :] = lane_pick(g1[at(a, i), :], inverse)
            mine[part(face_of[a], G2, i), :] = lane_pick(g2[across(a, i), :], inverse)
    scope("barrier")
    pl.semaphore_wait(barrier, expected)
    scope("send1")

    @pl.when(carrier)
    def _():
        landed(bag.at[pl.ds(0, 4 * FACE)], bag_recv.at[0])
        carry(theirs, 0, 4 * FACE, 2 * FACE, FAR_LD)
        carry(theirs, 2 * FACE, 6 * FACE, 2 * FACE, FAR_G)

    sent_ld = swap(mine, theirs, 1, 4 * FACE, 2 * FACE, FAR_LD, 0, 0)
    sent_g = swap(mine, theirs, 1, 6 * FACE, 2 * FACE, FAR_G, 2 * FACE, 0)
    sent_near = swap(mine, theirs, 0, 0, 4 * FACE, NEAR)
    greet(hello.at[0], y_near)

    @pl.when(core == 1)
    def _():
        def lower(z_to, _):
            greet(hello.at[2], [me + (z_to - z_at) * line])
            return 0

        lax.fori_loop(0, z_at, lower, 0)

    scope("diag")
    inner_diagonal(g0, g1, g2, ms, dg, tmp)
    scope("reorder")
    for a in INSIDE:
        for b in range(N):
            rows = at(a, b)
            dg[rows, :] = lane_pick(dg[rows, :], inverse)
            moved_load = lane_pick(ld[rows, :], inverse)
            ld[rows, :] = moved_load
            r[rows, :] = moved_load
    reorder(g0, g0, inverse)
    scope("sums")
    sum_yz([(v, a) for a in INSIDE for v in (dg, r)], lanes)

    def inner_z(a, _):
        for b in range(N):
            inv = 1.0 / dg[at(a, b), :]
            dg[at(a, b), :] = inv
            z[at(a, b), :] = inv * r[at(a, b), :]
        return 0

    lax.fori_loop(1, LAST, inner_z, 0, unroll=3)
    for b in range(N):
        g = [float(DERIV[m, 0] * DERIV[m, LAST]) * g0[at(m, b), :] for m in range(N)]
        cross[at(0, b), :] = added_up(g)
    scope("La1")
    stiffness_a(z, g0, y)

    def full(f, b):
        return tile(row_of[f] + b * N)

    def face_z(f):
        for b in range(N):
            rf[at(f, b), :] = mine[part(f, LOAD, b), :] + theirs[part(f, LOAD, b), :]
            total = mine[part(f, DIAG, b), :] + theirs[part(f, DIAG, b), :]
            a_sum[at(f, b), :] = total
            df[at(f, b), :] = total
        sum_yz([(rf, f), (df, f)], lanes)
        for b in range(N):
            inv = 1.0 / df[at(f, b), :]
            df[at(f, b), :] = inv
            zf[at(f, b), :] = inv * rf[at(f, b), :]

    def tell(f, k, carried=None):
        for b in range(N):
            w_mine[at(f, b), :] = y[full(f, b), :] + cross[at(0, b), :] * zf[at(1 - f, b), :]
        sum_yz([(w_mine, f)], lanes)
        return swap(w_mine, w_theirs, f, f * FACE, FACE, k, carried, 1)

    scope("x_near")
    sent_near.wait_recv()
    scope("z_near")
    face_z(0)
    sent_w = [None, tell(1, FAR_W, 4 * FACE)]
    scope("reorder2")
    reorder(g1, g1, inverse, INSIDE)
    for a in INSIDE:
        for c in range(N):
            g2t[at(a, c), :] = lane_pick(g2[across(a, c), :], inverse)
    reorder(ms, ms, inverse, INSIDE)
    scope("Lbc1")
    stiffness_bc(z, g1, g2t, ms, y, tmp, y)
    scope("hello")

    @pl.when(carrier)
    def _():
        landed(bag.at[pl.ds(4 * FACE, FACE)], bag_recv.at[1])
        carry(w_theirs, 4 * FACE, FACE, FACE, FAR_W)

    heard(hello.at[0], y_near)
    greet(hello.at[1], y_far)
    scope("g_near")
    first = pl.multiple_of((1 - core) * FACE, FACE)
    couplings(g0, first, coupling)
    loop(1, LAST, lambda a: couple(zf, 0, coupling, y, a))
    face_sums(0, mine, theirs, a_sum, a_sum, tmpf)
    s = face_terms(zf, 0, mine, theirs, a_sum, tmpf)
    for b in range(N):
        yf[at(0, b), :] = s[b]
    sum_yz([(yf, 0)], lanes)
    scope("x_far")
    sent_ld.wait_recv()
    scope("z_far")
    face_z(1)

    scope("inner2")
    for a in INSIDE:
        couple(zf, 1, coupling, y, a)
    sum_yz([(y, a) for a in INSIDE], lanes)
    zero = jnp.zeros((8, LANES), jnp.float32)

    def inner_p(a, num):
        for b in range(N):
            rows = at(a, b)
            p = COEF_Z * z[rows, :] - COEF_Q * (dg[rows, :] * y[rows, :])
            z[rows, :] = p
            num[b % 4] = num[b % 4] + ld[rows, :] * p
        return num

    num = lax.fori_loop(1, LAST, inner_p, [zero] * 4, unroll=True)
    scope("L2")
    den = energy_bc(z, g1, g2t, ms, [zero] * 4)
    den = energy_a(z, g0, u_ends, first, den)
    num, den = added_up(num), added_up(den)
    scope("g_far")
    sent_g.wait_recv()
    face_sums(1, mine, theirs, a_sum, a_sum, tmpf)
    s = face_terms(zf, 1, mine, theirs, a_sum, tmpf)
    for b in range(N):
        yf[at(1, b), :] = s[b]
    sum_yz([(yf, 1)], lanes)
    sent_w[0] = tell(0, NEAR_W)

    def face_p(f):
        for b in range(N):
            rows = at(f, b)
            total = yf[rows, :] + (w_mine[rows, :] + w_theirs[rows, :])
            pf[rows, :] = COEF_Z * zf[rows, :] - COEF_Q * (df[rows, :] * total)

    def face_dot(kind, f):
        return added_up([kind[part(f, LOAD, b), :] * pf[at(f, b), :] for b in range(N)])

    acc[tile(0), :] = num
    acc[tile(8), :] = den
    takes = jnp.where(2 * x >= xs, core, 1 - core) == 1
    gives = jnp.logical_not(takes)
    sent_q = remote(q_mine, q_theirs, x_recv.at[NEAR_Q], near_to)
    scope("w_near")

    @pl.when(takes)
    def _():
        sent_w[0].wait_recv()
        face_p(0)
        sent_q.wait_recv()
        acc[tile(0), :] = acc[tile(0), :] + (face_dot(mine, 0) + face_dot(theirs, 0))
        terms = [
            (2.0 * u_ends[at(0, b), :] + q_theirs[at(0, b), :]) * pf[at(0, b), :] for b in range(N)
        ]
        acc[tile(8), :] = acc[tile(8), :] + (face_energy(pf, 0, theirs, a_sum) + added_up(terms))
        for b in range(N):
            q_mine[at(0, b), :] = 2.0 * cross[at(0, b), :] * pf[at(0, b), :]

    scope("w_far")
    sent_w[1].wait_recv()
    scope("ends2")
    face_p(1)
    acc[tile(0), :] = acc[tile(0), :] + face_dot(mine, 1)
    terms = [2.0 * u_ends[at(1, b), :] * pf[at(1, b), :] for b in range(N)]
    acc[tile(8), :] = acc[tile(8), :] + (0.5 * face_energy(pf, 1, theirs, a_sum) + added_up(terms))

    @pl.when(takes)
    def _():
        terms = [q_mine[at(0, b), :] * pf[at(1, b), :] for b in range(N)]
        acc[tile(8), :] = acc[tile(8), :] + added_up(terms)

    @pl.when(gives)
    def _():
        for b in range(N):
            q_mine[at(0, b), :] = 2.0 * (
                u_ends[at(0, b), :] + cross[at(0, b), :] * pf[at(1, b), :]
            )
        sent_q.start()

    dots[0, 0:1, :] = jnp.sum(acc[tile(0), :], axis=0, keepdims=True)
    dots[0, 1:2, :] = jnp.sum(acc[tile(8), :], axis=0, keepdims=True)

    hops = sorted(
        ((dy, dx) for dy in range(ys) for dx in range(xs) if dy or dx),
        key=lambda d: -min(d[0], ys - d[0]) - min(d[1], xs - d[1]),
    )
    others = 2 * len(hops) + 1

    def send(src, dst, k, to):
        copy = pltpu.make_async_remote_copy(
            src_ref=src,
            dst_ref=dst,
            send_sem=s_send,
            recv_sem=s_recv.at[k],
            device_id=(to,),
            device_id_type=MESH,
        )
        copy.start()

    def arrived(ref, sem):
        pltpu.make_async_copy(ref, ref, sem).wait()

    def added(ref, first, total):
        part = [first, None, None, None]
        for j in range(total):
            part[j % 4] = plus(part[j % 4], ref[j])
        return functools.reduce(plus, [t for t in part if t is not None])

    heard(hello.at[1], y_far)
    for j, (dy, dx) in enumerate(hops):
        send(dots.at[0], got_a.at[2 * j + core], 0, moved(dy=dy, dx=dx) + 1 - core)

    @pl.when(core == 0)
    def _():
        send(dots.at[0], got_a.at[others - 1], 0, me + 1)

    scope("u_ends")

    @pl.when(gives)
    def _():
        sent_w[0].wait_recv()
        face_p(0)

    for f in faces:
        for b in range(N):
            i_mine[at(f, b), :] = u_ends[at(f, b), :] + cross[at(0, b), :] * pf[at(1 - f, b), :]
        swap(i_mine, i_theirs, f, f * FACE, FACE, IMAGE)
    for f in faces:
        s = face_terms(pf, f, mine, theirs, a_sum, tmpf)
        for b in range(N):
            yf[at(f, b), :] = s[b]
    stiffness_bc(z, g1, g2t, ms, y, tmp)
    stiffness_a(z, g0, u, INSIDE, y)

    def couple_both(a):
        couple(pf, 0, coupling, u, a)
        couple(pf, 1, coupling, u, a)

    loop(1, LAST, couple_both)
    scope("out_p_r")
    for src, ends, dst in ((z, pf, p_o), (r, rf, r_o)):
        reorder(src, dst, order, INSIDE)
        for f in faces:
            for b in range(N):
                dst[full(f, b), :] = lane_pick(ends[at(f, b), :], order)
    sum_yz([(u, a) for a in INSIDE], lanes)
    reorder(u, im_o, order, INSIDE)
    scope("plane")

    @pl.when(core == 1)
    def _():
        arrived(got_a.at[pl.ds(0, others)], s_recv.at[0])
        dots[1] = added(got_a, dots[0], others)

        @pl.when(z_at < zs - 1)
        def _():
            pl.semaphore_wait(hello.at[2], zs - 1 - z_at)

        for k in sorted(range(1, zs), key=lambda k: -min(k, zs - k)):
            for c in (0, 1):
                send(dots.at[1], got_b.at[k - 1], 1, moved(dz=k) - c)
        send(dots.at[1], got_b.at[zs - 1], 1, me - 1)
        got_b[zs - 1] = dots[1]

    scope("x3")
    landed(i_theirs, x_recv.at[IMAGE])
    for f in faces:
        for b in range(N):
            rows = at(f, b)
            yf[rows, :] = yf[rows, :] + (i_mine[rows, :] + i_theirs[rows, :])
    sum_yz([(yf, f) for f in faces], lanes)
    for f in faces:
        for b in range(N):
            im_o[full(f, b), :] = lane_pick(yf[at(f, b), :], order)
    scope("lines")

    @pl.when(core == 0)
    def _():
        arrived(got_b, s_recv.at[1])

    @pl.when(core == 1)
    def _():
        arrived(got_b.at[pl.ds(0, zs - 1)], s_recv.at[1])

    total = added(got_b, None, zs)
    scope("alpha")
    sums = jnp.sum(total, axis=1, keepdims=True)
    al_o[...] = jnp.broadcast_to(sums[0:1, :] / sums[1:2, :], (8, LANES))
    plane_sends, line_sends = len(hops), 2 * zs - 1

    @pl.when(core == 0)
    def _():
        arrived(sent_all.at[pl.ds(0, plane_sends + 1)], s_send)

    @pl.when(core == 1)
    def _():
        arrived(sent_all.at[pl.ds(0, plane_sends + line_sends)], s_send)

    for case, sends in (
        (takes & jnp.logical_not(carrier), 12),
        (takes & carrier, 17),
        (gives & jnp.logical_not(carrier), 13),
        (gives & carrier, 18),
    ):

        @pl.when(case)
        def _(sends=sends):
            landed(coef.at[pl.ds(0, sends * FACE)], x_send)

    scope(None)


CHUNKS = 4


def finish_kernel(p, r, im, al, x_h, r_h, both, sem):
    alpha = al[...]
    size = ROWS // CHUNKS
    for k in range(CHUNKS):
        for i in range(k * size, (k + 1) * size, N):
            both[tile(i), :] = alpha * p[tile(i), :]
        pltpu.make_async_copy(both.at[pl.ds(k * size, size)], x_h.at[pl.ds(k * size, size)], sem).start()
        for i in range(k * size, (k + 1) * size, N):
            both[tile(ROWS + i), :] = r[tile(i), :] - alpha * im[tile(i), :]
        rows = pl.ds(ROWS + k * size, size)
        pltpu.make_async_copy(both.at[rows], r_h.at[pl.ds(k * size, size)], sem).start()
    pltpu.make_async_copy(both, both, sem).wait()


def on_device(load_terms, geometry, mass_terms, element_order):
    flat = jax.ShapeDtypeStruct((ROWS, LANES), jnp.float32)
    vm = lambda *shape: pltpu.VMEM(shape, jnp.float32)
    field = vm(ROWS, LANES)
    pair = vm(2 * FACE, LANES)
    ys, zs, xs, cores = TORUS
    in_vmem = pl.BlockSpec(memory_space=pltpu.VMEM)
    in_hbm = pl.BlockSpec(memory_space=pltpu.HBM)
    parts = pl.pallas_call(
        step_kernel,
        out_shape=(field, field, field, vm(8, LANES)),
        in_specs=[in_hbm] * 4,
        out_specs=[in_vmem] * 4,
        scratch_shapes=[
            field, vm(4 * ROWS, LANES), *[field] * 7,
            *[vm(8 * FACE, LANES)] * 2,
            *[pair] * 4, vm(5 * FACE, LANES), *[pair] * 8, *[vm(FACE, LANES)] * 3,
            vm(12 * FACE, LANES), vm(16, LANES),
            vm(2, 2, LANES), vm(2 * ys * xs - 1, 2, LANES), vm(zs, 2, LANES),
            vm(ys * xs + 2 * zs, 2, LANES),
            pltpu.VMEM((1, LANES), jnp.int32),
            pltpu.SemaphoreType.DMA((3,)),
            pltpu.SemaphoreType.DMA(()),
            pltpu.SemaphoreType.DMA((7,)),
            pltpu.SemaphoreType.DMA((2,)),
            pltpu.SemaphoreType.DMA(()),
            pltpu.SemaphoreType.DMA((2,)),
            pltpu.SemaphoreType.REGULAR((3,)),
        ],
        compiler_params=pltpu.CompilerParams(
            collective_id=0, has_side_effects=True, vmem_limit_bytes=24 << 20
        ),
        name="cg_step",
    )(
        *[
            pltpu.with_memory_space_constraint(t, pltpu.HBM)
            for t in (
                load_terms.reshape(ROWS, LANES),
                geometry.reshape(3 * ROWS, LANES),
                mass_terms.reshape(ROWS, LANES),
                element_order,
            )
        ]
    )
    x, res = pl.pallas_call(
        finish_kernel,
        out_shape=(flat, flat),
        in_specs=[in_vmem] * 4,
        out_specs=[in_hbm] * 2,
        scratch_shapes=[vm(2 * ROWS, LANES), pltpu.SemaphoreType.DMA(())],
        compiler_params=pltpu.CompilerParams(vmem_limit_bytes=8 << 20),
        name="cg_finish",
    )(*[pltpu.with_memory_space_constraint(t, pltpu.VMEM) for t in parts])
    shape = load_terms.shape
    return x.reshape(shape), res.reshape(shape)


def solution(mesh):
    last = P(None, None, None, "slab")
    return jax.shard_map(
        on_device,
        mesh=mesh,
        in_specs=(last, P(None, None, None, None, "slab"), last, P("slab", None)),
        out_specs=(last, last),
        check_vma=False,
    )
```

```python
import functools

import jax
import jax.numpy as jnp
import numpy as np
from jax import lax
from jax.experimental import pallas as pl
from jax.experimental.pallas import tpu as pltpu
from jax.sharding import PartitionSpec as P

N = 8
LAST = N - 1
EL_Y = 8
EL_Z = 16
LANES = 128
ROWS = N * N * N
FACE = N * N
CENTRE = 1.65
HALF = 1.35
MESH = pl.DeviceIdType.MESH
TORUS = (8, 12, 4, 2)
ROOT = 1
INSIDE = range(1, LAST)
UNROLL_A = 4
UNROLL_BC = 3


def legendre_table(positions, points):
    columns = [positions * 0.0 + 1.0, positions]
    for degree in range(2, points):
        columns.append(
            ((2 * degree - 1) * positions * columns[-1] - (degree - 1) * columns[-2]) / degree
        )
    return np.stack(columns, axis=1)


def gll_derivative(points):
    degree = points - 1
    nodes = -np.cos(np.pi * np.arange(points) / degree)
    for _ in range(100):
        legendre = legendre_table(nodes, points)
        nodes = nodes - (nodes * legendre[:, degree] - legendre[:, degree - 1]) / (
            points * legendre[:, degree]
        )
    legendre = legendre_table(nodes, points)
    top = legendre[:, degree]
    same = np.eye(points, dtype=bool)
    spacing = np.where(same, 1.0, nodes[:, None] - nodes[None, :])
    table = np.where(same, 0.0, top[:, None] / (top[None, :] * spacing))
    table[0, 0] = -degree * points / 4.0
    table[degree, degree] = degree * points / 4.0
    return table


DERIV = gll_derivative(N).astype(np.float32).astype(np.float64)
SQUARED = DERIV * DERIV
SIGMA = CENTRE / HALF
RHO0 = 1.0 / SIGMA
RHO1 = 1.0 / (2.0 * SIGMA - RHO0)
COEF_Z = (1.0 + RHO1 * RHO0) / CENTRE + 2.0 * RHO1 / HALF
COEF_Q = 2.0 * RHO1 / HALF / CENTRE


def plus(x, y):
    return y if x is None else x + y


def contract(table, terms, sign, rows=range(N)):
    used = [j for j in range(N // 2) if terms[j] is not None]
    even = {j: terms[j] + terms[LAST - j] for j in used}
    odd = {j: terms[j] - terms[LAST - j] for j in used}
    out = [None] * N
    for i in range(N // 2):
        if i not in rows and LAST - i not in rows:
            continue
        e = o = None
        for j in used:
            e = plus(e, float(table[i, j] + table[i, LAST - j]) / 2 * even[j])
            o = plus(o, float(table[i, j] - table[i, LAST - j]) / 2 * odd[j])
        if i in rows:
            out[i] = e + o
        if LAST - i in rows:
            out[LAST - i] = (o - e) if sign < 0 else (e - o)
    return out


def tile(row):
    return pl.ds(row if isinstance(row, int) else pl.multiple_of(row, 8), 8)


def at(a, b):
    return tile((a * N + b) * N)


def across(a, c):
    return pl.ds(a * FACE + c, N, stride=N)


LOAD, DIAG, G1, G2 = range(4)
NEAR, FAR_LD, FAR_G, NEAR_W, FAR_W, IMAGE, NEAR_Q = range(7)


def part(f, kind, i):
    return tile(((f * 4 + kind) * N + i) * N)


def loop(start, stop, body):
    lax.fori_loop(start, stop, lambda i, _: (body(i), 0)[1], 0)


def stiffness_a(v, g0, out, rows=range(N), more=None):
    def along_a(b, _):
        va = [v[at(a, b), :] if a in INSIDE else None for a in range(N)]
        s = contract(DERIV, va, -1)
        s = contract(DERIV.T, [s[a] * g0[at(a, b), :] for a in range(N)], -1, rows)
        for a in rows:
            out[at(a, b), :] = s[a] if more is None else s[a] + more[at(a, b), :]
        return 0

    lax.fori_loop(0, N, along_a, 0, unroll=UNROLL_A)


def energy_a(v, g0, ends, first, total):
    def along_a(b, total):
        t = contract(DERIV, [v[at(a, b), :] if a in INSIDE else None for a in range(N)], -1)
        s = [t[a] * g0[at(a, b), :] for a in range(N)]
        total = [total[k] + s[k] * t[k] + s[k + 4] * t[k + 4] for k in range(4)]
        s = contract(DERIV.T, s, -1, (0, LAST))
        ends[tile(first + b * N), :] = s[0]
        ends[tile(FACE - first + b * N), :] = s[LAST]
        return total

    return lax.fori_loop(0, N, along_a, total, unroll=UNROLL_A)


def energy_bc(v, g1, g2t, ms, total):
    def along_bc(a, total):
        vb = [v[at(a, b), :] for b in range(N)]
        for own, g in (([v[across(a, c), :] for c in range(N)], g2t), (vb, g1)):
            t = contract(DERIV, own, -1)
            e = [t[i] * g[at(a, i), :] * t[i] for i in range(N)]
            total = [total[k] + (e[k] + e[k + 4]) for k in range(4)]
        e = [vb[b] * ms[at(a, b), :] * vb[b] for b in range(N)]
        return [total[k] + (e[k] + e[k + 4]) for k in range(4)]

    return lax.fori_loop(1, LAST, along_bc, total, unroll=UNROLL_BC)


def stiffness_bc(v, g1, g2t, ms, out, tmp, more=None):
    def along_bc(a, _):
        vt = [v[across(a, c), :] for c in range(N)]
        vb = [v[at(a, b), :] for b in range(N)]
        t = contract(DERIV, vt, -1)
        t = contract(DERIV.T, [t[c] * g2t[at(a, c), :] for c in range(N)], -1)
        for c in range(N):
            tmp[across(a, c), :] = t[c]
        s = contract(DERIV, vb, -1)
        s = contract(DERIV.T, [s[b] * g1[at(a, b), :] for b in range(N)], -1)
        for b in range(N):
            s[b] = s[b] + ms[at(a, b), :] * vb[b]
            if more is not None:
                s[b] = s[b] + more[at(a, b), :]
        for b in range(N):
            out[at(a, b), :] = s[b] + tmp[at(a, b), :]
        return 0

    lax.fori_loop(1, LAST, along_bc, 0, unroll=UNROLL_BC)


def inner_diagonal(g0, g1, g2, ms, out, tmp):
    def along_a(b, _):
        s = contract(SQUARED.T, [g0[at(a, b), :] for a in range(N)], 1, INSIDE)
        for a in INSIDE:
            out[at(a, b), :] = s[a] + ms[at(a, b), :]
        return 0

    lax.fori_loop(0, N, along_a, 0, unroll=UNROLL_A)

    def along_bc(a, _):
        t = contract(SQUARED.T, [g2[across(a, c), :] for c in range(N)], 1)
        for c in range(N):
            tmp[across(a, c), :] = t[c]
        s = contract(SQUARED.T, [g1[at(a, b), :] for b in range(N)], 1)
        for b in range(N):
            s[b] = s[b] + out[at(a, b), :]
        for b in range(N):
            out[at(a, b), :] = s[b] + tmp[at(a, b), :]
        return 0

    lax.fori_loop(1, LAST, along_bc, 0, unroll=UNROLL_BC)


def face_terms(v, f, mine, theirs, a_sum, tmp):
    s = contract(DERIV, [v[across(f, c), :] for c in range(N)], -1)
    s = contract(DERIV.T, [s[c] * theirs[part(f, G2, c), :] for c in range(N)], -1)
    for c in range(N):
        tmp[across(f, c), :] = s[c]
    vb = [v[at(f, b), :] for b in range(N)]
    s = contract(DERIV, vb, -1)
    s = contract(DERIV.T, [s[b] * theirs[part(f, G1, b), :] for b in range(N)], -1)
    return [s[b] + a_sum[at(f, b), :] * vb[b] + tmp[at(f, b), :] for b in range(N)]


def face_energy(v, f, theirs, a_sum):
    vb = [v[at(f, b), :] for b in range(N)]
    e = [a_sum[at(f, b), :] * vb[b] * vb[b] for b in range(N)]
    for own, kind in (([v[across(f, c), :] for c in range(N)], G2), (vb, G1)):
        t = contract(DERIV, own, -1)
        e = [e[i] + t[i] * theirs[part(f, kind, i), :] * t[i] for i in range(N)]
    return added_up(e)


def added_up(terms):
    while len(terms) > 1:
        terms = [functools.reduce(plus, terms[i : i + 2]) for i in range(0, len(terms), 2)]
    return terms[0]


def face_sums(f, mine, theirs, diag, a_sum, tmp):
    g = [[mine[part(f, k, i), :] + theirs[part(f, k, i), :] for i in range(N)] for k in (G1, G2)]
    for k in (G1, G2):
        for i in range(N):
            theirs[part(f, k, i), :] = g[k - G1][i]
    s = contract(SQUARED.T, g[1], 1)
    for c in range(N):
        tmp[across(f, c), :] = s[c]
    s = contract(SQUARED.T, g[0], 1)
    for b in range(N):
        a_sum[at(f, b), :] = diag[at(f, b), :] - s[b] - tmp[at(f, b), :]


def couplings(g0, first, out):
    def one(b, _):
        g = [g0[at(a, b), :] for a in range(N)]
        for a_end, row in ((0, first), (LAST, FACE - first)):
            s = contract(DERIV.T, [float(DERIV[m, a_end]) * g[m] for m in range(N)], -1, INSIDE)
            for a in INSIDE:
                out[tile(row * 6 + ((a - 1) * N + b) * N), :] = s[a]
        return 0

    lax.fori_loop(0, N, one, 0, unroll=2)


def couple(v, f, coupling, out, a):
    for b in range(N):
        out[at(a, b), :] = (
            out[at(a, b), :] + coupling[tile(((f * 6 + a - 1) * N + b) * N), :] * v[at(f, b), :]
        )


def lane_pick(x, idx):
    return jnp.take_along_axis(x, idx, axis=1, mode="promise_in_bounds")


def sum_yz(planes, lanes):
    ends = [(v[at(a, 0), :], v[at(a, LAST), :]) for v, a in planes]
    rims = [(v[across(a, 0), :], v[across(a, LAST), :]) for v, a in planes]
    ups = [jnp.where(lanes["up"], pltpu.roll(low, LANES - EL_Z, 1), 0.0) for low, _ in ends]
    downs = [jnp.where(lanes["down"], pltpu.roll(high, EL_Z, 1), 0.0) for _, high in ends]
    nexts = [lane_pick(low, lanes["next"]) for low, _ in rims]
    prevs = [lane_pick(high, lanes["prev"]) for _, high in rims]

    def corners(rim, idx):
        turned = jnp.where(lanes["first"], pltpu.roll(rim, 1, 0), pltpu.roll(rim, LAST, 0))
        return jnp.where(lanes["corner"], lane_pick(turned, idx), 0.0)

    far_nexts = [corners(low, lanes["corner_next"]) for low, _ in rims]
    far_prevs = [corners(high, lanes["corner_prev"]) for _, high in rims]
    for k, (v, a) in enumerate(planes):
        v[across(a, LAST), :] = rims[k][1] + (nexts[k] + far_nexts[k])
        v[across(a, 0), :] = rims[k][0] + (prevs[k] + far_prevs[k])
        v[at(a, LAST), :] = v[at(a, LAST), :] + ups[k]
        v[at(a, 0), :] = v[at(a, 0), :] + downs[k]


def step_kernel(
    load_h, geom_h, mass_h, order_h, p_o, r_o, im_o, al_o,
    ld, coef, g2t, r, dg, z, y, u, tmp,
    mine, theirs, w_mine, w_theirs, i_mine, i_theirs, bag, rf, df, zf, pf, yf, a_sum, tmpf,
    u_ends, cross, q_mine, q_theirs, coupling, acc,
    dots, fold, got_a, got_b, got_one, sent_all, order_v, in_sems, x_send, x_recv, bag_recv, s_send, s_recv, one_send, one_recv, hello,
):
    stack = []

    def scope(name):
        if stack:
            stack.pop().__exit__(None, None, None)
        if name:
            stack.append(jax.named_scope(name))
            stack[-1].__enter__()

    scope("enter")
    ys, zs, xs, cores = TORUS
    line, plane_size, count = xs * cores, zs * xs * cores, ys * zs * xs * cores
    me = lax.axis_index("slab")
    core = lax.rem(me, cores)
    in_plane = lax.rem(me, plane_size)

    def greet(sem, who):
        for q in who:
            pl.semaphore_signal(sem, inc=1, device_id=(q,), device_id_type=MESH)

    def heard(sem, who):
        if who:
            pl.semaphore_wait(sem, len(who))

    near_to = me + 1 - 2 * core
    far_to = me + 2 * core - 1
    far_to = jnp.where(far_to < 0, count - 1, jnp.where(far_to == count, 0, far_to))
    early, carrier, late = in_plane == 0, in_plane == line - 1, in_plane == plane_size - 1
    barrier = pltpu.get_barrier_semaphore()
    greet(barrier, [jnp.where(late, me + line - plane_size, far_to)])
    loads = [
        pltpu.make_async_copy(src, dst, in_sems.at[k])
        for k, src, dst in (
            (0, order_h, order_v),
            (1, load_h, ld),
            (2, geom_h, coef.at[pl.ds(0, 3 * ROWS)]),
            (2, mass_h, coef.at[pl.ds(3 * ROWS, ROWS)]),
        )
    ]
    for copy in loads:
        copy.start()
    g0, g1, g2, ms = (coef.at[pl.ds(k * ROWS, ROWS)] for k in range(4))

    y_at = me // plane_size
    z_at = in_plane // line
    x = lax.rem(me, line) // cores

    def moved(dy=0, dz=0, dx=0):
        to = me
        if dy:
            to = to + (lax.rem(y_at + dy, ys) - y_at) * plane_size
        if dz:
            to = to + (lax.rem(z_at + dz, zs) - z_at) * line
        if dx:
            to = to + (lax.rem(x + dx, xs) - x) * cores
        return to

    def ring(size, stop, start=1):
        return sorted({j % size for k in range(start, stop) for j in (k, -k)} - {0})

    sides = (near_to, far_to)
    row_of = (pl.multiple_of((1 - core) * (ROWS - FACE), FACE), pl.multiple_of(core * (ROWS - FACE), FACE))
    face_of = {0: 1 - core, LAST: core}
    carrier_of_early = lax.rem(y_at + ys - 1, ys) * plane_size + line - 1
    early_of_carrier = lax.rem(y_at + 1, ys) * plane_size
    late_of_carrier = me + plane_size - line

    row = [moved(dx=k) + c for k in range(xs) for c in (0, 1 - 2 * core) if k or not isinstance(c, int)]
    y_near = [moved(dy=k) for k in ring(ys, 3)]
    y_far = [moved(dy=k) for k in ring(ys, ys // 2 + 1, 3)]
    greet(barrier, [near_to] + row + y_near)

    @pl.when(early | carrier)
    def _():
        greet(barrier, [jnp.where(early, carrier_of_early, early_of_carrier)])

    def higher(z_to, _):
        greet(barrier, [me + (z_to - z_at) * line + 1 - core])
        return 0

    lax.fori_loop(z_at + 1, zs, higher, 0)
    is_root = me == ROOT
    others_than_root = jnp.logical_not(is_root)

    @pl.when(is_root)
    def _():
        def everyone(q, _):
            @pl.when(q != ROOT)
            def _():
                greet(barrier, [q])

            return 0

        lax.fori_loop(0, count, everyone, 0)

    expected = (
        len(row)
        + len(y_near)
        + 2
        + 2 * carrier.astype(jnp.int32)
        + 2 * core * z_at
        + others_than_root.astype(jnp.int32)
    )

    scope("idx")
    loads[0].wait()
    order = jnp.broadcast_to(order_v[...], (8, LANES))
    hit = (
        jnp.broadcast_to(order_v[...], (LANES, LANES))
        == lax.broadcasted_iota(jnp.int32, (LANES, LANES), 0)
    ).astype(jnp.float32)
    lane = lax.broadcasted_iota(jnp.int32, (8, LANES), 1)
    inverse = lax.dot_general(
        lane.astype(jnp.float32), hit, (((1,), (1,)), ((), ())), preferred_element_type=jnp.float32
    )
    inverse = (inverse + 0.5).astype(jnp.int32)
    in_row = lane & (EL_Z - 1)
    lanes = {
        "up": lane < LANES - EL_Z,
        "down": lane >= EL_Z,
        "next": lane - in_row + ((in_row + 1) & (EL_Z - 1)),
        "prev": lane - in_row + ((in_row + EL_Z - 1) & (EL_Z - 1)),
    }
    b_at = lax.broadcasted_iota(jnp.int32, (8, LANES), 0)
    lanes["first"] = b_at == 0
    lanes["corner"] = (lanes["first"] & lanes["down"]) | ((b_at == LAST) & lanes["up"])
    by_y = jnp.where(lanes["first"], LANES - EL_Z, EL_Z)
    lanes["corner_next"] = (lanes["next"] + by_y) & (LANES - 1)
    lanes["corner_prev"] = (lanes["prev"] + by_y) & (LANES - 1)

    def reorder(src, dst, idx, planes=range(N)):
        for a in planes:
            for b in range(N):
                dst[at(a, b), :] = lane_pick(src[at(a, b), :], idx)

    def remote(src, dst, recv, to):
        return pltpu.make_async_remote_copy(
            src_ref=src,
            dst_ref=dst,
            send_sem=x_send,
            recv_sem=recv,
            device_id=(to,),
            device_id_type=MESH,
        )

    def swap(src, dst, f, first, rows, k, carried=None, bag_k=None):
        src, dst = src.at[pl.ds(first, rows)], dst.at[pl.ds(first, rows)]
        copy = remote(src, dst, x_recv.at[k], sides[f])
        if carried is None:
            copy.start()
        else:
            by_bag = remote(src, bag.at[pl.ds(carried, rows)], bag_recv.at[bag_k], carrier_of_early)
            pl.when(early)(by_bag.start)
            pl.when(jnp.logical_not(early))(copy.start)
        return copy

    def carry(dst, carried, first, rows, k):
        src, dst = bag.at[pl.ds(carried, rows)], dst.at[pl.ds(first, rows)]
        remote(src, dst, x_recv.at[k], late_of_carrier).start()

    def landed(ref, sem):
        pltpu.make_async_copy(ref, ref, sem).wait()

    both = (0, LAST)
    faces = (0, 1)
    scope("load_ends")
    loads[1].wait()
    for a in both:
        for b in range(N):
            mine[part(face_of[a], LOAD, b), :] = lane_pick(ld[at(a, b), :], inverse)
    pltpu.make_async_copy(coef, coef, in_sems.at[2]).wait()
    for k, a in enumerate(both):
        s = contract(SQUARED.T, [g2[across(a, c), :] for c in range(N)], 1)
        for c in range(N):
            tmpf[across(k, c), :] = s[c]
    for b in range(N):
        s = contract(SQUARED.T, [g0[at(a, b), :] for a in range(N)], 1, both)
        for k, a in enumerate(both):
            yf[at(k, b), :] = s[a]
    for k, a in enumerate(both):
        s = contract(SQUARED.T, [g1[at(a, b), :] for b in range(N)], 1)
        for b in range(N):
            mine[part(face_of[a], DIAG, b), :] = lane_pick(
                s[b] + yf[at(k, b), :] + ms[at(a, b), :] + tmpf[at(k, b), :], inverse
            )
    for a in both:
        for i in range(N):
            mine[part(face_of[a], G1, i), :] = lane_pick(g1[at(a, i), :], inverse)
            mine[part(face_of[a], G2, i), :] = lane_pick(g2[across(a, i), :], inverse)
    scope("barrier")
    pl.semaphore_wait(barrier, expected)
    scope("send1")

    @pl.when(carrier)
    def _():
        landed(bag.at[pl.ds(0, 4 * FACE)], bag_recv.at[0])
        carry(theirs, 0, 4 * FACE, 2 * FACE, FAR_LD)
        carry(theirs, 2 * FACE, 6 * FACE, 2 * FACE, FAR_G)

    sent_ld = swap(mine, theirs, 1, 4 * FACE, 2 * FACE, FAR_LD, 0, 0)
    sent_g = swap(mine, theirs, 1, 6 * FACE, 2 * FACE, FAR_G, 2 * FACE, 0)
    sent_near = swap(mine, theirs, 0, 0, 4 * FACE, NEAR)
    greet(hello.at[0], y_near)

    @pl.when(core == 1)
    def _():
        def lower(z_to, _):
            greet(hello.at[2], [me + (z_to - z_at) * line])
            return 0

        lax.fori_loop(0, z_at, lower, 0)

    scope("diag")
    inner_diagonal(g0, g1, g2, ms, dg, tmp)
    scope("reorder")
    for a in INSIDE:
        for b in range(N):
            rows = at(a, b)
            dg[rows, :] = lane_pick(dg[rows, :], inverse)
            moved_load = lane_pick(ld[rows, :], inverse)
            ld[rows, :] = moved_load
            r[rows, :] = moved_load
    reorder(g0, g0, inverse)
    scope("sums")
    sum_yz([(v, a) for a in INSIDE for v in (dg, r)], lanes)

    def inner_z(a, _):
        for b in range(N):
            inv = 1.0 / dg[at(a, b), :]
            dg[at(a, b), :] = inv
            z[at(a, b), :] = inv * r[at(a, b), :]
        return 0

    lax.fori_loop(1, LAST, inner_z, 0, unroll=3)
    for b in range(N):
        g = [float(DERIV[m, 0] * DERIV[m, LAST]) * g0[at(m, b), :] for m in range(N)]
        cross[at(0, b), :] = added_up(g)
    scope("La1")
    stiffness_a(z, g0, y)

    def full(f, b):
        return tile(row_of[f] + b * N)

    def face_z(f):
        for b in range(N):
            rf[at(f, b), :] = mine[part(f, LOAD, b), :] + theirs[part(f, LOAD, b), :]
            total = mine[part(f, DIAG, b), :] + theirs[part(f, DIAG, b), :]
            a_sum[at(f, b), :] = total
            df[at(f, b), :] = total
        sum_yz([(rf, f), (df, f)], lanes)
        for b in range(N):
            inv = 1.0 / df[at(f, b), :]
            df[at(f, b), :] = inv
            zf[at(f, b), :] = inv * rf[at(f, b), :]

    def tell(f, k, carried=None):
        for b in range(N):
            w_mine[at(f, b), :] = y[full(f, b), :] + cross[at(0, b), :] * zf[at(1 - f, b), :]
        sum_yz([(w_mine, f)], lanes)
        return swap(w_mine, w_theirs, f, f * FACE, FACE, k, carried, 1)

    scope("x_near")
    sent_near.wait_recv()
    scope("z_near")
    face_z(0)
    sent_w = [None, tell(1, FAR_W, 4 * FACE)]
    scope("reorder2")
    reorder(g1, g1, inverse, INSIDE)
    for a in INSIDE:
        for c in range(N):
            g2t[at(a, c), :] = lane_pick(g2[across(a, c), :], inverse)
    reorder(ms, ms, inverse, INSIDE)
    scope("Lbc1")
    stiffness_bc(z, g1, g2t, ms, y, tmp, y)
    scope("hello")

    @pl.when(carrier)
    def _():
        landed(bag.at[pl.ds(4 * FACE, FACE)], bag_recv.at[1])
        carry(w_theirs, 4 * FACE, FACE, FACE, FAR_W)

    heard(hello.at[0], y_near)
    greet(hello.at[1], y_far)
    scope("g_near")
    first = pl.multiple_of((1 - core) * FACE, FACE)
    couplings(g0, first, coupling)
    loop(1, LAST, lambda a: couple(zf, 0, coupling, y, a))
    face_sums(0, mine, theirs, a_sum, a_sum, tmpf)
    s = face_terms(zf, 0, mine, theirs, a_sum, tmpf)
    for b in range(N):
        yf[at(0, b), :] = s[b]
    sum_yz([(yf, 0)], lanes)
    scope("x_far")
    sent_ld.wait_recv()
    scope("z_far")
    face_z(1)

    scope("inner2")
    for a in INSIDE:
        couple(zf, 1, coupling, y, a)
    sum_yz([(y, a) for a in INSIDE], lanes)
    zero = jnp.zeros((8, LANES), jnp.float32)

    def inner_p(a, num):
        for b in range(N):
            rows = at(a, b)
            p = COEF_Z * z[rows, :] - COEF_Q * (dg[rows, :] * y[rows, :])
            z[rows, :] = p
            num[b % 4] = num[b % 4] + ld[rows, :] * p
        return num

    num = lax.fori_loop(1, LAST, inner_p, [zero] * 4, unroll=True)
    scope("L2")
    den = energy_bc(z, g1, g2t, ms, [zero] * 4)
    den = energy_a(z, g0, u_ends, first, den)
    num, den = added_up(num), added_up(den)
    scope("g_far")
    sent_g.wait_recv()
    face_sums(1, mine, theirs, a_sum, a_sum, tmpf)
    s = face_terms(zf, 1, mine, theirs, a_sum, tmpf)
    for b in range(N):
        yf[at(1, b), :] = s[b]
    sum_yz([(yf, 1)], lanes)
    sent_w[0] = tell(0, NEAR_W)

    def face_p(f):
        for b in range(N):
            rows = at(f, b)
            total = yf[rows, :] + (w_mine[rows, :] + w_theirs[rows, :])
            pf[rows, :] = COEF_Z * zf[rows, :] - COEF_Q * (df[rows, :] * total)

    def face_dot(kind, f):
        return added_up([kind[part(f, LOAD, b), :] * pf[at(f, b), :] for b in range(N)])

    acc[tile(0), :] = num
    acc[tile(8), :] = den
    takes = jnp.where(2 * x >= xs, core, 1 - core) == 1
    gives = jnp.logical_not(takes)
    sent_q = remote(q_mine, q_theirs, x_recv.at[NEAR_Q], near_to)
    scope("w_near")

    @pl.when(takes)
    def _():
        sent_w[0].wait_recv()
        face_p(0)
        sent_q.wait_recv()
        acc[tile(0), :] = acc[tile(0), :] + (face_dot(mine, 0) + face_dot(theirs, 0))
        terms = [
            (2.0 * u_ends[at(0, b), :] + q_theirs[at(0, b), :]) * pf[at(0, b), :] for b in range(N)
        ]
        acc[tile(8), :] = acc[tile(8), :] + (face_energy(pf, 0, theirs, a_sum) + added_up(terms))
        for b in range(N):
            q_mine[at(0, b), :] = 2.0 * cross[at(0, b), :] * pf[at(0, b), :]

    scope("w_far")
    sent_w[1].wait_recv()
    scope("ends2")
    face_p(1)
    acc[tile(0), :] = acc[tile(0), :] + face_dot(mine, 1)
    terms = [2.0 * u_ends[at(1, b), :] * pf[at(1, b), :] for b in range(N)]
    acc[tile(8), :] = acc[tile(8), :] + (0.5 * face_energy(pf, 1, theirs, a_sum) + added_up(terms))

    @pl.when(takes)
    def _():
        terms = [q_mine[at(0, b), :] * pf[at(1, b), :] for b in range(N)]
        acc[tile(8), :] = acc[tile(8), :] + added_up(terms)

    @pl.when(gives)
    def _():
        for b in range(N):
            q_mine[at(0, b), :] = 2.0 * (
                u_ends[at(0, b), :] + cross[at(0, b), :] * pf[at(1, b), :]
            )
        sent_q.start()

    num_row = jnp.sum(acc[tile(0), :], axis=0, keepdims=True)
    den_row = jnp.sum(acc[tile(8), :], axis=0, keepdims=True)
    dots[0, 0:1, :] = num_row
    dots[0, 1:2, :] = den_row
    half = LANES // 2
    first_half = lane[0:1, :] < half
    fold[0, 0:1, :] = jnp.where(
        first_half, num_row + pltpu.roll(num_row, half, 1), den_row + pltpu.roll(den_row, half, 1)
    )

    hops = sorted(
        ((dy, dx) for dy in range(ys) for dx in range(xs) if dy or dx),
        key=lambda d: -min(d[0], ys - d[0]) - min(d[1], xs - d[1]),
    )
    others = 2 * len(hops) + 1

    def send(src, dst, k, to):
        copy = pltpu.make_async_remote_copy(
            src_ref=src,
            dst_ref=dst,
            send_sem=s_send,
            recv_sem=s_recv.at[k],
            device_id=(to,),
            device_id_type=MESH,
        )
        copy.start()

    def arrived(ref, sem):
        pltpu.make_async_copy(ref, ref, sem).wait()

    def added(ref, first, total):
        part = [first, None, None, None]
        for j in range(total):
            part[j % 4] = plus(part[j % 4], ref[j])
        return functools.reduce(plus, [t for t in part if t is not None])

    heard(hello.at[1], y_far)
    by_z = z_at * ys * line + y_at * line + lax.rem(me, line)
    for j, (dy, dx) in enumerate(hops):
        send(dots.at[0], got_a.at[2 * j + core], 0, moved(dy=dy, dx=dx) + 1 - core)
        if j == len(hops) // 2:

            @pl.when(others_than_root)
            def _():
                pltpu.make_async_remote_copy(
                    src_ref=fold.at[0],
                    dst_ref=got_one.at[jnp.maximum(by_z - 1, 0)],
                    send_sem=one_send,
                    recv_sem=one_recv.at[jnp.where(z_at < zs // 2, 0, 1)],
                    device_id=(ROOT,),
                    device_id_type=MESH,
                ).start()

    @pl.when(core == 0)
    def _():
        send(dots.at[0], got_a.at[others - 1], 0, me + 1)

    scope("u_ends")

    @pl.when(gives)
    def _():
        sent_w[0].wait_recv()
        face_p(0)

    for f in faces:
        for b in range(N):
            i_mine[at(f, b), :] = u_ends[at(f, b), :] + cross[at(0, b), :] * pf[at(1 - f, b), :]
        swap(i_mine, i_theirs, f, f * FACE, FACE, IMAGE)
    for f in faces:
        s = face_terms(pf, f, mine, theirs, a_sum, tmpf)
        for b in range(N):
            yf[at(f, b), :] = s[b]
    stiffness_bc(z, g1, g2t, ms, y, tmp)
    stiffness_a(z, g0, u, INSIDE, y)

    def couple_both(a):
        couple(pf, 0, coupling, u, a)
        couple(pf, 1, coupling, u, a)

    loop(1, LAST, couple_both)
    scope("out_p_r")
    for src, ends, dst in ((z, pf, p_o), (r, rf, r_o)):
        reorder(src, dst, order, INSIDE)
        for f in faces:
            for b in range(N):
                dst[full(f, b), :] = lane_pick(ends[at(f, b), :], order)
    sum_yz([(u, a) for a in INSIDE], lanes)
    reorder(u, im_o, order, INSIDE)
    scope("plane")

    @pl.when(core == 1)
    def _():
        arrived(got_a.at[pl.ds(0, others)], s_recv.at[0])
        dots[1] = added(got_a, dots[0], others)

        @pl.when(z_at < zs - 1)
        def _():
            pl.semaphore_wait(hello.at[2], zs - 1 - z_at)

        for k in sorted(range(1, zs), key=lambda k: -min(k, zs - k)):
            send(dots.at[1], got_b.at[k - 1], 1, moved(dz=k) - 1)

            @pl.when(moved(dz=k) != ROOT)
            def _(k=k):
                send(dots.at[1], got_b.at[k - 1], 1, moved(dz=k))

        send(dots.at[1], got_b.at[zs - 1], 1, me - 1)
        got_b[zs - 1] = dots[1]

    scope("x3")
    landed(i_theirs, x_recv.at[IMAGE])
    for f in faces:
        for b in range(N):
            rows = at(f, b)
            yf[rows, :] = yf[rows, :] + (i_mine[rows, :] + i_theirs[rows, :])
    sum_yz([(yf, f) for f in faces], lanes)
    for f in faces:
        for b in range(N):
            im_o[full(f, b), :] = lane_pick(yf[at(f, b), :], order)
    scope("lines")

    @pl.when(core == 0)
    def _():
        arrived(got_b, s_recv.at[1])

    @pl.when((core == 1) & others_than_root)
    def _():
        arrived(got_b.at[pl.ds(0, zs - 1)], s_recv.at[1])

    @pl.when(others_than_root)
    def _():
        dots[2] = added(got_b, None, zs)

    @pl.when(is_root)
    def _():
        early_ones = count // 2 - 1
        arrived(got_one.at[pl.ds(0, early_ones)], one_recv.at[0])
        arrived(got_one.at[pl.ds(early_ones, count // 2)], one_recv.at[1])
        width = 16

        def some(k, sums):
            for i in range(width):
                sums[i % 8] = sums[i % 8] + got_one[k * width + i]
            return sums

        blank = jnp.zeros((1, LANES), jnp.float32)
        whole = (count - 1) // width
        sums = lax.fori_loop(0, whole, some, [blank] * 8)
        for k in range(whole * width, count - 1):
            sums[k % 8] = sums[k % 8] + got_one[k]
        row_sum = added_up(sums) + fold[0]
        dots[2, 0:1, :] = jnp.where(first_half, row_sum, 0.0)
        dots[2, 1:2, :] = jnp.where(first_half, 0.0, row_sum)

    total = dots[2]
    scope("alpha")
    sums = jnp.sum(total, axis=1, keepdims=True)
    al_o[...] = jnp.broadcast_to(sums[0:1, :] / sums[1:2, :], (8, LANES))
    plane_sends, line_sends = len(hops), 2 * zs - 1
    above_root = lax.rem(me, plane_size) // line * line + ROOT == me
    above_root = above_root & others_than_root & (y_at == 0)

    @pl.when(others_than_root)
    def _():
        arrived(fold.at[0], one_send)

    for case, sends in (
        (core == 0, plane_sends + 1),
        ((core == 1) & above_root, plane_sends + line_sends - 1),
        ((core == 1) & jnp.logical_not(above_root), plane_sends + line_sends),
    ):

        @pl.when(case)
        def _(sends=sends):
            arrived(sent_all.at[pl.ds(0, sends)], s_send)

    for case, sends in (
        (takes & jnp.logical_not(carrier), 12),
        (takes & carrier, 17),
        (gives & jnp.logical_not(carrier), 13),
        (gives & carrier, 18),
    ):

        @pl.when(case)
        def _(sends=sends):
            landed(coef.at[pl.ds(0, sends * FACE)], x_send)

    scope(None)


CHUNKS = 4


def finish_kernel(p, r, im, al, x_h, r_h, both, sem):
    alpha = al[...]
    size = ROWS // CHUNKS
    for k in range(CHUNKS):
        for i in range(k * size, (k + 1) * size, N):
            both[tile(i), :] = alpha * p[tile(i), :]
        pltpu.make_async_copy(both.at[pl.ds(k * size, size)], x_h.at[pl.ds(k * size, size)], sem).start()
        for i in range(k * size, (k + 1) * size, N):
            both[tile(ROWS + i), :] = r[tile(i), :] - alpha * im[tile(i), :]
        rows = pl.ds(ROWS + k * size, size)
        pltpu.make_async_copy(both.at[rows], r_h.at[pl.ds(k * size, size)], sem).start()
    pltpu.make_async_copy(both, both, sem).wait()


def on_device(load_terms, geometry, mass_terms, element_order):
    flat = jax.ShapeDtypeStruct((ROWS, LANES), jnp.float32)
    vm = lambda *shape: pltpu.VMEM(shape, jnp.float32)
    field = vm(ROWS, LANES)
    pair = vm(2 * FACE, LANES)
    ys, zs, xs, cores = TORUS
    in_vmem = pl.BlockSpec(memory_space=pltpu.VMEM)
    in_hbm = pl.BlockSpec(memory_space=pltpu.HBM)
    parts = pl.pallas_call(
        step_kernel,
        out_shape=(field, field, field, vm(8, LANES)),
        in_specs=[in_hbm] * 4,
        out_specs=[in_vmem] * 4,
        scratch_shapes=[
            field, vm(4 * ROWS, LANES), *[field] * 7,
            *[vm(8 * FACE, LANES)] * 2,
            *[pair] * 4, vm(5 * FACE, LANES), *[pair] * 8, *[vm(FACE, LANES)] * 3,
            vm(12 * FACE, LANES), vm(16, LANES),
            vm(3, 2, LANES), vm(1, 1, LANES), vm(2 * ys * xs - 1, 2, LANES), vm(zs, 2, LANES),
            vm(ys * zs * xs * cores - 1, 1, LANES),
            vm(ys * xs + 2 * zs, 2, LANES),
            pltpu.VMEM((1, LANES), jnp.int32),
            pltpu.SemaphoreType.DMA((3,)),
            pltpu.SemaphoreType.DMA(()),
            pltpu.SemaphoreType.DMA((7,)),
            pltpu.SemaphoreType.DMA((2,)),
            pltpu.SemaphoreType.DMA(()),
            pltpu.SemaphoreType.DMA((2,)),
            pltpu.SemaphoreType.DMA(()),
            pltpu.SemaphoreType.DMA((2,)),
            pltpu.SemaphoreType.REGULAR((3,)),
        ],
        compiler_params=pltpu.CompilerParams(
            collective_id=0, has_side_effects=True, vmem_limit_bytes=24 << 20
        ),
        name="cg_step",
    )(
        *[
            pltpu.with_memory_space_constraint(t, pltpu.HBM)
            for t in (
                load_terms.reshape(ROWS, LANES),
                geometry.reshape(3 * ROWS, LANES),
                mass_terms.reshape(ROWS, LANES),
                element_order,
            )
        ]
    )
    x, res = pl.pallas_call(
        finish_kernel,
        out_shape=(flat, flat),
        in_specs=[in_vmem] * 4,
        out_specs=[in_hbm] * 2,
        scratch_shapes=[vm(2 * ROWS, LANES), pltpu.SemaphoreType.DMA(())],
        compiler_params=pltpu.CompilerParams(vmem_limit_bytes=8 << 20),
        name="cg_finish",
    )(*[pltpu.with_memory_space_constraint(t, pltpu.VMEM) for t in parts])
    shape = load_terms.shape
    return x.reshape(shape), res.reshape(shape)


def solution(mesh):
    last = P(None, None, None, "slab")
    return jax.shard_map(
        on_device,
        mesh=mesh,
        in_specs=(last, P(None, None, None, None, "slab"), last, P("slab", None)),
        out_specs=(last, last),
        check_vma=False,
    )
```

```python
import functools

import jax
import jax.numpy as jnp
import numpy as np
from jax import lax
from jax.experimental import pallas as pl
from jax.experimental.pallas import tpu as pltpu
from jax.sharding import PartitionSpec as P

N = 8
LAST = N - 1
EL_Y = 8
EL_Z = 16
LANES = 128
ROWS = N * N * N
FACE = N * N
CENTRE = 1.65
HALF = 1.35
MESH = pl.DeviceIdType.MESH
TORUS = (8, 12, 4, 2)
ROOT = 1
INSIDE = range(1, LAST)
UNROLL_A = 4
UNROLL_BC = 3


def legendre_table(positions, points):
    columns = [positions * 0.0 + 1.0, positions]
    for degree in range(2, points):
        columns.append(
            ((2 * degree - 1) * positions * columns[-1] - (degree - 1) * columns[-2]) / degree
        )
    return np.stack(columns, axis=1)


def gll_derivative(points):
    degree = points - 1
    nodes = -np.cos(np.pi * np.arange(points) / degree)
    for _ in range(100):
        legendre = legendre_table(nodes, points)
        nodes = nodes - (nodes * legendre[:, degree] - legendre[:, degree - 1]) / (
            points * legendre[:, degree]
        )
    legendre = legendre_table(nodes, points)
    top = legendre[:, degree]
    same = np.eye(points, dtype=bool)
    spacing = np.where(same, 1.0, nodes[:, None] - nodes[None, :])
    table = np.where(same, 0.0, top[:, None] / (top[None, :] * spacing))
    table[0, 0] = -degree * points / 4.0
    table[degree, degree] = degree * points / 4.0
    return table


DERIV = gll_derivative(N).astype(np.float32).astype(np.float64)
SQUARED = DERIV * DERIV
SIGMA = CENTRE / HALF
RHO0 = 1.0 / SIGMA
RHO1 = 1.0 / (2.0 * SIGMA - RHO0)
COEF_Z = (1.0 + RHO1 * RHO0) / CENTRE + 2.0 * RHO1 / HALF
COEF_Q = 2.0 * RHO1 / HALF / CENTRE


def plus(x, y):
    return y if x is None else x + y


def contract(table, terms, sign, rows=range(N)):
    used = [j for j in range(N // 2) if terms[j] is not None]
    even = {j: terms[j] + terms[LAST - j] for j in used}
    odd = {j: terms[j] - terms[LAST - j] for j in used}
    out = [None] * N
    for i in range(N // 2):
        if i not in rows and LAST - i not in rows:
            continue
        e = o = None
        for j in used:
            e = plus(e, float(table[i, j] + table[i, LAST - j]) / 2 * even[j])
            o = plus(o, float(table[i, j] - table[i, LAST - j]) / 2 * odd[j])
        if i in rows:
            out[i] = e + o
        if LAST - i in rows:
            out[LAST - i] = (o - e) if sign < 0 else (e - o)
    return out


def tile(row):
    return pl.ds(row if isinstance(row, int) else pl.multiple_of(row, 8), 8)


def at(a, b):
    return tile((a * N + b) * N)


def across(a, c):
    return pl.ds(a * FACE + c, N, stride=N)


LOAD, DIAG, G1, G2 = range(4)
NEAR, FAR_LD, FAR_G, NEAR_W, FAR_W, IMAGE = range(6)


def part(f, kind, i):
    return tile(((f * 4 + kind) * N + i) * N)


def loop(start, stop, body):
    lax.fori_loop(start, stop, lambda i, _: (body(i), 0)[1], 0)


def stiffness_a(v, g0, out, rows=range(N), more=None):
    def along_a(b, _):
        va = [v[at(a, b), :] if a in INSIDE else None for a in range(N)]
        s = contract(DERIV, va, -1)
        s = contract(DERIV.T, [s[a] * g0[at(a, b), :] for a in range(N)], -1, rows)
        for a in rows:
            out[at(a, b), :] = s[a] if more is None else s[a] + more[at(a, b), :]
        return 0

    lax.fori_loop(0, N, along_a, 0, unroll=UNROLL_A)


def energy_a(v, g0, ends, first, total):
    def along_a(b, total):
        t = contract(DERIV, [v[at(a, b), :] if a in INSIDE else None for a in range(N)], -1)
        s = [t[a] * g0[at(a, b), :] for a in range(N)]
        total = [total[k] + s[k] * t[k] + s[k + 4] * t[k + 4] for k in range(4)]
        s = contract(DERIV.T, s, -1, (0, LAST))
        ends[tile(first + b * N), :] = s[0]
        ends[tile(FACE - first + b * N), :] = s[LAST]
        return total

    return lax.fori_loop(0, N, along_a, total, unroll=UNROLL_A)


def energy_bc(v, g1, g2t, ms, total):
    def along_bc(a, total):
        vb = [v[at(a, b), :] for b in range(N)]
        for own, g in (([v[across(a, c), :] for c in range(N)], g2t), (vb, g1)):
            t = contract(DERIV, own, -1)
            e = [t[i] * g[at(a, i), :] * t[i] for i in range(N)]
            total = [total[k] + (e[k] + e[k + 4]) for k in range(4)]
        e = [vb[b] * ms[at(a, b), :] * vb[b] for b in range(N)]
        return [total[k] + (e[k] + e[k + 4]) for k in range(4)]

    return lax.fori_loop(1, LAST, along_bc, total, unroll=UNROLL_BC)


def stiffness_bc(v, g1, g2t, ms, out, tmp, more=None):
    def along_bc(a, _):
        vt = [v[across(a, c), :] for c in range(N)]
        vb = [v[at(a, b), :] for b in range(N)]
        t = contract(DERIV, vt, -1)
        t = contract(DERIV.T, [t[c] * g2t[at(a, c), :] for c in range(N)], -1)
        for c in range(N):
            tmp[across(a, c), :] = t[c]
        s = contract(DERIV, vb, -1)
        s = contract(DERIV.T, [s[b] * g1[at(a, b), :] for b in range(N)], -1)
        for b in range(N):
            s[b] = s[b] + ms[at(a, b), :] * vb[b]
            if more is not None:
                s[b] = s[b] + more[at(a, b), :]
        for b in range(N):
            out[at(a, b), :] = s[b] + tmp[at(a, b), :]
        return 0

    lax.fori_loop(1, LAST, along_bc, 0, unroll=UNROLL_BC)


def inner_diagonal(g0, g1, g2, ms, out, tmp):
    def along_a(b, _):
        s = contract(SQUARED.T, [g0[at(a, b), :] for a in range(N)], 1, INSIDE)
        for a in INSIDE:
            out[at(a, b), :] = s[a] + ms[at(a, b), :]
        return 0

    lax.fori_loop(0, N, along_a, 0, unroll=UNROLL_A)

    def along_bc(a, _):
        t = contract(SQUARED.T, [g2[across(a, c), :] for c in range(N)], 1)
        for c in range(N):
            tmp[across(a, c), :] = t[c]
        s = contract(SQUARED.T, [g1[at(a, b), :] for b in range(N)], 1)
        for b in range(N):
            s[b] = s[b] + out[at(a, b), :]
        for b in range(N):
            out[at(a, b), :] = s[b] + tmp[at(a, b), :]
        return 0

    lax.fori_loop(1, LAST, along_bc, 0, unroll=UNROLL_BC)


def face_terms(v, f, mine, theirs, a_sum, tmp):
    s = contract(DERIV, [v[across(f, c), :] for c in range(N)], -1)
    s = contract(DERIV.T, [s[c] * theirs[part(f, G2, c), :] for c in range(N)], -1)
    for c in range(N):
        tmp[across(f, c), :] = s[c]
    vb = [v[at(f, b), :] for b in range(N)]
    s = contract(DERIV, vb, -1)
    s = contract(DERIV.T, [s[b] * theirs[part(f, G1, b), :] for b in range(N)], -1)
    return [s[b] + a_sum[at(f, b), :] * vb[b] + tmp[at(f, b), :] for b in range(N)]


def face_energy(v, f, theirs, a_sum):
    vb = [v[at(f, b), :] for b in range(N)]
    e = [a_sum[at(f, b), :] * vb[b] * vb[b] for b in range(N)]
    for own, kind in (([v[across(f, c), :] for c in range(N)], G2), (vb, G1)):
        t = contract(DERIV, own, -1)
        e = [e[i] + t[i] * theirs[part(f, kind, i), :] * t[i] for i in range(N)]
    return added_up(e)


def added_up(terms):
    while len(terms) > 1:
        terms = [functools.reduce(plus, terms[i : i + 2]) for i in range(0, len(terms), 2)]
    return terms[0]


def face_sums(f, mine, theirs, diag, a_sum, tmp):
    g = [[mine[part(f, k, i), :] + theirs[part(f, k, i), :] for i in range(N)] for k in (G1, G2)]
    for k in (G1, G2):
        for i in range(N):
            theirs[part(f, k, i), :] = g[k - G1][i]
    s = contract(SQUARED.T, g[1], 1)
    for c in range(N):
        tmp[across(f, c), :] = s[c]
    s = contract(SQUARED.T, g[0], 1)
    for b in range(N):
        a_sum[at(f, b), :] = diag[at(f, b), :] - s[b] - tmp[at(f, b), :]


def couplings(g0, first, out):
    def one(b, _):
        g = [g0[at(a, b), :] for a in range(N)]
        for a_end, row in ((0, first), (LAST, FACE - first)):
            s = contract(DERIV.T, [float(DERIV[m, a_end]) * g[m] for m in range(N)], -1, INSIDE)
            for a in INSIDE:
                out[tile(row * 6 + ((a - 1) * N + b) * N), :] = s[a]
        return 0

    lax.fori_loop(0, N, one, 0, unroll=2)


def couple(v, f, coupling, out, a):
    for b in range(N):
        out[at(a, b), :] = (
            out[at(a, b), :] + coupling[tile(((f * 6 + a - 1) * N + b) * N), :] * v[at(f, b), :]
        )


def lane_pick(x, idx):
    return jnp.take_along_axis(x, idx, axis=1, mode="promise_in_bounds")


def sum_yz(planes, lanes):
    ends = [(v[at(a, 0), :], v[at(a, LAST), :]) for v, a in planes]
    rims = [(v[across(a, 0), :], v[across(a, LAST), :]) for v, a in planes]
    ups = [jnp.where(lanes["up"], pltpu.roll(low, LANES - EL_Z, 1), 0.0) for low, _ in ends]
    downs = [jnp.where(lanes["down"], pltpu.roll(high, EL_Z, 1), 0.0) for _, high in ends]
    nexts = [lane_pick(low, lanes["next"]) for low, _ in rims]
    prevs = [lane_pick(high, lanes["prev"]) for _, high in rims]

    def corners(rim, idx):
        turned = jnp.where(lanes["first"], pltpu.roll(rim, 1, 0), pltpu.roll(rim, LAST, 0))
        return jnp.where(lanes["corner"], lane_pick(turned, idx), 0.0)

    far_nexts = [corners(low, lanes["corner_next"]) for low, _ in rims]
    far_prevs = [corners(high, lanes["corner_prev"]) for _, high in rims]
    for k, (v, a) in enumerate(planes):
        v[across(a, LAST), :] = rims[k][1] + (nexts[k] + far_nexts[k])
        v[across(a, 0), :] = rims[k][0] + (prevs[k] + far_prevs[k])
        v[at(a, LAST), :] = v[at(a, LAST), :] + ups[k]
        v[at(a, 0), :] = v[at(a, 0), :] + downs[k]


def step_kernel(
    load_h, geom_h, mass_h, order_h, p_o, r_o, im_o, al_o,
    coef, g2t, r, dg, z, y, u, tmp,
    mine, theirs, w_mine, w_theirs, i_mine, i_theirs, bag, rf, df, zf, pf, yf, a_sum, tmpf,
    u_ends, cross, q_mine, q_theirs, coupling, acc,
    dots, got_a, got_b, got_one, all_sent, order_v, in_sems, x_send, x_recv, bag_recv, s_recv, one_recv, hello,
):
    stack = []

    def scope(name):
        if stack:
            stack.pop().__exit__(None, None, None)
        if name:
            stack.append(jax.named_scope(name))
            stack[-1].__enter__()

    scope("enter")
    ys, zs, xs, cores = TORUS
    line, plane_size, count = xs * cores, zs * xs * cores, ys * zs * xs * cores
    me = lax.axis_index("slab")
    core = lax.rem(me, cores)
    in_plane = lax.rem(me, plane_size)

    def greet(sem, who):
        for q in who:
            pl.semaphore_signal(sem, inc=1, device_id=(q,), device_id_type=MESH)

    def heard(sem, who):
        if who:
            pl.semaphore_wait(sem, len(who))

    near_to = me + 1 - 2 * core
    far_to = me + 2 * core - 1
    far_to = jnp.where(far_to < 0, count - 1, jnp.where(far_to == count, 0, far_to))
    early, carrier, late = in_plane == 0, in_plane == line - 1, in_plane == plane_size - 1
    barrier = pltpu.get_barrier_semaphore()
    greet(barrier, [jnp.where(late, me + line - plane_size, far_to)])
    loads = [
        pltpu.make_async_copy(src, dst, in_sems.at[k])
        for k, src, dst in (
            (0, order_h, order_v),
            (1, load_h, coef.at[pl.ds(4 * ROWS, ROWS)]),
            (1, geom_h, coef.at[pl.ds(0, 3 * ROWS)]),
            (1, mass_h, coef.at[pl.ds(3 * ROWS, ROWS)]),
        )
    ]
    for copy in loads:
        copy.start()
    g0, g1, g2, ms, ld = (coef.at[pl.ds(k * ROWS, ROWS)] for k in range(5))

    y_at = me // plane_size
    z_at = in_plane // line
    x = lax.rem(me, line) // cores

    def moved(dy=0, dz=0, dx=0):
        to = me
        if dy:
            to = to + (lax.rem(y_at + dy, ys) - y_at) * plane_size
        if dz:
            to = to + (lax.rem(z_at + dz, zs) - z_at) * line
        if dx:
            to = to + (lax.rem(x + dx, xs) - x) * cores
        return to

    def ring(size, stop, start=1):
        return sorted({j % size for k in range(start, stop) for j in (k, -k)} - {0})

    sides = (near_to, far_to)
    row_of = (pl.multiple_of((1 - core) * (ROWS - FACE), FACE), pl.multiple_of(core * (ROWS - FACE), FACE))
    face_of = {0: 1 - core, LAST: core}
    carrier_of_early = lax.rem(y_at + ys - 1, ys) * plane_size + line - 1
    early_of_carrier = lax.rem(y_at + 1, ys) * plane_size
    late_of_carrier = me + plane_size - line

    row = [moved(dx=k) + c for k in range(xs) for c in (0, 1 - 2 * core) if k or not isinstance(c, int)]
    y_near = [moved(dy=k) for k in ring(ys, 3)]
    y_far = [moved(dy=k) for k in ring(ys, ys // 2 + 1, 3)]
    greet(barrier, [near_to] + row + y_near)

    @pl.when(early | carrier)
    def _():
        greet(barrier, [jnp.where(early, carrier_of_early, early_of_carrier)])

    def higher(z_to, _):
        greet(barrier, [me + (z_to - z_at) * line + 1 - core])
        return 0

    lax.fori_loop(z_at + 1, zs, higher, 0)
    is_root = me == ROOT
    others_than_root = jnp.logical_not(is_root)

    @pl.when(is_root)
    def _():
        def everyone(q, _):
            @pl.when(q != ROOT)
            def _():
                greet(barrier, [q])

            return 0

        lax.fori_loop(0, count, everyone, 0)

    expected = (
        len(row)
        + len(y_near)
        + 2
        + 2 * carrier.astype(jnp.int32)
        + 2 * core * z_at
        + others_than_root.astype(jnp.int32)
    )

    scope("idx")
    loads[0].wait()
    order = jnp.broadcast_to(order_v[...], (8, LANES))
    hit = (
        jnp.broadcast_to(order_v[...], (LANES, LANES))
        == lax.broadcasted_iota(jnp.int32, (LANES, LANES), 0)
    ).astype(jnp.float32)
    lane = lax.broadcasted_iota(jnp.int32, (8, LANES), 1)
    inverse = lax.dot_general(
        lane.astype(jnp.float32), hit, (((1,), (1,)), ((), ())), preferred_element_type=jnp.float32
    )
    inverse = (inverse + 0.5).astype(jnp.int32)
    in_row = lane & (EL_Z - 1)
    lanes = {
        "up": lane < LANES - EL_Z,
        "down": lane >= EL_Z,
        "next": lane - in_row + ((in_row + 1) & (EL_Z - 1)),
        "prev": lane - in_row + ((in_row + EL_Z - 1) & (EL_Z - 1)),
    }
    b_at = lax.broadcasted_iota(jnp.int32, (8, LANES), 0)
    lanes["first"] = b_at == 0
    lanes["corner"] = (lanes["first"] & lanes["down"]) | ((b_at == LAST) & lanes["up"])
    by_y = jnp.where(lanes["first"], LANES - EL_Z, EL_Z)
    lanes["corner_next"] = (lanes["next"] + by_y) & (LANES - 1)
    lanes["corner_prev"] = (lanes["prev"] + by_y) & (LANES - 1)

    def reorder(src, dst, idx, planes=range(N)):
        for a in planes:
            for b in range(N):
                dst[at(a, b), :] = lane_pick(src[at(a, b), :], idx)

    def remote(src, dst, recv, to):
        return pltpu.make_async_remote_copy(
            src_ref=src,
            dst_ref=dst,
            send_sem=x_send,
            recv_sem=recv,
            device_id=(to,),
            device_id_type=MESH,
        )

    def swap(src, dst, f, first, rows, k, carried=None):
        src, dst = src.at[pl.ds(first, rows)], dst.at[pl.ds(first, rows)]
        copy = remote(src, dst, x_recv.at[k], sides[f])
        if carried is None:
            copy.start()
        else:
            by_bag = remote(src, bag.at[pl.ds(carried, rows)], bag_recv, carrier_of_early)
            pl.when(early)(by_bag.start)
            pl.when(jnp.logical_not(early))(copy.start)
        return copy

    def carry(dst, carried, first, rows, k):
        src, dst = bag.at[pl.ds(carried, rows)], dst.at[pl.ds(first, rows)]
        remote(src, dst, x_recv.at[k], late_of_carrier).start()

    def landed(ref, sem):
        pltpu.make_async_copy(ref, ref, sem).wait()

    both = (0, LAST)
    faces = (0, 1)
    scope("load_ends")
    pltpu.make_async_copy(coef, coef, in_sems.at[1]).wait()
    for a in both:
        for b in range(N):
            mine[part(face_of[a], LOAD, b), :] = lane_pick(ld[at(a, b), :], inverse)
    for k, a in enumerate(both):
        s = contract(SQUARED.T, [g2[across(a, c), :] for c in range(N)], 1)
        for c in range(N):
            tmpf[across(k, c), :] = s[c]
    for b in range(N):
        s = contract(SQUARED.T, [g0[at(a, b), :] for a in range(N)], 1, both)
        for k, a in enumerate(both):
            yf[at(k, b), :] = s[a]
    for k, a in enumerate(both):
        s = contract(SQUARED.T, [g1[at(a, b), :] for b in range(N)], 1)
        for b in range(N):
            mine[part(face_of[a], DIAG, b), :] = lane_pick(
                s[b] + yf[at(k, b), :] + ms[at(a, b), :] + tmpf[at(k, b), :], inverse
            )
    for a in both:
        for i in range(N):
            mine[part(face_of[a], G1, i), :] = lane_pick(g1[at(a, i), :], inverse)
            mine[part(face_of[a], G2, i), :] = lane_pick(g2[across(a, i), :], inverse)
    scope("barrier")
    pl.semaphore_wait(barrier, expected)
    scope("send1")

    sent_ld = swap(mine, theirs, 1, 4 * FACE, 2 * FACE, FAR_LD, 0)
    sent_g = swap(mine, theirs, 1, 6 * FACE, 2 * FACE, FAR_G, 2 * FACE)
    sent_near = swap(mine, theirs, 0, 0, 4 * FACE, NEAR)

    @pl.when(carrier)
    def _():
        landed(bag, bag_recv)
        carry(theirs, 0, 4 * FACE, 2 * FACE, FAR_LD)
        carry(theirs, 2 * FACE, 6 * FACE, 2 * FACE, FAR_G)
        carry(w_theirs, 4 * FACE, FACE, FACE, FAR_W)

    greet(hello.at[0], y_near)

    @pl.when(core == 1)
    def _():
        def lower(z_to, _):
            greet(hello.at[2], [me + (z_to - z_at) * line])
            return 0

        lax.fori_loop(0, z_at, lower, 0)

    scope("diag")
    inner_diagonal(g0, g1, g2, ms, dg, tmp)
    scope("reorder")
    for a in INSIDE:
        for b in range(N):
            rows = at(a, b)
            dg[rows, :] = lane_pick(dg[rows, :], inverse)
            moved_load = lane_pick(ld[rows, :], inverse)
            ld[rows, :] = moved_load
            r[rows, :] = moved_load
    reorder(g0, g0, inverse)
    scope("sums")
    sum_yz([(v, a) for a in INSIDE for v in (dg, r)], lanes)

    def inner_z(a, _):
        for b in range(N):
            inv = 1.0 / dg[at(a, b), :]
            dg[at(a, b), :] = inv
            z[at(a, b), :] = inv * r[at(a, b), :]
        return 0

    lax.fori_loop(1, LAST, inner_z, 0, unroll=3)
    for b in range(N):
        g = [float(DERIV[m, 0] * DERIV[m, LAST]) * g0[at(m, b), :] for m in range(N)]
        cross[at(0, b), :] = added_up(g)
    scope("La1")
    stiffness_a(z, g0, y)

    def full(f, b):
        return tile(row_of[f] + b * N)

    def face_z(f):
        for b in range(N):
            rf[at(f, b), :] = mine[part(f, LOAD, b), :] + theirs[part(f, LOAD, b), :]
            total = mine[part(f, DIAG, b), :] + theirs[part(f, DIAG, b), :]
            a_sum[at(f, b), :] = total
            df[at(f, b), :] = total
        sum_yz([(rf, f), (df, f)], lanes)
        for b in range(N):
            inv = 1.0 / df[at(f, b), :]
            df[at(f, b), :] = inv
            zf[at(f, b), :] = inv * rf[at(f, b), :]

    def tell(f, k, carried=None):
        for b in range(N):
            w_mine[at(f, b), :] = y[full(f, b), :] + cross[at(0, b), :] * zf[at(1 - f, b), :]
        sum_yz([(w_mine, f)], lanes)
        return swap(w_mine, w_theirs, f, f * FACE, FACE, k, carried)

    scope("x_near")
    sent_near.wait_recv()
    scope("z_near")
    face_z(0)
    sent_w = [None, tell(1, FAR_W, 4 * FACE)]
    scope("reorder2")
    reorder(g1, g1, inverse, INSIDE)
    for a in INSIDE:
        for c in range(N):
            g2t[at(a, c), :] = lane_pick(g2[across(a, c), :], inverse)
    reorder(ms, ms, inverse, INSIDE)
    scope("Lbc1")
    stiffness_bc(z, g1, g2t, ms, y, tmp, y)
    scope("hello")

    heard(hello.at[0], y_near)
    greet(hello.at[1], y_far)
    scope("g_near")
    first = pl.multiple_of((1 - core) * FACE, FACE)
    couplings(g0, first, coupling)
    loop(1, LAST, lambda a: couple(zf, 0, coupling, y, a))
    face_sums(0, mine, theirs, a_sum, a_sum, tmpf)
    s = face_terms(zf, 0, mine, theirs, a_sum, tmpf)
    for b in range(N):
        yf[at(0, b), :] = s[b]
    sum_yz([(yf, 0)], lanes)
    scope("x_far")
    sent_ld.wait_recv()
    scope("z_far")
    face_z(1)

    scope("inner2")
    for a in INSIDE:
        couple(zf, 1, coupling, y, a)
    sum_yz([(y, a) for a in INSIDE], lanes)
    zero = jnp.zeros((8, LANES), jnp.float32)

    def inner_p(a, num):
        for b in range(N):
            rows = at(a, b)
            p = COEF_Z * z[rows, :] - COEF_Q * (dg[rows, :] * y[rows, :])
            z[rows, :] = p
            num[b % 4] = num[b % 4] + ld[rows, :] * p
        return num

    num = lax.fori_loop(1, LAST, inner_p, [zero] * 4, unroll=True)
    scope("L2")
    den = energy_bc(z, g1, g2t, ms, [zero] * 4)
    den = energy_a(z, g0, u_ends, first, den)
    num, den = added_up(num), added_up(den)
    scope("g_far")
    sent_g.wait_recv()
    face_sums(1, mine, theirs, a_sum, a_sum, tmpf)
    s = face_terms(zf, 1, mine, theirs, a_sum, tmpf)
    for b in range(N):
        yf[at(1, b), :] = s[b]
    sum_yz([(yf, 1)], lanes)
    sent_w[0] = tell(0, NEAR_W)

    def face_p(f):
        for b in range(N):
            rows = at(f, b)
            total = yf[rows, :] + (w_mine[rows, :] + w_theirs[rows, :])
            pf[rows, :] = COEF_Z * zf[rows, :] - COEF_Q * (df[rows, :] * total)

    def face_dot(kind, f):
        return added_up([kind[part(f, LOAD, b), :] * pf[at(f, b), :] for b in range(N)])

    acc[tile(0), :] = num
    acc[tile(8), :] = den
    takes = jnp.where(2 * x >= xs, core, 1 - core) == 1
    gives = jnp.logical_not(takes)
    sent_q = remote(q_mine, q_theirs, x_recv.at[NEAR_W], near_to)
    scope("w_near")

    @pl.when(takes)
    def _():
        landed(w_mine, x_recv.at[NEAR_W])
        face_p(0)
        acc[tile(0), :] = acc[tile(0), :] + (face_dot(mine, 0) + face_dot(theirs, 0))
        terms = [
            (2.0 * u_ends[at(0, b), :] + q_theirs[at(0, b), :]) * pf[at(0, b), :] for b in range(N)
        ]
        acc[tile(8), :] = acc[tile(8), :] + (face_energy(pf, 0, theirs, a_sum) + added_up(terms))
        for b in range(N):
            q_mine[at(0, b), :] = 2.0 * cross[at(0, b), :] * pf[at(0, b), :]

    scope("w_far")
    sent_w[1].wait_recv()
    scope("ends2")
    face_p(1)
    acc[tile(0), :] = acc[tile(0), :] + face_dot(mine, 1)
    terms = [2.0 * u_ends[at(1, b), :] * pf[at(1, b), :] for b in range(N)]
    acc[tile(8), :] = acc[tile(8), :] + (0.5 * face_energy(pf, 1, theirs, a_sum) + added_up(terms))

    @pl.when(takes)
    def _():
        terms = [q_mine[at(0, b), :] * pf[at(1, b), :] for b in range(N)]
        acc[tile(8), :] = acc[tile(8), :] + added_up(terms)

    @pl.when(gives)
    def _():
        for b in range(N):
            q_mine[at(0, b), :] = 2.0 * (
                u_ends[at(0, b), :] + cross[at(0, b), :] * pf[at(1, b), :]
            )
        sent_q.start()

    num_row = jnp.sum(acc[tile(0), :], axis=0, keepdims=True)
    den_row = jnp.sum(acc[tile(8), :], axis=0, keepdims=True)
    dots[0, 0:1, :] = num_row
    dots[0, 1:2, :] = den_row
    hops = sorted(
        ((dy, dx) for dy in range(ys) for dx in range(xs) if dy or dx),
        key=lambda d: -min(d[0], ys - d[0]) - min(d[1], xs - d[1]),
    )
    others = 2 * len(hops) + 1

    def send(src, dst, k, to):
        copy = pltpu.make_async_remote_copy(
            src_ref=src,
            dst_ref=dst,
            send_sem=x_send,
            recv_sem=s_recv.at[k],
            device_id=(to,),
            device_id_type=MESH,
        )
        copy.start()

    def arrived(ref, sem):
        pltpu.make_async_copy(ref, ref, sem).wait()

    def added(ref, first, total):
        part = [first, None, None, None]
        for j in range(total):
            part[j % 4] = plus(part[j % 4], ref[j])
        return functools.reduce(plus, [t for t in part if t is not None])

    heard(hello.at[1], y_far)
    last_from, last_to = zs // 2, zs // 2 + max(zs // 4, 1)
    is_last = (z_at >= last_from) & (z_at < last_to)
    rank = jnp.where(
        is_last, z_at + zs - last_to, jnp.where(z_at < last_from, z_at, z_at - (last_to - last_from))
    )
    by_z = rank * ys * line + y_at * line + lax.rem(me, line)

    @pl.when(others_than_root)
    def _():
        pltpu.make_async_remote_copy(
            src_ref=dots.at[0],
            dst_ref=got_one.at[jnp.maximum(by_z - 1, 0)],
            send_sem=x_send,
            recv_sem=one_recv.at[jnp.where(is_last, 1, 0)],
            device_id=(ROOT,),
            device_id_type=MESH,
        ).start()

    for j, (dy, dx) in enumerate(hops):
        send(dots.at[0], got_a.at[2 * j + core], 0, moved(dy=dy, dx=dx) + 1 - core)

    @pl.when(core == 0)
    def _():
        send(dots.at[0], got_a.at[others - 1], 0, me + 1)

    scope("u_ends")

    @pl.when(gives)
    def _():
        sent_w[0].wait_recv()
        face_p(0)

    for f in faces:
        for b in range(N):
            i_mine[at(f, b), :] = u_ends[at(f, b), :] + cross[at(0, b), :] * pf[at(1 - f, b), :]
        swap(i_mine, i_theirs, f, f * FACE, FACE, IMAGE)
    for f in faces:
        s = face_terms(pf, f, mine, theirs, a_sum, tmpf)
        for b in range(N):
            yf[at(f, b), :] = s[b]
    stiffness_bc(z, g1, g2t, ms, y, tmp)
    stiffness_a(z, g0, u, INSIDE, y)

    def couple_both(a):
        couple(pf, 0, coupling, u, a)
        couple(pf, 1, coupling, u, a)

    loop(1, LAST, couple_both)
    scope("out_p_r")
    for src, ends, dst in ((z, pf, p_o), (r, rf, r_o)):
        reorder(src, dst, order, INSIDE)
        for f in faces:
            for b in range(N):
                dst[full(f, b), :] = lane_pick(ends[at(f, b), :], order)
    sum_yz([(u, a) for a in INSIDE], lanes)
    reorder(u, im_o, order, INSIDE)
    scope("plane")

    @pl.when(core == 1)
    def _():
        arrived(got_a.at[pl.ds(0, others)], s_recv.at[0])
        dots[1] = added(got_a, dots[0], others)

        @pl.when(z_at < zs - 1)
        def _():
            pl.semaphore_wait(hello.at[2], zs - 1 - z_at)

        for k in sorted(range(1, zs), key=lambda k: -min(k, zs - k)):
            send(dots.at[1], got_b.at[k - 1], 1, moved(dz=k) - 1)

            @pl.when(moved(dz=k) != ROOT)
            def _(k=k):
                send(dots.at[1], got_b.at[k - 1], 1, moved(dz=k))

        send(dots.at[1], got_b.at[zs - 1], 1, me - 1)
        got_b[zs - 1] = dots[1]

    scope("x3")
    landed(i_theirs, x_recv.at[IMAGE])
    for f in faces:
        for b in range(N):
            rows = at(f, b)
            yf[rows, :] = yf[rows, :] + (i_mine[rows, :] + i_theirs[rows, :])
    sum_yz([(yf, f) for f in faces], lanes)
    for f in faces:
        for b in range(N):
            im_o[full(f, b), :] = lane_pick(yf[at(f, b), :], order)
    scope("lines")

    @pl.when(core == 0)
    def _():
        arrived(got_b, s_recv.at[1])

    @pl.when((core == 1) & others_than_root)
    def _():
        arrived(got_b.at[pl.ds(0, zs - 1)], s_recv.at[1])

    @pl.when(others_than_root)
    def _():
        dots[2] = added(got_b, None, zs)

    @pl.when(is_root)
    def _():
        width = 16
        last_ones = (last_to - last_from) * ys * line
        early_ones = count - 1 - last_ones

        def sum_of(start, number, sums):
            def some(k, sums):
                for i in range(width):
                    sums[i % 8] = sums[i % 8] + got_one[start + k * width + i]
                return sums

            whole = number // width
            sums = lax.fori_loop(0, whole, some, sums)
            for k in range(whole * width, number):
                sums[k % 8] = sums[k % 8] + got_one[start + k]
            return sums

        arrived(got_one.at[pl.ds(0, early_ones)], one_recv.at[0])
        sums = sum_of(0, early_ones, [jnp.zeros((2, LANES), jnp.float32)] * 8)
        sums[0] = sums[0] + dots[0]
        arrived(got_one.at[pl.ds(early_ones, last_ones)], one_recv.at[1])
        sums = sum_of(early_ones, last_ones, sums)
        dots[2] = added_up(sums)

    total = dots[2]
    scope("alpha")
    sums = jnp.sum(total, axis=1, keepdims=True)
    al_o[...] = jnp.broadcast_to(sums[0:1, :] / sums[1:2, :], (8, LANES))
    face_rows = FACE // 2
    above_root = (core == 1) & (in_plane // line * line + ROOT == me) & others_than_root
    sums_0, sums_1 = len(hops) + 2, len(hops) + 2 * zs
    for sums_sent, many in (
        (core == 0, sums_0),
        ((core == 1) & jnp.logical_not(above_root | is_root), sums_1),
        (above_root | is_root, sums_1 - 1),
    ):
        for faces_sent, faces in (
            (takes & jnp.logical_not(carrier), 12),
            (takes & carrier, 17),
            (gives & jnp.logical_not(carrier), 13),
            (gives & carrier, 18),
        ):

            @pl.when(sums_sent & faces_sent)
            def _(sent=many + faces * face_rows):
                arrived(all_sent.at[pl.ds(0, sent)], x_send)

    scope(None)


CHUNKS = 4


def finish_kernel(p, r, im, al, x_h, r_h, both, sem):
    alpha = al[...]
    size = ROWS // CHUNKS
    for k in range(CHUNKS):
        for i in range(k * size, (k + 1) * size, N):
            both[tile(i), :] = alpha * p[tile(i), :]
        pltpu.make_async_copy(both.at[pl.ds(k * size, size)], x_h.at[pl.ds(k * size, size)], sem).start()
        for i in range(k * size, (k + 1) * size, N):
            both[tile(ROWS + i), :] = r[tile(i), :] - alpha * im[tile(i), :]
        rows = pl.ds(ROWS + k * size, size)
        pltpu.make_async_copy(both.at[rows], r_h.at[pl.ds(k * size, size)], sem).start()
    pltpu.make_async_copy(both, both, sem).wait()


def on_device(load_terms, geometry, mass_terms, element_order):
    flat = jax.ShapeDtypeStruct((ROWS, LANES), jnp.float32)
    vm = lambda *shape: pltpu.VMEM(shape, jnp.float32)
    field = vm(ROWS, LANES)
    pair = vm(2 * FACE, LANES)
    ys, zs, xs, cores = TORUS
    in_vmem = pl.BlockSpec(memory_space=pltpu.VMEM)
    in_hbm = pl.BlockSpec(memory_space=pltpu.HBM)
    parts = pl.pallas_call(
        step_kernel,
        out_shape=(field, field, field, vm(8, LANES)),
        in_specs=[in_hbm] * 4,
        out_specs=[in_vmem] * 4,
        scratch_shapes=[
            vm(5 * ROWS, LANES), *[field] * 7,
            *[vm(8 * FACE, LANES)] * 2,
            *[pair] * 4, vm(5 * FACE, LANES), *[pair] * 8, *[vm(FACE, LANES)] * 3,
            vm(12 * FACE, LANES), vm(16, LANES),
            vm(3, 2, LANES), vm(2 * ys * xs - 1, 2, LANES), vm(zs, 2, LANES),
            vm(ys * zs * xs * cores - 1, 2, LANES),
            vm(18 * FACE // 2 + ys * xs + 2 * zs, 2, LANES),
            pltpu.VMEM((1, LANES), jnp.int32),
            pltpu.SemaphoreType.DMA((2,)),
            pltpu.SemaphoreType.DMA(()),
            pltpu.SemaphoreType.DMA((6,)),
            pltpu.SemaphoreType.DMA(()),
            pltpu.SemaphoreType.DMA((2,)),
            pltpu.SemaphoreType.DMA((2,)),
            pltpu.SemaphoreType.REGULAR((3,)),
        ],
        compiler_params=pltpu.CompilerParams(
            collective_id=0, has_side_effects=True, vmem_limit_bytes=24 << 20
        ),
        name="cg_step",
    )(
        *[
            pltpu.with_memory_space_constraint(t, pltpu.HBM)
            for t in (
                load_terms.reshape(ROWS, LANES),
                geometry.reshape(3 * ROWS, LANES),
                mass_terms.reshape(ROWS, LANES),
                element_order,
            )
        ]
    )
    x, res = pl.pallas_call(
        finish_kernel,
        out_shape=(flat, flat),
        in_specs=[in_vmem] * 4,
        out_specs=[in_hbm] * 2,
        scratch_shapes=[vm(2 * ROWS, LANES), pltpu.SemaphoreType.DMA(())],
        compiler_params=pltpu.CompilerParams(vmem_limit_bytes=8 << 20),
        name="cg_finish",
    )(*[pltpu.with_memory_space_constraint(t, pltpu.VMEM) for t in parts])
    shape = load_terms.shape
    return x.reshape(shape), res.reshape(shape)


def solution(mesh):
    last = P(None, None, None, "slab")
    return jax.shard_map(
        on_device,
        mesh=mesh,
        in_specs=(last, P(None, None, None, None, "slab"), last, P("slab", None)),
        out_specs=(last, last),
        check_vma=False,
    )
```

```python
import functools

import jax
import jax.numpy as jnp
import numpy as np
from jax import lax
from jax.experimental import pallas as pl
from jax.experimental.pallas import tpu as pltpu
from jax.sharding import PartitionSpec as P

N = 8
LAST = N - 1
EL_Y = 8
EL_Z = 16
LANES = 128
ROWS = N * N * N
FACE = N * N
CENTRE = 1.65
HALF = 1.35
MESH = pl.DeviceIdType.MESH
TORUS = (8, 12, 4, 2)
ROOTS = (1, 3, 97, 2, 96)
INSIDE = range(1, LAST)
UNROLL_A = 4
UNROLL_BC = 3


def legendre_table(positions, points):
    columns = [positions * 0.0 + 1.0, positions]
    for degree in range(2, points):
        columns.append(
            ((2 * degree - 1) * positions * columns[-1] - (degree - 1) * columns[-2]) / degree
        )
    return np.stack(columns, axis=1)


def gll_derivative(points):
    degree = points - 1
    nodes = -np.cos(np.pi * np.arange(points) / degree)
    for _ in range(100):
        legendre = legendre_table(nodes, points)
        nodes = nodes - (nodes * legendre[:, degree] - legendre[:, degree - 1]) / (
            points * legendre[:, degree]
        )
    legendre = legendre_table(nodes, points)
    top = legendre[:, degree]
    same = np.eye(points, dtype=bool)
    spacing = np.where(same, 1.0, nodes[:, None] - nodes[None, :])
    table = np.where(same, 0.0, top[:, None] / (top[None, :] * spacing))
    table[0, 0] = -degree * points / 4.0
    table[degree, degree] = degree * points / 4.0
    return table


DERIV = gll_derivative(N).astype(np.float32).astype(np.float64)
SQUARED = DERIV * DERIV
SIGMA = CENTRE / HALF
RHO0 = 1.0 / SIGMA
RHO1 = 1.0 / (2.0 * SIGMA - RHO0)
COEF_Z = (1.0 + RHO1 * RHO0) / CENTRE + 2.0 * RHO1 / HALF
COEF_Q = 2.0 * RHO1 / HALF / CENTRE


def plus(x, y):
    return y if x is None else x + y


def contract(table, terms, sign, rows=range(N)):
    used = [j for j in range(N // 2) if terms[j] is not None]
    even = {j: terms[j] + terms[LAST - j] for j in used}
    odd = {j: terms[j] - terms[LAST - j] for j in used}
    out = [None] * N
    for i in range(N // 2):
        if i not in rows and LAST - i not in rows:
            continue
        e = o = None
        for j in used:
            e = plus(e, float(table[i, j] + table[i, LAST - j]) / 2 * even[j])
            o = plus(o, float(table[i, j] - table[i, LAST - j]) / 2 * odd[j])
        if i in rows:
            out[i] = e + o
        if LAST - i in rows:
            out[LAST - i] = (o - e) if sign < 0 else (e - o)
    return out


def tile(row):
    return pl.ds(row if isinstance(row, int) else pl.multiple_of(row, 8), 8)


def at(a, b):
    return tile((a * N + b) * N)


def across(a, c):
    return pl.ds(a * FACE + c, N, stride=N)


LOAD, DIAG, G1, G2 = range(4)
NEAR, FAR_LD, FAR_G, NEAR_W, FAR_W, IMAGE = range(6)


def part(f, kind, i):
    return tile(((f * 4 + kind) * N + i) * N)


def loop(start, stop, body):
    lax.fori_loop(start, stop, lambda i, _: (body(i), 0)[1], 0)


def stiffness_a(v, g0, out, rows=range(N), more=None):
    def along_a(b, _):
        va = [v[at(a, b), :] if a in INSIDE else None for a in range(N)]
        s = contract(DERIV, va, -1)
        s = contract(DERIV.T, [s[a] * g0[at(a, b), :] for a in range(N)], -1, rows)
        for a in rows:
            out[at(a, b), :] = s[a] if more is None else s[a] + more[at(a, b), :]
        return 0

    lax.fori_loop(0, N, along_a, 0, unroll=UNROLL_A)


def energy_a(v, g0, ends, first, total):
    def along_a(b, total):
        t = contract(DERIV, [v[at(a, b), :] if a in INSIDE else None for a in range(N)], -1)
        s = [t[a] * g0[at(a, b), :] for a in range(N)]
        total = [total[k] + s[k] * t[k] + s[k + 4] * t[k + 4] for k in range(4)]
        s = contract(DERIV.T, s, -1, (0, LAST))
        ends[tile(first + b * N), :] = s[0]
        ends[tile(FACE - first + b * N), :] = s[LAST]
        return total

    return lax.fori_loop(0, N, along_a, total, unroll=UNROLL_A)


def energy_bc(v, g1, g2t, ms, total):
    def along_bc(a, total):
        vb = [v[at(a, b), :] for b in range(N)]
        for own, g in (([v[across(a, c), :] for c in range(N)], g2t), (vb, g1)):
            t = contract(DERIV, own, -1)
            e = [t[i] * g[at(a, i), :] * t[i] for i in range(N)]
            total = [total[k] + (e[k] + e[k + 4]) for k in range(4)]
        e = [vb[b] * ms[at(a, b), :] * vb[b] for b in range(N)]
        return [total[k] + (e[k] + e[k + 4]) for k in range(4)]

    return lax.fori_loop(1, LAST, along_bc, total, unroll=UNROLL_BC)


def stiffness_bc(v, g1, g2t, ms, out, tmp, more=None):
    def along_bc(a, _):
        vt = [v[across(a, c), :] for c in range(N)]
        vb = [v[at(a, b), :] for b in range(N)]
        t = contract(DERIV, vt, -1)
        t = contract(DERIV.T, [t[c] * g2t[at(a, c), :] for c in range(N)], -1)
        for c in range(N):
            tmp[across(a, c), :] = t[c]
        s = contract(DERIV, vb, -1)
        s = contract(DERIV.T, [s[b] * g1[at(a, b), :] for b in range(N)], -1)
        for b in range(N):
            s[b] = s[b] + ms[at(a, b), :] * vb[b]
            if more is not None:
                s[b] = s[b] + more[at(a, b), :]
        for b in range(N):
            out[at(a, b), :] = s[b] + tmp[at(a, b), :]
        return 0

    lax.fori_loop(1, LAST, along_bc, 0, unroll=UNROLL_BC)


def inner_diagonal(g0, g1, g2, ms, out, tmp):
    def along_a(b, _):
        s = contract(SQUARED.T, [g0[at(a, b), :] for a in range(N)], 1, INSIDE)
        for a in INSIDE:
            out[at(a, b), :] = s[a] + ms[at(a, b), :]
        return 0

    lax.fori_loop(0, N, along_a, 0, unroll=UNROLL_A)

    def along_bc(a, _):
        t = contract(SQUARED.T, [g2[across(a, c), :] for c in range(N)], 1)
        for c in range(N):
            tmp[across(a, c), :] = t[c]
        s = contract(SQUARED.T, [g1[at(a, b), :] for b in range(N)], 1)
        for b in range(N):
            s[b] = s[b] + out[at(a, b), :]
        for b in range(N):
            out[at(a, b), :] = s[b] + tmp[at(a, b), :]
        return 0

    lax.fori_loop(1, LAST, along_bc, 0, unroll=UNROLL_BC)


def face_terms(v, f, mine, theirs, a_sum, tmp):
    s = contract(DERIV, [v[across(f, c), :] for c in range(N)], -1)
    s = contract(DERIV.T, [s[c] * theirs[part(f, G2, c), :] for c in range(N)], -1)
    for c in range(N):
        tmp[across(f, c), :] = s[c]
    vb = [v[at(f, b), :] for b in range(N)]
    s = contract(DERIV, vb, -1)
    s = contract(DERIV.T, [s[b] * theirs[part(f, G1, b), :] for b in range(N)], -1)
    return [s[b] + a_sum[at(f, b), :] * vb[b] + tmp[at(f, b), :] for b in range(N)]


def face_energy(v, f, theirs, a_sum):
    vb = [v[at(f, b), :] for b in range(N)]
    e = [a_sum[at(f, b), :] * vb[b] * vb[b] for b in range(N)]
    for own, kind in (([v[across(f, c), :] for c in range(N)], G2), (vb, G1)):
        t = contract(DERIV, own, -1)
        e = [e[i] + t[i] * theirs[part(f, kind, i), :] * t[i] for i in range(N)]
    return added_up(e)


def added_up(terms):
    while len(terms) > 1:
        terms = [functools.reduce(plus, terms[i : i + 2]) for i in range(0, len(terms), 2)]
    return terms[0]


def face_sums(f, mine, theirs, diag, a_sum, tmp):
    g = [[mine[part(f, k, i), :] + theirs[part(f, k, i), :] for i in range(N)] for k in (G1, G2)]
    for k in (G1, G2):
        for i in range(N):
            theirs[part(f, k, i), :] = g[k - G1][i]
    s = contract(SQUARED.T, g[1], 1)
    for c in range(N):
        tmp[across(f, c), :] = s[c]
    s = contract(SQUARED.T, g[0], 1)
    for b in range(N):
        a_sum[at(f, b), :] = diag[at(f, b), :] - s[b] - tmp[at(f, b), :]


def couplings(g0, first, out):
    def one(b, _):
        g = [g0[at(a, b), :] for a in range(N)]
        for a_end, row in ((0, first), (LAST, FACE - first)):
            s = contract(DERIV.T, [float(DERIV[m, a_end]) * g[m] for m in range(N)], -1, INSIDE)
            for a in INSIDE:
                out[tile(row * 6 + ((a - 1) * N + b) * N), :] = s[a]
        return 0

    lax.fori_loop(0, N, one, 0, unroll=2)


def couple(v, f, coupling, out, a):
    for b in range(N):
        out[at(a, b), :] = (
            out[at(a, b), :] + coupling[tile(((f * 6 + a - 1) * N + b) * N), :] * v[at(f, b), :]
        )


def lane_pick(x, idx):
    return jnp.take_along_axis(x, idx, axis=1, mode="promise_in_bounds")


def sum_yz(planes, lanes):
    ends = [(v[at(a, 0), :], v[at(a, LAST), :]) for v, a in planes]
    rims = [(v[across(a, 0), :], v[across(a, LAST), :]) for v, a in planes]
    ups = [jnp.where(lanes["up"], pltpu.roll(low, LANES - EL_Z, 1), 0.0) for low, _ in ends]
    downs = [jnp.where(lanes["down"], pltpu.roll(high, EL_Z, 1), 0.0) for _, high in ends]
    nexts = [lane_pick(low, lanes["next"]) for low, _ in rims]
    prevs = [lane_pick(high, lanes["prev"]) for _, high in rims]

    def corners(rim, idx):
        turned = jnp.where(lanes["first"], pltpu.roll(rim, 1, 0), pltpu.roll(rim, LAST, 0))
        return jnp.where(lanes["corner"], lane_pick(turned, idx), 0.0)

    far_nexts = [corners(low, lanes["corner_next"]) for low, _ in rims]
    far_prevs = [corners(high, lanes["corner_prev"]) for _, high in rims]
    for k, (v, a) in enumerate(planes):
        v[across(a, LAST), :] = rims[k][1] + (nexts[k] + far_nexts[k])
        v[across(a, 0), :] = rims[k][0] + (prevs[k] + far_prevs[k])
        v[at(a, LAST), :] = v[at(a, LAST), :] + ups[k]
        v[at(a, 0), :] = v[at(a, 0), :] + downs[k]


def step_kernel(
    load_h, geom_h, mass_h, order_h, p_o, r_o, im_o, al_o,
    coef, g2t, r, dg, z, y, u, tmp,
    mine, theirs, w_mine, w_theirs, i_mine, i_theirs, bag, rf, df, zf, pf, yf, a_sum, tmpf,
    u_ends, cross, q_mine, q_theirs, coupling, acc,
    dots, got_a, got_b, got_one, all_sent, order_v, in_sems, x_send, x_recv, bag_recv, s_recv, one_recv, hello,
):
    stack = []

    def scope(name):
        if stack:
            stack.pop().__exit__(None, None, None)
        if name:
            stack.append(jax.named_scope(name))
            stack[-1].__enter__()

    scope("enter")
    ys, zs, xs, cores = TORUS
    line, plane_size, count = xs * cores, zs * xs * cores, ys * zs * xs * cores
    me = lax.axis_index("slab")
    core = lax.rem(me, cores)
    in_plane = lax.rem(me, plane_size)

    def greet(sem, who):
        for q in who:
            pl.semaphore_signal(sem, inc=1, device_id=(q,), device_id_type=MESH)

    def heard(sem, who):
        if who:
            pl.semaphore_wait(sem, len(who))

    near_to = me + 1 - 2 * core
    far_to = me + 2 * core - 1
    far_to = jnp.where(far_to < 0, count - 1, jnp.where(far_to == count, 0, far_to))
    early, carrier, late = in_plane == 0, in_plane == line - 1, in_plane == plane_size - 1
    barrier = pltpu.get_barrier_semaphore()
    greet(barrier, [jnp.where(late, me + line - plane_size, far_to)])
    loads = [
        pltpu.make_async_copy(src, dst, in_sems.at[k])
        for k, src, dst in (
            (0, order_h, order_v),
            (1, load_h, coef.at[pl.ds(4 * ROWS, ROWS)]),
            (1, geom_h, coef.at[pl.ds(0, 3 * ROWS)]),
            (1, mass_h, coef.at[pl.ds(3 * ROWS, ROWS)]),
        )
    ]
    for copy in loads:
        copy.start()
    g0, g1, g2, ms, ld = (coef.at[pl.ds(k * ROWS, ROWS)] for k in range(5))

    y_at = me // plane_size
    z_at = in_plane // line
    x = lax.rem(me, line) // cores

    def moved(dy=0, dz=0, dx=0):
        to = me
        if dy:
            to = to + (lax.rem(y_at + dy, ys) - y_at) * plane_size
        if dz:
            to = to + (lax.rem(z_at + dz, zs) - z_at) * line
        if dx:
            to = to + (lax.rem(x + dx, xs) - x) * cores
        return to

    def ring(size, stop, start=1):
        return sorted({j % size for k in range(start, stop) for j in (k, -k)} - {0})

    sides = (near_to, far_to)
    row_of = (pl.multiple_of((1 - core) * (ROWS - FACE), FACE), pl.multiple_of(core * (ROWS - FACE), FACE))
    face_of = {0: 1 - core, LAST: core}
    carrier_of_early = lax.rem(y_at + ys - 1, ys) * plane_size + line - 1
    early_of_carrier = lax.rem(y_at + 1, ys) * plane_size
    late_of_carrier = me + plane_size - line

    row = [moved(dx=k) + c for k in range(xs) for c in (0, 1 - 2 * core) if k or not isinstance(c, int)]
    y_near = [moved(dy=k) for k in ring(ys, 3)]
    y_far = [moved(dy=k) for k in ring(ys, ys // 2 + 1, 3)]
    greet(barrier, [near_to] + row + y_near)

    @pl.when(early | carrier)
    def _():
        greet(barrier, [jnp.where(early, carrier_of_early, early_of_carrier)])

    def higher(z_to, _):
        greet(barrier, [me + (z_to - z_at) * line + 1 - core])
        return 0

    lax.fori_loop(z_at + 1, zs, higher, 0)
    roots = [r for r in ROOTS if r < count]

    def one_of(device, some):
        return functools.reduce(jnp.logical_or, [device == r for r in some])

    is_root = one_of(me, roots)
    others_than_root = jnp.logical_not(is_root)

    @pl.when(is_root)
    def _():
        width = next(k for k in range(16, 0, -1) if (count - 1) % k == 0)

        def everyone(k, _):
            for i in range(width):
                q = me + 1 + k * width + i
                greet(barrier, [jnp.where(q >= count, q - count, q)])
            return 0

        lax.fori_loop(0, (count - 1) // width, everyone, 0)

    expected = (
        len(row)
        + len(y_near)
        + 2
        + 2 * carrier.astype(jnp.int32)
        + 2 * core * z_at
        + len(roots)
        - is_root.astype(jnp.int32)
    )

    scope("idx")
    loads[0].wait()
    order = jnp.broadcast_to(order_v[...], (8, LANES))
    hit = (
        jnp.broadcast_to(order_v[...], (LANES, LANES))
        == lax.broadcasted_iota(jnp.int32, (LANES, LANES), 0)
    ).astype(jnp.float32)
    lane = lax.broadcasted_iota(jnp.int32, (8, LANES), 1)
    inverse = lax.dot_general(
        lane.astype(jnp.float32), hit, (((1,), (1,)), ((), ())), preferred_element_type=jnp.float32
    )
    inverse = (inverse + 0.5).astype(jnp.int32)
    in_row = lane & (EL_Z - 1)
    lanes = {
        "up": lane < LANES - EL_Z,
        "down": lane >= EL_Z,
        "next": lane - in_row + ((in_row + 1) & (EL_Z - 1)),
        "prev": lane - in_row + ((in_row + EL_Z - 1) & (EL_Z - 1)),
    }
    b_at = lax.broadcasted_iota(jnp.int32, (8, LANES), 0)
    lanes["first"] = b_at == 0
    lanes["corner"] = (lanes["first"] & lanes["down"]) | ((b_at == LAST) & lanes["up"])
    by_y = jnp.where(lanes["first"], LANES - EL_Z, EL_Z)
    lanes["corner_next"] = (lanes["next"] + by_y) & (LANES - 1)
    lanes["corner_prev"] = (lanes["prev"] + by_y) & (LANES - 1)

    def reorder(src, dst, idx, planes=range(N)):
        for a in planes:
            for b in range(N):
                dst[at(a, b), :] = lane_pick(src[at(a, b), :], idx)

    def remote(src, dst, recv, to):
        return pltpu.make_async_remote_copy(
            src_ref=src,
            dst_ref=dst,
            send_sem=x_send,
            recv_sem=recv,
            device_id=(to,),
            device_id_type=MESH,
        )

    def swap(src, dst, f, first, rows, k, carried=None):
        src, dst = src.at[pl.ds(first, rows)], dst.at[pl.ds(first, rows)]
        copy = remote(src, dst, x_recv.at[k], sides[f])
        if carried is None:
            copy.start()
        else:
            by_bag = remote(src, bag.at[pl.ds(carried, rows)], bag_recv, carrier_of_early)
            pl.when(early)(by_bag.start)
            pl.when(jnp.logical_not(early))(copy.start)
        return copy

    def carry(dst, carried, first, rows, k):
        src, dst = bag.at[pl.ds(carried, rows)], dst.at[pl.ds(first, rows)]
        remote(src, dst, x_recv.at[k], late_of_carrier).start()

    def landed(ref, sem):
        pltpu.make_async_copy(ref, ref, sem).wait()

    both = (0, LAST)
    faces = (0, 1)
    scope("load_ends")
    pltpu.make_async_copy(coef, coef, in_sems.at[1]).wait()
    for a in both:
        for b in range(N):
            mine[part(face_of[a], LOAD, b), :] = lane_pick(ld[at(a, b), :], inverse)
    for k, a in enumerate(both):
        s = contract(SQUARED.T, [g2[across(a, c), :] for c in range(N)], 1)
        for c in range(N):
            tmpf[across(k, c), :] = s[c]
    for b in range(N):
        s = contract(SQUARED.T, [g0[at(a, b), :] for a in range(N)], 1, both)
        for k, a in enumerate(both):
            yf[at(k, b), :] = s[a]
    for k, a in enumerate(both):
        s = contract(SQUARED.T, [g1[at(a, b), :] for b in range(N)], 1)
        for b in range(N):
            mine[part(face_of[a], DIAG, b), :] = lane_pick(
                s[b] + yf[at(k, b), :] + ms[at(a, b), :] + tmpf[at(k, b), :], inverse
            )
    for a in both:
        for i in range(N):
            mine[part(face_of[a], G1, i), :] = lane_pick(g1[at(a, i), :], inverse)
            mine[part(face_of[a], G2, i), :] = lane_pick(g2[across(a, i), :], inverse)
    scope("barrier")
    pl.semaphore_wait(barrier, expected)
    scope("send1")

    sent_ld = swap(mine, theirs, 1, 4 * FACE, 2 * FACE, FAR_LD, 0)
    sent_g = swap(mine, theirs, 1, 6 * FACE, 2 * FACE, FAR_G, 2 * FACE)
    sent_near = swap(mine, theirs, 0, 0, 4 * FACE, NEAR)

    @pl.when(carrier)
    def _():
        landed(bag, bag_recv)
        carry(theirs, 0, 4 * FACE, 2 * FACE, FAR_LD)
        carry(theirs, 2 * FACE, 6 * FACE, 2 * FACE, FAR_G)
        carry(w_theirs, 4 * FACE, FACE, FACE, FAR_W)

    greet(hello.at[0], y_near)

    @pl.when(core == 1)
    def _():
        def lower(z_to, _):
            greet(hello.at[2], [me + (z_to - z_at) * line])
            return 0

        lax.fori_loop(0, z_at, lower, 0)

    scope("diag")
    inner_diagonal(g0, g1, g2, ms, dg, tmp)
    scope("reorder")
    for a in INSIDE:
        for b in range(N):
            rows = at(a, b)
            dg[rows, :] = lane_pick(dg[rows, :], inverse)
            moved_load = lane_pick(ld[rows, :], inverse)
            ld[rows, :] = moved_load
            r[rows, :] = moved_load
    reorder(g0, g0, inverse)
    scope("sums")
    sum_yz([(v, a) for a in INSIDE for v in (dg, r)], lanes)

    def inner_z(a, _):
        for b in range(N):
            inv = 1.0 / dg[at(a, b), :]
            dg[at(a, b), :] = inv
            z[at(a, b), :] = inv * r[at(a, b), :]
        return 0

    lax.fori_loop(1, LAST, inner_z, 0, unroll=3)
    for b in range(N):
        g = [float(DERIV[m, 0] * DERIV[m, LAST]) * g0[at(m, b), :] for m in range(N)]
        cross[at(0, b), :] = added_up(g)
    scope("La1")
    stiffness_a(z, g0, y)

    def full(f, b):
        return tile(row_of[f] + b * N)

    def face_z(f):
        for b in range(N):
            rf[at(f, b), :] = mine[part(f, LOAD, b), :] + theirs[part(f, LOAD, b), :]
            total = mine[part(f, DIAG, b), :] + theirs[part(f, DIAG, b), :]
            a_sum[at(f, b), :] = total
            df[at(f, b), :] = total
        sum_yz([(rf, f), (df, f)], lanes)
        for b in range(N):
            inv = 1.0 / df[at(f, b), :]
            df[at(f, b), :] = inv
            zf[at(f, b), :] = inv * rf[at(f, b), :]

    def tell(f, k, carried=None):
        for b in range(N):
            w_mine[at(f, b), :] = y[full(f, b), :] + cross[at(0, b), :] * zf[at(1 - f, b), :]
        sum_yz([(w_mine, f)], lanes)
        return swap(w_mine, w_theirs, f, f * FACE, FACE, k, carried)

    scope("x_near")
    sent_near.wait_recv()
    scope("z_near")
    face_z(0)
    sent_w = [None, tell(1, FAR_W, 4 * FACE)]
    scope("reorder2")
    reorder(g1, g1, inverse, INSIDE)
    for a in INSIDE:
        for c in range(N):
            g2t[at(a, c), :] = lane_pick(g2[across(a, c), :], inverse)
    reorder(ms, ms, inverse, INSIDE)
    scope("Lbc1")
    stiffness_bc(z, g1, g2t, ms, y, tmp, y)
    scope("hello")

    heard(hello.at[0], y_near)
    greet(hello.at[1], y_far)
    scope("g_near")
    first = pl.multiple_of((1 - core) * FACE, FACE)
    couplings(g0, first, coupling)
    loop(1, LAST, lambda a: couple(zf, 0, coupling, y, a))
    face_sums(0, mine, theirs, a_sum, a_sum, tmpf)
    s = face_terms(zf, 0, mine, theirs, a_sum, tmpf)
    for b in range(N):
        yf[at(0, b), :] = s[b]
    sum_yz([(yf, 0)], lanes)
    scope("x_far")
    sent_ld.wait_recv()
    scope("z_far")
    face_z(1)

    scope("inner2")
    for a in INSIDE:
        couple(zf, 1, coupling, y, a)
    sum_yz([(y, a) for a in INSIDE], lanes)
    zero = jnp.zeros((8, LANES), jnp.float32)

    def inner_p(a, num):
        for b in range(N):
            rows = at(a, b)
            p = COEF_Z * z[rows, :] - COEF_Q * (dg[rows, :] * y[rows, :])
            z[rows, :] = p
            num[b % 4] = num[b % 4] + ld[rows, :] * p
        return num

    num = lax.fori_loop(1, LAST, inner_p, [zero] * 4, unroll=True)
    scope("L2")
    den = energy_bc(z, g1, g2t, ms, [zero] * 4)
    den = energy_a(z, g0, u_ends, first, den)
    num, den = added_up(num), added_up(den)
    scope("g_far")
    sent_g.wait_recv()
    face_sums(1, mine, theirs, a_sum, a_sum, tmpf)
    s = face_terms(zf, 1, mine, theirs, a_sum, tmpf)
    for b in range(N):
        yf[at(1, b), :] = s[b]
    sum_yz([(yf, 1)], lanes)
    sent_w[0] = tell(0, NEAR_W)

    def face_p(f):
        for b in range(N):
            rows = at(f, b)
            total = yf[rows, :] + (w_mine[rows, :] + w_theirs[rows, :])
            pf[rows, :] = COEF_Z * zf[rows, :] - COEF_Q * (df[rows, :] * total)

    def face_dot(kind, f):
        return added_up([kind[part(f, LOAD, b), :] * pf[at(f, b), :] for b in range(N)])

    acc[tile(0), :] = num
    acc[tile(8), :] = den
    takes = jnp.where(2 * x >= xs, core, 1 - core) == 1
    gives = jnp.logical_not(takes)
    sent_q = remote(q_mine, q_theirs, x_recv.at[NEAR_W], near_to)
    scope("w_near")

    @pl.when(takes)
    def _():
        landed(w_mine, x_recv.at[NEAR_W])
        face_p(0)
        acc[tile(0), :] = acc[tile(0), :] + (face_dot(mine, 0) + face_dot(theirs, 0))
        terms = [
            (2.0 * u_ends[at(0, b), :] + q_theirs[at(0, b), :]) * pf[at(0, b), :] for b in range(N)
        ]
        acc[tile(8), :] = acc[tile(8), :] + (face_energy(pf, 0, theirs, a_sum) + added_up(terms))
        for b in range(N):
            q_mine[at(0, b), :] = 2.0 * cross[at(0, b), :] * pf[at(0, b), :]

    scope("w_far")
    sent_w[1].wait_recv()
    scope("ends2")
    face_p(1)
    acc[tile(0), :] = acc[tile(0), :] + face_dot(mine, 1)
    terms = [2.0 * u_ends[at(1, b), :] * pf[at(1, b), :] for b in range(N)]
    acc[tile(8), :] = acc[tile(8), :] + (0.5 * face_energy(pf, 1, theirs, a_sum) + added_up(terms))

    @pl.when(takes)
    def _():
        terms = [q_mine[at(0, b), :] * pf[at(1, b), :] for b in range(N)]
        acc[tile(8), :] = acc[tile(8), :] + added_up(terms)

    @pl.when(gives)
    def _():
        for b in range(N):
            q_mine[at(0, b), :] = 2.0 * (
                u_ends[at(0, b), :] + cross[at(0, b), :] * pf[at(1, b), :]
            )
        sent_q.start()

    num_row = jnp.sum(acc[tile(0), :], axis=0, keepdims=True)
    den_row = jnp.sum(acc[tile(8), :], axis=0, keepdims=True)
    dots[0, 0:1, :] = num_row
    dots[0, 1:2, :] = den_row
    hops = sorted(
        ((dy, dx) for dy in range(ys) for dx in range(xs) if dy or dx),
        key=lambda d: -min(d[0], ys - d[0]) - min(d[1], xs - d[1]),
    )
    others = 2 * len(hops) + 1

    def send(src, dst, k, to):
        copy = pltpu.make_async_remote_copy(
            src_ref=src,
            dst_ref=dst,
            send_sem=x_send,
            recv_sem=s_recv.at[k],
            device_id=(to,),
            device_id_type=MESH,
        )
        copy.start()

    def arrived(ref, sem):
        pltpu.make_async_copy(ref, ref, sem).wait()

    def added(ref, first, total):
        part = [first, None, None, None]
        for j in range(total):
            part[j % 4] = plus(part[j % 4], ref[j])
        return functools.reduce(plus, [t for t in part if t is not None])

    half_z, pair_z = zs // 2, zs // 2 + zs // 8
    in_line = y_at * line + lax.rem(me, line)
    slow_low = (z_at == pair_z) & (x == xs - 1) & (core == 1)
    slow_high = (z_at == pair_z + 1) & (x == 0) & (core == 0)
    slow_ones = ys * (2 if pair_z + 1 < zs else 1)
    slow_before = jnp.where(
        z_at > pair_z + 1,
        slow_ones,
        jnp.where(
            z_at == pair_z + 1,
            ys + y_at + (lax.rem(me, line) > 0).astype(jnp.int32),
            jnp.where(z_at == pair_z, y_at, 0),
        ),
    )
    slot = jnp.where(
        slow_low | slow_high,
        count - slow_ones + jnp.where(slow_high, ys, 0) + y_at,
        z_at * ys * line + in_line - slow_before,
    )
    group = jnp.where(slow_low | slow_high, 2, jnp.where(z_at < half_z, 0, 1))
    group_0 = half_z * ys * line - 1
    groups = (group_0, count - 1 - group_0 - slow_ones, slow_ones)

    def root_sum(k, total):
        width, start, number = 16, sum(groups[:k]), groups[k]
        arrived(got_one.at[pl.ds(start, number)], one_recv.at[k])
        sums = [total] + [jnp.zeros((2, LANES), jnp.float32)] * 7

        def some(i, sums):
            return [
                sums[j] + got_one[start + i * width + j] + got_one[start + i * width + j + 8]
                for j in range(8)
            ]

        whole = number // width
        sums = lax.fori_loop(0, whole, some, sums)
        for i in range(whole * width, number):
            sums[i % 8] = sums[i % 8] + got_one[start + i]
        return added_up(sums)

    def send_to_root(r):
        at_root = r // plane_size * line + r % line

        @pl.when(me != r)
        def _():
            pltpu.make_async_remote_copy(
                src_ref=dots.at[0],
                dst_ref=got_one.at[slot - (slot > at_root).astype(jnp.int32)],
                send_sem=x_send,
                recv_sem=one_recv.at[group],
                device_id=(r,),
                device_id_type=MESH,
            ).start()

    send_to_root(roots[0])
    heard(hello.at[1], y_far)
    for j, (dy, dx) in enumerate(hops):
        send(dots.at[0], got_a.at[2 * j + core], 0, moved(dy=dy, dx=dx) + 1 - core)

    @pl.when(core == 0)
    def _():
        send(dots.at[0], got_a.at[others - 1], 0, me + 1)

    for other_root in roots[1:]:
        send_to_root(other_root)

    scope("u_ends")

    @pl.when(gives)
    def _():
        sent_w[0].wait_recv()
        face_p(0)

    for f in faces:
        for b in range(N):
            i_mine[at(f, b), :] = u_ends[at(f, b), :] + cross[at(0, b), :] * pf[at(1 - f, b), :]
        swap(i_mine, i_theirs, f, f * FACE, FACE, IMAGE)
    for f in faces:
        s = face_terms(pf, f, mine, theirs, a_sum, tmpf)
        for b in range(N):
            yf[at(f, b), :] = s[b]
    stiffness_bc(z, g1, g2t, ms, y, tmp)
    stiffness_a(z, g0, u, INSIDE, y)

    def couple_both(a):
        couple(pf, 0, coupling, u, a)
        couple(pf, 1, coupling, u, a)

    loop(1, LAST, couple_both)
    scope("out_p_r")
    for src, ends, dst in ((z, pf, p_o), (r, rf, r_o)):
        reorder(src, dst, order, INSIDE)
        for f in faces:
            for b in range(N):
                dst[full(f, b), :] = lane_pick(ends[at(f, b), :], order)
    sum_yz([(u, a) for a in INSIDE], lanes)
    reorder(u, im_o, order, INSIDE)
    scope("root_0")

    @pl.when(is_root)
    def _():
        dots[2] = root_sum(0, dots[0])

    scope("plane")
    first_of_column = me - z_at * line
    skip_0 = one_of(first_of_column - 1, [r for r in roots if r % cores == 0] or [-1])
    skip_1 = one_of(first_of_column, [r for r in roots if r % cores == 1])

    @pl.when(core == 1)
    def _():
        arrived(got_a.at[pl.ds(0, others)], s_recv.at[0])
        dots[1] = added(got_a, dots[0], others)

        @pl.when(z_at < zs - 1)
        def _():
            pl.semaphore_wait(hello.at[2], zs - 1 - z_at)

        for k in sorted(range(1, zs), key=lambda k: -min(k, zs - k)):
            to_first = z_at == zs - k
            for c, skip in ((1, skip_0), (0, skip_1)):

                @pl.when(jnp.logical_not(to_first & skip))
                def _(k=k, c=c):
                    send(dots.at[1], got_b.at[k - 1], 1, moved(dz=k) - c)

        @pl.when(jnp.logical_not((z_at == 0) & skip_0))
        def _():
            send(dots.at[1], got_b.at[zs - 1], 1, me - 1)

        got_b[zs - 1] = dots[1]

    scope("x3")
    landed(i_theirs, x_recv.at[IMAGE])
    for f in faces:
        for b in range(N):
            rows = at(f, b)
            yf[rows, :] = yf[rows, :] + (i_mine[rows, :] + i_theirs[rows, :])
    sum_yz([(yf, f) for f in faces], lanes)
    for f in faces:
        for b in range(N):
            im_o[full(f, b), :] = lane_pick(yf[at(f, b), :], order)
    face_rows = FACE // 2
    skipped = is_root.astype(jnp.int32) + jnp.where(
        core == 1,
        skip_0.astype(jnp.int32) + jnp.where(z_at > 0, skip_1.astype(jnp.int32), 0),
        0,
    )
    sums_0, sums_1 = len(hops) + 1 + len(roots), len(hops) + 2 * zs - 1 + len(roots)
    kinds = [(takes & jnp.logical_not(carrier), 12), (gives & jnp.logical_not(carrier), 13)]
    kinds += [(carrier & takes, 17)] + ([(carrier & gives, 18)] if xs == 1 else [])
    for faces_sent, face_count in kinds:
        for c, most, left_out in ((0, sums_0, 2), (1, sums_1, 3)):
            for less in range(left_out):

                @pl.when(faces_sent & (core == c) & (skipped == less))
                def _(sent=most - less + face_count * face_rows):
                    arrived(all_sent.at[pl.ds(0, sent)], x_send)

    scope("lines")

    @pl.when((core == 0) & others_than_root)
    def _():
        arrived(got_b, s_recv.at[1])

    @pl.when((core == 1) & others_than_root)
    def _():
        arrived(got_b.at[pl.ds(0, zs - 1)], s_recv.at[1])

    @pl.when(others_than_root)
    def _():
        dots[2] = added(got_b, None, zs)

    @pl.when(is_root)
    def _():
        dots[2] = root_sum(2, root_sum(1, dots[2]))

    total = dots[2]
    scope("alpha")
    sums = jnp.sum(total, axis=1, keepdims=True)
    al_o[...] = jnp.broadcast_to(sums[0:1, :] / sums[1:2, :], (8, LANES))
    scope(None)


CHUNKS = 4


def finish_kernel(p, r, im, al, x_h, r_h, both, sem):
    alpha = al[...]
    size = ROWS // CHUNKS
    for k in range(CHUNKS):
        for i in range(k * size, (k + 1) * size, N):
            both[tile(i), :] = alpha * p[tile(i), :]
        pltpu.make_async_copy(both.at[pl.ds(k * size, size)], x_h.at[pl.ds(k * size, size)], sem).start()
        for i in range(k * size, (k + 1) * size, N):
            both[tile(ROWS + i), :] = r[tile(i), :] - alpha * im[tile(i), :]
        rows = pl.ds(ROWS + k * size, size)
        pltpu.make_async_copy(both.at[rows], r_h.at[pl.ds(k * size, size)], sem).start()
    pltpu.make_async_copy(both, both, sem).wait()


def on_device(load_terms, geometry, mass_terms, element_order):
    flat = jax.ShapeDtypeStruct((ROWS, LANES), jnp.float32)
    vm = lambda *shape: pltpu.VMEM(shape, jnp.float32)
    field = vm(ROWS, LANES)
    pair = vm(2 * FACE, LANES)
    ys, zs, xs, cores = TORUS
    in_vmem = pl.BlockSpec(memory_space=pltpu.VMEM)
    in_hbm = pl.BlockSpec(memory_space=pltpu.HBM)
    parts = pl.pallas_call(
        step_kernel,
        out_shape=(field, field, field, vm(8, LANES)),
        in_specs=[in_hbm] * 4,
        out_specs=[in_vmem] * 4,
        scratch_shapes=[
            vm(5 * ROWS, LANES), *[field] * 7,
            *[vm(8 * FACE, LANES)] * 2,
            *[pair] * 4, vm(5 * FACE, LANES), *[pair] * 8, *[vm(FACE, LANES)] * 3,
            vm(12 * FACE, LANES), vm(16, LANES),
            vm(3, 2, LANES), vm(2 * ys * xs - 1, 2, LANES), vm(zs, 2, LANES),
            vm(ys * zs * xs * cores - 1, 2, LANES),
            vm(18 * FACE // 2 + ys * xs + 2 * zs + len(ROOTS), 2, LANES),
            pltpu.VMEM((1, LANES), jnp.int32),
            pltpu.SemaphoreType.DMA((2,)),
            pltpu.SemaphoreType.DMA(()),
            pltpu.SemaphoreType.DMA((6,)),
            pltpu.SemaphoreType.DMA(()),
            pltpu.SemaphoreType.DMA((2,)),
            pltpu.SemaphoreType.DMA((3,)),
            pltpu.SemaphoreType.REGULAR((3,)),
        ],
        compiler_params=pltpu.CompilerParams(
            collective_id=0, has_side_effects=True, vmem_limit_bytes=24 << 20
        ),
        name="cg_step",
    )(
        *[
            pltpu.with_memory_space_constraint(t, pltpu.HBM)
            for t in (
                load_terms.reshape(ROWS, LANES),
                geometry.reshape(3 * ROWS, LANES),
                mass_terms.reshape(ROWS, LANES),
                element_order,
            )
        ]
    )
    x, res = pl.pallas_call(
        finish_kernel,
        out_shape=(flat, flat),
        in_specs=[in_vmem] * 4,
        out_specs=[in_hbm] * 2,
        scratch_shapes=[vm(2 * ROWS, LANES), pltpu.SemaphoreType.DMA(())],
        compiler_params=pltpu.CompilerParams(vmem_limit_bytes=8 << 20),
        name="cg_finish",
    )(*[pltpu.with_memory_space_constraint(t, pltpu.VMEM) for t in parts])
    shape = load_terms.shape
    return x.reshape(shape), res.reshape(shape)


def solution(mesh):
    last = P(None, None, None, "slab")
    return jax.shard_map(
        on_device,
        mesh=mesh,
        in_specs=(last, P(None, None, None, None, "slab"), last, P("slab", None)),
        out_specs=(last, last),
        check_vma=False,
    )
```

```python
import functools

import jax
import jax.numpy as jnp
import numpy as np
from jax import lax
from jax.experimental import pallas as pl
from jax.experimental.pallas import tpu as pltpu
from jax.sharding import PartitionSpec as P

N = 8
LAST = N - 1
EL_Y = 8
EL_Z = 16
LANES = 128
ROWS = N * N * N
FACE = N * N
CENTRE = 1.65
HALF = 1.35
MESH = pl.DeviceIdType.MESH
TORUS = (8, 12, 4, 2)
ROOTS = (1, 3, 97, 2, 96)
INSIDE = range(1, LAST)
UNROLL_A = 4
UNROLL_BC = 3


def legendre_table(positions, points):
    columns = [positions * 0.0 + 1.0, positions]
    for degree in range(2, points):
        columns.append(
            ((2 * degree - 1) * positions * columns[-1] - (degree - 1) * columns[-2]) / degree
        )
    return np.stack(columns, axis=1)


def gll_derivative(points):
    degree = points - 1
    nodes = -np.cos(np.pi * np.arange(points) / degree)
    for _ in range(100):
        legendre = legendre_table(nodes, points)
        nodes = nodes - (nodes * legendre[:, degree] - legendre[:, degree - 1]) / (
            points * legendre[:, degree]
        )
    legendre = legendre_table(nodes, points)
    top = legendre[:, degree]
    same = np.eye(points, dtype=bool)
    spacing = np.where(same, 1.0, nodes[:, None] - nodes[None, :])
    table = np.where(same, 0.0, top[:, None] / (top[None, :] * spacing))
    table[0, 0] = -degree * points / 4.0
    table[degree, degree] = degree * points / 4.0
    return table


DERIV = gll_derivative(N).astype(np.float32).astype(np.float64)
SQUARED = DERIV * DERIV
SIGMA = CENTRE / HALF
RHO0 = 1.0 / SIGMA
RHO1 = 1.0 / (2.0 * SIGMA - RHO0)
COEF_Z = (1.0 + RHO1 * RHO0) / CENTRE + 2.0 * RHO1 / HALF
COEF_Q = 2.0 * RHO1 / HALF / CENTRE


def plus(x, y):
    return y if x is None else x + y


def contract(table, terms, sign, rows=range(N)):
    used = [j for j in range(N // 2) if terms[j] is not None]
    even = {j: terms[j] + terms[LAST - j] for j in used}
    odd = {j: terms[j] - terms[LAST - j] for j in used}
    out = [None] * N
    for i in range(N // 2):
        if i not in rows and LAST - i not in rows:
            continue
        e = o = None
        for j in used:
            e = plus(e, float(table[i, j] + table[i, LAST - j]) / 2 * even[j])
            o = plus(o, float(table[i, j] - table[i, LAST - j]) / 2 * odd[j])
        if i in rows:
            out[i] = e + o
        if LAST - i in rows:
            out[LAST - i] = (o - e) if sign < 0 else (e - o)
    return out


def tile(row):
    return pl.ds(row if isinstance(row, int) else pl.multiple_of(row, 8), 8)


def at(a, b):
    return tile((a * N + b) * N)


def across(a, c):
    return pl.ds(a * FACE + c, N, stride=N)


LOAD, DIAG, G1, G2 = range(4)
NEAR, FAR_LD, FAR_G, NEAR_W, FAR_W, IMAGE = range(6)


def part(f, kind, i):
    return tile(((f * 4 + kind) * N + i) * N)


def loop(start, stop, body):
    lax.fori_loop(start, stop, lambda i, _: (body(i), 0)[1], 0)


def stiffness_a(v, g0, out, rows=range(N), more=None):
    def along_a(b, _):
        va = [v[at(a, b), :] if a in INSIDE else None for a in range(N)]
        s = contract(DERIV, va, -1)
        s = contract(DERIV.T, [s[a] * g0[at(a, b), :] for a in range(N)], -1, rows)
        for a in rows:
            out[at(a, b), :] = s[a] if more is None else s[a] + more[at(a, b), :]
        return 0

    lax.fori_loop(0, N, along_a, 0, unroll=UNROLL_A)


def energy_a(v, g0, ends, first, total):
    def along_a(b, total):
        t = contract(DERIV, [v[at(a, b), :] if a in INSIDE else None for a in range(N)], -1)
        s = [t[a] * g0[at(a, b), :] for a in range(N)]
        total = [total[k] + s[k] * t[k] + s[k + 4] * t[k + 4] for k in range(4)]
        s = contract(DERIV.T, s, -1, (0, LAST))
        ends[tile(first + b * N), :] = s[0]
        ends[tile(FACE - first + b * N), :] = s[LAST]
        return total

    return lax.fori_loop(0, N, along_a, total, unroll=UNROLL_A)


def energy_bc(v, g1, g2t, ms, total):
    def along_bc(a, total):
        vb = [v[at(a, b), :] for b in range(N)]
        for own, g in (([v[across(a, c), :] for c in range(N)], g2t), (vb, g1)):
            t = contract(DERIV, own, -1)
            e = [t[i] * g[at(a, i), :] * t[i] for i in range(N)]
            total = [total[k] + (e[k] + e[k + 4]) for k in range(4)]
        e = [vb[b] * ms[at(a, b), :] * vb[b] for b in range(N)]
        return [total[k] + (e[k] + e[k + 4]) for k in range(4)]

    return lax.fori_loop(1, LAST, along_bc, total, unroll=UNROLL_BC)


def stiffness_bc(v, g1, g2t, ms, out, tmp, more=None):
    def along_bc(a, _):
        vt = [v[across(a, c), :] for c in range(N)]
        vb = [v[at(a, b), :] for b in range(N)]
        t = contract(DERIV, vt, -1)
        t = contract(DERIV.T, [t[c] * g2t[at(a, c), :] for c in range(N)], -1)
        for c in range(N):
            tmp[across(a, c), :] = t[c]
        s = contract(DERIV, vb, -1)
        s = contract(DERIV.T, [s[b] * g1[at(a, b), :] for b in range(N)], -1)
        for b in range(N):
            s[b] = s[b] + ms[at(a, b), :] * vb[b]
            if more is not None:
                s[b] = s[b] + more[at(a, b), :]
        for b in range(N):
            out[at(a, b), :] = s[b] + tmp[at(a, b), :]
        return 0

    lax.fori_loop(1, LAST, along_bc, 0, unroll=UNROLL_BC)


def inner_diagonal(g0, g1, g2, ms, out, tmp):
    def along_a(b, _):
        s = contract(SQUARED.T, [g0[at(a, b), :] for a in range(N)], 1, INSIDE)
        for a in INSIDE:
            out[at(a, b), :] = s[a] + ms[at(a, b), :]
        return 0

    lax.fori_loop(0, N, along_a, 0, unroll=UNROLL_A)

    def along_bc(a, _):
        t = contract(SQUARED.T, [g2[across(a, c), :] for c in range(N)], 1)
        for c in range(N):
            tmp[across(a, c), :] = t[c]
        s = contract(SQUARED.T, [g1[at(a, b), :] for b in range(N)], 1)
        for b in range(N):
            s[b] = s[b] + out[at(a, b), :]
        for b in range(N):
            out[at(a, b), :] = s[b] + tmp[at(a, b), :]
        return 0

    lax.fori_loop(1, LAST, along_bc, 0, unroll=UNROLL_BC)


def face_terms(v, f, mine, theirs, a_sum, tmp):
    s = contract(DERIV, [v[across(f, c), :] for c in range(N)], -1)
    s = contract(DERIV.T, [s[c] * theirs[part(f, G2, c), :] for c in range(N)], -1)
    for c in range(N):
        tmp[across(f, c), :] = s[c]
    vb = [v[at(f, b), :] for b in range(N)]
    s = contract(DERIV, vb, -1)
    s = contract(DERIV.T, [s[b] * theirs[part(f, G1, b), :] for b in range(N)], -1)
    return [s[b] + a_sum[at(f, b), :] * vb[b] + tmp[at(f, b), :] for b in range(N)]


def face_energy(v, f, theirs, a_sum):
    vb = [v[at(f, b), :] for b in range(N)]
    e = [a_sum[at(f, b), :] * vb[b] * vb[b] for b in range(N)]
    for own, kind in (([v[across(f, c), :] for c in range(N)], G2), (vb, G1)):
        t = contract(DERIV, own, -1)
        e = [e[i] + t[i] * theirs[part(f, kind, i), :] * t[i] for i in range(N)]
    return added_up(e)


def added_up(terms):
    while len(terms) > 1:
        terms = [functools.reduce(plus, terms[i : i + 2]) for i in range(0, len(terms), 2)]
    return terms[0]


def face_sums(f, mine, theirs, diag, a_sum, tmp):
    g = [[mine[part(f, k, i), :] + theirs[part(f, k, i), :] for i in range(N)] for k in (G1, G2)]
    for k in (G1, G2):
        for i in range(N):
            theirs[part(f, k, i), :] = g[k - G1][i]
    s = contract(SQUARED.T, g[1], 1)
    for c in range(N):
        tmp[across(f, c), :] = s[c]
    s = contract(SQUARED.T, g[0], 1)
    for b in range(N):
        a_sum[at(f, b), :] = diag[at(f, b), :] - s[b] - tmp[at(f, b), :]


def couplings(g0, first, out):
    def one(b, _):
        g = [g0[at(a, b), :] for a in range(N)]
        for a_end, row in ((0, first), (LAST, FACE - first)):
            s = contract(DERIV.T, [float(DERIV[m, a_end]) * g[m] for m in range(N)], -1, INSIDE)
            for a in INSIDE:
                out[tile(row * 6 + ((a - 1) * N + b) * N), :] = s[a]
        return 0

    lax.fori_loop(0, N, one, 0, unroll=2)


def couple(v, f, coupling, out, a):
    for b in range(N):
        out[at(a, b), :] = (
            out[at(a, b), :] + coupling[tile(((f * 6 + a - 1) * N + b) * N), :] * v[at(f, b), :]
        )


def lane_pick(x, idx):
    return jnp.take_along_axis(x, idx, axis=1, mode="promise_in_bounds")


def sum_yz(planes, lanes):
    ends = [(v[at(a, 0), :], v[at(a, LAST), :]) for v, a in planes]
    rims = [(v[across(a, 0), :], v[across(a, LAST), :]) for v, a in planes]
    ups = [jnp.where(lanes["up"], pltpu.roll(low, LANES - EL_Z, 1), 0.0) for low, _ in ends]
    downs = [jnp.where(lanes["down"], pltpu.roll(high, EL_Z, 1), 0.0) for _, high in ends]
    nexts = [lane_pick(low, lanes["next"]) for low, _ in rims]
    prevs = [lane_pick(high, lanes["prev"]) for _, high in rims]

    def corners(rim, idx):
        turned = jnp.where(lanes["first"], pltpu.roll(rim, 1, 0), pltpu.roll(rim, LAST, 0))
        return jnp.where(lanes["corner"], lane_pick(turned, idx), 0.0)

    far_nexts = [corners(low, lanes["corner_next"]) for low, _ in rims]
    far_prevs = [corners(high, lanes["corner_prev"]) for _, high in rims]
    for k, (v, a) in enumerate(planes):
        v[across(a, LAST), :] = rims[k][1] + (nexts[k] + far_nexts[k])
        v[across(a, 0), :] = rims[k][0] + (prevs[k] + far_prevs[k])
        v[at(a, LAST), :] = v[at(a, LAST), :] + ups[k]
        v[at(a, 0), :] = v[at(a, 0), :] + downs[k]


def step_kernel(
    load_h, geom_h, mass_h, order_h, p_o, r_o, im_o, al_o,
    coef, g2t, r, dg, z, y, u, tmp,
    mine, theirs, w_mine, w_theirs, i_mine, i_theirs, bag, rf, df, zf, pf, yf, a_sum, tmpf,
    u_ends, cross, q_mine, q_theirs, coupling, acc,
    dots, got_a, got_b, got_one, all_sent, order_v, in_sems, x_send, x_recv, bag_recv, s_recv, one_recv, hello,
):
    stack = []

    def scope(name):
        if stack:
            stack.pop().__exit__(None, None, None)
        if name:
            stack.append(jax.named_scope(name))
            stack[-1].__enter__()

    scope("enter")
    ys, zs, xs, cores = TORUS
    line, plane_size, count = xs * cores, zs * xs * cores, ys * zs * xs * cores
    me = lax.axis_index("slab")
    core = lax.rem(me, cores)
    in_plane = lax.rem(me, plane_size)

    def greet(sem, who):
        for q in who:
            pl.semaphore_signal(sem, inc=1, device_id=(q,), device_id_type=MESH)

    def heard(sem, who):
        if who:
            pl.semaphore_wait(sem, len(who))

    near_to = me + 1 - 2 * core
    far_to = me + 2 * core - 1
    far_to = jnp.where(far_to < 0, count - 1, jnp.where(far_to == count, 0, far_to))
    in_line = lax.rem(me, line)
    early, late = in_line == 0, in_line == line - 1
    at_turn = in_plane < line
    carrier = (jnp.logical_not(at_turn) & (in_line == 1)) | (at_turn & late)
    carrier_of_late = jnp.where(in_plane == plane_size - 1, me + line - plane_size, me + 2)
    barrier = pltpu.get_barrier_semaphore()
    greet(barrier, [jnp.where(late, carrier_of_late, far_to)])
    loads = [
        pltpu.make_async_copy(src, dst, in_sems.at[k])
        for k, src, dst in (
            (0, order_h, order_v),
            (1, load_h, coef.at[pl.ds(4 * ROWS, ROWS)]),
            (1, geom_h, coef.at[pl.ds(0, 3 * ROWS)]),
            (1, mass_h, coef.at[pl.ds(3 * ROWS, ROWS)]),
        )
    ]
    for copy in loads:
        copy.start()
    g0, g1, g2, ms, ld = (coef.at[pl.ds(k * ROWS, ROWS)] for k in range(5))

    y_at = me // plane_size
    z_at = in_plane // line
    x = in_line // cores

    def moved(dy=0, dz=0, dx=0):
        to = me
        if dy:
            to = to + (lax.rem(y_at + dy, ys) - y_at) * plane_size
        if dz:
            to = to + (lax.rem(z_at + dz, zs) - z_at) * line
        if dx:
            to = to + (lax.rem(x + dx, xs) - x) * cores
        return to

    def ring(size, stop, start=1):
        return sorted({j % size for k in range(start, stop) for j in (k, -k)} - {0})

    sides = (near_to, far_to)
    row_of = (pl.multiple_of((1 - core) * (ROWS - FACE), FACE), pl.multiple_of(core * (ROWS - FACE), FACE))
    face_of = {0: 1 - core, LAST: core}
    carrier_of_early = jnp.where(
        at_turn, lax.rem(y_at + ys - 1, ys) * plane_size + line - 1, me + 1
    )
    early_of_carrier = lax.rem(y_at + 1, ys) * plane_size
    late_of_carrier = jnp.where(at_turn, me + plane_size - line, me - 2)

    y_near = [moved(dy=k) for k in ring(ys, 3)]
    y_far = [moved(dy=k) for k in ring(ys, ys // 2 + 1, 3)]
    greet(barrier, [near_to])
    not_early = jnp.logical_not(early)
    for k in range(1, line):

        @pl.when(in_line != k)
        def _(k=k):
            greet(barrier, [me - in_line + k])

    @pl.when(not_early)
    def _():
        greet(barrier, y_near)

    @pl.when(at_turn & (early | late))
    def _():
        greet(barrier, [jnp.where(early, carrier_of_early, early_of_carrier)])

    def higher(z_to, _):
        greet(barrier, [me + (z_to - z_at) * line + 1 - core])
        return 0

    lax.fori_loop(z_at + 1, zs, higher, 0)
    roots = [r for r in ROOTS if r < count]

    def one_of(device, some):
        return functools.reduce(jnp.logical_or, [device == r for r in some])

    is_root = one_of(me, roots)
    others_than_root = jnp.logical_not(is_root)

    @pl.when(is_root)
    def _():
        width = next(k for k in range(16, 0, -1) if (count - 1) % k == 0)

        def everyone(k, _):
            for i in range(width):
                q = me + 1 + k * width + i
                greet(barrier, [jnp.where(q >= count, q - count, q)])
            return 0

        lax.fori_loop(0, (count - 1) // width, everyone, 0)

    expected = jnp.where(
        early,
        1 + at_turn.astype(jnp.int32),
        (line - 1)
        + len(y_near)
        + 2
        + carrier.astype(jnp.int32)
        + (carrier & at_turn).astype(jnp.int32)
        + 2 * core * z_at,
    )
    expected = expected + len(roots) - is_root.astype(jnp.int32)

    scope("idx")
    loads[0].wait()
    order = jnp.broadcast_to(order_v[...], (8, LANES))
    hit = (
        jnp.broadcast_to(order_v[...], (LANES, LANES))
        == lax.broadcasted_iota(jnp.int32, (LANES, LANES), 0)
    ).astype(jnp.float32)
    lane = lax.broadcasted_iota(jnp.int32, (8, LANES), 1)
    inverse = lax.dot_general(
        lane.astype(jnp.float32), hit, (((1,), (1,)), ((), ())), preferred_element_type=jnp.float32
    )
    inverse = (inverse + 0.5).astype(jnp.int32)
    in_row = lane & (EL_Z - 1)
    lanes = {
        "up": lane < LANES - EL_Z,
        "down": lane >= EL_Z,
        "next": lane - in_row + ((in_row + 1) & (EL_Z - 1)),
        "prev": lane - in_row + ((in_row + EL_Z - 1) & (EL_Z - 1)),
    }
    b_at = lax.broadcasted_iota(jnp.int32, (8, LANES), 0)
    lanes["first"] = b_at == 0
    lanes["corner"] = (lanes["first"] & lanes["down"]) | ((b_at == LAST) & lanes["up"])
    by_y = jnp.where(lanes["first"], LANES - EL_Z, EL_Z)
    lanes["corner_next"] = (lanes["next"] + by_y) & (LANES - 1)
    lanes["corner_prev"] = (lanes["prev"] + by_y) & (LANES - 1)

    def reorder(src, dst, idx, planes=range(N)):
        for a in planes:
            for b in range(N):
                dst[at(a, b), :] = lane_pick(src[at(a, b), :], idx)

    def remote(src, dst, recv, to):
        return pltpu.make_async_remote_copy(
            src_ref=src,
            dst_ref=dst,
            send_sem=x_send,
            recv_sem=recv,
            device_id=(to,),
            device_id_type=MESH,
        )

    def swap(src, dst, f, first, rows, k, carried=None):
        src, dst = src.at[pl.ds(first, rows)], dst.at[pl.ds(first, rows)]
        copy = remote(src, dst, x_recv.at[k], sides[f])
        if carried is None:
            copy.start()
        else:
            by_bag = remote(src, bag.at[pl.ds(carried, rows)], bag_recv.at[1], carrier_of_early)
            pl.when(early)(by_bag.start)
            pl.when(jnp.logical_not(early))(copy.start)
        return copy

    def carry(dst, carried, first, rows, k):
        src, dst = bag.at[pl.ds(carried, rows)], dst.at[pl.ds(first, rows)]
        remote(src, dst, x_recv.at[k], late_of_carrier).start()

    def landed(ref, sem):
        pltpu.make_async_copy(ref, ref, sem).wait()

    @pl.when(early)
    def _():
        pl.semaphore_wait(barrier, expected)
        greet(hello.at[3], [near_to])

    both = (0, LAST)
    faces = (0, 1)
    scope("load_ends")
    pltpu.make_async_copy(coef, coef, in_sems.at[1]).wait()
    for a in both:
        for b in range(N):
            mine[part(face_of[a], LOAD, b), :] = lane_pick(ld[at(a, b), :], inverse)
    for k, a in enumerate(both):
        s = contract(SQUARED.T, [g2[across(a, c), :] for c in range(N)], 1)
        for c in range(N):
            tmpf[across(k, c), :] = s[c]
    for b in range(N):
        s = contract(SQUARED.T, [g0[at(a, b), :] for a in range(N)], 1, both)
        for k, a in enumerate(both):
            yf[at(k, b), :] = s[a]
    for k, a in enumerate(both):
        s = contract(SQUARED.T, [g1[at(a, b), :] for b in range(N)], 1)
        for b in range(N):
            mine[part(face_of[a], DIAG, b), :] = lane_pick(
                s[b] + yf[at(k, b), :] + ms[at(a, b), :] + tmpf[at(k, b), :], inverse
            )
    for a in both:
        for i in range(N):
            mine[part(face_of[a], G1, i), :] = lane_pick(g1[at(a, i), :], inverse)
            mine[part(face_of[a], G2, i), :] = lane_pick(g2[across(a, i), :], inverse)
    sent_near = remote(
        mine.at[pl.ds(0, 4 * FACE)], theirs.at[pl.ds(0, 4 * FACE)], x_recv.at[NEAR], near_to
    )
    beside_early = in_line == 1

    @pl.when(beside_early)
    def _():
        pl.semaphore_wait(hello.at[3], 1)
        sent_near.start()

    scope("barrier")

    @pl.when(not_early)
    def _():
        pl.semaphore_wait(barrier, expected)

    scope("send1")

    @pl.when(carrier)
    def _():
        landed(bag.at[pl.ds(0, 4 * FACE)], bag_recv.at[0])
        carry(theirs, 0, 4 * FACE, 2 * FACE, FAR_LD)
        carry(theirs, 2 * FACE, 6 * FACE, 2 * FACE, FAR_G)

    @pl.when(early)
    def _():
        remote(
            mine.at[pl.ds(4 * FACE, 4 * FACE)],
            bag.at[pl.ds(0, 4 * FACE)],
            bag_recv.at[0],
            carrier_of_early,
        ).start()

    sent_ld, sent_g = (
        remote(mine.at[rows], theirs.at[rows], x_recv.at[k], far_to)
        for k, rows in ((FAR_LD, pl.ds(4 * FACE, 2 * FACE)), (FAR_G, pl.ds(6 * FACE, 2 * FACE)))
    )

    @pl.when(not_early)
    def _():
        sent_ld.start()
        sent_g.start()

    pl.when(jnp.logical_not(beside_early))(sent_near.start)

    @pl.when(not_early)
    def _():
        greet(hello.at[0], y_near)


    @pl.when(core == 1)
    def _():
        def lower(z_to, _):
            greet(hello.at[2], [me + (z_to - z_at) * line])
            return 0

        lax.fori_loop(0, z_at, lower, 0)

    scope("diag")
    inner_diagonal(g0, g1, g2, ms, dg, tmp)
    scope("reorder")
    for a in INSIDE:
        for b in range(N):
            rows = at(a, b)
            dg[rows, :] = lane_pick(dg[rows, :], inverse)
            moved_load = lane_pick(ld[rows, :], inverse)
            ld[rows, :] = moved_load
            r[rows, :] = moved_load
    reorder(g0, g0, inverse)

    @pl.when(carrier)
    def _():
        landed(bag.at[pl.ds(4 * FACE, FACE)], bag_recv.at[1])
        carry(w_theirs, 4 * FACE, FACE, FACE, FAR_W)

    scope("sums")
    sum_yz([(v, a) for a in INSIDE for v in (dg, r)], lanes)

    def inner_z(a, _):
        for b in range(N):
            inv = 1.0 / dg[at(a, b), :]
            dg[at(a, b), :] = inv
            z[at(a, b), :] = inv * r[at(a, b), :]
        return 0

    lax.fori_loop(1, LAST, inner_z, 0, unroll=3)
    for b in range(N):
        g = [float(DERIV[m, 0] * DERIV[m, LAST]) * g0[at(m, b), :] for m in range(N)]
        cross[at(0, b), :] = added_up(g)
    scope("La1")
    stiffness_a(z, g0, y)

    def full(f, b):
        return tile(row_of[f] + b * N)

    def face_z(f):
        for b in range(N):
            rf[at(f, b), :] = mine[part(f, LOAD, b), :] + theirs[part(f, LOAD, b), :]
            total = mine[part(f, DIAG, b), :] + theirs[part(f, DIAG, b), :]
            a_sum[at(f, b), :] = total
            df[at(f, b), :] = total
        sum_yz([(rf, f), (df, f)], lanes)
        for b in range(N):
            inv = 1.0 / df[at(f, b), :]
            df[at(f, b), :] = inv
            zf[at(f, b), :] = inv * rf[at(f, b), :]

    def tell(f, k, carried=None):
        for b in range(N):
            w_mine[at(f, b), :] = y[full(f, b), :] + cross[at(0, b), :] * zf[at(1 - f, b), :]
        sum_yz([(w_mine, f)], lanes)
        return swap(w_mine, w_theirs, f, f * FACE, FACE, k, carried)

    scope("x_near")
    sent_near.wait_recv()
    scope("z_near")
    face_z(0)
    sent_w = [None, tell(1, FAR_W, 4 * FACE)]
    scope("reorder2")
    reorder(g1, g1, inverse, INSIDE)
    for a in INSIDE:
        for c in range(N):
            g2t[at(a, c), :] = lane_pick(g2[across(a, c), :], inverse)
    reorder(ms, ms, inverse, INSIDE)
    scope("Lbc1")
    stiffness_bc(z, g1, g2t, ms, y, tmp, y)
    scope("hello")

    @pl.when(not_early)
    def _():
        heard(hello.at[0], y_near)
        greet(hello.at[1], y_far)

    scope("g_near")
    first = pl.multiple_of((1 - core) * FACE, FACE)
    couplings(g0, first, coupling)
    loop(1, LAST, lambda a: couple(zf, 0, coupling, y, a))
    face_sums(0, mine, theirs, a_sum, a_sum, tmpf)
    s = face_terms(zf, 0, mine, theirs, a_sum, tmpf)
    for b in range(N):
        yf[at(0, b), :] = s[b]
    sum_yz([(yf, 0)], lanes)
    scope("x_far")
    sent_ld.wait_recv()
    scope("z_far")
    face_z(1)

    scope("inner2")
    for a in INSIDE:
        couple(zf, 1, coupling, y, a)
    sum_yz([(y, a) for a in INSIDE], lanes)
    zero = jnp.zeros((8, LANES), jnp.float32)

    def inner_p(a, num):
        for b in range(N):
            rows = at(a, b)
            p = COEF_Z * z[rows, :] - COEF_Q * (dg[rows, :] * y[rows, :])
            z[rows, :] = p
            num[b % 4] = num[b % 4] + ld[rows, :] * p
        return num

    num = lax.fori_loop(1, LAST, inner_p, [zero] * 4, unroll=True)
    scope("L2")
    den = energy_bc(z, g1, g2t, ms, [zero] * 4)
    den = energy_a(z, g0, u_ends, first, den)
    num, den = added_up(num), added_up(den)
    scope("g_far")
    sent_g.wait_recv()
    face_sums(1, mine, theirs, a_sum, a_sum, tmpf)
    s = face_terms(zf, 1, mine, theirs, a_sum, tmpf)
    for b in range(N):
        yf[at(1, b), :] = s[b]
    sum_yz([(yf, 1)], lanes)
    sent_w[0] = tell(0, NEAR_W)

    def face_p(f):
        for b in range(N):
            rows = at(f, b)
            total = yf[rows, :] + (w_mine[rows, :] + w_theirs[rows, :])
            pf[rows, :] = COEF_Z * zf[rows, :] - COEF_Q * (df[rows, :] * total)

    def face_dot(kind, f):
        return added_up([kind[part(f, LOAD, b), :] * pf[at(f, b), :] for b in range(N)])

    acc[tile(0), :] = num
    acc[tile(8), :] = den
    takes = jnp.where(2 * x >= xs, core, 1 - core) == 1
    gives = jnp.logical_not(takes)
    sent_q = remote(q_mine, q_theirs, x_recv.at[NEAR_W], near_to)
    scope("w_near")

    @pl.when(takes)
    def _():
        landed(w_mine, x_recv.at[NEAR_W])
        face_p(0)
        acc[tile(0), :] = acc[tile(0), :] + (face_dot(mine, 0) + face_dot(theirs, 0))
        terms = [
            (2.0 * u_ends[at(0, b), :] + q_theirs[at(0, b), :]) * pf[at(0, b), :] for b in range(N)
        ]
        acc[tile(8), :] = acc[tile(8), :] + (face_energy(pf, 0, theirs, a_sum) + added_up(terms))
        for b in range(N):
            q_mine[at(0, b), :] = 2.0 * cross[at(0, b), :] * pf[at(0, b), :]

    scope("w_far")
    sent_w[1].wait_recv()
    scope("ends2")
    face_p(1)
    acc[tile(0), :] = acc[tile(0), :] + face_dot(mine, 1)
    terms = [2.0 * u_ends[at(1, b), :] * pf[at(1, b), :] for b in range(N)]
    acc[tile(8), :] = acc[tile(8), :] + (0.5 * face_energy(pf, 1, theirs, a_sum) + added_up(terms))

    @pl.when(takes)
    def _():
        terms = [q_mine[at(0, b), :] * pf[at(1, b), :] for b in range(N)]
        acc[tile(8), :] = acc[tile(8), :] + added_up(terms)

    @pl.when(gives)
    def _():
        for b in range(N):
            q_mine[at(0, b), :] = 2.0 * (
                u_ends[at(0, b), :] + cross[at(0, b), :] * pf[at(1, b), :]
            )
        sent_q.start()

    num_row = jnp.sum(acc[tile(0), :], axis=0, keepdims=True)
    den_row = jnp.sum(acc[tile(8), :], axis=0, keepdims=True)
    dots[0, 0:1, :] = num_row
    dots[0, 1:2, :] = den_row
    hops = sorted(
        ((dy, dx) for dy in range(ys) for dx in range(xs) if dy or dx),
        key=lambda d: -min(d[0], ys - d[0]) - min(d[1], xs - d[1]),
    )
    others = 2 * len(hops) + 1

    def send(src, dst, k, to):
        copy = pltpu.make_async_remote_copy(
            src_ref=src,
            dst_ref=dst,
            send_sem=x_send,
            recv_sem=s_recv.at[k],
            device_id=(to,),
            device_id_type=MESH,
        )
        copy.start()

    def arrived(ref, sem):
        pltpu.make_async_copy(ref, ref, sem).wait()

    def added(ref, first, total):
        part = [first, None, None, None]
        for j in range(total):
            part[j % 4] = plus(part[j % 4], ref[j])
        return functools.reduce(plus, [t for t in part if t is not None])

    half_z, pair_z = zs // 2, zs // 2 + zs // 8
    in_first = y_at * line + in_line
    slow_low = (z_at == pair_z) & (x == xs - 1) & (core == 1)
    slow_high = (z_at == pair_z + 1) & (x == 0) & (core == 0)
    slow_ones = ys * (2 if pair_z + 1 < zs else 1)
    slow_before = jnp.where(
        z_at > pair_z + 1,
        slow_ones,
        jnp.where(
            z_at == pair_z + 1,
            ys + y_at + (in_line > 0).astype(jnp.int32),
            jnp.where(z_at == pair_z, y_at, 0),
        ),
    )
    slot = jnp.where(
        slow_low | slow_high,
        count - slow_ones + jnp.where(slow_high, ys, 0) + y_at,
        z_at * ys * line + in_first - slow_before,
    )
    group = jnp.where(slow_low | slow_high, 2, jnp.where(z_at < half_z, 0, 1))
    group_0 = half_z * ys * line - 1
    groups = (group_0, count - 1 - group_0 - slow_ones, slow_ones)

    def root_sum(k, total):
        width, start, number = 16, sum(groups[:k]), groups[k]
        arrived(got_one.at[pl.ds(start, number)], one_recv.at[k])
        sums = [total] + [jnp.zeros((2, LANES), jnp.float32)] * 7

        def some(i, sums):
            return [
                sums[j] + got_one[start + i * width + j] + got_one[start + i * width + j + 8]
                for j in range(8)
            ]

        whole = number // width
        sums = lax.fori_loop(0, whole, some, sums)
        for i in range(whole * width, number):
            sums[i % 8] = sums[i % 8] + got_one[start + i]
        return added_up(sums)

    def send_to_root(r):
        at_root = r // plane_size * line + r % line

        @pl.when(me != r)
        def _():
            pltpu.make_async_remote_copy(
                src_ref=dots.at[0],
                dst_ref=got_one.at[slot - (slot > at_root).astype(jnp.int32)],
                send_sem=x_send,
                recv_sem=one_recv.at[group],
                device_id=(r,),
                device_id_type=MESH,
            ).start()

    send_to_root(roots[0])

    @pl.when(not_early)
    def _():
        heard(hello.at[1], y_far)

    @pl.when(beside_early)
    def _():
        greet(hello.at[0], [near_to])

    @pl.when(early)
    def _():
        pl.semaphore_wait(hello.at[0], 1)

    for j, (dy, dx) in enumerate(hops):
        send(dots.at[0], got_a.at[2 * j + core], 0, moved(dy=dy, dx=dx) + 1 - core)

    @pl.when(core == 0)
    def _():
        send(dots.at[0], got_a.at[others - 1], 0, me + 1)

    for other_root in roots[1:]:
        send_to_root(other_root)

    scope("u_ends")

    @pl.when(gives)
    def _():
        sent_w[0].wait_recv()
        face_p(0)

    for f in faces:
        for b in range(N):
            i_mine[at(f, b), :] = u_ends[at(f, b), :] + cross[at(0, b), :] * pf[at(1 - f, b), :]
        swap(i_mine, i_theirs, f, f * FACE, FACE, IMAGE)
    for f in faces:
        s = face_terms(pf, f, mine, theirs, a_sum, tmpf)
        for b in range(N):
            yf[at(f, b), :] = s[b]
    stiffness_bc(z, g1, g2t, ms, y, tmp)
    stiffness_a(z, g0, u, INSIDE, y)

    def couple_both(a):
        couple(pf, 0, coupling, u, a)
        couple(pf, 1, coupling, u, a)

    loop(1, LAST, couple_both)
    scope("out_p_r")
    for src, ends, dst in ((z, pf, p_o), (r, rf, r_o)):
        reorder(src, dst, order, INSIDE)
        for f in faces:
            for b in range(N):
                dst[full(f, b), :] = lane_pick(ends[at(f, b), :], order)
    sum_yz([(u, a) for a in INSIDE], lanes)
    reorder(u, im_o, order, INSIDE)
    scope("root_0")

    @pl.when(is_root)
    def _():
        dots[2] = root_sum(0, dots[0])

    scope("plane")
    first_of_column = me - z_at * line
    skip_0 = one_of(first_of_column - 1, [r for r in roots if r % cores == 0] or [-1])
    skip_1 = one_of(first_of_column, [r for r in roots if r % cores == 1])

    @pl.when(core == 1)
    def _():
        arrived(got_a.at[pl.ds(0, others)], s_recv.at[0])
        dots[1] = added(got_a, dots[0], others)

        @pl.when(z_at < zs - 1)
        def _():
            pl.semaphore_wait(hello.at[2], zs - 1 - z_at)

        for k in sorted(range(1, zs), key=lambda k: -min(k, zs - k)):
            to_first = z_at == zs - k
            for c, skip in ((1, skip_0), (0, skip_1)):

                @pl.when(jnp.logical_not(to_first & skip))
                def _(k=k, c=c):
                    send(dots.at[1], got_b.at[k - 1], 1, moved(dz=k) - c)

        @pl.when(jnp.logical_not((z_at == 0) & skip_0))
        def _():
            send(dots.at[1], got_b.at[zs - 1], 1, me - 1)

        got_b[zs - 1] = dots[1]

    scope("x3")
    landed(i_theirs, x_recv.at[IMAGE])
    for f in faces:
        for b in range(N):
            rows = at(f, b)
            yf[rows, :] = yf[rows, :] + (i_mine[rows, :] + i_theirs[rows, :])
    sum_yz([(yf, f) for f in faces], lanes)
    for f in faces:
        for b in range(N):
            im_o[full(f, b), :] = lane_pick(yf[at(f, b), :], order)
    face_rows = FACE // 2
    skipped = is_root.astype(jnp.int32) + jnp.where(
        core == 1,
        skip_0.astype(jnp.int32) + jnp.where(z_at > 0, skip_1.astype(jnp.int32), 0),
        0,
    )
    sums_0, sums_1 = len(hops) + 1 + len(roots), len(hops) + 2 * zs - 1 + len(roots)
    kinds = [(takes & jnp.logical_not(carrier), 12), (gives & jnp.logical_not(carrier), 13)]
    kinds += [(carrier & takes, 17), (carrier & gives, 18)]
    for faces_sent, face_count in kinds:
        for c, most, left_out in ((0, sums_0, 2), (1, sums_1, 3)):
            for less in range(left_out):

                @pl.when(faces_sent & (core == c) & (skipped == less))
                def _(sent=most - less + face_count * face_rows):
                    arrived(all_sent.at[pl.ds(0, sent)], x_send)

    scope("lines")

    @pl.when((core == 0) & others_than_root)
    def _():
        arrived(got_b, s_recv.at[1])

    @pl.when((core == 1) & others_than_root)
    def _():
        arrived(got_b.at[pl.ds(0, zs - 1)], s_recv.at[1])

    @pl.when(others_than_root)
    def _():
        dots[2] = added(got_b, None, zs)

    @pl.when(is_root)
    def _():
        dots[2] = root_sum(2, root_sum(1, dots[2]))

    total = dots[2]
    scope("alpha")
    sums = jnp.sum(total, axis=1, keepdims=True)
    al_o[...] = jnp.broadcast_to(sums[0:1, :] / sums[1:2, :], (8, LANES))
    scope(None)


CHUNKS = 4


def finish_kernel(p, r, im, al, x_h, r_h, both, sem):
    alpha = al[...]
    size = ROWS // CHUNKS
    for k in range(CHUNKS):
        for i in range(k * size, (k + 1) * size, N):
            both[tile(i), :] = alpha * p[tile(i), :]
        pltpu.make_async_copy(both.at[pl.ds(k * size, size)], x_h.at[pl.ds(k * size, size)], sem).start()
        for i in range(k * size, (k + 1) * size, N):
            both[tile(ROWS + i), :] = r[tile(i), :] - alpha * im[tile(i), :]
        rows = pl.ds(ROWS + k * size, size)
        pltpu.make_async_copy(both.at[rows], r_h.at[pl.ds(k * size, size)], sem).start()
    pltpu.make_async_copy(both, both, sem).wait()


def on_device(load_terms, geometry, mass_terms, element_order):
    flat = jax.ShapeDtypeStruct((ROWS, LANES), jnp.float32)
    vm = lambda *shape: pltpu.VMEM(shape, jnp.float32)
    field = vm(ROWS, LANES)
    pair = vm(2 * FACE, LANES)
    ys, zs, xs, cores = TORUS
    in_vmem = pl.BlockSpec(memory_space=pltpu.VMEM)
    in_hbm = pl.BlockSpec(memory_space=pltpu.HBM)
    parts = pl.pallas_call(
        step_kernel,
        out_shape=(field, field, field, vm(8, LANES)),
        in_specs=[in_hbm] * 4,
        out_specs=[in_vmem] * 4,
        scratch_shapes=[
            vm(5 * ROWS, LANES), *[field] * 7,
            *[vm(8 * FACE, LANES)] * 2,
            *[pair] * 4, vm(5 * FACE, LANES), *[pair] * 8, *[vm(FACE, LANES)] * 3,
            vm(12 * FACE, LANES), vm(16, LANES),
            vm(3, 2, LANES), vm(2 * ys * xs - 1, 2, LANES), vm(zs, 2, LANES),
            vm(ys * zs * xs * cores - 1, 2, LANES),
            vm(18 * FACE // 2 + ys * xs + 2 * zs + len(ROOTS), 2, LANES),
            pltpu.VMEM((1, LANES), jnp.int32),
            pltpu.SemaphoreType.DMA((2,)),
            pltpu.SemaphoreType.DMA(()),
            pltpu.SemaphoreType.DMA((6,)),
            pltpu.SemaphoreType.DMA((2,)),
            pltpu.SemaphoreType.DMA((2,)),
            pltpu.SemaphoreType.DMA((3,)),
            pltpu.SemaphoreType.REGULAR((4,)),
        ],
        compiler_params=pltpu.CompilerParams(
            collective_id=0, has_side_effects=True, vmem_limit_bytes=24 << 20
        ),
        name="cg_step",
    )(
        *[
            pltpu.with_memory_space_constraint(t, pltpu.HBM)
            for t in (
                load_terms.reshape(ROWS, LANES),
                geometry.reshape(3 * ROWS, LANES),
                mass_terms.reshape(ROWS, LANES),
                element_order,
            )
        ]
    )
    x, res = pl.pallas_call(
        finish_kernel,
        out_shape=(flat, flat),
        in_specs=[in_vmem] * 4,
        out_specs=[in_hbm] * 2,
        scratch_shapes=[vm(2 * ROWS, LANES), pltpu.SemaphoreType.DMA(())],
        compiler_params=pltpu.CompilerParams(vmem_limit_bytes=8 << 20),
        name="cg_finish",
    )(*[pltpu.with_memory_space_constraint(t, pltpu.VMEM) for t in parts])
    shape = load_terms.shape
    return x.reshape(shape), res.reshape(shape)


def solution(mesh):
    last = P(None, None, None, "slab")
    return jax.shard_map(
        on_device,
        mesh=mesh,
        in_specs=(last, P(None, None, None, None, "slab"), last, P("slab", None)),
        out_specs=(last, last),
        check_vma=False,
    )
```

```python
import functools

import jax
import jax.numpy as jnp
import numpy as np
from jax import lax
from jax.experimental import pallas as pl
from jax.experimental.pallas import tpu as pltpu
from jax.sharding import PartitionSpec as P

N = 8
LAST = N - 1
EL_Y = 8
EL_Z = 16
LANES = 128
ROWS = N * N * N
FACE = N * N
CENTRE = 1.65
HALF = 1.35
MESH = pl.DeviceIdType.MESH
TORUS = (8, 12, 4, 2)
ROOTS = (1, 3, 97, 2, 96, 7, 193, 192, 5, 6)
INSIDE = range(1, LAST)
UNROLL_A = 4
UNROLL_BC = 3


def legendre_table(positions, points):
    columns = [positions * 0.0 + 1.0, positions]
    for degree in range(2, points):
        columns.append(
            ((2 * degree - 1) * positions * columns[-1] - (degree - 1) * columns[-2]) / degree
        )
    return np.stack(columns, axis=1)


def gll_derivative(points):
    degree = points - 1
    nodes = -np.cos(np.pi * np.arange(points) / degree)
    for _ in range(100):
        legendre = legendre_table(nodes, points)
        nodes = nodes - (nodes * legendre[:, degree] - legendre[:, degree - 1]) / (
            points * legendre[:, degree]
        )
    legendre = legendre_table(nodes, points)
    top = legendre[:, degree]
    same = np.eye(points, dtype=bool)
    spacing = np.where(same, 1.0, nodes[:, None] - nodes[None, :])
    table = np.where(same, 0.0, top[:, None] / (top[None, :] * spacing))
    table[0, 0] = -degree * points / 4.0
    table[degree, degree] = degree * points / 4.0
    return table


DERIV = gll_derivative(N).astype(np.float32).astype(np.float64)
SQUARED = DERIV * DERIV
SIGMA = CENTRE / HALF
RHO0 = 1.0 / SIGMA
RHO1 = 1.0 / (2.0 * SIGMA - RHO0)
COEF_Z = (1.0 + RHO1 * RHO0) / CENTRE + 2.0 * RHO1 / HALF
COEF_Q = 2.0 * RHO1 / HALF / CENTRE


def plus(x, y):
    return y if x is None else x + y


def contract(table, terms, sign, rows=range(N)):
    used = [j for j in range(N // 2) if terms[j] is not None]
    even = {j: terms[j] + terms[LAST - j] for j in used}
    odd = {j: terms[j] - terms[LAST - j] for j in used}
    out = [None] * N
    for i in range(N // 2):
        if i not in rows and LAST - i not in rows:
            continue
        e = o = None
        for j in used:
            e = plus(e, float(table[i, j] + table[i, LAST - j]) / 2 * even[j])
            o = plus(o, float(table[i, j] - table[i, LAST - j]) / 2 * odd[j])
        if i in rows:
            out[i] = e + o
        if LAST - i in rows:
            out[LAST - i] = (o - e) if sign < 0 else (e - o)
    return out


def tile(row):
    return pl.ds(row if isinstance(row, int) else pl.multiple_of(row, 8), 8)


def at(a, b):
    return tile((a * N + b) * N)


def across(a, c):
    return pl.ds(a * FACE + c, N, stride=N)


LOAD, DIAG, G1, G2 = range(4)
NEAR, FAR_LD, FAR_G, NEAR_W, FAR_W, IMAGE = range(6)


def part(f, kind, i):
    return tile(((f * 4 + kind) * N + i) * N)


def loop(start, stop, body):
    lax.fori_loop(start, stop, lambda i, _: (body(i), 0)[1], 0)


def stiffness_a(v, g0, out, rows=range(N), more=None):
    def along_a(b, _):
        va = [v[at(a, b), :] if a in INSIDE else None for a in range(N)]
        s = contract(DERIV, va, -1)
        s = contract(DERIV.T, [s[a] * g0[at(a, b), :] for a in range(N)], -1, rows)
        for a in rows:
            out[at(a, b), :] = s[a] if more is None else s[a] + more[at(a, b), :]
        return 0

    lax.fori_loop(0, N, along_a, 0, unroll=UNROLL_A)


def energy_a(v, g0, ends, first, total):
    def along_a(b, total):
        t = contract(DERIV, [v[at(a, b), :] if a in INSIDE else None for a in range(N)], -1)
        s = [t[a] * g0[at(a, b), :] for a in range(N)]
        total = [total[k] + s[k] * t[k] + s[k + 4] * t[k + 4] for k in range(4)]
        s = contract(DERIV.T, s, -1, (0, LAST))
        ends[tile(first + b * N), :] = s[0]
        ends[tile(FACE - first + b * N), :] = s[LAST]
        return total

    return lax.fori_loop(0, N, along_a, total, unroll=UNROLL_A)


def energy_bc(v, g1, g2t, ms, total):
    def along_bc(a, total):
        vb = [v[at(a, b), :] for b in range(N)]
        for own, g in (([v[across(a, c), :] for c in range(N)], g2t), (vb, g1)):
            t = contract(DERIV, own, -1)
            e = [t[i] * g[at(a, i), :] * t[i] for i in range(N)]
            total = [total[k] + (e[k] + e[k + 4]) for k in range(4)]
        e = [vb[b] * ms[at(a, b), :] * vb[b] for b in range(N)]
        return [total[k] + (e[k] + e[k + 4]) for k in range(4)]

    return lax.fori_loop(1, LAST, along_bc, total, unroll=UNROLL_BC)


def stiffness_bc(v, g1, g2t, ms, out, tmp, more=None):
    def along_bc(a, _):
        vt = [v[across(a, c), :] for c in range(N)]
        vb = [v[at(a, b), :] for b in range(N)]
        t = contract(DERIV, vt, -1)
        t = contract(DERIV.T, [t[c] * g2t[at(a, c), :] for c in range(N)], -1)
        for c in range(N):
            tmp[across(a, c), :] = t[c]
        s = contract(DERIV, vb, -1)
        s = contract(DERIV.T, [s[b] * g1[at(a, b), :] for b in range(N)], -1)
        for b in range(N):
            s[b] = s[b] + ms[at(a, b), :] * vb[b]
            if more is not None:
                s[b] = s[b] + more[at(a, b), :]
        for b in range(N):
            out[at(a, b), :] = s[b] + tmp[at(a, b), :]
        return 0

    lax.fori_loop(1, LAST, along_bc, 0, unroll=UNROLL_BC)


def inner_diagonal(g0, g1, g2, ms, out, tmp):
    def along_a(b, _):
        s = contract(SQUARED.T, [g0[at(a, b), :] for a in range(N)], 1, INSIDE)
        for a in INSIDE:
            out[at(a, b), :] = s[a] + ms[at(a, b), :]
        return 0

    lax.fori_loop(0, N, along_a, 0, unroll=UNROLL_A)

    def along_bc(a, _):
        t = contract(SQUARED.T, [g2[across(a, c), :] for c in range(N)], 1)
        for c in range(N):
            tmp[across(a, c), :] = t[c]
        s = contract(SQUARED.T, [g1[at(a, b), :] for b in range(N)], 1)
        for b in range(N):
            s[b] = s[b] + out[at(a, b), :]
        for b in range(N):
            out[at(a, b), :] = s[b] + tmp[at(a, b), :]
        return 0

    lax.fori_loop(1, LAST, along_bc, 0, unroll=UNROLL_BC)


def face_terms(v, f, mine, theirs, a_sum, tmp):
    s = contract(DERIV, [v[across(f, c), :] for c in range(N)], -1)
    s = contract(DERIV.T, [s[c] * theirs[part(f, G2, c), :] for c in range(N)], -1)
    for c in range(N):
        tmp[across(f, c), :] = s[c]
    vb = [v[at(f, b), :] for b in range(N)]
    s = contract(DERIV, vb, -1)
    s = contract(DERIV.T, [s[b] * theirs[part(f, G1, b), :] for b in range(N)], -1)
    return [s[b] + a_sum[at(f, b), :] * vb[b] + tmp[at(f, b), :] for b in range(N)]


def face_energy(v, f, theirs, a_sum):
    vb = [v[at(f, b), :] for b in range(N)]
    e = [a_sum[at(f, b), :] * vb[b] * vb[b] for b in range(N)]
    for own, kind in (([v[across(f, c), :] for c in range(N)], G2), (vb, G1)):
        t = contract(DERIV, own, -1)
        e = [e[i] + t[i] * theirs[part(f, kind, i), :] * t[i] for i in range(N)]
    return added_up(e)


def added_up(terms):
    while len(terms) > 1:
        terms = [functools.reduce(plus, terms[i : i + 2]) for i in range(0, len(terms), 2)]
    return terms[0]


def face_sums(f, mine, theirs, diag, a_sum, tmp):
    g = [[mine[part(f, k, i), :] + theirs[part(f, k, i), :] for i in range(N)] for k in (G1, G2)]
    for k in (G1, G2):
        for i in range(N):
            theirs[part(f, k, i), :] = g[k - G1][i]
    s = contract(SQUARED.T, g[1], 1)
    for c in range(N):
        tmp[across(f, c), :] = s[c]
    s = contract(SQUARED.T, g[0], 1)
    for b in range(N):
        a_sum[at(f, b), :] = diag[at(f, b), :] - s[b] - tmp[at(f, b), :]


def couplings(g0, first, out):
    def one(b, _):
        g = [g0[at(a, b), :] for a in range(N)]
        for a_end, row in ((0, first), (LAST, FACE - first)):
            s = contract(DERIV.T, [float(DERIV[m, a_end]) * g[m] for m in range(N)], -1, INSIDE)
            for a in INSIDE:
                out[tile(row * 6 + ((a - 1) * N + b) * N), :] = s[a]
        return 0

    lax.fori_loop(0, N, one, 0, unroll=2)


def couple(v, f, coupling, out, a):
    for b in range(N):
        out[at(a, b), :] = (
            out[at(a, b), :] + coupling[tile(((f * 6 + a - 1) * N + b) * N), :] * v[at(f, b), :]
        )


def lane_pick(x, idx):
    return jnp.take_along_axis(x, idx, axis=1, mode="promise_in_bounds")


def sum_yz(planes, lanes):
    ends = [(v[at(a, 0), :], v[at(a, LAST), :]) for v, a in planes]
    rims = [(v[across(a, 0), :], v[across(a, LAST), :]) for v, a in planes]
    ups = [jnp.where(lanes["up"], pltpu.roll(low, LANES - EL_Z, 1), 0.0) for low, _ in ends]
    downs = [jnp.where(lanes["down"], pltpu.roll(high, EL_Z, 1), 0.0) for _, high in ends]
    nexts = [lane_pick(low, lanes["next"]) for low, _ in rims]
    prevs = [lane_pick(high, lanes["prev"]) for _, high in rims]

    def corners(rim, idx):
        turned = jnp.where(lanes["first"], pltpu.roll(rim, 1, 0), pltpu.roll(rim, LAST, 0))
        return jnp.where(lanes["corner"], lane_pick(turned, idx), 0.0)

    far_nexts = [corners(low, lanes["corner_next"]) for low, _ in rims]
    far_prevs = [corners(high, lanes["corner_prev"]) for _, high in rims]
    for k, (v, a) in enumerate(planes):
        v[across(a, LAST), :] = rims[k][1] + (nexts[k] + far_nexts[k])
        v[across(a, 0), :] = rims[k][0] + (prevs[k] + far_prevs[k])
        v[at(a, LAST), :] = v[at(a, LAST), :] + ups[k]
        v[at(a, 0), :] = v[at(a, 0), :] + downs[k]


def step_kernel(
    load_h, geom_h, mass_h, order_h, p_o, r_o, im_o, al_o,
    coef, g2t, r, dg, z, y, u, tmp,
    mine, theirs, w_mine, w_theirs, i_mine, i_theirs, bag, rf, df, zf, pf, yf, a_sum, tmpf,
    u_ends, cross, q_mine, q_theirs, coupling, acc,
    dots, fold, got_a, got_b, got_one, all_sent, order_v, in_sems, x_send, x_recv, bag_recv, s_recv, one_send, one_recv, hello,
):
    stack = []

    def scope(name):
        if stack:
            stack.pop().__exit__(None, None, None)
        if name:
            stack.append(jax.named_scope(name))
            stack[-1].__enter__()

    scope("enter")
    ys, zs, xs, cores = TORUS
    line, plane_size, count = xs * cores, zs * xs * cores, ys * zs * xs * cores
    me = lax.axis_index("slab")
    core = lax.rem(me, cores)
    in_plane = lax.rem(me, plane_size)

    def greet(sem, who):
        for q in who:
            pl.semaphore_signal(sem, inc=1, device_id=(q,), device_id_type=MESH)

    def heard(sem, who):
        if who:
            pl.semaphore_wait(sem, len(who))

    near_to = me + 1 - 2 * core
    far_to = me + 2 * core - 1
    far_to = jnp.where(far_to < 0, count - 1, jnp.where(far_to == count, 0, far_to))
    in_line = lax.rem(me, line)
    early, late = in_line == 0, in_line == line - 1
    at_turn = in_plane < line
    carrier = (jnp.logical_not(at_turn) & (in_line == 1)) | (at_turn & late)
    carrier_of_late = jnp.where(in_plane == plane_size - 1, me + line - plane_size, me + 2)
    barrier = pltpu.get_barrier_semaphore()
    greet(barrier, [jnp.where(late, carrier_of_late, far_to)])
    loads = [
        pltpu.make_async_copy(src, dst, in_sems.at[k])
        for k, src, dst in (
            (0, order_h, order_v),
            (1, load_h, coef.at[pl.ds(4 * ROWS, ROWS)]),
            (1, geom_h, coef.at[pl.ds(0, 3 * ROWS)]),
            (1, mass_h, coef.at[pl.ds(3 * ROWS, ROWS)]),
        )
    ]
    for copy in loads:
        copy.start()
    g0, g1, g2, ms, ld = (coef.at[pl.ds(k * ROWS, ROWS)] for k in range(5))

    y_at = me // plane_size
    z_at = in_plane // line
    x = in_line // cores

    def moved(dy=0, dz=0, dx=0):
        to = me
        if dy:
            to = to + (lax.rem(y_at + dy, ys) - y_at) * plane_size
        if dz:
            to = to + (lax.rem(z_at + dz, zs) - z_at) * line
        if dx:
            to = to + (lax.rem(x + dx, xs) - x) * cores
        return to

    def ring(size, stop, start=1):
        return sorted({j % size for k in range(start, stop) for j in (k, -k)} - {0})

    sides = (near_to, far_to)
    row_of = (pl.multiple_of((1 - core) * (ROWS - FACE), FACE), pl.multiple_of(core * (ROWS - FACE), FACE))
    face_of = {0: 1 - core, LAST: core}
    carrier_of_early = jnp.where(
        at_turn, lax.rem(y_at + ys - 1, ys) * plane_size + line - 1, me + 1
    )
    early_of_carrier = lax.rem(y_at + 1, ys) * plane_size
    late_of_carrier = jnp.where(at_turn, me + plane_size - line, me - 2)

    y_near = [moved(dy=k) for k in ring(ys, 3)]
    y_far = [moved(dy=k) for k in ring(ys, ys // 2 + 1, 3)]
    greet(barrier, [near_to])
    not_early = jnp.logical_not(early)
    for k in range(1, line):

        @pl.when(in_line != k)
        def _(k=k):
            greet(barrier, [me - in_line + k])

    @pl.when(not_early)
    def _():
        greet(barrier, y_near)

    @pl.when(at_turn & (early | late))
    def _():
        greet(barrier, [jnp.where(early, carrier_of_early, early_of_carrier)])

    def higher(z_to, _):
        greet(barrier, [me + (z_to - z_at) * line + 1 - core])
        return 0

    lax.fori_loop(z_at + 1, zs, higher, 0)
    roots = [r for r in ROOTS if r < count]

    def one_of(device, some):
        return functools.reduce(jnp.logical_or, [device == r for r in some])

    is_root = one_of(me, roots)
    others_than_root = jnp.logical_not(is_root)

    @pl.when(is_root)
    def _():
        width = next(k for k in range(16, 0, -1) if (count - 1) % k == 0)

        def everyone(k, _):
            for i in range(width):
                q = me + 1 + k * width + i
                greet(barrier, [jnp.where(q >= count, q - count, q)])
            return 0

        lax.fori_loop(0, (count - 1) // width, everyone, 0)

    expected = jnp.where(
        early,
        1 + at_turn.astype(jnp.int32),
        (line - 1)
        + len(y_near)
        + 2
        + carrier.astype(jnp.int32)
        + (carrier & at_turn).astype(jnp.int32)
        + 2 * core * z_at,
    )
    expected = expected + len(roots) - is_root.astype(jnp.int32)

    scope("idx")
    loads[0].wait()
    order = jnp.broadcast_to(order_v[...], (8, LANES))
    hit = (
        jnp.broadcast_to(order_v[...], (LANES, LANES))
        == lax.broadcasted_iota(jnp.int32, (LANES, LANES), 0)
    ).astype(jnp.float32)
    lane = lax.broadcasted_iota(jnp.int32, (8, LANES), 1)
    inverse = lax.dot_general(
        lane.astype(jnp.float32), hit, (((1,), (1,)), ((), ())), preferred_element_type=jnp.float32
    )
    inverse = (inverse + 0.5).astype(jnp.int32)
    in_row = lane & (EL_Z - 1)
    lanes = {
        "up": lane < LANES - EL_Z,
        "down": lane >= EL_Z,
        "next": lane - in_row + ((in_row + 1) & (EL_Z - 1)),
        "prev": lane - in_row + ((in_row + EL_Z - 1) & (EL_Z - 1)),
    }
    b_at = lax.broadcasted_iota(jnp.int32, (8, LANES), 0)
    lanes["first"] = b_at == 0
    lanes["corner"] = (lanes["first"] & lanes["down"]) | ((b_at == LAST) & lanes["up"])
    by_y = jnp.where(lanes["first"], LANES - EL_Z, EL_Z)
    lanes["corner_next"] = (lanes["next"] + by_y) & (LANES - 1)
    lanes["corner_prev"] = (lanes["prev"] + by_y) & (LANES - 1)

    def reorder(src, dst, idx, planes=range(N)):
        for a in planes:
            for b in range(N):
                dst[at(a, b), :] = lane_pick(src[at(a, b), :], idx)

    def remote(src, dst, recv, to):
        return pltpu.make_async_remote_copy(
            src_ref=src,
            dst_ref=dst,
            send_sem=x_send,
            recv_sem=recv,
            device_id=(to,),
            device_id_type=MESH,
        )

    def swap(src, dst, f, first, rows, k, carried=None):
        src, dst = src.at[pl.ds(first, rows)], dst.at[pl.ds(first, rows)]
        copy = remote(src, dst, x_recv.at[k], sides[f])
        if carried is None:
            copy.start()
        else:
            by_bag = remote(src, bag.at[pl.ds(carried, rows)], bag_recv.at[1], carrier_of_early)
            pl.when(early)(by_bag.start)
            pl.when(jnp.logical_not(early))(copy.start)
        return copy

    def carry(dst, carried, first, rows, k):
        src, dst = bag.at[pl.ds(carried, rows)], dst.at[pl.ds(first, rows)]
        remote(src, dst, x_recv.at[k], late_of_carrier).start()

    def landed(ref, sem):
        pltpu.make_async_copy(ref, ref, sem).wait()

    @pl.when(early)
    def _():
        pl.semaphore_wait(barrier, expected)
        greet(hello.at[3], [near_to])

    both = (0, LAST)
    faces = (0, 1)
    scope("load_ends")
    pltpu.make_async_copy(coef, coef, in_sems.at[1]).wait()
    for a in both:
        for b in range(N):
            mine[part(face_of[a], LOAD, b), :] = lane_pick(ld[at(a, b), :], inverse)
    for k, a in enumerate(both):
        s = contract(SQUARED.T, [g2[across(a, c), :] for c in range(N)], 1)
        for c in range(N):
            tmpf[across(k, c), :] = s[c]
    for b in range(N):
        s = contract(SQUARED.T, [g0[at(a, b), :] for a in range(N)], 1, both)
        for k, a in enumerate(both):
            yf[at(k, b), :] = s[a]
    for k, a in enumerate(both):
        s = contract(SQUARED.T, [g1[at(a, b), :] for b in range(N)], 1)
        for b in range(N):
            mine[part(face_of[a], DIAG, b), :] = lane_pick(
                s[b] + yf[at(k, b), :] + ms[at(a, b), :] + tmpf[at(k, b), :], inverse
            )
    for a in both:
        for i in range(N):
            mine[part(face_of[a], G1, i), :] = lane_pick(g1[at(a, i), :], inverse)
            mine[part(face_of[a], G2, i), :] = lane_pick(g2[across(a, i), :], inverse)
    sent_near = remote(
        mine.at[pl.ds(0, 4 * FACE)], theirs.at[pl.ds(0, 4 * FACE)], x_recv.at[NEAR], near_to
    )
    beside_early = in_line == 1

    @pl.when(beside_early)
    def _():
        pl.semaphore_wait(hello.at[3], 1)
        sent_near.start()

    scope("barrier")

    @pl.when(not_early)
    def _():
        pl.semaphore_wait(barrier, expected)

    scope("send1")

    @pl.when(carrier)
    def _():
        landed(bag.at[pl.ds(0, 4 * FACE)], bag_recv.at[0])
        carry(theirs, 0, 4 * FACE, 2 * FACE, FAR_LD)
        carry(theirs, 2 * FACE, 6 * FACE, 2 * FACE, FAR_G)

    @pl.when(early)
    def _():
        remote(
            mine.at[pl.ds(4 * FACE, 4 * FACE)],
            bag.at[pl.ds(0, 4 * FACE)],
            bag_recv.at[0],
            carrier_of_early,
        ).start()

    sent_ld, sent_g = (
        remote(mine.at[rows], theirs.at[rows], x_recv.at[k], far_to)
        for k, rows in ((FAR_LD, pl.ds(4 * FACE, 2 * FACE)), (FAR_G, pl.ds(6 * FACE, 2 * FACE)))
    )

    @pl.when(not_early)
    def _():
        sent_ld.start()
        sent_g.start()

    pl.when(jnp.logical_not(beside_early))(sent_near.start)

    @pl.when(not_early)
    def _():
        greet(hello.at[0], y_near)


    @pl.when(core == 1)
    def _():
        def lower(z_to, _):
            greet(hello.at[2], [me + (z_to - z_at) * line])
            return 0

        lax.fori_loop(0, z_at, lower, 0)

    scope("diag")
    inner_diagonal(g0, g1, g2, ms, dg, tmp)
    scope("reorder")
    for a in INSIDE:
        for b in range(N):
            rows = at(a, b)
            dg[rows, :] = lane_pick(dg[rows, :], inverse)
            moved_load = lane_pick(ld[rows, :], inverse)
            ld[rows, :] = moved_load
            r[rows, :] = moved_load
    reorder(g0, g0, inverse)

    @pl.when(carrier)
    def _():
        landed(bag.at[pl.ds(4 * FACE, FACE)], bag_recv.at[1])
        carry(w_theirs, 4 * FACE, FACE, FACE, FAR_W)

    scope("sums")
    sum_yz([(v, a) for a in INSIDE for v in (dg, r)], lanes)

    def inner_z(a, _):
        for b in range(N):
            inv = 1.0 / dg[at(a, b), :]
            dg[at(a, b), :] = inv
            z[at(a, b), :] = inv * r[at(a, b), :]
        return 0

    lax.fori_loop(1, LAST, inner_z, 0, unroll=3)
    for b in range(N):
        g = [float(DERIV[m, 0] * DERIV[m, LAST]) * g0[at(m, b), :] for m in range(N)]
        cross[at(0, b), :] = added_up(g)
    scope("La1")
    stiffness_a(z, g0, y)

    def full(f, b):
        return tile(row_of[f] + b * N)

    def face_z(f):
        for b in range(N):
            rf[at(f, b), :] = mine[part(f, LOAD, b), :] + theirs[part(f, LOAD, b), :]
            total = mine[part(f, DIAG, b), :] + theirs[part(f, DIAG, b), :]
            a_sum[at(f, b), :] = total
            df[at(f, b), :] = total
        sum_yz([(rf, f), (df, f)], lanes)
        for b in range(N):
            inv = 1.0 / df[at(f, b), :]
            df[at(f, b), :] = inv
            zf[at(f, b), :] = inv * rf[at(f, b), :]

    def tell(f, k, carried=None):
        for b in range(N):
            w_mine[at(f, b), :] = y[full(f, b), :] + cross[at(0, b), :] * zf[at(1 - f, b), :]
        sum_yz([(w_mine, f)], lanes)
        return swap(w_mine, w_theirs, f, f * FACE, FACE, k, carried)

    scope("x_near")
    sent_near.wait_recv()
    scope("z_near")
    face_z(0)
    sent_w = [None, tell(1, FAR_W, 4 * FACE)]
    scope("reorder2")
    reorder(g1, g1, inverse, INSIDE)
    for a in INSIDE:
        for c in range(N):
            g2t[at(a, c), :] = lane_pick(g2[across(a, c), :], inverse)
    reorder(ms, ms, inverse, INSIDE)
    scope("Lbc1")
    stiffness_bc(z, g1, g2t, ms, y, tmp, y)
    scope("hello")

    @pl.when(not_early)
    def _():
        heard(hello.at[0], y_near)
        greet(hello.at[1], y_far)

    scope("g_near")
    first = pl.multiple_of((1 - core) * FACE, FACE)
    couplings(g0, first, coupling)
    loop(1, LAST, lambda a: couple(zf, 0, coupling, y, a))
    face_sums(0, mine, theirs, a_sum, a_sum, tmpf)
    s = face_terms(zf, 0, mine, theirs, a_sum, tmpf)
    for b in range(N):
        yf[at(0, b), :] = s[b]
    sum_yz([(yf, 0)], lanes)
    scope("x_far")
    sent_ld.wait_recv()
    scope("z_far")
    face_z(1)

    scope("inner2")
    for a in INSIDE:
        couple(zf, 1, coupling, y, a)
    sum_yz([(y, a) for a in INSIDE], lanes)
    zero = jnp.zeros((8, LANES), jnp.float32)

    def inner_p(a, num):
        for b in range(N):
            rows = at(a, b)
            p = COEF_Z * z[rows, :] - COEF_Q * (dg[rows, :] * y[rows, :])
            z[rows, :] = p
            num[b % 4] = num[b % 4] + ld[rows, :] * p
        return num

    num = lax.fori_loop(1, LAST, inner_p, [zero] * 4, unroll=True)
    scope("L2")
    den = energy_bc(z, g1, g2t, ms, [zero] * 4)
    den = energy_a(z, g0, u_ends, first, den)
    num, den = added_up(num), added_up(den)
    sent_w[0] = tell(0, NEAR_W)
    scope("g_far")
    sent_g.wait_recv()
    face_sums(1, mine, theirs, a_sum, a_sum, tmpf)
    s = face_terms(zf, 1, mine, theirs, a_sum, tmpf)
    for b in range(N):
        yf[at(1, b), :] = s[b]
    sum_yz([(yf, 1)], lanes)

    def face_p(f):
        for b in range(N):
            rows = at(f, b)
            total = yf[rows, :] + (w_mine[rows, :] + w_theirs[rows, :])
            pf[rows, :] = COEF_Z * zf[rows, :] - COEF_Q * (df[rows, :] * total)

    def face_dot(kind, f):
        return added_up([kind[part(f, LOAD, b), :] * pf[at(f, b), :] for b in range(N)])

    acc[tile(0), :] = num
    acc[tile(8), :] = den
    takes = jnp.where(2 * x >= xs, core, 1 - core) == 1
    gives = jnp.logical_not(takes)
    sent_q = remote(q_mine, q_theirs, x_recv.at[NEAR_W], near_to)
    scope("w_near")

    @pl.when(takes)
    def _():
        landed(w_mine, x_recv.at[NEAR_W])
        face_p(0)
        acc[tile(0), :] = acc[tile(0), :] + (face_dot(mine, 0) + face_dot(theirs, 0))
        terms = [
            (2.0 * u_ends[at(0, b), :] + q_theirs[at(0, b), :]) * pf[at(0, b), :] for b in range(N)
        ]
        acc[tile(8), :] = acc[tile(8), :] + (face_energy(pf, 0, theirs, a_sum) + added_up(terms))
        for b in range(N):
            q_mine[at(0, b), :] = 2.0 * cross[at(0, b), :] * pf[at(0, b), :]

    scope("w_far")
    sent_w[1].wait_recv()
    scope("ends2")
    face_p(1)
    acc[tile(0), :] = acc[tile(0), :] + face_dot(mine, 1)
    terms = [2.0 * u_ends[at(1, b), :] * pf[at(1, b), :] for b in range(N)]
    acc[tile(8), :] = acc[tile(8), :] + (0.5 * face_energy(pf, 1, theirs, a_sum) + added_up(terms))

    @pl.when(takes)
    def _():
        terms = [q_mine[at(0, b), :] * pf[at(1, b), :] for b in range(N)]
        acc[tile(8), :] = acc[tile(8), :] + added_up(terms)

    @pl.when(gives)
    def _():
        for b in range(N):
            q_mine[at(0, b), :] = 2.0 * (
                u_ends[at(0, b), :] + cross[at(0, b), :] * pf[at(1, b), :]
            )
        sent_q.start()

    num_row = jnp.sum(acc[tile(0), :], axis=0, keepdims=True)
    den_row = jnp.sum(acc[tile(8), :], axis=0, keepdims=True)
    dots[0, 0:1, :] = num_row
    dots[0, 1:2, :] = den_row
    half = LANES // 2
    first_half = lane[0:1, :] < half
    fold[0] = jnp.where(
        first_half, num_row + pltpu.roll(num_row, half, 1), den_row + pltpu.roll(den_row, half, 1)
    )
    hops = sorted(
        ((dy, dx) for dy in range(ys) for dx in range(xs) if dy or dx),
        key=lambda d: -min(d[0], ys - d[0]) - min(d[1], xs - d[1]),
    )
    others = 2 * len(hops) + 1

    def send(src, dst, k, to):
        copy = pltpu.make_async_remote_copy(
            src_ref=src,
            dst_ref=dst,
            send_sem=x_send,
            recv_sem=s_recv.at[k],
            device_id=(to,),
            device_id_type=MESH,
        )
        copy.start()

    def arrived(ref, sem):
        pltpu.make_async_copy(ref, ref, sem).wait()

    def added(ref, first, total):
        part = [first, None, None, None]
        for j in range(total):
            part[j % 4] = plus(part[j % 4], ref[j])
        return functools.reduce(plus, [t for t in part if t is not None])

    half_z, pair_z = zs // 2, zs // 2 + zs // 8
    in_first = y_at * line + in_line
    slow_low = (z_at == pair_z) & (x == xs - 1) & (core == 1)
    slow_high = (z_at == pair_z + 1) & (x == 0) & (core == 0)
    slow_ones = ys * (2 if pair_z + 1 < zs else 1)
    slow_before = jnp.where(
        z_at > pair_z + 1,
        slow_ones,
        jnp.where(
            z_at == pair_z + 1,
            ys + y_at + (in_line > 0).astype(jnp.int32),
            jnp.where(z_at == pair_z, y_at, 0),
        ),
    )
    slot = jnp.where(
        slow_low | slow_high,
        count - slow_ones + jnp.where(slow_high, ys, 0) + y_at,
        z_at * ys * line + in_first - slow_before,
    )
    group = jnp.where(slow_low | slow_high, 2, jnp.where(z_at < half_z, 0, 1))
    group_0 = half_z * ys * line - 1
    groups = (group_0, count - 1 - group_0 - slow_ones, slow_ones)

    def root_sum(k, total):
        width, start, number = 16, sum(groups[:k]), groups[k]
        arrived(got_one.at[pl.ds(start, number)], one_recv.at[k])
        sums = [total] + [jnp.zeros((1, LANES), jnp.float32)] * 7

        def some(i, sums):
            return [
                sums[j] + got_one[start + i * width + j] + got_one[start + i * width + j + 8]
                for j in range(8)
            ]

        whole = number // width
        sums = lax.fori_loop(0, whole, some, sums)
        for i in range(whole * width, number):
            sums[i % 8] = sums[i % 8] + got_one[start + i]
        return added_up(sums)

    def send_to_root(r):
        at_root = r // plane_size * line + r % line

        @pl.when(me != r)
        def _():
            pltpu.make_async_remote_copy(
                src_ref=fold.at[0],
                dst_ref=got_one.at[slot - (slot > at_root).astype(jnp.int32)],
                send_sem=one_send,
                recv_sem=one_recv.at[group],
                device_id=(r,),
                device_id_type=MESH,
            ).start()

    send_to_root(roots[0])

    @pl.when(not_early)
    def _():
        heard(hello.at[1], y_far)

    @pl.when(beside_early)
    def _():
        greet(hello.at[0], [near_to])

    @pl.when(early)
    def _():
        pl.semaphore_wait(hello.at[0], 1)

    for j, (dy, dx) in enumerate(hops):
        send(dots.at[0], got_a.at[2 * j + core], 0, moved(dy=dy, dx=dx) + 1 - core)

    @pl.when(core == 0)
    def _():
        send(dots.at[0], got_a.at[others - 1], 0, me + 1)

    for other_root in roots[1:]:
        send_to_root(other_root)

    scope("u_ends")

    @pl.when(gives)
    def _():
        sent_w[0].wait_recv()
        face_p(0)

    for f in faces:
        for b in range(N):
            i_mine[at(f, b), :] = u_ends[at(f, b), :] + cross[at(0, b), :] * pf[at(1 - f, b), :]
        swap(i_mine, i_theirs, f, f * FACE, FACE, IMAGE)
    for f in faces:
        s = face_terms(pf, f, mine, theirs, a_sum, tmpf)
        for b in range(N):
            yf[at(f, b), :] = s[b]
    stiffness_bc(z, g1, g2t, ms, y, tmp)
    stiffness_a(z, g0, u, INSIDE, y)

    def couple_both(a):
        couple(pf, 0, coupling, u, a)
        couple(pf, 1, coupling, u, a)

    loop(1, LAST, couple_both)
    scope("out_p_r")
    for src, ends, dst in ((z, pf, p_o), (r, rf, r_o)):
        reorder(src, dst, order, INSIDE)
        for f in faces:
            for b in range(N):
                dst[full(f, b), :] = lane_pick(ends[at(f, b), :], order)
    sum_yz([(u, a) for a in INSIDE], lanes)
    reorder(u, im_o, order, INSIDE)
    scope("root_0")

    @pl.when(is_root)
    def _():
        fold[1] = root_sum(0, fold[0])

    scope("plane")
    first_of_column = me - z_at * line
    skip_0 = one_of(first_of_column - 1, [r for r in roots if r % cores == 0] or [-1])
    skip_1 = one_of(first_of_column, [r for r in roots if r % cores == 1])

    @pl.when(core == 1)
    def _():
        arrived(got_a.at[pl.ds(0, others)], s_recv.at[0])
        dots[1] = added(got_a, dots[0], others)

        @pl.when(z_at < zs - 1)
        def _():
            pl.semaphore_wait(hello.at[2], zs - 1 - z_at)

        for k in sorted(range(1, zs), key=lambda k: -min(k, zs - k)):
            to_first = z_at == zs - k
            for c, skip in ((1, skip_0), (0, skip_1)):

                @pl.when(jnp.logical_not(to_first & skip))
                def _(k=k, c=c):
                    send(dots.at[1], got_b.at[k - 1], 1, moved(dz=k) - c)

        @pl.when(jnp.logical_not((z_at == 0) & skip_0))
        def _():
            send(dots.at[1], got_b.at[zs - 1], 1, me - 1)

        got_b[zs - 1] = dots[1]

    scope("x3")
    landed(i_theirs, x_recv.at[IMAGE])
    for f in faces:
        for b in range(N):
            rows = at(f, b)
            yf[rows, :] = yf[rows, :] + (i_mine[rows, :] + i_theirs[rows, :])
    sum_yz([(yf, f) for f in faces], lanes)
    for f in faces:
        for b in range(N):
            im_o[full(f, b), :] = lane_pick(yf[at(f, b), :], order)
    face_rows = FACE // 2
    skipped = jnp.where(
        core == 1,
        skip_0.astype(jnp.int32) + jnp.where(z_at > 0, skip_1.astype(jnp.int32), 0),
        0,
    )
    sums_0, sums_1 = len(hops) + 1, len(hops) + 2 * zs - 1
    kinds = [(takes & jnp.logical_not(carrier), 12), (gives & jnp.logical_not(carrier), 13)]
    kinds += [(carrier & takes, 17), (carrier & gives, 18)]

    def all_left(who, to_roots):
        for faces_sent, face_count in kinds:
            for c, most, left_out in ((0, sums_0, 1), (1, sums_1, 3)):
                for less in range(left_out):

                    @pl.when(faces_sent & (core == c) & (skipped == less) & who)
                    def _(sent=most - less + face_count * face_rows):
                        arrived(all_sent.at[pl.ds(0, sent)], x_send)

        @pl.when(who)
        def _():
            arrived(got_one.at[pl.ds(0, to_roots)], one_send)

    all_left(others_than_root, len(roots))

    scope("lines")

    @pl.when((core == 0) & others_than_root)
    def _():
        arrived(got_b, s_recv.at[1])

    @pl.when((core == 1) & others_than_root)
    def _():
        arrived(got_b.at[pl.ds(0, zs - 1)], s_recv.at[1])

    @pl.when(others_than_root)
    def _():
        dots[2] = added(got_b, None, zs)

    @pl.when(is_root)
    def _():
        both_sums = root_sum(2, root_sum(1, fold[1]))
        dots[2, 0:1, :] = jnp.where(first_half, both_sums, 0.0)
        dots[2, 1:2, :] = jnp.where(first_half, 0.0, both_sums)

    total = dots[2]
    scope("alpha")
    sums = jnp.sum(total, axis=1, keepdims=True)
    al_o[...] = jnp.broadcast_to(sums[0:1, :] / sums[1:2, :], (8, LANES))
    all_left(is_root, len(roots) - 1)
    scope(None)


CHUNKS = 4


def finish_kernel(p, r, im, al, x_h, r_h, both, sem):
    alpha = al[...]
    size = ROWS // CHUNKS
    for k in range(CHUNKS):
        for i in range(k * size, (k + 1) * size, N):
            both[tile(i), :] = alpha * p[tile(i), :]
        pltpu.make_async_copy(both.at[pl.ds(k * size, size)], x_h.at[pl.ds(k * size, size)], sem).start()
        for i in range(k * size, (k + 1) * size, N):
            both[tile(ROWS + i), :] = r[tile(i), :] - alpha * im[tile(i), :]
        rows = pl.ds(ROWS + k * size, size)
        pltpu.make_async_copy(both.at[rows], r_h.at[pl.ds(k * size, size)], sem).start()
    pltpu.make_async_copy(both, both, sem).wait()


def on_device(load_terms, geometry, mass_terms, element_order):
    flat = jax.ShapeDtypeStruct((ROWS, LANES), jnp.float32)
    vm = lambda *shape: pltpu.VMEM(shape, jnp.float32)
    field = vm(ROWS, LANES)
    pair = vm(2 * FACE, LANES)
    ys, zs, xs, cores = TORUS
    in_vmem = pl.BlockSpec(memory_space=pltpu.VMEM)
    in_hbm = pl.BlockSpec(memory_space=pltpu.HBM)
    parts = pl.pallas_call(
        step_kernel,
        out_shape=(field, field, field, vm(8, LANES)),
        in_specs=[in_hbm] * 4,
        out_specs=[in_vmem] * 4,
        scratch_shapes=[
            vm(5 * ROWS, LANES), *[field] * 7,
            *[vm(8 * FACE, LANES)] * 2,
            *[pair] * 4, vm(5 * FACE, LANES), *[pair] * 8, *[vm(FACE, LANES)] * 3,
            vm(12 * FACE, LANES), vm(16, LANES),
            vm(3, 2, LANES), vm(2, 1, LANES), vm(2 * ys * xs - 1, 2, LANES), vm(zs, 2, LANES),
            vm(ys * zs * xs * cores - 1, 1, LANES),
            vm(18 * FACE // 2 + ys * xs + 2 * zs + len(ROOTS), 2, LANES),
            pltpu.VMEM((1, LANES), jnp.int32),
            pltpu.SemaphoreType.DMA((2,)),
            pltpu.SemaphoreType.DMA(()),
            pltpu.SemaphoreType.DMA((6,)),
            pltpu.SemaphoreType.DMA((2,)),
            pltpu.SemaphoreType.DMA((2,)),
            pltpu.SemaphoreType.DMA(()),
            pltpu.SemaphoreType.DMA((3,)),
            pltpu.SemaphoreType.REGULAR((4,)),
        ],
        compiler_params=pltpu.CompilerParams(
            collective_id=0, has_side_effects=True, vmem_limit_bytes=24 << 20
        ),
        name="cg_step",
    )(
        *[
            pltpu.with_memory_space_constraint(t, pltpu.HBM)
            for t in (
                load_terms.reshape(ROWS, LANES),
                geometry.reshape(3 * ROWS, LANES),
                mass_terms.reshape(ROWS, LANES),
                element_order,
            )
        ]
    )
    x, res = pl.pallas_call(
        finish_kernel,
        out_shape=(flat, flat),
        in_specs=[in_vmem] * 4,
        out_specs=[in_hbm] * 2,
        scratch_shapes=[vm(2 * ROWS, LANES), pltpu.SemaphoreType.DMA(())],
        compiler_params=pltpu.CompilerParams(vmem_limit_bytes=8 << 20),
        name="cg_finish",
    )(*[pltpu.with_memory_space_constraint(t, pltpu.VMEM) for t in parts])
    shape = load_terms.shape
    return x.reshape(shape), res.reshape(shape)


def solution(mesh):
    last = P(None, None, None, "slab")
    return jax.shard_map(
        on_device,
        mesh=mesh,
        in_specs=(last, P(None, None, None, None, "slab"), last, P("slab", None)),
        out_specs=(last, last),
        check_vma=False,
    )
```

```python
import functools

import jax
import jax.numpy as jnp
import numpy as np
from jax import lax
from jax.experimental import pallas as pl
from jax.experimental.pallas import tpu as pltpu
from jax.sharding import PartitionSpec as P

N = 8
LAST = N - 1
EL_Y = 8
EL_Z = 16
LANES = 128
ROWS = N * N * N
FACE = N * N
CENTRE = 1.65
HALF = 1.35
MESH = pl.DeviceIdType.MESH
TORUS = (8, 12, 4, 2)
ROOTS = (1, 3, 97, 2, 96, 7, 193, 192, 5, 6)
INSIDE = range(1, LAST)
UNROLL_A = 4
UNROLL_BC = 3


def legendre_table(positions, points):
    columns = [positions * 0.0 + 1.0, positions]
    for degree in range(2, points):
        columns.append(
            ((2 * degree - 1) * positions * columns[-1] - (degree - 1) * columns[-2]) / degree
        )
    return np.stack(columns, axis=1)


def gll_derivative(points):
    degree = points - 1
    nodes = -np.cos(np.pi * np.arange(points) / degree)
    for _ in range(100):
        legendre = legendre_table(nodes, points)
        nodes = nodes - (nodes * legendre[:, degree] - legendre[:, degree - 1]) / (
            points * legendre[:, degree]
        )
    legendre = legendre_table(nodes, points)
    top = legendre[:, degree]
    same = np.eye(points, dtype=bool)
    spacing = np.where(same, 1.0, nodes[:, None] - nodes[None, :])
    table = np.where(same, 0.0, top[:, None] / (top[None, :] * spacing))
    table[0, 0] = -degree * points / 4.0
    table[degree, degree] = degree * points / 4.0
    return table


DERIV = gll_derivative(N).astype(np.float32).astype(np.float64)
SQUARED = DERIV * DERIV
SIGMA = CENTRE / HALF
RHO0 = 1.0 / SIGMA
RHO1 = 1.0 / (2.0 * SIGMA - RHO0)
COEF_Z = (1.0 + RHO1 * RHO0) / CENTRE + 2.0 * RHO1 / HALF
COEF_Q = 2.0 * RHO1 / HALF / CENTRE


def plus(x, y):
    return y if x is None else x + y


def contract(table, terms, sign, rows=range(N)):
    used = [j for j in range(N // 2) if terms[j] is not None]
    even = {j: terms[j] + terms[LAST - j] for j in used}
    odd = {j: terms[j] - terms[LAST - j] for j in used}
    out = [None] * N
    for i in range(N // 2):
        if i not in rows and LAST - i not in rows:
            continue
        e = o = None
        for j in used:
            e = plus(e, float(table[i, j] + table[i, LAST - j]) / 2 * even[j])
            o = plus(o, float(table[i, j] - table[i, LAST - j]) / 2 * odd[j])
        if i in rows:
            out[i] = e + o
        if LAST - i in rows:
            out[LAST - i] = (o - e) if sign < 0 else (e - o)
    return out


def tile(row):
    return pl.ds(row if isinstance(row, int) else pl.multiple_of(row, 8), 8)


def at(a, b):
    return tile((a * N + b) * N)


def across(a, c):
    return pl.ds(a * FACE + c, N, stride=N)


LOAD, DIAG, G1, G2 = range(4)
NEAR, FAR_LD, FAR_G, NEAR_W, FAR_W, IMAGE = range(6)


def part(f, kind, i):
    return tile(((f * 4 + kind) * N + i) * N)


def loop(start, stop, body):
    lax.fori_loop(start, stop, lambda i, _: (body(i), 0)[1], 0)


def stiffness_a(v, g0, out, rows=range(N), more=None):
    def along_a(b, _):
        va = [v[at(a, b), :] if a in INSIDE else None for a in range(N)]
        s = contract(DERIV, va, -1)
        s = contract(DERIV.T, [s[a] * g0[at(a, b), :] for a in range(N)], -1, rows)
        for a in rows:
            out[at(a, b), :] = s[a] if more is None else s[a] + more[at(a, b), :]
        return 0

    lax.fori_loop(0, N, along_a, 0, unroll=UNROLL_A)


def energy_a(v, g0, ends, first, total):
    def along_a(b, total):
        t = contract(DERIV, [v[at(a, b), :] if a in INSIDE else None for a in range(N)], -1)
        s = [t[a] * g0[at(a, b), :] for a in range(N)]
        total = [total[k] + s[k] * t[k] + s[k + 4] * t[k + 4] for k in range(4)]
        s = contract(DERIV.T, s, -1, (0, LAST))
        ends[tile(first + b * N), :] = s[0]
        ends[tile(FACE - first + b * N), :] = s[LAST]
        return total

    return lax.fori_loop(0, N, along_a, total, unroll=UNROLL_A)


def energy_bc(v, g1, g2t, ms, total):
    def along_bc(a, total):
        vb = [v[at(a, b), :] for b in range(N)]
        for own, g in (([v[across(a, c), :] for c in range(N)], g2t), (vb, g1)):
            t = contract(DERIV, own, -1)
            e = [t[i] * g[at(a, i), :] * t[i] for i in range(N)]
            total = [total[k] + (e[k] + e[k + 4]) for k in range(4)]
        e = [vb[b] * ms[at(a, b), :] * vb[b] for b in range(N)]
        return [total[k] + (e[k] + e[k + 4]) for k in range(4)]

    return lax.fori_loop(1, LAST, along_bc, total, unroll=UNROLL_BC)


def stiffness_bc(v, g1, g2t, ms, out, tmp, more=None):
    def along_bc(a, _):
        vt = [v[across(a, c), :] for c in range(N)]
        vb = [v[at(a, b), :] for b in range(N)]
        t = contract(DERIV, vt, -1)
        t = contract(DERIV.T, [t[c] * g2t[at(a, c), :] for c in range(N)], -1)
        for c in range(N):
            tmp[across(a, c), :] = t[c]
        s = contract(DERIV, vb, -1)
        s = contract(DERIV.T, [s[b] * g1[at(a, b), :] for b in range(N)], -1)
        for b in range(N):
            s[b] = s[b] + ms[at(a, b), :] * vb[b]
            if more is not None:
                s[b] = s[b] + more[at(a, b), :]
        for b in range(N):
            out[at(a, b), :] = s[b] + tmp[at(a, b), :]
        return 0

    lax.fori_loop(1, LAST, along_bc, 0, unroll=UNROLL_BC)


def inner_diagonal(g0, g1, g2, ms, out, tmp):
    def along_a(b, _):
        s = contract(SQUARED.T, [g0[at(a, b), :] for a in range(N)], 1, INSIDE)
        for a in INSIDE:
            out[at(a, b), :] = s[a] + ms[at(a, b), :]
        return 0

    lax.fori_loop(0, N, along_a, 0, unroll=UNROLL_A)

    def along_bc(a, _):
        t = contract(SQUARED.T, [g2[across(a, c), :] for c in range(N)], 1)
        for c in range(N):
            tmp[across(a, c), :] = t[c]
        s = contract(SQUARED.T, [g1[at(a, b), :] for b in range(N)], 1)
        for b in range(N):
            s[b] = s[b] + out[at(a, b), :]
        for b in range(N):
            out[at(a, b), :] = s[b] + tmp[at(a, b), :]
        return 0

    lax.fori_loop(1, LAST, along_bc, 0, unroll=UNROLL_BC)


def face_terms(v, f, mine, theirs, a_sum, tmp):
    s = contract(DERIV, [v[across(f, c), :] for c in range(N)], -1)
    s = contract(DERIV.T, [s[c] * theirs[part(f, G2, c), :] for c in range(N)], -1)
    for c in range(N):
        tmp[across(f, c), :] = s[c]
    vb = [v[at(f, b), :] for b in range(N)]
    s = contract(DERIV, vb, -1)
    s = contract(DERIV.T, [s[b] * theirs[part(f, G1, b), :] for b in range(N)], -1)
    return [s[b] + a_sum[at(f, b), :] * vb[b] + tmp[at(f, b), :] for b in range(N)]


def face_energy(v, f, theirs, a_sum):
    vb = [v[at(f, b), :] for b in range(N)]
    e = [a_sum[at(f, b), :] * vb[b] * vb[b] for b in range(N)]
    for own, kind in (([v[across(f, c), :] for c in range(N)], G2), (vb, G1)):
        t = contract(DERIV, own, -1)
        e = [e[i] + t[i] * theirs[part(f, kind, i), :] * t[i] for i in range(N)]
    return added_up(e)


def added_up(terms):
    while len(terms) > 1:
        terms = [functools.reduce(plus, terms[i : i + 2]) for i in range(0, len(terms), 2)]
    return terms[0]


def face_sums(f, mine, theirs, diag, a_sum, tmp):
    g = [[mine[part(f, k, i), :] + theirs[part(f, k, i), :] for i in range(N)] for k in (G1, G2)]
    for k in (G1, G2):
        for i in range(N):
            theirs[part(f, k, i), :] = g[k - G1][i]
    s = contract(SQUARED.T, g[1], 1)
    for c in range(N):
        tmp[across(f, c), :] = s[c]
    s = contract(SQUARED.T, g[0], 1)
    for b in range(N):
        a_sum[at(f, b), :] = diag[at(f, b), :] - s[b] - tmp[at(f, b), :]


def couplings(g0, first, out):
    def one(b, _):
        g = [g0[at(a, b), :] for a in range(N)]
        for a_end, row in ((0, first), (LAST, FACE - first)):
            s = contract(DERIV.T, [float(DERIV[m, a_end]) * g[m] for m in range(N)], -1, INSIDE)
            for a in INSIDE:
                out[tile(row * 6 + ((a - 1) * N + b) * N), :] = s[a]
        return 0

    lax.fori_loop(0, N, one, 0, unroll=2)


def couple(v, f, coupling, out, a):
    for b in range(N):
        out[at(a, b), :] = (
            out[at(a, b), :] + coupling[tile(((f * 6 + a - 1) * N + b) * N), :] * v[at(f, b), :]
        )


def lane_pick(x, idx):
    return jnp.take_along_axis(x, idx, axis=1, mode="promise_in_bounds")


def sum_yz(planes, lanes):
    ends = [(v[at(a, 0), :], v[at(a, LAST), :]) for v, a in planes]
    rims = [(v[across(a, 0), :], v[across(a, LAST), :]) for v, a in planes]
    ups = [jnp.where(lanes["up"], pltpu.roll(low, LANES - EL_Z, 1), 0.0) for low, _ in ends]
    downs = [jnp.where(lanes["down"], pltpu.roll(high, EL_Z, 1), 0.0) for _, high in ends]
    nexts = [lane_pick(low, lanes["next"]) for low, _ in rims]
    prevs = [lane_pick(high, lanes["prev"]) for _, high in rims]

    def corners(rim, idx):
        turned = jnp.where(lanes["first"], pltpu.roll(rim, 1, 0), pltpu.roll(rim, LAST, 0))
        return jnp.where(lanes["corner"], lane_pick(turned, idx), 0.0)

    far_nexts = [corners(low, lanes["corner_next"]) for low, _ in rims]
    far_prevs = [corners(high, lanes["corner_prev"]) for _, high in rims]
    for k, (v, a) in enumerate(planes):
        v[across(a, LAST), :] = rims[k][1] + (nexts[k] + far_nexts[k])
        v[across(a, 0), :] = rims[k][0] + (prevs[k] + far_prevs[k])
        v[at(a, LAST), :] = v[at(a, LAST), :] + ups[k]
        v[at(a, 0), :] = v[at(a, 0), :] + downs[k]


def step_kernel(
    load_h, geom_h, mass_h, order_h, p_o, r_o, im_o, al_o,
    coef, g2t, r, dg, z, y, u, tmp,
    mine, theirs, w_mine, w_theirs, i_mine, i_theirs, bag, rf, df, zf, pf, yf, a_sum, tmpf,
    u_ends, cross, q_mine, q_theirs, coupling, acc,
    dots, fold, got_a, got_b, got_one, got_two, all_sent, order_v, in_sems, x_send, x_recv, bag_recv, s_recv, one_send, hello,
):
    stack = []

    def scope(name):
        if stack:
            stack.pop().__exit__(None, None, None)
        if name:
            stack.append(jax.named_scope(name))
            stack[-1].__enter__()

    scope("enter")
    ys, zs, xs, cores = TORUS
    line, plane_size, count = xs * cores, zs * xs * cores, ys * zs * xs * cores
    me = lax.axis_index("slab")
    core = lax.rem(me, cores)
    in_plane = lax.rem(me, plane_size)

    def greet(sem, who):
        for q in who:
            pl.semaphore_signal(sem, inc=1, device_id=(q,), device_id_type=MESH)

    def heard(sem, who):
        if who:
            pl.semaphore_wait(sem, len(who))

    near_to = me + 1 - 2 * core
    far_to = me + 2 * core - 1
    far_to = jnp.where(far_to < 0, count - 1, jnp.where(far_to == count, 0, far_to))
    in_line = lax.rem(me, line)
    early, late = in_line == 0, in_line == line - 1
    at_turn = in_plane < line
    carrier = (jnp.logical_not(at_turn) & (in_line == 1)) | (at_turn & late)
    carrier_of_late = jnp.where(in_plane == plane_size - 1, me + line - plane_size, me + 2)
    barrier = pltpu.get_barrier_semaphore()
    greet(barrier, [jnp.where(late, carrier_of_late, far_to)])
    loads = [
        pltpu.make_async_copy(src, dst, in_sems.at[k])
        for k, src, dst in (
            (0, order_h, order_v),
            (1, load_h, coef.at[pl.ds(4 * ROWS, ROWS)]),
            (1, geom_h, coef.at[pl.ds(0, 3 * ROWS)]),
            (1, mass_h, coef.at[pl.ds(3 * ROWS, ROWS)]),
        )
    ]
    for copy in loads:
        copy.start()
    g0, g1, g2, ms, ld = (coef.at[pl.ds(k * ROWS, ROWS)] for k in range(5))

    y_at = me // plane_size
    z_at = in_plane // line
    x = in_line // cores

    def moved(dy=0, dz=0, dx=0):
        to = me
        if dy:
            to = to + (lax.rem(y_at + dy, ys) - y_at) * plane_size
        if dz:
            to = to + (lax.rem(z_at + dz, zs) - z_at) * line
        if dx:
            to = to + (lax.rem(x + dx, xs) - x) * cores
        return to

    def ring(size, stop, start=1):
        return sorted({j % size for k in range(start, stop) for j in (k, -k)} - {0})

    sides = (near_to, far_to)
    row_of = (pl.multiple_of((1 - core) * (ROWS - FACE), FACE), pl.multiple_of(core * (ROWS - FACE), FACE))
    face_of = {0: 1 - core, LAST: core}
    carrier_of_early = jnp.where(
        at_turn, lax.rem(y_at + ys - 1, ys) * plane_size + line - 1, me + 1
    )
    early_of_carrier = lax.rem(y_at + 1, ys) * plane_size
    late_of_carrier = jnp.where(at_turn, me + plane_size - line, me - 2)

    y_near = [moved(dy=k) for k in ring(ys, 3)]
    y_far = [moved(dy=k) for k in ring(ys, ys // 2 + 1, 3)]
    greet(barrier, [near_to])
    not_early = jnp.logical_not(early)
    for k in range(1, line):

        @pl.when(in_line != k)
        def _(k=k):
            greet(barrier, [me - in_line + k])

    @pl.when(not_early)
    def _():
        greet(barrier, y_near)

    @pl.when(at_turn & (early | late))
    def _():
        greet(barrier, [jnp.where(early, carrier_of_early, early_of_carrier)])

    def higher(z_to, _):
        greet(barrier, [me + (z_to - z_at) * line + 1 - core])
        return 0

    lax.fori_loop(z_at + 1, zs, higher, 0)
    roots = [r for r in ROOTS if r < count]

    def one_of(device, some):
        return functools.reduce(jnp.logical_or, [device == r for r in some])

    is_root = one_of(me, roots)
    others_than_root = jnp.logical_not(is_root)

    @pl.when(is_root)
    def _():
        width = next(k for k in range(16, 0, -1) if (count - 1) % k == 0)

        def everyone(k, _):
            for i in range(width):
                q = me + 1 + k * width + i
                greet(barrier, [jnp.where(q >= count, q - count, q)])
            return 0

        lax.fori_loop(0, (count - 1) // width, everyone, 0)

    expected = jnp.where(
        early,
        1 + at_turn.astype(jnp.int32),
        (line - 1)
        + len(y_near)
        + 2
        + carrier.astype(jnp.int32)
        + (carrier & at_turn).astype(jnp.int32)
        + 2 * core * z_at,
    )
    expected = expected + len(roots) - is_root.astype(jnp.int32)

    scope("idx")
    loads[0].wait()
    order = jnp.broadcast_to(order_v[...], (8, LANES))
    hit = (
        jnp.broadcast_to(order_v[...], (LANES, LANES))
        == lax.broadcasted_iota(jnp.int32, (LANES, LANES), 0)
    ).astype(jnp.float32)
    lane = lax.broadcasted_iota(jnp.int32, (8, LANES), 1)
    inverse = lax.dot_general(
        lane.astype(jnp.float32), hit, (((1,), (1,)), ((), ())), preferred_element_type=jnp.float32
    )
    inverse = (inverse + 0.5).astype(jnp.int32)
    in_row = lane & (EL_Z - 1)
    lanes = {
        "up": lane < LANES - EL_Z,
        "down": lane >= EL_Z,
        "next": lane - in_row + ((in_row + 1) & (EL_Z - 1)),
        "prev": lane - in_row + ((in_row + EL_Z - 1) & (EL_Z - 1)),
    }
    b_at = lax.broadcasted_iota(jnp.int32, (8, LANES), 0)
    lanes["first"] = b_at == 0
    lanes["corner"] = (lanes["first"] & lanes["down"]) | ((b_at == LAST) & lanes["up"])
    by_y = jnp.where(lanes["first"], LANES - EL_Z, EL_Z)
    lanes["corner_next"] = (lanes["next"] + by_y) & (LANES - 1)
    lanes["corner_prev"] = (lanes["prev"] + by_y) & (LANES - 1)

    def reorder(src, dst, idx, planes=range(N)):
        for a in planes:
            for b in range(N):
                dst[at(a, b), :] = lane_pick(src[at(a, b), :], idx)

    def remote(src, dst, recv, to):
        return pltpu.make_async_remote_copy(
            src_ref=src,
            dst_ref=dst,
            send_sem=x_send,
            recv_sem=recv,
            device_id=(to,),
            device_id_type=MESH,
        )

    def swap(src, dst, f, first, rows, k, carried=None):
        src, dst = src.at[pl.ds(first, rows)], dst.at[pl.ds(first, rows)]
        copy = remote(src, dst, x_recv.at[k], sides[f])
        if carried is None:
            copy.start()
        else:
            by_bag = remote(src, bag.at[pl.ds(carried, rows)], bag_recv.at[1], carrier_of_early)
            pl.when(early)(by_bag.start)
            pl.when(jnp.logical_not(early))(copy.start)
        return copy

    def carry(dst, carried, first, rows, k):
        src, dst = bag.at[pl.ds(carried, rows)], dst.at[pl.ds(first, rows)]
        remote(src, dst, x_recv.at[k], late_of_carrier).start()

    def landed(ref, sem):
        pltpu.make_async_copy(ref, ref, sem).wait()

    @pl.when(early)
    def _():
        pl.semaphore_wait(barrier, expected)
        greet(hello.at[3], [near_to])

    both = (0, LAST)
    faces = (0, 1)
    scope("load_ends")
    pltpu.make_async_copy(coef, coef, in_sems.at[1]).wait()
    for a in both:
        for b in range(N):
            mine[part(face_of[a], LOAD, b), :] = lane_pick(ld[at(a, b), :], inverse)
    for k, a in enumerate(both):
        s = contract(SQUARED.T, [g2[across(a, c), :] for c in range(N)], 1)
        for c in range(N):
            tmpf[across(k, c), :] = s[c]
    for b in range(N):
        s = contract(SQUARED.T, [g0[at(a, b), :] for a in range(N)], 1, both)
        for k, a in enumerate(both):
            yf[at(k, b), :] = s[a]
    for k, a in enumerate(both):
        s = contract(SQUARED.T, [g1[at(a, b), :] for b in range(N)], 1)
        for b in range(N):
            mine[part(face_of[a], DIAG, b), :] = lane_pick(
                s[b] + yf[at(k, b), :] + ms[at(a, b), :] + tmpf[at(k, b), :], inverse
            )
    for a in both:
        for i in range(N):
            mine[part(face_of[a], G1, i), :] = lane_pick(g1[at(a, i), :], inverse)
            mine[part(face_of[a], G2, i), :] = lane_pick(g2[across(a, i), :], inverse)
    sent_near = remote(
        mine.at[pl.ds(0, 4 * FACE)], theirs.at[pl.ds(0, 4 * FACE)], x_recv.at[NEAR], near_to
    )
    beside_early = in_line == 1

    @pl.when(beside_early)
    def _():
        pl.semaphore_wait(hello.at[3], 1)
        sent_near.start()

    scope("barrier")

    @pl.when(not_early)
    def _():
        pl.semaphore_wait(barrier, expected)

    scope("send1")

    @pl.when(carrier)
    def _():
        landed(bag.at[pl.ds(0, 4 * FACE)], bag_recv.at[0])
        carry(theirs, 0, 4 * FACE, 2 * FACE, FAR_LD)
        carry(theirs, 2 * FACE, 6 * FACE, 2 * FACE, FAR_G)

    @pl.when(early)
    def _():
        remote(
            mine.at[pl.ds(4 * FACE, 4 * FACE)],
            bag.at[pl.ds(0, 4 * FACE)],
            bag_recv.at[0],
            carrier_of_early,
        ).start()

    sent_ld, sent_g = (
        remote(mine.at[rows], theirs.at[rows], x_recv.at[k], far_to)
        for k, rows in ((FAR_LD, pl.ds(4 * FACE, 2 * FACE)), (FAR_G, pl.ds(6 * FACE, 2 * FACE)))
    )

    @pl.when(not_early)
    def _():
        sent_ld.start()
        sent_g.start()

    pl.when(jnp.logical_not(beside_early))(sent_near.start)

    @pl.when(not_early)
    def _():
        greet(hello.at[0], y_near)


    @pl.when(core == 1)
    def _():
        def lower(z_to, _):
            greet(hello.at[2], [me + (z_to - z_at) * line])
            return 0

        lax.fori_loop(0, z_at, lower, 0)

    scope("diag")
    inner_diagonal(g0, g1, g2, ms, dg, tmp)
    scope("reorder")
    for a in INSIDE:
        for b in range(N):
            rows = at(a, b)
            dg[rows, :] = lane_pick(dg[rows, :], inverse)
            moved_load = lane_pick(ld[rows, :], inverse)
            ld[rows, :] = moved_load
            r[rows, :] = moved_load
    reorder(g0, g0, inverse)

    @pl.when(carrier)
    def _():
        landed(bag.at[pl.ds(4 * FACE, FACE)], bag_recv.at[1])
        carry(w_theirs, 4 * FACE, FACE, FACE, FAR_W)

    scope("sums")
    sum_yz([(v, a) for a in INSIDE for v in (dg, r)], lanes)

    def inner_z(a, _):
        for b in range(N):
            inv = 1.0 / dg[at(a, b), :]
            dg[at(a, b), :] = inv
            z[at(a, b), :] = inv * r[at(a, b), :]
        return 0

    lax.fori_loop(1, LAST, inner_z, 0, unroll=3)
    for b in range(N):
        g = [float(DERIV[m, 0] * DERIV[m, LAST]) * g0[at(m, b), :] for m in range(N)]
        cross[at(0, b), :] = added_up(g)
    scope("La1")
    stiffness_a(z, g0, y)

    def full(f, b):
        return tile(row_of[f] + b * N)

    def face_z(f):
        for b in range(N):
            rf[at(f, b), :] = mine[part(f, LOAD, b), :] + theirs[part(f, LOAD, b), :]
            total = mine[part(f, DIAG, b), :] + theirs[part(f, DIAG, b), :]
            a_sum[at(f, b), :] = total
            df[at(f, b), :] = total
        sum_yz([(rf, f), (df, f)], lanes)
        for b in range(N):
            inv = 1.0 / df[at(f, b), :]
            df[at(f, b), :] = inv
            zf[at(f, b), :] = inv * rf[at(f, b), :]

    def tell(f, k, carried=None):
        for b in range(N):
            w_mine[at(f, b), :] = y[full(f, b), :] + cross[at(0, b), :] * zf[at(1 - f, b), :]
        sum_yz([(w_mine, f)], lanes)
        return swap(w_mine, w_theirs, f, f * FACE, FACE, k, carried)

    scope("x_near")
    sent_near.wait_recv()
    scope("z_near")
    face_z(0)
    sent_w = [None, tell(1, FAR_W, 4 * FACE)]
    scope("reorder2")
    reorder(g1, g1, inverse, INSIDE)
    for a in INSIDE:
        for c in range(N):
            g2t[at(a, c), :] = lane_pick(g2[across(a, c), :], inverse)
    reorder(ms, ms, inverse, INSIDE)
    scope("Lbc1")
    stiffness_bc(z, g1, g2t, ms, y, tmp, y)
    scope("hello")

    @pl.when(not_early)
    def _():
        heard(hello.at[0], y_near)
        greet(hello.at[1], y_far)

    scope("g_near")
    first = pl.multiple_of((1 - core) * FACE, FACE)
    couplings(g0, first, coupling)
    loop(1, LAST, lambda a: couple(zf, 0, coupling, y, a))
    face_sums(0, mine, theirs, a_sum, a_sum, tmpf)
    s = face_terms(zf, 0, mine, theirs, a_sum, tmpf)
    for b in range(N):
        yf[at(0, b), :] = s[b]
    sum_yz([(yf, 0)], lanes)
    scope("x_far")
    sent_ld.wait_recv()
    scope("z_far")
    face_z(1)

    scope("inner2")
    for a in INSIDE:
        couple(zf, 1, coupling, y, a)
    sum_yz([(y, a) for a in INSIDE], lanes)
    zero = jnp.zeros((8, LANES), jnp.float32)

    def inner_p(a, num):
        for b in range(N):
            rows = at(a, b)
            p = COEF_Z * z[rows, :] - COEF_Q * (dg[rows, :] * y[rows, :])
            z[rows, :] = p
            num[b % 4] = num[b % 4] + ld[rows, :] * p
        return num

    num = lax.fori_loop(1, LAST, inner_p, [zero] * 4, unroll=True)
    scope("L2")
    den = energy_bc(z, g1, g2t, ms, [zero] * 4)
    den = energy_a(z, g0, u_ends, first, den)
    num, den = added_up(num), added_up(den)
    sent_w[0] = tell(0, NEAR_W)
    scope("g_far")
    sent_g.wait_recv()
    face_sums(1, mine, theirs, a_sum, a_sum, tmpf)
    s = face_terms(zf, 1, mine, theirs, a_sum, tmpf)
    for b in range(N):
        yf[at(1, b), :] = s[b]
    sum_yz([(yf, 1)], lanes)

    def face_p(f):
        for b in range(N):
            rows = at(f, b)
            total = yf[rows, :] + (w_mine[rows, :] + w_theirs[rows, :])
            pf[rows, :] = COEF_Z * zf[rows, :] - COEF_Q * (df[rows, :] * total)

    def face_dot(kind, f):
        return added_up([kind[part(f, LOAD, b), :] * pf[at(f, b), :] for b in range(N)])

    acc[tile(0), :] = num
    acc[tile(8), :] = den
    takes = jnp.where(2 * x >= xs, core, 1 - core) == 1
    gives = jnp.logical_not(takes)
    sent_q = remote(q_mine, q_theirs, x_recv.at[NEAR_W], near_to)
    scope("w_near")

    @pl.when(takes)
    def _():
        landed(w_mine, x_recv.at[NEAR_W])
        face_p(0)
        acc[tile(0), :] = acc[tile(0), :] + (face_dot(mine, 0) + face_dot(theirs, 0))
        terms = [
            (2.0 * u_ends[at(0, b), :] + q_theirs[at(0, b), :]) * pf[at(0, b), :] for b in range(N)
        ]
        acc[tile(8), :] = acc[tile(8), :] + (face_energy(pf, 0, theirs, a_sum) + added_up(terms))
        for b in range(N):
            q_mine[at(0, b), :] = 2.0 * cross[at(0, b), :] * pf[at(0, b), :]

    scope("w_far")
    sent_w[1].wait_recv()
    scope("ends2")
    face_p(1)
    acc[tile(0), :] = acc[tile(0), :] + face_dot(mine, 1)
    terms = [2.0 * u_ends[at(1, b), :] * pf[at(1, b), :] for b in range(N)]
    acc[tile(8), :] = acc[tile(8), :] + (0.5 * face_energy(pf, 1, theirs, a_sum) + added_up(terms))

    @pl.when(takes)
    def _():
        terms = [q_mine[at(0, b), :] * pf[at(1, b), :] for b in range(N)]
        acc[tile(8), :] = acc[tile(8), :] + added_up(terms)

    @pl.when(gives)
    def _():
        for b in range(N):
            q_mine[at(0, b), :] = 2.0 * (
                u_ends[at(0, b), :] + cross[at(0, b), :] * pf[at(1, b), :]
            )
        sent_q.start()

    num_row = jnp.sum(acc[tile(0), :], axis=0, keepdims=True)
    den_row = jnp.sum(acc[tile(8), :], axis=0, keepdims=True)
    dots[0, 0:1, :] = num_row
    dots[0, 1:2, :] = den_row
    hops = sorted(
        ((dy, dx) for dy in range(ys) for dx in range(xs) if dy or dx),
        key=lambda d: -min(d[0], ys - d[0]) - min(d[1], xs - d[1]),
    )
    others = 2 * len(hops) + 1

    def send(src, dst, k, to):
        copy = pltpu.make_async_remote_copy(
            src_ref=src,
            dst_ref=dst,
            send_sem=x_send,
            recv_sem=s_recv.at[k],
            device_id=(to,),
            device_id_type=MESH,
        )
        copy.start()

    def arrived(ref, sem):
        pltpu.make_async_copy(ref, ref, sem).wait()

    def added(ref, first, total):
        part = [first, None, None, None]
        for j in range(total):
            part[j % 4] = plus(part[j % 4], ref[j])
        return functools.reduce(plus, [t for t in part if t is not None])

    half_z, pair_z = zs // 2, zs // 2 + zs // 8
    in_first = y_at * line + in_line
    slow_low = (z_at == pair_z) & (x == xs - 1) & (core == 1)
    slow_high = (z_at == pair_z + 1) & (x == 0) & (core == 0)
    slow_ones = ys * (2 if pair_z + 1 < zs else 1)
    slow_before = jnp.where(
        z_at > pair_z + 1,
        slow_ones,
        jnp.where(
            z_at == pair_z + 1,
            ys + y_at + (in_line > 0).astype(jnp.int32),
            jnp.where(z_at == pair_z, y_at, 0),
        ),
    )
    slot = jnp.where(
        slow_low | slow_high,
        count - slow_ones + jnp.where(slow_high, ys, 0) + y_at,
        z_at * ys * line + in_first - slow_before,
    )
    group = jnp.where(slow_low | slow_high, 2, jnp.where(z_at < half_z, 0, 1))
    group_0 = half_z * ys * line - 1
    groups = (group_0, count - 1 - group_0 - slow_ones, slow_ones)

    def root_sum(got, k, total):
        width, start, number = 16, sum(groups[:k]), groups[k]
        arrived(got.at[pl.ds(start, number)], root_recv[k])
        sums = [total] + [jnp.zeros_like(total)] * 7

        def some(i, sums):
            return [
                sums[j] + got[start + i * width + j] + got[start + i * width + j + 8]
                for j in range(8)
            ]

        whole = number // width
        sums = lax.fori_loop(0, whole, some, sums)
        for i in range(whole * width, number):
            sums[i % 8] = sums[i % 8] + got[start + i]
        return added_up(sums)

    root_recv = (s_recv.at[2], s_recv.at[3], s_recv.at[1])
    root_sem = s_recv.at[jnp.where(group == 2, 1, group + 2)]

    def send_to_root(r):
        at_root = r // plane_size * line + r % line

        @pl.when(me != r)
        def _():
            first_root = r == roots[0]
            pltpu.make_async_remote_copy(
                src_ref=dots.at[0] if first_root else fold.at[0],
                dst_ref=(got_two if first_root else got_one).at[
                    slot - (slot > at_root).astype(jnp.int32)
                ],
                send_sem=x_send if first_root else one_send,
                recv_sem=root_sem,
                device_id=(r,),
                device_id_type=MESH,
            ).start()

    send_to_root(roots[0])
    half = LANES // 2
    first_half = lane[0:1, :] < half
    fold[0] = jnp.where(
        first_half, num_row + pltpu.roll(num_row, half, 1), den_row + pltpu.roll(den_row, half, 1)
    )

    @pl.when(not_early)
    def _():
        heard(hello.at[1], y_far)

    @pl.when(beside_early)
    def _():
        greet(hello.at[0], [near_to])

    @pl.when(early)
    def _():
        pl.semaphore_wait(hello.at[0], 1)

    for j, (dy, dx) in enumerate(hops):
        send(dots.at[0], got_a.at[2 * j + core], 0, moved(dy=dy, dx=dx) + 1 - core)

    @pl.when(core == 0)
    def _():
        send(dots.at[0], got_a.at[others - 1], 0, me + 1)

    for other_root in roots[1:]:
        send_to_root(other_root)

    scope("u_ends")

    @pl.when(gives)
    def _():
        sent_w[0].wait_recv()
        face_p(0)

    for f in faces:
        for b in range(N):
            i_mine[at(f, b), :] = u_ends[at(f, b), :] + cross[at(0, b), :] * pf[at(1 - f, b), :]
        swap(i_mine, i_theirs, f, f * FACE, FACE, IMAGE)
    for f in faces:
        s = face_terms(pf, f, mine, theirs, a_sum, tmpf)
        for b in range(N):
            yf[at(f, b), :] = s[b]
    stiffness_bc(z, g1, g2t, ms, y, tmp)
    stiffness_a(z, g0, u, INSIDE, y)

    def couple_both(a):
        couple(pf, 0, coupling, u, a)
        couple(pf, 1, coupling, u, a)

    loop(1, LAST, couple_both)
    scope("out_p_r")
    for src, ends, dst in ((z, pf, p_o), (r, rf, r_o)):
        reorder(src, dst, order, INSIDE)
        for f in faces:
            for b in range(N):
                dst[full(f, b), :] = lane_pick(ends[at(f, b), :], order)
    sum_yz([(u, a) for a in INSIDE], lanes)
    reorder(u, im_o, order, INSIDE)
    scope("root_0")
    is_first, not_first = me == roots[0], me != roots[0]

    @pl.when(is_root)
    def _():
        @pl.when(is_first)
        def _():
            dots[2] = root_sum(got_two, 0, dots[0])

        @pl.when(not_first)
        def _():
            fold[1] = root_sum(got_one, 0, fold[0])

    scope("plane")
    first_of_column = me - z_at * line
    skip_0 = one_of(first_of_column - 1, [r for r in roots if r % cores == 0] or [-1])
    skip_1 = one_of(first_of_column, [r for r in roots if r % cores == 1])

    @pl.when(core == 1)
    def _():
        arrived(got_a.at[pl.ds(0, others)], s_recv.at[0])
        dots[1] = added(got_a, dots[0], others)

        @pl.when(z_at < zs - 1)
        def _():
            pl.semaphore_wait(hello.at[2], zs - 1 - z_at)

        for k in sorted(range(1, zs), key=lambda k: -min(k, zs - k)):
            to_first = z_at == zs - k
            for c, skip in ((1, skip_0), (0, skip_1)):

                @pl.when(jnp.logical_not(to_first & skip))
                def _(k=k, c=c):
                    send(dots.at[1], got_b.at[k - 1], 1, moved(dz=k) - c)

        @pl.when(jnp.logical_not((z_at == 0) & skip_0))
        def _():
            send(dots.at[1], got_b.at[zs - 1], 1, me - 1)

        got_b[zs - 1] = dots[1]

    scope("x3")
    landed(i_theirs, x_recv.at[IMAGE])
    for f in faces:
        for b in range(N):
            rows = at(f, b)
            yf[rows, :] = yf[rows, :] + (i_mine[rows, :] + i_theirs[rows, :])
    sum_yz([(yf, f) for f in faces], lanes)
    for f in faces:
        for b in range(N):
            im_o[full(f, b), :] = lane_pick(yf[at(f, b), :], order)
    face_rows = FACE // 2
    skipped = jnp.where(
        core == 1,
        skip_0.astype(jnp.int32) + jnp.where(z_at > 0, skip_1.astype(jnp.int32), 0),
        0,
    )
    sums_0, sums_1 = len(hops) + 2, len(hops) + 2 * zs
    skipped = skipped + is_first.astype(jnp.int32)
    kinds = [(takes & jnp.logical_not(carrier), 12), (gives & jnp.logical_not(carrier), 13)]
    kinds += [(carrier & takes, 17), (carrier & gives, 18)]

    def all_left(who, to_roots):
        for faces_sent, face_count in kinds:
            for c, most, left_out in ((0, sums_0, 2), (1, sums_1, 4)):
                for less in range(left_out):

                    @pl.when(faces_sent & (core == c) & (skipped == less) & who)
                    def _(sent=most - less + face_count * face_rows):
                        arrived(all_sent.at[pl.ds(0, sent)], x_send)

        for whose, number in to_roots:

            @pl.when(whose)
            def _(number=number):
                arrived(got_one.at[pl.ds(0, number)], one_send)

    all_left(others_than_root, [(others_than_root, len(roots) - 1)])

    scope("lines")

    @pl.when((core == 0) & others_than_root)
    def _():
        arrived(got_b, s_recv.at[1])

    @pl.when((core == 1) & others_than_root)
    def _():
        arrived(got_b.at[pl.ds(0, zs - 1)], s_recv.at[1])

    def divide(total):
        sums = jnp.sum(total, axis=1, keepdims=True)
        al_o[...] = jnp.broadcast_to(sums[0:1, :] / sums[1:2, :], (8, LANES))

    @pl.when(others_than_root)
    def _():
        divide(added(got_b, None, zs))

    @pl.when(is_first)
    def _():
        divide(root_sum(got_two, 2, root_sum(got_two, 1, dots[2])))

    @pl.when(is_root & not_first)
    def _():
        row_sum = root_sum(got_one, 2, root_sum(got_one, 1, fold[1]))
        own_half = (lane[0:2, :] < half) == (b_at[0:2, :] == 0)
        divide(jnp.where(own_half, jnp.broadcast_to(row_sum, (2, LANES)), 0.0))

    scope("alpha")
    all_left(is_root, [(is_first, len(roots) - 1), (is_root & not_first, len(roots) - 2)])
    scope(None)


CHUNKS = 4


def finish_kernel(p, r, im, al, x_h, r_h, both, sem):
    alpha = al[...]
    size = ROWS // CHUNKS
    for k in range(CHUNKS):
        for i in range(k * size, (k + 1) * size, N):
            both[tile(i), :] = alpha * p[tile(i), :]
        pltpu.make_async_copy(both.at[pl.ds(k * size, size)], x_h.at[pl.ds(k * size, size)], sem).start()
        for i in range(k * size, (k + 1) * size, N):
            both[tile(ROWS + i), :] = r[tile(i), :] - alpha * im[tile(i), :]
        rows = pl.ds(ROWS + k * size, size)
        pltpu.make_async_copy(both.at[rows], r_h.at[pl.ds(k * size, size)], sem).start()
    pltpu.make_async_copy(both, both, sem).wait()


def on_device(load_terms, geometry, mass_terms, element_order):
    flat = jax.ShapeDtypeStruct((ROWS, LANES), jnp.float32)
    vm = lambda *shape: pltpu.VMEM(shape, jnp.float32)
    field = vm(ROWS, LANES)
    pair = vm(2 * FACE, LANES)
    ys, zs, xs, cores = TORUS
    in_vmem = pl.BlockSpec(memory_space=pltpu.VMEM)
    in_hbm = pl.BlockSpec(memory_space=pltpu.HBM)
    parts = pl.pallas_call(
        step_kernel,
        out_shape=(field, field, field, vm(8, LANES)),
        in_specs=[in_hbm] * 4,
        out_specs=[in_vmem] * 4,
        scratch_shapes=[
            vm(5 * ROWS, LANES), *[field] * 7,
            *[vm(8 * FACE, LANES)] * 2,
            *[pair] * 4, vm(5 * FACE, LANES), *[pair] * 8, *[vm(FACE, LANES)] * 3,
            vm(12 * FACE, LANES), vm(16, LANES),
            vm(3, 2, LANES), vm(2, 1, LANES), vm(2 * ys * xs - 1, 2, LANES), vm(zs, 2, LANES),
            vm(ys * zs * xs * cores - 1, 1, LANES), vm(ys * zs * xs * cores - 1, 2, LANES),
            vm(18 * FACE // 2 + ys * xs + 2 * zs + 1, 2, LANES),
            pltpu.VMEM((1, LANES), jnp.int32),
            pltpu.SemaphoreType.DMA((2,)),
            pltpu.SemaphoreType.DMA(()),
            pltpu.SemaphoreType.DMA((6,)),
            pltpu.SemaphoreType.DMA((2,)),
            pltpu.SemaphoreType.DMA((4,)),
            pltpu.SemaphoreType.DMA(()),
            pltpu.SemaphoreType.REGULAR((4,)),
        ],
        compiler_params=pltpu.CompilerParams(
            collective_id=0, has_side_effects=True, vmem_limit_bytes=24 << 20
        ),
        name="cg_step",
    )(
        *[
            pltpu.with_memory_space_constraint(t, pltpu.HBM)
            for t in (
                load_terms.reshape(ROWS, LANES),
                geometry.reshape(3 * ROWS, LANES),
                mass_terms.reshape(ROWS, LANES),
                element_order,
            )
        ]
    )
    x, res = pl.pallas_call(
        finish_kernel,
        out_shape=(flat, flat),
        in_specs=[in_vmem] * 4,
        out_specs=[in_hbm] * 2,
        scratch_shapes=[vm(2 * ROWS, LANES), pltpu.SemaphoreType.DMA(())],
        compiler_params=pltpu.CompilerParams(vmem_limit_bytes=8 << 20),
        name="cg_finish",
    )(*[pltpu.with_memory_space_constraint(t, pltpu.VMEM) for t in parts])
    shape = load_terms.shape
    return x.reshape(shape), res.reshape(shape)


def solution(mesh):
    last = P(None, None, None, "slab")
    return jax.shard_map(
        on_device,
        mesh=mesh,
        in_specs=(last, P(None, None, None, None, "slab"), last, P("slab", None)),
        out_specs=(last, last),
        check_vma=False,
    )
```

```python
import functools

import jax
import jax.numpy as jnp
import numpy as np
from jax import lax
from jax.experimental import pallas as pl
from jax.experimental.pallas import tpu as pltpu
from jax.sharding import PartitionSpec as P

N = 8
LAST = N - 1
EL_Y = 8
EL_Z = 16
LANES = 128
ROWS = N * N * N
FACE = N * N
CENTRE = 1.65
HALF = 1.35
MESH = pl.DeviceIdType.MESH
TORUS = (8, 12, 4, 2)
ROOTS = (1, 3, 97, 2, 96, 7, 193, 192, 5, 6)
INSIDE = range(1, LAST)
UNROLL_A = 4
UNROLL_BC = 3


def legendre_table(positions, points):
    columns = [positions * 0.0 + 1.0, positions]
    for degree in range(2, points):
        columns.append(
            ((2 * degree - 1) * positions * columns[-1] - (degree - 1) * columns[-2]) / degree
        )
    return np.stack(columns, axis=1)


def gll_derivative(points):
    degree = points - 1
    nodes = -np.cos(np.pi * np.arange(points) / degree)
    for _ in range(100):
        legendre = legendre_table(nodes, points)
        nodes = nodes - (nodes * legendre[:, degree] - legendre[:, degree - 1]) / (
            points * legendre[:, degree]
        )
    legendre = legendre_table(nodes, points)
    top = legendre[:, degree]
    same = np.eye(points, dtype=bool)
    spacing = np.where(same, 1.0, nodes[:, None] - nodes[None, :])
    table = np.where(same, 0.0, top[:, None] / (top[None, :] * spacing))
    table[0, 0] = -degree * points / 4.0
    table[degree, degree] = degree * points / 4.0
    return table


DERIV = gll_derivative(N).astype(np.float32).astype(np.float64)
SQUARED = DERIV * DERIV
SIGMA = CENTRE / HALF
RHO0 = 1.0 / SIGMA
RHO1 = 1.0 / (2.0 * SIGMA - RHO0)
COEF_Z = (1.0 + RHO1 * RHO0) / CENTRE + 2.0 * RHO1 / HALF
COEF_Q = 2.0 * RHO1 / HALF / CENTRE


def plus(x, y):
    return y if x is None else x + y


def contract(table, terms, sign, rows=range(N)):
    used = [j for j in range(N // 2) if terms[j] is not None]
    even = {j: terms[j] + terms[LAST - j] for j in used}
    odd = {j: terms[j] - terms[LAST - j] for j in used}
    out = [None] * N
    for i in range(N // 2):
        if i not in rows and LAST - i not in rows:
            continue
        e = o = None
        for j in used:
            e = plus(e, float(table[i, j] + table[i, LAST - j]) / 2 * even[j])
            o = plus(o, float(table[i, j] - table[i, LAST - j]) / 2 * odd[j])
        if i in rows:
            out[i] = e + o
        if LAST - i in rows:
            out[LAST - i] = (o - e) if sign < 0 else (e - o)
    return out


def tile(row):
    return pl.ds(row if isinstance(row, int) else pl.multiple_of(row, 8), 8)


def at(a, b):
    return tile((a * N + b) * N)


def across(a, c):
    return pl.ds(a * FACE + c, N, stride=N)


LOAD, DIAG, G1, G2 = range(4)
NEAR, FAR_LD, FAR_G, NEAR_W, FAR_W, IMAGE = range(6)


def part(f, kind, i):
    return tile(((f * 4 + kind) * N + i) * N)


def loop(start, stop, body):
    lax.fori_loop(start, stop, lambda i, _: (body(i), 0)[1], 0)


def stiffness_a(v, g0, out, rows=range(N), more=None):
    def along_a(b, _):
        va = [v[at(a, b), :] if a in INSIDE else None for a in range(N)]
        s = contract(DERIV, va, -1)
        s = contract(DERIV.T, [s[a] * g0[at(a, b), :] for a in range(N)], -1, rows)
        for a in rows:
            out[at(a, b), :] = s[a] if more is None else s[a] + more[at(a, b), :]
        return 0

    lax.fori_loop(0, N, along_a, 0, unroll=UNROLL_A)


def energy_a(v, g0, ends, first, total):
    def along_a(b, total):
        t = contract(DERIV, [v[at(a, b), :] if a in INSIDE else None for a in range(N)], -1)
        s = [t[a] * g0[at(a, b), :] for a in range(N)]
        total = [total[k] + s[k] * t[k] + s[k + 4] * t[k + 4] for k in range(4)]
        s = contract(DERIV.T, s, -1, (0, LAST))
        ends[tile(first + b * N), :] = s[0]
        ends[tile(FACE - first + b * N), :] = s[LAST]
        return total

    return lax.fori_loop(0, N, along_a, total, unroll=UNROLL_A)


def energy_bc(v, g1, g2t, ms, total):
    def along_bc(a, total):
        vb = [v[at(a, b), :] for b in range(N)]
        for own, g in (([v[across(a, c), :] for c in range(N)], g2t), (vb, g1)):
            t = contract(DERIV, own, -1)
            e = [t[i] * g[at(a, i), :] * t[i] for i in range(N)]
            total = [total[k] + (e[k] + e[k + 4]) for k in range(4)]
        e = [vb[b] * ms[at(a, b), :] * vb[b] for b in range(N)]
        return [total[k] + (e[k] + e[k + 4]) for k in range(4)]

    return lax.fori_loop(1, LAST, along_bc, total, unroll=UNROLL_BC)


def stiffness_bc(v, g1, g2t, ms, out, tmp, more=None):
    def along_bc(a, _):
        vt = [v[across(a, c), :] for c in range(N)]
        vb = [v[at(a, b), :] for b in range(N)]
        t = contract(DERIV, vt, -1)
        t = contract(DERIV.T, [t[c] * g2t[at(a, c), :] for c in range(N)], -1)
        for c in range(N):
            tmp[across(a, c), :] = t[c]
        s = contract(DERIV, vb, -1)
        s = contract(DERIV.T, [s[b] * g1[at(a, b), :] for b in range(N)], -1)
        for b in range(N):
            s[b] = s[b] + ms[at(a, b), :] * vb[b]
            if more is not None:
                s[b] = s[b] + more[at(a, b), :]
        for b in range(N):
            out[at(a, b), :] = s[b] + tmp[at(a, b), :]
        return 0

    lax.fori_loop(1, LAST, along_bc, 0, unroll=UNROLL_BC)


def inner_diagonal(g0, g1, g2, ms, out, tmp):
    def along_a(b, _):
        s = contract(SQUARED.T, [g0[at(a, b), :] for a in range(N)], 1, INSIDE)
        for a in INSIDE:
            out[at(a, b), :] = s[a] + ms[at(a, b), :]
        return 0

    lax.fori_loop(0, N, along_a, 0, unroll=UNROLL_A)

    def along_bc(a, _):
        t = contract(SQUARED.T, [g2[across(a, c), :] for c in range(N)], 1)
        for c in range(N):
            tmp[across(a, c), :] = t[c]
        s = contract(SQUARED.T, [g1[at(a, b), :] for b in range(N)], 1)
        for b in range(N):
            s[b] = s[b] + out[at(a, b), :]
        for b in range(N):
            out[at(a, b), :] = s[b] + tmp[at(a, b), :]
        return 0

    lax.fori_loop(1, LAST, along_bc, 0, unroll=UNROLL_BC)


def face_terms(v, f, mine, theirs, a_sum, tmp):
    s = contract(DERIV, [v[across(f, c), :] for c in range(N)], -1)
    s = contract(DERIV.T, [s[c] * theirs[part(f, G2, c), :] for c in range(N)], -1)
    for c in range(N):
        tmp[across(f, c), :] = s[c]
    vb = [v[at(f, b), :] for b in range(N)]
    s = contract(DERIV, vb, -1)
    s = contract(DERIV.T, [s[b] * theirs[part(f, G1, b), :] for b in range(N)], -1)
    return [s[b] + a_sum[at(f, b), :] * vb[b] + tmp[at(f, b), :] for b in range(N)]


def face_energy(v, f, theirs, a_sum):
    vb = [v[at(f, b), :] for b in range(N)]
    e = [a_sum[at(f, b), :] * vb[b] * vb[b] for b in range(N)]
    for own, kind in (([v[across(f, c), :] for c in range(N)], G2), (vb, G1)):
        t = contract(DERIV, own, -1)
        e = [e[i] + t[i] * theirs[part(f, kind, i), :] * t[i] for i in range(N)]
    return added_up(e)


def added_up(terms):
    while len(terms) > 1:
        terms = [functools.reduce(plus, terms[i : i + 2]) for i in range(0, len(terms), 2)]
    return terms[0]


def face_sums(f, mine, theirs, diag, a_sum, tmp):
    g = [[mine[part(f, k, i), :] + theirs[part(f, k, i), :] for i in range(N)] for k in (G1, G2)]
    for k in (G1, G2):
        for i in range(N):
            theirs[part(f, k, i), :] = g[k - G1][i]
    s = contract(SQUARED.T, g[1], 1)
    for c in range(N):
        tmp[across(f, c), :] = s[c]
    s = contract(SQUARED.T, g[0], 1)
    for b in range(N):
        a_sum[at(f, b), :] = diag[at(f, b), :] - s[b] - tmp[at(f, b), :]


def couplings(g0, first, out):
    def one(b, _):
        g = [g0[at(a, b), :] for a in range(N)]
        for a_end, row in ((0, first), (LAST, FACE - first)):
            s = contract(DERIV.T, [float(DERIV[m, a_end]) * g[m] for m in range(N)], -1, INSIDE)
            for a in INSIDE:
                out[tile(row * 6 + ((a - 1) * N + b) * N), :] = s[a]
        return 0

    lax.fori_loop(0, N, one, 0, unroll=2)


def couple(v, f, coupling, out, a):
    for b in range(N):
        out[at(a, b), :] = (
            out[at(a, b), :] + coupling[tile(((f * 6 + a - 1) * N + b) * N), :] * v[at(f, b), :]
        )


def lane_pick(x, idx):
    return jnp.take_along_axis(x, idx, axis=1, mode="promise_in_bounds")


def sum_yz(planes, lanes):
    ends = [(v[at(a, 0), :], v[at(a, LAST), :]) for v, a in planes]
    rims = [(v[across(a, 0), :], v[across(a, LAST), :]) for v, a in planes]
    ups = [jnp.where(lanes["up"], pltpu.roll(low, LANES - EL_Z, 1), 0.0) for low, _ in ends]
    downs = [jnp.where(lanes["down"], pltpu.roll(high, EL_Z, 1), 0.0) for _, high in ends]
    nexts = [lane_pick(low, lanes["next"]) for low, _ in rims]
    prevs = [lane_pick(high, lanes["prev"]) for _, high in rims]

    def corners(rim, idx):
        turned = jnp.where(lanes["first"], pltpu.roll(rim, 1, 0), pltpu.roll(rim, LAST, 0))
        return jnp.where(lanes["corner"], lane_pick(turned, idx), 0.0)

    far_nexts = [corners(low, lanes["corner_next"]) for low, _ in rims]
    far_prevs = [corners(high, lanes["corner_prev"]) for _, high in rims]
    for k, (v, a) in enumerate(planes):
        v[across(a, LAST), :] = rims[k][1] + (nexts[k] + far_nexts[k])
        v[across(a, 0), :] = rims[k][0] + (prevs[k] + far_prevs[k])
        v[at(a, LAST), :] = v[at(a, LAST), :] + ups[k]
        v[at(a, 0), :] = v[at(a, 0), :] + downs[k]


def step_kernel(
    load_h, geom_h, mass_h, order_h, p_o, r_o, im_o, al_o,
    coef, g2t, r, dg, z, y, u, tmp,
    mine, theirs, w_mine, w_theirs, i_mine, i_theirs, bag, rf, df, zf, pf, yf, a_sum, tmpf,
    u_ends, cross, q_mine, q_theirs, coupling, acc,
    dots, fold, got_a, got_b, got_one, got_two, all_sent, order_v, in_sems, x_send, x_recv, bag_recv, s_recv, one_send, hello,
):
    stack = []

    def scope(name):
        if stack:
            stack.pop().__exit__(None, None, None)
        if name:
            stack.append(jax.named_scope(name))
            stack[-1].__enter__()

    scope("enter")
    ys, zs, xs, cores = TORUS
    line, plane_size, count = xs * cores, zs * xs * cores, ys * zs * xs * cores
    me = lax.axis_index("slab")
    core = lax.rem(me, cores)
    in_plane = lax.rem(me, plane_size)

    def greet(sem, who):
        for q in who:
            pl.semaphore_signal(sem, inc=1, device_id=(q,), device_id_type=MESH)

    def heard(sem, who):
        if who:
            pl.semaphore_wait(sem, len(who))

    near_to = me + 1 - 2 * core
    far_to = me + 2 * core - 1
    far_to = jnp.where(far_to < 0, count - 1, jnp.where(far_to == count, 0, far_to))
    in_line = lax.rem(me, line)
    early, late = in_line == 0, in_line == line - 1
    at_turn = in_plane < line
    carrier = (jnp.logical_not(at_turn) & (in_line == 1)) | (at_turn & late)
    carrier_of_late = jnp.where(in_plane == plane_size - 1, me + line - plane_size, me + 2)
    barrier = pltpu.get_barrier_semaphore()
    greet(barrier, [jnp.where(late, carrier_of_late, far_to)])
    loads = [
        pltpu.make_async_copy(src, dst, in_sems.at[k])
        for k, src, dst in (
            (0, order_h, order_v),
            (1, load_h, coef.at[pl.ds(4 * ROWS, ROWS)]),
            (1, geom_h, coef.at[pl.ds(0, 3 * ROWS)]),
            (1, mass_h, coef.at[pl.ds(3 * ROWS, ROWS)]),
        )
    ]
    for copy in loads:
        copy.start()
    g0, g1, g2, ms, ld = (coef.at[pl.ds(k * ROWS, ROWS)] for k in range(5))

    y_at = me // plane_size
    z_at = in_plane // line
    x = in_line // cores

    def moved(dy=0, dz=0, dx=0):
        to = me
        if dy:
            to = to + (lax.rem(y_at + dy, ys) - y_at) * plane_size
        if dz:
            to = to + (lax.rem(z_at + dz, zs) - z_at) * line
        if dx:
            to = to + (lax.rem(x + dx, xs) - x) * cores
        return to

    def ring(size, stop, start=1):
        return sorted({j % size for k in range(start, stop) for j in (k, -k)} - {0})

    sides = (near_to, far_to)
    row_of = (pl.multiple_of((1 - core) * (ROWS - FACE), FACE), pl.multiple_of(core * (ROWS - FACE), FACE))
    face_of = {0: 1 - core, LAST: core}
    carrier_of_early = jnp.where(
        at_turn, lax.rem(y_at + ys - 1, ys) * plane_size + line - 1, me + 1
    )
    early_of_carrier = lax.rem(y_at + 1, ys) * plane_size
    late_of_carrier = jnp.where(at_turn, me + plane_size - line, me - 2)

    y_near = [moved(dy=k) for k in ring(ys, 3)]
    y_far = [moved(dy=k) for k in ring(ys, ys // 2 + 1, 3)]
    greet(barrier, [near_to])
    not_early = jnp.logical_not(early)
    for k in range(1, line):

        @pl.when(in_line != k)
        def _(k=k):
            greet(barrier, [me - in_line + k])

    @pl.when(not_early)
    def _():
        greet(barrier, y_near)

    @pl.when(at_turn & (early | late))
    def _():
        greet(barrier, [jnp.where(early, carrier_of_early, early_of_carrier)])

    def higher(z_to, _):
        greet(barrier, [me + (z_to - z_at) * line + 1 - core])
        return 0

    lax.fori_loop(z_at + 1, zs, higher, 0)
    roots = [r for r in ROOTS if r < count]

    def one_of(device, some):
        return functools.reduce(jnp.logical_or, [device == r for r in some])

    is_root = one_of(me, roots)
    others_than_root = jnp.logical_not(is_root)

    @pl.when(is_root)
    def _():
        width = next(k for k in range(16, 0, -1) if (count - 1) % k == 0)

        def everyone(k, _):
            for i in range(width):
                q = me + 1 + k * width + i
                greet(barrier, [jnp.where(q >= count, q - count, q)])
            return 0

        lax.fori_loop(0, (count - 1) // width, everyone, 0)

    expected = jnp.where(
        early,
        1 + at_turn.astype(jnp.int32),
        (line - 1)
        + len(y_near)
        + 2
        + carrier.astype(jnp.int32)
        + (carrier & at_turn).astype(jnp.int32)
        + 2 * core * z_at,
    )
    expected = expected + len(roots) - is_root.astype(jnp.int32)

    scope("idx")
    loads[0].wait()
    order = jnp.broadcast_to(order_v[...], (8, LANES))
    hit = (
        jnp.broadcast_to(order_v[...], (LANES, LANES))
        == lax.broadcasted_iota(jnp.int32, (LANES, LANES), 0)
    ).astype(jnp.float32)
    lane = lax.broadcasted_iota(jnp.int32, (8, LANES), 1)
    inverse = lax.dot_general(
        lane.astype(jnp.float32), hit, (((1,), (1,)), ((), ())), preferred_element_type=jnp.float32
    )
    inverse = (inverse + 0.5).astype(jnp.int32)
    in_row = lane & (EL_Z - 1)
    lanes = {
        "up": lane < LANES - EL_Z,
        "down": lane >= EL_Z,
        "next": lane - in_row + ((in_row + 1) & (EL_Z - 1)),
        "prev": lane - in_row + ((in_row + EL_Z - 1) & (EL_Z - 1)),
    }
    b_at = lax.broadcasted_iota(jnp.int32, (8, LANES), 0)
    lanes["first"] = b_at == 0
    lanes["corner"] = (lanes["first"] & lanes["down"]) | ((b_at == LAST) & lanes["up"])
    by_y = jnp.where(lanes["first"], LANES - EL_Z, EL_Z)
    lanes["corner_next"] = (lanes["next"] + by_y) & (LANES - 1)
    lanes["corner_prev"] = (lanes["prev"] + by_y) & (LANES - 1)

    def reorder(src, dst, idx, planes=range(N)):
        for a in planes:
            for b in range(N):
                dst[at(a, b), :] = lane_pick(src[at(a, b), :], idx)

    def remote(src, dst, recv, to):
        return pltpu.make_async_remote_copy(
            src_ref=src,
            dst_ref=dst,
            send_sem=x_send,
            recv_sem=recv,
            device_id=(to,),
            device_id_type=MESH,
        )

    def swap(src, dst, f, first, rows, k, carried=None):
        src, dst = src.at[pl.ds(first, rows)], dst.at[pl.ds(first, rows)]
        copy = remote(src, dst, x_recv.at[k], sides[f])
        if carried is None:
            copy.start()
        else:
            by_bag = remote(src, bag.at[pl.ds(carried, rows)], bag_recv.at[1], carrier_of_early)
            pl.when(early)(by_bag.start)
            pl.when(jnp.logical_not(early))(copy.start)
        return copy

    def carry(dst, carried, first, rows, k):
        src, dst = bag.at[pl.ds(carried, rows)], dst.at[pl.ds(first, rows)]
        remote(src, dst, x_recv.at[k], late_of_carrier).start()

    def landed(ref, sem):
        pltpu.make_async_copy(ref, ref, sem).wait()

    @pl.when(early)
    def _():
        pl.semaphore_wait(barrier, expected)
        greet(hello.at[3], [near_to])

    both = (0, LAST)
    faces = (0, 1)
    scope("load_ends")
    pltpu.make_async_copy(coef, coef, in_sems.at[1]).wait()
    for a in both:
        for b in range(N):
            mine[part(face_of[a], LOAD, b), :] = lane_pick(ld[at(a, b), :], inverse)
    for k, a in enumerate(both):
        s = contract(SQUARED.T, [g2[across(a, c), :] for c in range(N)], 1)
        for c in range(N):
            tmpf[across(k, c), :] = s[c]
    for b in range(N):
        s = contract(SQUARED.T, [g0[at(a, b), :] for a in range(N)], 1, both)
        for k, a in enumerate(both):
            yf[at(k, b), :] = s[a]
    for k, a in enumerate(both):
        s = contract(SQUARED.T, [g1[at(a, b), :] for b in range(N)], 1)
        for b in range(N):
            mine[part(face_of[a], DIAG, b), :] = lane_pick(
                s[b] + yf[at(k, b), :] + ms[at(a, b), :] + tmpf[at(k, b), :], inverse
            )
    for a in both:
        for i in range(N):
            mine[part(face_of[a], G1, i), :] = lane_pick(g1[at(a, i), :], inverse)
            mine[part(face_of[a], G2, i), :] = lane_pick(g2[across(a, i), :], inverse)
    sent_near = remote(
        mine.at[pl.ds(0, 4 * FACE)], theirs.at[pl.ds(0, 4 * FACE)], x_recv.at[NEAR], near_to
    )
    beside_early = in_line == 1

    @pl.when(beside_early)
    def _():
        pl.semaphore_wait(hello.at[3], 1)
        sent_near.start()

    scope("barrier")

    @pl.when(not_early)
    def _():
        pl.semaphore_wait(barrier, expected)

    scope("send1")

    @pl.when(carrier)
    def _():
        landed(bag.at[pl.ds(0, 4 * FACE)], bag_recv.at[0])
        carry(theirs, 0, 4 * FACE, 2 * FACE, FAR_LD)
        carry(theirs, 2 * FACE, 6 * FACE, 2 * FACE, FAR_G)

    @pl.when(early)
    def _():
        remote(
            mine.at[pl.ds(4 * FACE, 4 * FACE)],
            bag.at[pl.ds(0, 4 * FACE)],
            bag_recv.at[0],
            carrier_of_early,
        ).start()

    sent_ld, sent_g = (
        remote(mine.at[rows], theirs.at[rows], x_recv.at[k], far_to)
        for k, rows in ((FAR_LD, pl.ds(4 * FACE, 2 * FACE)), (FAR_G, pl.ds(6 * FACE, 2 * FACE)))
    )

    @pl.when(not_early)
    def _():
        sent_ld.start()
        sent_g.start()

    pl.when(jnp.logical_not(beside_early))(sent_near.start)

    @pl.when(not_early)
    def _():
        greet(hello.at[0], y_near)


    @pl.when(core == 1)
    def _():
        def lower(z_to, _):
            greet(hello.at[2], [me + (z_to - z_at) * line])
            return 0

        lax.fori_loop(0, z_at, lower, 0)

    scope("diag")
    inner_diagonal(g0, g1, g2, ms, dg, tmp)
    scope("reorder")
    for a in INSIDE:
        for b in range(N):
            rows = at(a, b)
            dg[rows, :] = lane_pick(dg[rows, :], inverse)
            moved_load = lane_pick(ld[rows, :], inverse)
            ld[rows, :] = moved_load
            r[rows, :] = moved_load
    reorder(g0, g0, inverse)

    @pl.when(carrier)
    def _():
        landed(bag.at[pl.ds(4 * FACE, FACE)], bag_recv.at[1])
        carry(w_theirs, 4 * FACE, FACE, FACE, FAR_W)

    scope("sums")
    sum_yz([(v, a) for a in INSIDE for v in (dg, r)], lanes)

    def inner_z(a, _):
        for b in range(N):
            inv = 1.0 / dg[at(a, b), :]
            dg[at(a, b), :] = inv
            z[at(a, b), :] = inv * r[at(a, b), :]
        return 0

    lax.fori_loop(1, LAST, inner_z, 0, unroll=3)
    for b in range(N):
        g = [float(DERIV[m, 0] * DERIV[m, LAST]) * g0[at(m, b), :] for m in range(N)]
        cross[at(0, b), :] = added_up(g)
    scope("La1")
    stiffness_a(z, g0, y)

    def full(f, b):
        return tile(row_of[f] + b * N)

    def face_z(f):
        for b in range(N):
            rf[at(f, b), :] = mine[part(f, LOAD, b), :] + theirs[part(f, LOAD, b), :]
            total = mine[part(f, DIAG, b), :] + theirs[part(f, DIAG, b), :]
            a_sum[at(f, b), :] = total
            df[at(f, b), :] = total
        sum_yz([(rf, f), (df, f)], lanes)
        for b in range(N):
            inv = 1.0 / df[at(f, b), :]
            df[at(f, b), :] = inv
            zf[at(f, b), :] = inv * rf[at(f, b), :]

    def tell(f, k, carried=None):
        for b in range(N):
            w_mine[at(f, b), :] = y[full(f, b), :] + cross[at(0, b), :] * zf[at(1 - f, b), :]
        sum_yz([(w_mine, f)], lanes)
        return swap(w_mine, w_theirs, f, f * FACE, FACE, k, carried)

    scope("x_near")
    sent_near.wait_recv()
    scope("z_near")
    face_z(0)
    sent_w = [None, tell(1, FAR_W, 4 * FACE)]
    scope("reorder2")
    reorder(g1, g1, inverse, INSIDE)
    for a in INSIDE:
        for c in range(N):
            g2t[at(a, c), :] = lane_pick(g2[across(a, c), :], inverse)
    reorder(ms, ms, inverse, INSIDE)
    scope("Lbc1")
    stiffness_bc(z, g1, g2t, ms, y, tmp, y)
    scope("hello")

    @pl.when(not_early)
    def _():
        heard(hello.at[0], y_near)
        greet(hello.at[1], y_far)

    scope("g_near")
    first = pl.multiple_of((1 - core) * FACE, FACE)
    couplings(g0, first, coupling)
    loop(1, LAST, lambda a: couple(zf, 0, coupling, y, a))
    face_sums(0, mine, theirs, a_sum, a_sum, tmpf)
    s = face_terms(zf, 0, mine, theirs, a_sum, tmpf)
    for b in range(N):
        yf[at(0, b), :] = s[b]
    sum_yz([(yf, 0)], lanes)
    scope("x_far")
    sent_ld.wait_recv()
    scope("z_far")
    face_z(1)

    scope("inner2")
    for a in INSIDE:
        couple(zf, 1, coupling, y, a)
    sum_yz([(y, a) for a in INSIDE], lanes)
    zero = jnp.zeros((8, LANES), jnp.float32)

    def inner_p(a, num):
        for b in range(N):
            rows = at(a, b)
            p = COEF_Z * z[rows, :] - COEF_Q * (dg[rows, :] * y[rows, :])
            z[rows, :] = p
            num[b % 4] = num[b % 4] + ld[rows, :] * p
        return num

    num = lax.fori_loop(1, LAST, inner_p, [zero] * 4, unroll=True)
    scope("L2")
    den = energy_bc(z, g1, g2t, ms, [zero] * 4)
    den = energy_a(z, g0, u_ends, first, den)
    num, den = added_up(num), added_up(den)
    sent_w[0] = tell(0, NEAR_W)
    scope("g_far")
    sent_g.wait_recv()
    face_sums(1, mine, theirs, a_sum, a_sum, tmpf)
    s = face_terms(zf, 1, mine, theirs, a_sum, tmpf)
    for b in range(N):
        yf[at(1, b), :] = s[b]
    sum_yz([(yf, 1)], lanes)

    def face_p(f):
        for b in range(N):
            rows = at(f, b)
            total = yf[rows, :] + (w_mine[rows, :] + w_theirs[rows, :])
            pf[rows, :] = COEF_Z * zf[rows, :] - COEF_Q * (df[rows, :] * total)

    def face_dot(kind, f):
        return added_up([kind[part(f, LOAD, b), :] * pf[at(f, b), :] for b in range(N)])

    acc[tile(0), :] = num
    acc[tile(8), :] = den
    takes = jnp.where(2 * x >= xs, core, 1 - core) == 1
    gives = jnp.logical_not(takes)
    sent_q = remote(q_mine, q_theirs, x_recv.at[NEAR_W], near_to)
    scope("w_near")

    @pl.when(takes)
    def _():
        landed(w_mine, x_recv.at[NEAR_W])
        face_p(0)
        acc[tile(0), :] = acc[tile(0), :] + (face_dot(mine, 0) + face_dot(theirs, 0))
        terms = [
            (2.0 * u_ends[at(0, b), :] + q_theirs[at(0, b), :]) * pf[at(0, b), :] for b in range(N)
        ]
        acc[tile(8), :] = acc[tile(8), :] + (face_energy(pf, 0, theirs, a_sum) + added_up(terms))
        for b in range(N):
            q_mine[at(0, b), :] = 2.0 * cross[at(0, b), :] * pf[at(0, b), :]

    scope("w_far")
    sent_w[1].wait_recv()
    scope("ends2")
    face_p(1)
    acc[tile(0), :] = acc[tile(0), :] + face_dot(mine, 1)
    terms = [2.0 * u_ends[at(1, b), :] * pf[at(1, b), :] for b in range(N)]
    acc[tile(8), :] = acc[tile(8), :] + (0.5 * face_energy(pf, 1, theirs, a_sum) + added_up(terms))

    @pl.when(takes)
    def _():
        terms = [q_mine[at(0, b), :] * pf[at(1, b), :] for b in range(N)]
        acc[tile(8), :] = acc[tile(8), :] + added_up(terms)

    @pl.when(gives)
    def _():
        for b in range(N):
            q_mine[at(0, b), :] = 2.0 * (
                u_ends[at(0, b), :] + cross[at(0, b), :] * pf[at(1, b), :]
            )
        sent_q.start()

    num_row = jnp.sum(acc[tile(0), :], axis=0, keepdims=True)
    den_row = jnp.sum(acc[tile(8), :], axis=0, keepdims=True)
    dots[0, 0:1, :] = num_row
    dots[0, 1:2, :] = den_row
    hops = sorted(
        ((dy, dx) for dy in range(ys) for dx in range(xs) if dy or dx),
        key=lambda d: -min(d[0], ys - d[0]) - min(d[1], xs - d[1]),
    )
    others = 2 * len(hops) + 1

    def send(src, dst, k, to):
        copy = pltpu.make_async_remote_copy(
            src_ref=src,
            dst_ref=dst,
            send_sem=x_send,
            recv_sem=s_recv.at[k],
            device_id=(to,),
            device_id_type=MESH,
        )
        copy.start()

    def arrived(ref, sem):
        pltpu.make_async_copy(ref, ref, sem).wait()

    def added(ref, first, total):
        part = [first, None, None, None]
        for j in range(total):
            part[j % 4] = plus(part[j % 4], ref[j])
        return functools.reduce(plus, [t for t in part if t is not None])

    half_z, pair_z = zs // 2, zs // 2 + zs // 8
    in_first = y_at * line + in_line
    slow_low = (z_at == pair_z) & (x == xs - 1) & (core == 1)
    slow_high = (z_at == pair_z + 1) & (x == 0) & (core == 0)
    slow_ones = ys * (2 if pair_z + 1 < zs else 1)
    slow_before = jnp.where(
        z_at > pair_z + 1,
        slow_ones,
        jnp.where(
            z_at == pair_z + 1,
            ys + y_at + (in_line > 0).astype(jnp.int32),
            jnp.where(z_at == pair_z, y_at, 0),
        ),
    )
    slot = jnp.where(
        slow_low | slow_high,
        count - slow_ones + jnp.where(slow_high, ys, 0) + y_at,
        z_at * ys * line + in_first - slow_before,
    )
    group = jnp.where(slow_low | slow_high, 2, jnp.where(z_at < half_z, 0, 1))
    group_0 = half_z * ys * line - 1
    groups = (group_0, count - 1 - group_0 - slow_ones, slow_ones)

    def root_sum(got, k, total):
        width, start, number = 16, sum(groups[:k]), groups[k]
        arrived(got.at[pl.ds(start, number)], root_recv[k])
        sums = [total] + [jnp.zeros_like(total)] * 7

        def some(i, sums):
            return [
                sums[j] + got[start + i * width + j] + got[start + i * width + j + 8]
                for j in range(8)
            ]

        whole = number // width
        sums = lax.fori_loop(0, whole, some, sums)
        for i in range(whole * width, number):
            sums[i % 8] = sums[i % 8] + got[start + i]
        return added_up(sums)

    root_recv = (s_recv.at[2], s_recv.at[3], s_recv.at[1])
    root_sem = s_recv.at[jnp.where(group == 2, 1, group + 2)]

    def send_to_root(r):
        at_root = r // plane_size * line + r % line

        @pl.when(me != r)
        def _():
            first_root = r == roots[0]
            pltpu.make_async_remote_copy(
                src_ref=dots.at[0] if first_root else fold.at[0],
                dst_ref=(got_two if first_root else got_one).at[
                    slot - (slot > at_root).astype(jnp.int32)
                ],
                send_sem=x_send if first_root else one_send,
                recv_sem=root_sem,
                device_id=(r,),
                device_id_type=MESH,
            ).start()

    send_to_root(roots[0])
    half = LANES // 2
    first_half = lane[0:1, :] < half
    fold[0] = jnp.where(
        first_half, num_row + pltpu.roll(num_row, half, 1), den_row + pltpu.roll(den_row, half, 1)
    )

    @pl.when(not_early)
    def _():
        heard(hello.at[1], y_far)

    @pl.when(beside_early)
    def _():
        greet(hello.at[0], [near_to])

    @pl.when(early)
    def _():
        pl.semaphore_wait(hello.at[0], 1)

    for j, (dy, dx) in enumerate(hops):
        send(dots.at[0], got_a.at[2 * j + core], 0, moved(dy=dy, dx=dx) + 1 - core)

    @pl.when(core == 0)
    def _():
        send(dots.at[0], got_a.at[others - 1], 0, me + 1)

    for other_root in roots[1:]:
        send_to_root(other_root)

    scope("u_ends")

    @pl.when(gives)
    def _():
        sent_w[0].wait_recv()
        face_p(0)

    for f in faces:
        for b in range(N):
            i_mine[at(f, b), :] = u_ends[at(f, b), :] + cross[at(0, b), :] * pf[at(1 - f, b), :]
        swap(i_mine, i_theirs, f, f * FACE, FACE, IMAGE)
    for f in faces:
        s = face_terms(pf, f, mine, theirs, a_sum, tmpf)
        for b in range(N):
            yf[at(f, b), :] = s[b]
    stiffness_bc(z, g1, g2t, ms, y, tmp)
    stiffness_a(z, g0, u, INSIDE, y)

    def couple_both(a):
        couple(pf, 0, coupling, u, a)
        couple(pf, 1, coupling, u, a)

    loop(1, LAST, couple_both)
    scope("out_p_r")
    for src, ends, dst in ((z, pf, p_o), (r, rf, r_o)):
        reorder(src, dst, order, INSIDE)
        for f in faces:
            for b in range(N):
                dst[full(f, b), :] = lane_pick(ends[at(f, b), :], order)
    sum_yz([(u, a) for a in INSIDE], lanes)
    reorder(u, im_o, order, INSIDE)
    scope("x3_root")
    is_first, not_first = me == roots[0], me != roots[0]

    def image_ends():
        landed(i_theirs, x_recv.at[IMAGE])
        for f in faces:
            for b in range(N):
                rows = at(f, b)
                yf[rows, :] = yf[rows, :] + (i_mine[rows, :] + i_theirs[rows, :])
        sum_yz([(yf, f) for f in faces], lanes)
        for f in faces:
            for b in range(N):
                im_o[full(f, b), :] = lane_pick(yf[at(f, b), :], order)

    @pl.when(is_root)
    def _():
        image_ends()

    scope("plane")
    first_of_column = me - z_at * line
    skip_0 = one_of(first_of_column - 1, [r for r in roots if r % cores == 0] or [-1])
    skip_1 = one_of(first_of_column, [r for r in roots if r % cores == 1])

    @pl.when(core == 1)
    def _():
        arrived(got_a.at[pl.ds(0, others)], s_recv.at[0])
        dots[1] = added(got_a, dots[0], others)

        @pl.when(z_at < zs - 1)
        def _():
            pl.semaphore_wait(hello.at[2], zs - 1 - z_at)

        for k in sorted(range(1, zs), key=lambda k: -min(k, zs - k)):
            to_first = z_at == zs - k
            for c, skip in ((1, skip_0), (0, skip_1)):

                @pl.when(jnp.logical_not(to_first & skip))
                def _(k=k, c=c):
                    send(dots.at[1], got_b.at[k - 1], 1, moved(dz=k) - c)

        @pl.when(jnp.logical_not((z_at == 0) & skip_0))
        def _():
            send(dots.at[1], got_b.at[zs - 1], 1, me - 1)

        got_b[zs - 1] = dots[1]

    scope("root_0")

    @pl.when(is_root)
    def _():
        @pl.when(is_first)
        def _():
            dots[2] = root_sum(got_two, 0, dots[0])

        @pl.when(not_first)
        def _():
            fold[1] = root_sum(got_one, 0, fold[0])

    scope("x3")

    @pl.when(others_than_root)
    def _():
        image_ends()

    face_rows = FACE // 2
    skipped = jnp.where(
        core == 1,
        skip_0.astype(jnp.int32) + jnp.where(z_at > 0, skip_1.astype(jnp.int32), 0),
        0,
    )
    sums_0, sums_1 = len(hops) + 2, len(hops) + 2 * zs
    skipped = skipped + is_first.astype(jnp.int32)
    kinds = [(takes & jnp.logical_not(carrier), 12), (gives & jnp.logical_not(carrier), 13)]
    kinds += [(carrier & takes, 17), (carrier & gives, 18)]

    def all_left(who, to_roots):
        for faces_sent, face_count in kinds:
            for c, most, left_out in ((0, sums_0, 2), (1, sums_1, 4)):
                for less in range(left_out):

                    @pl.when(faces_sent & (core == c) & (skipped == less) & who)
                    def _(sent=most - less + face_count * face_rows):
                        arrived(all_sent.at[pl.ds(0, sent)], x_send)

        for whose, number in to_roots:

            @pl.when(whose)
            def _(number=number):
                arrived(got_one.at[pl.ds(0, number)], one_send)

    all_left(others_than_root, [(others_than_root, len(roots) - 1)])

    scope("lines")

    @pl.when((core == 0) & others_than_root)
    def _():
        arrived(got_b, s_recv.at[1])

    @pl.when((core == 1) & others_than_root)
    def _():
        arrived(got_b.at[pl.ds(0, zs - 1)], s_recv.at[1])

    def divide(total):
        sums = jnp.sum(total, axis=1, keepdims=True)
        al_o[...] = jnp.broadcast_to(sums[0:1, :] / sums[1:2, :], (8, LANES))

    @pl.when(others_than_root)
    def _():
        divide(added(got_b, None, zs))

    @pl.when(is_first)
    def _():
        divide(root_sum(got_two, 2, root_sum(got_two, 1, dots[2])))

    @pl.when(is_root & not_first)
    def _():
        row_sum = root_sum(got_one, 2, root_sum(got_one, 1, fold[1]))
        own_half = (lane[0:2, :] < half) == (b_at[0:2, :] == 0)
        divide(jnp.where(own_half, jnp.broadcast_to(row_sum, (2, LANES)), 0.0))

    scope("alpha")
    all_left(is_root, [(is_first, len(roots) - 1), (is_root & not_first, len(roots) - 2)])
    scope(None)


CHUNKS = 8


def finish_kernel(p, r, im, al, x_h, r_h, both, sem):
    alpha = al[...]
    size = ROWS // CHUNKS
    for k in range(CHUNKS):
        for i in range(k * size, (k + 1) * size, N):
            both[tile(i), :] = alpha * p[tile(i), :]
        pltpu.make_async_copy(both.at[pl.ds(k * size, size)], x_h.at[pl.ds(k * size, size)], sem).start()
        for i in range(k * size, (k + 1) * size, N):
            both[tile(ROWS + i), :] = r[tile(i), :] - alpha * im[tile(i), :]
        rows = pl.ds(ROWS + k * size, size)
        pltpu.make_async_copy(both.at[rows], r_h.at[pl.ds(k * size, size)], sem).start()
    pltpu.make_async_copy(both, both, sem).wait()


def on_device(load_terms, geometry, mass_terms, element_order):
    flat = jax.ShapeDtypeStruct((ROWS, LANES), jnp.float32)
    vm = lambda *shape: pltpu.VMEM(shape, jnp.float32)
    field = vm(ROWS, LANES)
    pair = vm(2 * FACE, LANES)
    ys, zs, xs, cores = TORUS
    in_vmem = pl.BlockSpec(memory_space=pltpu.VMEM)
    in_hbm = pl.BlockSpec(memory_space=pltpu.HBM)
    parts = pl.pallas_call(
        step_kernel,
        out_shape=(field, field, field, vm(8, LANES)),
        in_specs=[in_hbm] * 4,
        out_specs=[in_vmem] * 4,
        scratch_shapes=[
            vm(5 * ROWS, LANES), *[field] * 7,
            *[vm(8 * FACE, LANES)] * 2,
            *[pair] * 4, vm(5 * FACE, LANES), *[pair] * 8, *[vm(FACE, LANES)] * 3,
            vm(12 * FACE, LANES), vm(16, LANES),
            vm(3, 2, LANES), vm(2, 1, LANES), vm(2 * ys * xs - 1, 2, LANES), vm(zs, 2, LANES),
            vm(ys * zs * xs * cores - 1, 1, LANES), vm(ys * zs * xs * cores - 1, 2, LANES),
            vm(18 * FACE // 2 + ys * xs + 2 * zs + 1, 2, LANES),
            pltpu.VMEM((1, LANES), jnp.int32),
            pltpu.SemaphoreType.DMA((2,)),
            pltpu.SemaphoreType.DMA(()),
            pltpu.SemaphoreType.DMA((6,)),
            pltpu.SemaphoreType.DMA((2,)),
            pltpu.SemaphoreType.DMA((4,)),
            pltpu.SemaphoreType.DMA(()),
            pltpu.SemaphoreType.REGULAR((4,)),
        ],
        compiler_params=pltpu.CompilerParams(
            collective_id=0, has_side_effects=True, vmem_limit_bytes=24 << 20
        ),
        name="cg_step",
    )(
        *[
            pltpu.with_memory_space_constraint(t, pltpu.HBM)
            for t in (
                load_terms.reshape(ROWS, LANES),
                geometry.reshape(3 * ROWS, LANES),
                mass_terms.reshape(ROWS, LANES),
                element_order,
            )
        ]
    )
    x, res = pl.pallas_call(
        finish_kernel,
        out_shape=(flat, flat),
        in_specs=[in_vmem] * 4,
        out_specs=[in_hbm] * 2,
        scratch_shapes=[vm(2 * ROWS, LANES), pltpu.SemaphoreType.DMA(())],
        compiler_params=pltpu.CompilerParams(vmem_limit_bytes=8 << 20),
        name="cg_finish",
    )(*[pltpu.with_memory_space_constraint(t, pltpu.VMEM) for t in parts])
    shape = load_terms.shape
    return x.reshape(shape), res.reshape(shape)


def solution(mesh):
    last = P(None, None, None, "slab")
    return jax.shard_map(
        on_device,
        mesh=mesh,
        in_specs=(last, P(None, None, None, None, "slab"), last, P("slab", None)),
        out_specs=(last, last),
        check_vma=False,
    )
```

```python
import functools

import jax
import jax.numpy as jnp
import numpy as np
from jax import lax
from jax.experimental import pallas as pl
from jax.experimental.pallas import tpu as pltpu
from jax.sharding import PartitionSpec as P

N = 8
LAST = N - 1
EL_Y = 8
EL_Z = 16
LANES = 128
ROWS = N * N * N
FACE = N * N
CENTRE = 1.65
HALF = 1.35
MESH = pl.DeviceIdType.MESH
TORUS = (8, 12, 4, 2)
ROOTS = (1, 3, 97, 2, 96, 7, 193, 192, 5, 6)
INSIDE = range(1, LAST)
UNROLL_A = 4
UNROLL_BC = 3


def legendre_table(positions, points):
    columns = [positions * 0.0 + 1.0, positions]
    for degree in range(2, points):
        columns.append(
            ((2 * degree - 1) * positions * columns[-1] - (degree - 1) * columns[-2]) / degree
        )
    return np.stack(columns, axis=1)


def gll_derivative(points):
    degree = points - 1
    nodes = -np.cos(np.pi * np.arange(points) / degree)
    for _ in range(100):
        legendre = legendre_table(nodes, points)
        nodes = nodes - (nodes * legendre[:, degree] - legendre[:, degree - 1]) / (
            points * legendre[:, degree]
        )
    legendre = legendre_table(nodes, points)
    top = legendre[:, degree]
    same = np.eye(points, dtype=bool)
    spacing = np.where(same, 1.0, nodes[:, None] - nodes[None, :])
    table = np.where(same, 0.0, top[:, None] / (top[None, :] * spacing))
    table[0, 0] = -degree * points / 4.0
    table[degree, degree] = degree * points / 4.0
    return table


DERIV = gll_derivative(N).astype(np.float32).astype(np.float64)
SQUARED = DERIV * DERIV
SIGMA = CENTRE / HALF
RHO0 = 1.0 / SIGMA
RHO1 = 1.0 / (2.0 * SIGMA - RHO0)
COEF_Z = (1.0 + RHO1 * RHO0) / CENTRE + 2.0 * RHO1 / HALF
COEF_Q = 2.0 * RHO1 / HALF / CENTRE


def plus(x, y):
    return y if x is None else x + y


def contract(table, terms, sign, rows=range(N)):
    used = [j for j in range(N // 2) if terms[j] is not None]
    even = {j: terms[j] + terms[LAST - j] for j in used}
    odd = {j: terms[j] - terms[LAST - j] for j in used}
    out = [None] * N
    for i in range(N // 2):
        if i not in rows and LAST - i not in rows:
            continue
        e = o = None
        for j in used:
            e = plus(e, float(table[i, j] + table[i, LAST - j]) / 2 * even[j])
            o = plus(o, float(table[i, j] - table[i, LAST - j]) / 2 * odd[j])
        if i in rows:
            out[i] = e + o
        if LAST - i in rows:
            out[LAST - i] = (o - e) if sign < 0 else (e - o)
    return out


def tile(row):
    return pl.ds(row if isinstance(row, int) else pl.multiple_of(row, 8), 8)


def at(a, b):
    return tile((a * N + b) * N)


def across(a, c):
    return pl.ds(a * FACE + c, N, stride=N)


LOAD, DIAG, G1, G2 = range(4)
NEAR, FAR_LD, FAR_G, NEAR_W, FAR_W, IMAGE = range(6)


def part(f, kind, i):
    return tile(((f * 4 + kind) * N + i) * N)


def loop(start, stop, body):
    lax.fori_loop(start, stop, lambda i, _: (body(i), 0)[1], 0)


def stiffness_a(v, g0, out, rows=range(N), more=None):
    def along_a(b, _):
        va = [v[at(a, b), :] if a in INSIDE else None for a in range(N)]
        s = contract(DERIV, va, -1)
        s = contract(DERIV.T, [s[a] * g0[at(a, b), :] for a in range(N)], -1, rows)
        for a in rows:
            out[at(a, b), :] = s[a] if more is None else s[a] + more[at(a, b), :]
        return 0

    lax.fori_loop(0, N, along_a, 0, unroll=UNROLL_A)


def energy_a(v, g0, ends, first, total):
    def along_a(b, total):
        t = contract(DERIV, [v[at(a, b), :] if a in INSIDE else None for a in range(N)], -1)
        s = [t[a] * g0[at(a, b), :] for a in range(N)]
        total = [total[k] + s[k] * t[k] + s[k + 4] * t[k + 4] for k in range(4)]
        s = contract(DERIV.T, s, -1, (0, LAST))
        ends[tile(first + b * N), :] = s[0]
        ends[tile(FACE - first + b * N), :] = s[LAST]
        return total

    return lax.fori_loop(0, N, along_a, total, unroll=UNROLL_A)


def energy_bc(v, g1, g2t, ms, total):
    def along_bc(a, total):
        vb = [v[at(a, b), :] for b in range(N)]
        for own, g in (([v[across(a, c), :] for c in range(N)], g2t), (vb, g1)):
            t = contract(DERIV, own, -1)
            e = [t[i] * g[at(a, i), :] * t[i] for i in range(N)]
            total = [total[k] + (e[k] + e[k + 4]) for k in range(4)]
        e = [vb[b] * ms[at(a, b), :] * vb[b] for b in range(N)]
        return [total[k] + (e[k] + e[k + 4]) for k in range(4)]

    return lax.fori_loop(1, LAST, along_bc, total, unroll=UNROLL_BC)


def stiffness_bc(v, g1, g2t, ms, out, tmp, more=None):
    def along_bc(a, _):
        vt = [v[across(a, c), :] for c in range(N)]
        vb = [v[at(a, b), :] for b in range(N)]
        t = contract(DERIV, vt, -1)
        t = contract(DERIV.T, [t[c] * g2t[at(a, c), :] for c in range(N)], -1)
        for c in range(N):
            tmp[across(a, c), :] = t[c]
        s = contract(DERIV, vb, -1)
        s = contract(DERIV.T, [s[b] * g1[at(a, b), :] for b in range(N)], -1)
        for b in range(N):
            s[b] = s[b] + ms[at(a, b), :] * vb[b]
            if more is not None:
                s[b] = s[b] + more[at(a, b), :]
        for b in range(N):
            out[at(a, b), :] = s[b] + tmp[at(a, b), :]
        return 0

    lax.fori_loop(1, LAST, along_bc, 0, unroll=UNROLL_BC)


def inner_diagonal(g0, g1, g2, ms, out, tmp):
    def along_a(b, _):
        s = contract(SQUARED.T, [g0[at(a, b), :] for a in range(N)], 1, INSIDE)
        for a in INSIDE:
            out[at(a, b), :] = s[a] + ms[at(a, b), :]
        return 0

    lax.fori_loop(0, N, along_a, 0, unroll=UNROLL_A)

    def along_bc(a, _):
        t = contract(SQUARED.T, [g2[across(a, c), :] for c in range(N)], 1)
        for c in range(N):
            tmp[across(a, c), :] = t[c]
        s = contract(SQUARED.T, [g1[at(a, b), :] for b in range(N)], 1)
        for b in range(N):
            s[b] = s[b] + out[at(a, b), :]
        for b in range(N):
            out[at(a, b), :] = s[b] + tmp[at(a, b), :]
        return 0

    lax.fori_loop(1, LAST, along_bc, 0, unroll=UNROLL_BC)


def face_terms(v, f, mine, theirs, a_sum, tmp):
    s = contract(DERIV, [v[across(f, c), :] for c in range(N)], -1)
    s = contract(DERIV.T, [s[c] * theirs[part(f, G2, c), :] for c in range(N)], -1)
    for c in range(N):
        tmp[across(f, c), :] = s[c]
    vb = [v[at(f, b), :] for b in range(N)]
    s = contract(DERIV, vb, -1)
    s = contract(DERIV.T, [s[b] * theirs[part(f, G1, b), :] for b in range(N)], -1)
    return [s[b] + a_sum[at(f, b), :] * vb[b] + tmp[at(f, b), :] for b in range(N)]


def face_energy(v, f, theirs, a_sum):
    vb = [v[at(f, b), :] for b in range(N)]
    e = [a_sum[at(f, b), :] * vb[b] * vb[b] for b in range(N)]
    for own, kind in (([v[across(f, c), :] for c in range(N)], G2), (vb, G1)):
        t = contract(DERIV, own, -1)
        e = [e[i] + t[i] * theirs[part(f, kind, i), :] * t[i] for i in range(N)]
    return added_up(e)


def added_up(terms):
    while len(terms) > 1:
        terms = [functools.reduce(plus, terms[i : i + 2]) for i in range(0, len(terms), 2)]
    return terms[0]


def face_sums(f, mine, theirs, diag, a_sum, tmp):
    g = [[mine[part(f, k, i), :] + theirs[part(f, k, i), :] for i in range(N)] for k in (G1, G2)]
    for k in (G1, G2):
        for i in range(N):
            theirs[part(f, k, i), :] = g[k - G1][i]
    s = contract(SQUARED.T, g[1], 1)
    for c in range(N):
        tmp[across(f, c), :] = s[c]
    s = contract(SQUARED.T, g[0], 1)
    for b in range(N):
        a_sum[at(f, b), :] = diag[at(f, b), :] - s[b] - tmp[at(f, b), :]


def couplings(g0, first, out):
    def one(b, _):
        g = [g0[at(a, b), :] for a in range(N)]
        for a_end, row in ((0, first), (LAST, FACE - first)):
            s = contract(DERIV.T, [float(DERIV[m, a_end]) * g[m] for m in range(N)], -1, INSIDE)
            for a in INSIDE:
                out[tile(row * 6 + ((a - 1) * N + b) * N), :] = s[a]
        return 0

    lax.fori_loop(0, N, one, 0, unroll=2)


def couple(v, f, coupling, out, a):
    for b in range(N):
        out[at(a, b), :] = (
            out[at(a, b), :] + coupling[tile(((f * 6 + a - 1) * N + b) * N), :] * v[at(f, b), :]
        )


def lane_pick(x, idx):
    return jnp.take_along_axis(x, idx, axis=1, mode="promise_in_bounds")


def sum_yz(planes, lanes):
    ends = [(v[at(a, 0), :], v[at(a, LAST), :]) for v, a in planes]
    rims = [(v[across(a, 0), :], v[across(a, LAST), :]) for v, a in planes]
    ups = [jnp.where(lanes["up"], pltpu.roll(low, LANES - EL_Z, 1), 0.0) for low, _ in ends]
    downs = [jnp.where(lanes["down"], pltpu.roll(high, EL_Z, 1), 0.0) for _, high in ends]
    nexts = [lane_pick(low, lanes["next"]) for low, _ in rims]
    prevs = [lane_pick(high, lanes["prev"]) for _, high in rims]

    def corners(rim, idx):
        turned = jnp.where(lanes["first"], pltpu.roll(rim, 1, 0), pltpu.roll(rim, LAST, 0))
        return jnp.where(lanes["corner"], lane_pick(turned, idx), 0.0)

    far_nexts = [corners(low, lanes["corner_next"]) for low, _ in rims]
    far_prevs = [corners(high, lanes["corner_prev"]) for _, high in rims]
    for k, (v, a) in enumerate(planes):
        v[across(a, LAST), :] = rims[k][1] + (nexts[k] + far_nexts[k])
        v[across(a, 0), :] = rims[k][0] + (prevs[k] + far_prevs[k])
        v[at(a, LAST), :] = v[at(a, LAST), :] + ups[k]
        v[at(a, 0), :] = v[at(a, 0), :] + downs[k]


def step_kernel(
    load_h, geom_h, mass_h, order_h, p_o, r_o, im_o, al_o,
    coef, g2t, r, dg, z, y, u, tmp,
    mine, theirs, w_mine, w_theirs, i_mine, i_theirs, bag, rf, df, zf, pf, yf, a_sum, tmpf,
    u_ends, cross, q_mine, q_theirs, coupling, acc,
    dots, fold, got_a, got_b, got_one, got_two, all_sent, order_v, in_sems, x_send, x_recv, bag_recv, s_recv, one_send, hello,
):
    stack = []

    def scope(name):
        if stack:
            stack.pop().__exit__(None, None, None)
        if name:
            stack.append(jax.named_scope(name))
            stack[-1].__enter__()

    scope("enter")
    ys, zs, xs, cores = TORUS
    line, plane_size, count = xs * cores, zs * xs * cores, ys * zs * xs * cores
    me = lax.axis_index("slab")
    core = lax.rem(me, cores)
    in_plane = lax.rem(me, plane_size)

    def greet(sem, who):
        for q in who:
            pl.semaphore_signal(sem, inc=1, device_id=(q,), device_id_type=MESH)

    def heard(sem, who):
        if who:
            pl.semaphore_wait(sem, len(who))

    near_to = me + 1 - 2 * core
    far_to = me + 2 * core - 1
    far_to = jnp.where(far_to < 0, count - 1, jnp.where(far_to == count, 0, far_to))
    in_line = lax.rem(me, line)
    early, late = in_line == 0, in_line == line - 1
    at_turn = in_plane < line
    carrier = (jnp.logical_not(at_turn) & (in_line == 1)) | (at_turn & late)
    carrier_of_late = jnp.where(in_plane == plane_size - 1, me + line - plane_size, me + 2)
    barrier = pltpu.get_barrier_semaphore()
    greet(barrier, [jnp.where(late, carrier_of_late, far_to)])
    loads = [
        pltpu.make_async_copy(src, dst, in_sems.at[k])
        for k, src, dst in (
            (0, order_h, order_v),
            (1, load_h, coef.at[pl.ds(4 * ROWS, ROWS)]),
            (1, geom_h, coef.at[pl.ds(0, 3 * ROWS)]),
            (1, mass_h, coef.at[pl.ds(3 * ROWS, ROWS)]),
        )
    ]
    for copy in loads:
        copy.start()
    g0, g1, g2, ms, ld = (coef.at[pl.ds(k * ROWS, ROWS)] for k in range(5))

    y_at = me // plane_size
    z_at = in_plane // line
    x = in_line // cores

    def moved(dy=0, dz=0, dx=0):
        to = me
        if dy:
            to = to + (lax.rem(y_at + dy, ys) - y_at) * plane_size
        if dz:
            to = to + (lax.rem(z_at + dz, zs) - z_at) * line
        if dx:
            to = to + (lax.rem(x + dx, xs) - x) * cores
        return to

    def ring(size, stop, start=1):
        return sorted({j % size for k in range(start, stop) for j in (k, -k)} - {0})

    sides = (near_to, far_to)
    row_of = (pl.multiple_of((1 - core) * (ROWS - FACE), FACE), pl.multiple_of(core * (ROWS - FACE), FACE))
    face_of = {0: 1 - core, LAST: core}
    carrier_of_early = jnp.where(
        at_turn, lax.rem(y_at + ys - 1, ys) * plane_size + line - 1, me + 1
    )
    early_of_carrier = lax.rem(y_at + 1, ys) * plane_size
    late_of_carrier = jnp.where(at_turn, me + plane_size - line, me - 2)

    y_near = [moved(dy=k) for k in ring(ys, 3)]
    y_far = [moved(dy=k) for k in ring(ys, ys // 2 + 1, 3)]
    greet(barrier, [near_to])
    not_early = jnp.logical_not(early)
    for k in range(1, line):

        @pl.when(in_line != k)
        def _(k=k):
            greet(barrier, [me - in_line + k])

    @pl.when(not_early)
    def _():
        greet(barrier, y_near)

    @pl.when(at_turn & (early | late))
    def _():
        greet(barrier, [jnp.where(early, carrier_of_early, early_of_carrier)])

    def higher(z_to, _):
        greet(barrier, [me + (z_to - z_at) * line + 1 - core])
        return 0

    lax.fori_loop(z_at + 1, zs, higher, 0)
    roots = [r for r in ROOTS if r < count]

    def one_of(device, some):
        return functools.reduce(jnp.logical_or, [device == r for r in some])

    is_root = one_of(me, roots)
    others_than_root = jnp.logical_not(is_root)

    @pl.when(is_root)
    def _():
        width = next(k for k in range(16, 0, -1) if (count - 1) % k == 0)

        def everyone(k, _):
            for i in range(width):
                q = me + 1 + k * width + i
                greet(barrier, [jnp.where(q >= count, q - count, q)])
            return 0

        lax.fori_loop(0, (count - 1) // width, everyone, 0)

    expected = jnp.where(
        early,
        1 + at_turn.astype(jnp.int32),
        (line - 1)
        + len(y_near)
        + 2
        + carrier.astype(jnp.int32)
        + (carrier & at_turn).astype(jnp.int32)
        + 2 * core * z_at,
    )
    expected = expected + len(roots) - is_root.astype(jnp.int32)

    scope("idx")
    loads[0].wait()
    order = jnp.broadcast_to(order_v[...], (8, LANES))
    hit = (
        jnp.broadcast_to(order_v[...], (LANES, LANES))
        == lax.broadcasted_iota(jnp.int32, (LANES, LANES), 0)
    ).astype(jnp.float32)
    lane = lax.broadcasted_iota(jnp.int32, (8, LANES), 1)
    inverse = lax.dot_general(
        lane.astype(jnp.float32), hit, (((1,), (1,)), ((), ())), preferred_element_type=jnp.float32
    )
    inverse = (inverse + 0.5).astype(jnp.int32)
    in_row = lane & (EL_Z - 1)
    lanes = {
        "up": lane < LANES - EL_Z,
        "down": lane >= EL_Z,
        "next": lane - in_row + ((in_row + 1) & (EL_Z - 1)),
        "prev": lane - in_row + ((in_row + EL_Z - 1) & (EL_Z - 1)),
    }
    b_at = lax.broadcasted_iota(jnp.int32, (8, LANES), 0)
    lanes["first"] = b_at == 0
    lanes["corner"] = (lanes["first"] & lanes["down"]) | ((b_at == LAST) & lanes["up"])
    by_y = jnp.where(lanes["first"], LANES - EL_Z, EL_Z)
    lanes["corner_next"] = (lanes["next"] + by_y) & (LANES - 1)
    lanes["corner_prev"] = (lanes["prev"] + by_y) & (LANES - 1)

    def reorder(src, dst, idx, planes=range(N)):
        for a in planes:
            for b in range(N):
                dst[at(a, b), :] = lane_pick(src[at(a, b), :], idx)

    def remote(src, dst, recv, to):
        return pltpu.make_async_remote_copy(
            src_ref=src,
            dst_ref=dst,
            send_sem=x_send,
            recv_sem=recv,
            device_id=(to,),
            device_id_type=MESH,
        )

    def swap(src, dst, f, first, rows, k, carried=None):
        src, dst = src.at[pl.ds(first, rows)], dst.at[pl.ds(first, rows)]
        copy = remote(src, dst, x_recv.at[k], sides[f])
        if carried is None:
            copy.start()
        else:
            by_bag = remote(src, bag.at[pl.ds(carried, rows)], bag_recv.at[1], carrier_of_early)
            pl.when(early)(by_bag.start)
            pl.when(jnp.logical_not(early))(copy.start)
        return copy

    def carry(dst, carried, first, rows, k):
        src, dst = bag.at[pl.ds(carried, rows)], dst.at[pl.ds(first, rows)]
        remote(src, dst, x_recv.at[k], late_of_carrier).start()

    def landed(ref, sem):
        pltpu.make_async_copy(ref, ref, sem).wait()

    @pl.when(early)
    def _():
        pl.semaphore_wait(barrier, expected)
        greet(hello.at[3], [near_to])

    both = (0, LAST)
    faces = (0, 1)
    scope("load_ends")
    pltpu.make_async_copy(coef, coef, in_sems.at[1]).wait()
    for a in both:
        for b in range(N):
            mine[part(face_of[a], LOAD, b), :] = lane_pick(ld[at(a, b), :], inverse)
    for k, a in enumerate(both):
        s = contract(SQUARED.T, [g2[across(a, c), :] for c in range(N)], 1)
        for c in range(N):
            tmpf[across(k, c), :] = s[c]
    for b in range(N):
        s = contract(SQUARED.T, [g0[at(a, b), :] for a in range(N)], 1, both)
        for k, a in enumerate(both):
            yf[at(k, b), :] = s[a]
    for k, a in enumerate(both):
        s = contract(SQUARED.T, [g1[at(a, b), :] for b in range(N)], 1)
        for b in range(N):
            mine[part(face_of[a], DIAG, b), :] = lane_pick(
                s[b] + yf[at(k, b), :] + ms[at(a, b), :] + tmpf[at(k, b), :], inverse
            )
    for a in both:
        for i in range(N):
            mine[part(face_of[a], G1, i), :] = lane_pick(g1[at(a, i), :], inverse)
            mine[part(face_of[a], G2, i), :] = lane_pick(g2[across(a, i), :], inverse)
    sent_near = remote(
        mine.at[pl.ds(0, 4 * FACE)], theirs.at[pl.ds(0, 4 * FACE)], x_recv.at[NEAR], near_to
    )
    beside_early = in_line == 1

    @pl.when(beside_early)
    def _():
        pl.semaphore_wait(hello.at[3], 1)
        sent_near.start()

    scope("barrier")

    @pl.when(not_early)
    def _():
        pl.semaphore_wait(barrier, expected)

    scope("send1")

    @pl.when(carrier)
    def _():
        landed(bag.at[pl.ds(0, 4 * FACE)], bag_recv.at[0])
        carry(theirs, 0, 4 * FACE, 2 * FACE, FAR_LD)
        carry(theirs, 2 * FACE, 6 * FACE, 2 * FACE, FAR_G)

    @pl.when(early)
    def _():
        remote(
            mine.at[pl.ds(4 * FACE, 4 * FACE)],
            bag.at[pl.ds(0, 4 * FACE)],
            bag_recv.at[0],
            carrier_of_early,
        ).start()

    sent_ld, sent_g = (
        remote(mine.at[rows], theirs.at[rows], x_recv.at[k], far_to)
        for k, rows in ((FAR_LD, pl.ds(4 * FACE, 2 * FACE)), (FAR_G, pl.ds(6 * FACE, 2 * FACE)))
    )

    @pl.when(not_early)
    def _():
        sent_ld.start()
        sent_g.start()

    pl.when(jnp.logical_not(beside_early))(sent_near.start)

    @pl.when(not_early)
    def _():
        greet(hello.at[0], y_near)


    @pl.when(core == 1)
    def _():
        def lower(z_to, _):
            greet(hello.at[2], [me + (z_to - z_at) * line])
            return 0

        lax.fori_loop(0, z_at, lower, 0)

    scope("diag")
    inner_diagonal(g0, g1, g2, ms, dg, tmp)
    scope("reorder")
    for a in INSIDE:
        for b in range(N):
            rows = at(a, b)
            dg[rows, :] = lane_pick(dg[rows, :], inverse)
            moved_load = lane_pick(ld[rows, :], inverse)
            ld[rows, :] = moved_load
            r[rows, :] = moved_load
    reorder(g0, g0, inverse)

    @pl.when(carrier)
    def _():
        landed(bag.at[pl.ds(4 * FACE, FACE)], bag_recv.at[1])
        carry(w_theirs, 4 * FACE, FACE, FACE, FAR_W)

    scope("sums")
    sum_yz([(v, a) for a in INSIDE for v in (dg, r)], lanes)

    def inner_z(a, _):
        for b in range(N):
            inv = 1.0 / dg[at(a, b), :]
            dg[at(a, b), :] = inv
            z[at(a, b), :] = inv * r[at(a, b), :]
        return 0

    lax.fori_loop(1, LAST, inner_z, 0, unroll=3)
    for b in range(N):
        g = [float(DERIV[m, 0] * DERIV[m, LAST]) * g0[at(m, b), :] for m in range(N)]
        cross[at(0, b), :] = added_up(g)
    scope("La1")
    stiffness_a(z, g0, y)

    def full(f, b):
        return tile(row_of[f] + b * N)

    def face_z(f):
        for b in range(N):
            rf[at(f, b), :] = mine[part(f, LOAD, b), :] + theirs[part(f, LOAD, b), :]
            total = mine[part(f, DIAG, b), :] + theirs[part(f, DIAG, b), :]
            a_sum[at(f, b), :] = total
            df[at(f, b), :] = total
        sum_yz([(rf, f), (df, f)], lanes)
        for b in range(N):
            inv = 1.0 / df[at(f, b), :]
            df[at(f, b), :] = inv
            zf[at(f, b), :] = inv * rf[at(f, b), :]

    def tell(f, k, carried=None):
        for b in range(N):
            w_mine[at(f, b), :] = y[full(f, b), :] + cross[at(0, b), :] * zf[at(1 - f, b), :]
        sum_yz([(w_mine, f)], lanes)
        return swap(w_mine, w_theirs, f, f * FACE, FACE, k, carried)

    scope("x_near")
    sent_near.wait_recv()
    scope("z_near")
    face_z(0)
    sent_w = [None, tell(1, FAR_W, 4 * FACE)]
    scope("reorder2")
    reorder(g1, g1, inverse, INSIDE)
    for a in INSIDE:
        for c in range(N):
            g2t[at(a, c), :] = lane_pick(g2[across(a, c), :], inverse)
    reorder(ms, ms, inverse, INSIDE)
    scope("Lbc1")
    stiffness_bc(z, g1, g2t, ms, y, tmp, y)
    scope("hello")

    @pl.when(not_early)
    def _():
        heard(hello.at[0], y_near)
        greet(hello.at[1], y_far)

    scope("g_near")
    first = pl.multiple_of((1 - core) * FACE, FACE)
    couplings(g0, first, coupling)
    loop(1, LAST, lambda a: couple(zf, 0, coupling, y, a))
    face_sums(0, mine, theirs, a_sum, a_sum, tmpf)
    s = face_terms(zf, 0, mine, theirs, a_sum, tmpf)
    for b in range(N):
        yf[at(0, b), :] = s[b]
    sum_yz([(yf, 0)], lanes)
    scope("x_far")
    sent_ld.wait_recv()
    scope("z_far")
    face_z(1)

    scope("inner2")
    for a in INSIDE:
        couple(zf, 1, coupling, y, a)
    sum_yz([(y, a) for a in INSIDE], lanes)
    zero = jnp.zeros((8, LANES), jnp.float32)

    def inner_p(a, num):
        for b in range(N):
            rows = at(a, b)
            p = COEF_Z * z[rows, :] - COEF_Q * (dg[rows, :] * y[rows, :])
            z[rows, :] = p
            num[b % 4] = num[b % 4] + ld[rows, :] * p
        return num

    num = lax.fori_loop(1, LAST, inner_p, [zero] * 4, unroll=True)
    scope("L2")
    den = energy_bc(z, g1, g2t, ms, [zero] * 4)
    den = energy_a(z, g0, u_ends, first, den)
    num, den = added_up(num), added_up(den)
    sent_w[0] = tell(0, NEAR_W)
    scope("g_far")
    sent_g.wait_recv()
    face_sums(1, mine, theirs, a_sum, a_sum, tmpf)
    s = face_terms(zf, 1, mine, theirs, a_sum, tmpf)
    for b in range(N):
        yf[at(1, b), :] = s[b]
    sum_yz([(yf, 1)], lanes)

    def face_p(f):
        for b in range(N):
            rows = at(f, b)
            total = yf[rows, :] + (w_mine[rows, :] + w_theirs[rows, :])
            pf[rows, :] = COEF_Z * zf[rows, :] - COEF_Q * (df[rows, :] * total)

    def face_dot(kind, f):
        return added_up([kind[part(f, LOAD, b), :] * pf[at(f, b), :] for b in range(N)])

    acc[tile(0), :] = num
    acc[tile(8), :] = den
    takes = jnp.where(2 * x >= xs, core, 1 - core) == 1
    gives = jnp.logical_not(takes)
    sent_q = remote(q_mine, q_theirs, x_recv.at[NEAR_W], near_to)
    scope("w_near")

    @pl.when(takes)
    def _():
        landed(w_mine, x_recv.at[NEAR_W])
        face_p(0)
        acc[tile(0), :] = acc[tile(0), :] + (face_dot(mine, 0) + face_dot(theirs, 0))
        terms = [
            (2.0 * u_ends[at(0, b), :] + q_theirs[at(0, b), :]) * pf[at(0, b), :] for b in range(N)
        ]
        acc[tile(8), :] = acc[tile(8), :] + (face_energy(pf, 0, theirs, a_sum) + added_up(terms))
        for b in range(N):
            q_mine[at(0, b), :] = 2.0 * cross[at(0, b), :] * pf[at(0, b), :]

    scope("w_far")
    sent_w[1].wait_recv()
    scope("ends2")
    face_p(1)
    acc[tile(0), :] = acc[tile(0), :] + face_dot(mine, 1)
    terms = [2.0 * u_ends[at(1, b), :] * pf[at(1, b), :] for b in range(N)]
    acc[tile(8), :] = acc[tile(8), :] + (0.5 * face_energy(pf, 1, theirs, a_sum) + added_up(terms))

    @pl.when(takes)
    def _():
        terms = [q_mine[at(0, b), :] * pf[at(1, b), :] for b in range(N)]
        acc[tile(8), :] = acc[tile(8), :] + added_up(terms)

    @pl.when(gives)
    def _():
        for b in range(N):
            q_mine[at(0, b), :] = 2.0 * (
                u_ends[at(0, b), :] + cross[at(0, b), :] * pf[at(1, b), :]
            )
        sent_q.start()

    num_row = jnp.sum(acc[tile(0), :], axis=0, keepdims=True)
    den_row = jnp.sum(acc[tile(8), :], axis=0, keepdims=True)
    dots[0, 0:1, :] = num_row
    dots[0, 1:2, :] = den_row
    hops = sorted(
        ((dy, dx) for dy in range(ys) for dx in range(xs) if dy or dx),
        key=lambda d: -min(d[0], ys - d[0]) - min(d[1], xs - d[1]),
    )
    others = 2 * len(hops) + 1

    def send(src, dst, k, to):
        copy = pltpu.make_async_remote_copy(
            src_ref=src,
            dst_ref=dst,
            send_sem=x_send,
            recv_sem=s_recv.at[k],
            device_id=(to,),
            device_id_type=MESH,
        )
        copy.start()

    def arrived(ref, sem):
        pltpu.make_async_copy(ref, ref, sem).wait()

    def added(ref, first, total):
        part = [first, None, None, None]
        for j in range(total):
            part[j % 4] = plus(part[j % 4], ref[j])
        return functools.reduce(plus, [t for t in part if t is not None])

    half_z, pair_z = zs // 2, zs // 2 + zs // 8
    in_first = y_at * line + in_line
    slow_low = (z_at == pair_z) & (x == xs - 1) & (core == 1)
    slow_high = (z_at == pair_z + 1) & (x == 0) & (core == 0)
    slow_ones = ys * (2 if pair_z + 1 < zs else 1)
    slow_before = jnp.where(
        z_at > pair_z + 1,
        slow_ones,
        jnp.where(
            z_at == pair_z + 1,
            ys + y_at + (in_line > 0).astype(jnp.int32),
            jnp.where(z_at == pair_z, y_at, 0),
        ),
    )
    slot = jnp.where(
        slow_low | slow_high,
        count - slow_ones + jnp.where(slow_high, ys, 0) + y_at,
        z_at * ys * line + in_first - slow_before,
    )
    group = jnp.where(slow_low | slow_high, 2, jnp.where(z_at < half_z, 0, 1))
    group_0 = half_z * ys * line - 1
    groups = (group_0, count - 1 - group_0 - slow_ones, slow_ones)

    def root_sum(got, k, total):
        width, start, number = 16, sum(groups[:k]), groups[k]
        arrived(got.at[pl.ds(start, number)], root_recv[k])
        sums = [total] + [jnp.zeros_like(total)] * 7

        def some(i, sums):
            return [
                sums[j] + got[start + i * width + j] + got[start + i * width + j + 8]
                for j in range(8)
            ]

        whole = number // width
        sums = lax.fori_loop(0, whole, some, sums)
        for i in range(whole * width, number):
            sums[i % 8] = sums[i % 8] + got[start + i]
        return added_up(sums)

    root_recv = (s_recv.at[2], s_recv.at[3], s_recv.at[1])
    root_sem = s_recv.at[jnp.where(group == 2, 1, group + 2)]

    def send_to_root(r):
        at_root = r // plane_size * line + r % line

        @pl.when(me != r)
        def _():
            first_root = r == roots[0]
            pltpu.make_async_remote_copy(
                src_ref=dots.at[0] if first_root else fold.at[0],
                dst_ref=(got_two if first_root else got_one).at[
                    slot - (slot > at_root).astype(jnp.int32)
                ],
                send_sem=x_send if first_root else one_send,
                recv_sem=root_sem,
                device_id=(r,),
                device_id_type=MESH,
            ).start()

    send_to_root(roots[0])
    half = LANES // 2
    first_half = lane[0:1, :] < half
    fold[0] = jnp.where(
        first_half, num_row + pltpu.roll(num_row, half, 1), den_row + pltpu.roll(den_row, half, 1)
    )

    @pl.when(not_early)
    def _():
        heard(hello.at[1], y_far)

    @pl.when(beside_early)
    def _():
        greet(hello.at[0], [near_to])

    @pl.when(early)
    def _():
        pl.semaphore_wait(hello.at[0], 1)

    for j, (dy, dx) in enumerate(hops):
        send(dots.at[0], got_a.at[2 * j + core], 0, moved(dy=dy, dx=dx) + 1 - core)

    @pl.when(core == 0)
    def _():
        send(dots.at[0], got_a.at[others - 1], 0, me + 1)

    for other_root in roots[1:]:
        send_to_root(other_root)

    scope("u_ends")

    @pl.when(gives)
    def _():
        sent_w[0].wait_recv()
        face_p(0)

    for f in faces:
        for b in range(N):
            i_mine[at(f, b), :] = u_ends[at(f, b), :] + cross[at(0, b), :] * pf[at(1 - f, b), :]
        swap(i_mine, i_theirs, f, f * FACE, FACE, IMAGE)
    for f in faces:
        s = face_terms(pf, f, mine, theirs, a_sum, tmpf)
        for b in range(N):
            yf[at(f, b), :] = s[b]
    stiffness_bc(z, g1, g2t, ms, y, tmp)
    stiffness_a(z, g0, u, INSIDE, y)

    def couple_both(a):
        couple(pf, 0, coupling, u, a)
        couple(pf, 1, coupling, u, a)

    loop(1, LAST, couple_both)
    scope("out_p_r")
    for src, ends, dst in ((z, pf, p_o), (r, rf, r_o)):
        reorder(src, dst, order, INSIDE)
        for f in faces:
            for b in range(N):
                dst[full(f, b), :] = lane_pick(ends[at(f, b), :], order)
    sum_yz([(u, a) for a in INSIDE], lanes)
    reorder(u, im_o, order, INSIDE)
    scope("root_0")
    is_first, not_first = me == roots[0], me != roots[0]

    @pl.when(is_root)
    def _():
        @pl.when(is_first)
        def _():
            dots[2] = root_sum(got_two, 0, dots[0])

        @pl.when(not_first)
        def _():
            fold[1] = root_sum(got_one, 0, fold[0])

    scope("plane")
    first_of_column = me - z_at * line
    skip_0 = one_of(first_of_column - 1, [r for r in roots if r % cores == 0] or [-1])
    skip_1 = one_of(first_of_column, [r for r in roots if r % cores == 1])

    @pl.when(core == 1)
    def _():
        arrived(got_a.at[pl.ds(0, others)], s_recv.at[0])
        dots[1] = added(got_a, dots[0], others)

        @pl.when(z_at < zs - 1)
        def _():
            pl.semaphore_wait(hello.at[2], zs - 1 - z_at)

        for k in sorted(range(1, zs), key=lambda k: -min(k, zs - k)):
            to_first = z_at == zs - k
            for c, skip in ((1, skip_0), (0, skip_1)):

                @pl.when(jnp.logical_not(to_first & skip))
                def _(k=k, c=c):
                    send(dots.at[1], got_b.at[k - 1], 1, moved(dz=k) - c)

        @pl.when(jnp.logical_not((z_at == 0) & skip_0))
        def _():
            send(dots.at[1], got_b.at[zs - 1], 1, me - 1)

        got_b[zs - 1] = dots[1]

    scope("x3")
    landed(i_theirs, x_recv.at[IMAGE])
    for f in faces:
        for b in range(N):
            rows = at(f, b)
            yf[rows, :] = yf[rows, :] + (i_mine[rows, :] + i_theirs[rows, :])
    sum_yz([(yf, f) for f in faces], lanes)
    for f in faces:
        for b in range(N):
            im_o[full(f, b), :] = lane_pick(yf[at(f, b), :], order)
    face_rows = FACE // 2
    skipped = jnp.where(
        core == 1,
        skip_0.astype(jnp.int32) + jnp.where(z_at > 0, skip_1.astype(jnp.int32), 0),
        0,
    )
    sums_0, sums_1 = len(hops) + 2, len(hops) + 2 * zs
    skipped = skipped + is_first.astype(jnp.int32)
    kinds = [(takes & jnp.logical_not(carrier), 12), (gives & jnp.logical_not(carrier), 13)]
    kinds += [(carrier & takes, 17), (carrier & gives, 18)]

    def all_left(who, to_roots):
        for faces_sent, face_count in kinds:
            for c, most, left_out in ((0, sums_0, 2), (1, sums_1, 4)):
                for less in range(left_out):

                    @pl.when(faces_sent & (core == c) & (skipped == less) & who)
                    def _(sent=most - less + face_count * face_rows):
                        arrived(all_sent.at[pl.ds(0, sent)], x_send)

        for whose, number in to_roots:

            @pl.when(whose)
            def _(number=number):
                arrived(got_one.at[pl.ds(0, number)], one_send)

    all_left(others_than_root, [(others_than_root, len(roots) - 1)])

    scope("lines")

    @pl.when((core == 0) & others_than_root)
    def _():
        arrived(got_b, s_recv.at[1])

    @pl.when((core == 1) & others_than_root)
    def _():
        arrived(got_b.at[pl.ds(0, zs - 1)], s_recv.at[1])

    def divide(total):
        sums = jnp.sum(total, axis=1, keepdims=True)
        al_o[...] = jnp.broadcast_to(sums[0:1, :] / sums[1:2, :], (8, LANES))

    @pl.when(others_than_root)
    def _():
        divide(added(got_b, None, zs))

    @pl.when(is_first)
    def _():
        divide(root_sum(got_two, 2, root_sum(got_two, 1, dots[2])))

    @pl.when(is_root & not_first)
    def _():
        row_sum = root_sum(got_one, 2, root_sum(got_one, 1, fold[1]))
        own_half = (lane[0:2, :] < half) == (b_at[0:2, :] == 0)
        divide(jnp.where(own_half, jnp.broadcast_to(row_sum, (2, LANES)), 0.0))

    scope("alpha")
    all_left(is_root, [(is_first, len(roots) - 1), (is_root & not_first, len(roots) - 2)])
    scope(None)


CHUNKS = 8


def finish_kernel(p, r, im, al, x_h, r_h, both, sem):
    alpha = al[...]
    size = ROWS // CHUNKS
    for k in range(CHUNKS):
        for i in range(k * size, (k + 1) * size, N):
            both[tile(i), :] = alpha * p[tile(i), :]
        pltpu.make_async_copy(both.at[pl.ds(k * size, size)], x_h.at[pl.ds(k * size, size)], sem).start()
        for i in range(k * size, (k + 1) * size, N):
            both[tile(ROWS + i), :] = r[tile(i), :] - alpha * im[tile(i), :]
        rows = pl.ds(ROWS + k * size, size)
        pltpu.make_async_copy(both.at[rows], r_h.at[pl.ds(k * size, size)], sem).start()
    pltpu.make_async_copy(both, both, sem).wait()


def on_device(load_terms, geometry, mass_terms, element_order):
    flat = jax.ShapeDtypeStruct((ROWS, LANES), jnp.float32)
    vm = lambda *shape: pltpu.VMEM(shape, jnp.float32)
    field = vm(ROWS, LANES)
    pair = vm(2 * FACE, LANES)
    ys, zs, xs, cores = TORUS
    in_vmem = pl.BlockSpec(memory_space=pltpu.VMEM)
    in_hbm = pl.BlockSpec(memory_space=pltpu.HBM)
    parts = pl.pallas_call(
        step_kernel,
        out_shape=(field, field, field, vm(8, LANES)),
        in_specs=[in_hbm] * 4,
        out_specs=[in_vmem] * 4,
        scratch_shapes=[
            vm(5 * ROWS, LANES), *[field] * 7,
            *[vm(8 * FACE, LANES)] * 2,
            *[pair] * 4, vm(5 * FACE, LANES), *[pair] * 8, *[vm(FACE, LANES)] * 3,
            vm(12 * FACE, LANES), vm(16, LANES),
            vm(3, 2, LANES), vm(2, 1, LANES), vm(2 * ys * xs - 1, 2, LANES), vm(zs, 2, LANES),
            vm(ys * zs * xs * cores - 1, 1, LANES), vm(ys * zs * xs * cores - 1, 2, LANES),
            vm(18 * FACE // 2 + ys * xs + 2 * zs + 1, 2, LANES),
            pltpu.VMEM((1, LANES), jnp.int32),
            pltpu.SemaphoreType.DMA((2,)),
            pltpu.SemaphoreType.DMA(()),
            pltpu.SemaphoreType.DMA((6,)),
            pltpu.SemaphoreType.DMA((2,)),
            pltpu.SemaphoreType.DMA((4,)),
            pltpu.SemaphoreType.DMA(()),
            pltpu.SemaphoreType.REGULAR((4,)),
        ],
        compiler_params=pltpu.CompilerParams(
            collective_id=0, has_side_effects=True, vmem_limit_bytes=24 << 20
        ),
        name="cg_step",
    )(
        *[
            pltpu.with_memory_space_constraint(t, pltpu.HBM)
            for t in (
                load_terms.reshape(ROWS, LANES),
                geometry.reshape(3 * ROWS, LANES),
                mass_terms.reshape(ROWS, LANES),
                element_order,
            )
        ]
    )
    x, res = pl.pallas_call(
        finish_kernel,
        out_shape=(flat, flat),
        in_specs=[in_vmem] * 4,
        out_specs=[in_hbm] * 2,
        scratch_shapes=[vm(2 * ROWS, LANES), pltpu.SemaphoreType.DMA(())],
        compiler_params=pltpu.CompilerParams(vmem_limit_bytes=8 << 20),
        name="cg_finish",
    )(*[pltpu.with_memory_space_constraint(t, pltpu.VMEM) for t in parts])
    shape = load_terms.shape
    return x.reshape(shape), res.reshape(shape)


def solution(mesh):
    last = P(None, None, None, "slab")
    return jax.shard_map(
        on_device,
        mesh=mesh,
        in_specs=(last, P(None, None, None, None, "slab"), last, P("slab", None)),
        out_specs=(last, last),
        check_vma=False,
    )
```
